32 devices in a mesh: seq: 4 (over z), fsdp: 8 (over y, x, core).
Axes of the slice: x: 2, y: 2, z: 4, core: 2. Of those that a mesh axis runs over, the one named last changes fastest.
Arguments:
- tokens: bfloat16 [8, 1024, 2048], P('fsdp', 'seq'), may hold values from -6 to 6
- cotangent: bfloat16 [8, 1024, 2048], P('fsdp', 'seq'), may hold values from -6 to 6
- lengths: int32 [8], P('fsdp'), may hold values from 256 to 1024, as said below
- routes: int32 [8, 1024, 8], P('fsdp', 'seq'), may hold values from 0 to 31, as said below
- slots: int32 [8, 1024, 8], P('fsdp', 'seq'), may hold values from -1 to 79, as said below
- w_qkv: bfloat16 [2048, 5120], P(('seq', 'fsdp')), may hold values from -0.125 to 0.125
- w_out: bfloat16 [4096, 2048], P(('seq', 'fsdp')), may hold values from -1.5 to 1.5
- w_router: bfloat16 [2048, 32], P(('seq', 'fsdp')), may hold values from -0.25 to 0.25
- norm_gains: bfloat16 [4352], P(('seq', 'fsdp')), may hold values from 0.25 to 1.75
- w_gate_up: bfloat16 [32, 2048, 1536], P('fsdp', 'seq'), may hold values from -0.125 to 0.125
- w_down: bfloat16 [32, 768, 2048], P('fsdp', None, 'seq'), may hold values from -0.625 to 0.625
Outputs:
- output: bfloat16 [8, 1024, 2048], P('fsdp', 'seq')
- d_input: float32 [8, 1024, 2048], P('fsdp', 'seq')
- grad_qkv: float32 [2048, 5120], P(('seq', 'fsdp'))
- grad_out: float32 [4096, 2048], P(('seq', 'fsdp'))
- grad_router: float32 [2048, 32], P(('seq', 'fsdp'))
- grad_gains: float32 [4352], P(('seq', 'fsdp'))
- grad_gate_up: float32 [32, 2048, 1536], P('fsdp', 'seq')
- grad_down: float32 [32, 768, 2048], P('fsdp', None, 'seq')
The draws below stay inside these ranges and needn't reach their ends.
Inputs may be any that keep to these rules, and one draw needn't show every extreme that they name: `lengths`: every length is at least a quarter of 1024, and some sequence is 1024 long. `routes`: each token names 8 different experts. Among the valid tokens of one device (aligned blocks of 256 positions of a sequence) that route to one expert, the slots count 0, 1, 2 and so on in order of position while below 80; later ones and all padded slots are -1. In every draw some device sends 80 rows to some expert.
All inputs are finite; a program needn't handle non-finite values.
Results may differ from the reference program's by a relative error of at most 0.019.
Values may be sent and summed in bfloat16 or wider, within the bound.
A program may use at most 384 MiB of HBM per device.

```python
import jax
import jax.numpy as jnp
from jax import lax

D = 2048
QH = 32
KH = 4
HD = 128
FF = 768
TOPK = 8
TOK_DEV = 256
EXPERTS = 32
SEQ_LEN = 1024
SEQS = 8
CAP = 80


def route_tables(key):
    block_count = SEQ_LEN // TOK_DEV
    drawn = jax.random.randint(jax.random.fold_in(key, 11), (SEQS,), SEQ_LEN // 4, SEQ_LEN + 1)
    longest = jax.random.randint(jax.random.fold_in(key, 12), (), 0, SEQS)
    lengths = jnp.where(jnp.arange(SEQS) == longest, SEQ_LEN, drawn).astype(jnp.int32)
    expert_ids = jnp.arange(EXPERTS, dtype=jnp.int32)
    score = jax.random.randint(jax.random.fold_in(key, 13), (SEQS, SEQ_LEN, EXPERTS), 0, 65536)
    favour = jax.random.randint(jax.random.fold_in(key, 14), (EXPERTS,), 0, 65536)
    hottest = jax.random.randint(jax.random.fold_in(key, 15), (), 0, EXPERTS)
    total = score + favour[None, None, :] + jnp.where(expert_ids == hottest, 262144, 0)[None, None, :]
    total = total * EXPERTS + expert_ids[None, None, :]
    picked_scores, picked = lax.top_k(total, TOPK)
    turn = jax.random.randint(jax.random.fold_in(key, 16), (SEQS, SEQ_LEN, 1), 0, TOPK)
    order = (jnp.arange(TOPK, dtype=jnp.int32)[None, None, :] + turn) % TOPK
    routes = jnp.take_along_axis(picked.astype(jnp.int32), order, axis=-1)
    valid = jnp.arange(SEQ_LEN, dtype=jnp.int32)[None, :] < lengths[:, None]
    hits = jnp.sum((routes[..., None] == expert_ids[None, None, None, :]).astype(jnp.int32), axis=2)
    hits = hits * valid[..., None].astype(jnp.int32)
    hits = hits.reshape(SEQS, block_count, TOK_DEV, EXPERTS)
    before = (jnp.cumsum(hits, axis=2) - hits).reshape(SEQS, SEQ_LEN, EXPERTS)
    rank = jnp.take_along_axis(before, routes, axis=-1)
    slots = jnp.where(valid[..., None] & (rank < CAP), rank, -1).astype(jnp.int32)
    return (lengths, routes, slots)


def draw_lengths(key, part):
    return route_tables(key)[0]


def draw_routes(key, part):
    return route_tables(key)[1]


def draw_slots(key, part):
    return route_tables(key)[2]


def block_scale(stream_key, shape, shards, low, largest):
    level, own = 1.0, jax.random.fold_in(stream_key, 6)
    for axis_at, shards_of in shards:
        heights = jnp.exp(jax.random.uniform(jax.random.fold_in(own, axis_at), (shards_of,), jnp.float32, low / len(shards), largest / len(shards)))
        level = level * jnp.repeat(heights, shape[axis_at] // shards_of).reshape([-1 if axis == axis_at else 1 for axis in range(len(shape))])
    return level


def gaussian(own_key, extent, spread, limit, cuts=(), kind=jnp.bfloat16):
    values = spread * jax.random.normal(own_key, extent, jnp.float32)
    if cuts:
        values = values * block_scale(own_key, extent, cuts, -0.22, 0.18)
    return jnp.clip(values, -limit, limit).astype(kind)


def setup_inputs(seed: int = 0) -> dict:
    seeds = jax.random.split(jax.random.key(seed), 12)
    return {
        "tokens": gaussian(seeds[0], (SEQS, SEQ_LEN, D), 1.0, 6.0, ((0, 8), (1, 4))),
        "cotangent": gaussian(seeds[1], (SEQS, SEQ_LEN, D), 1.0, 6.0, ((0, 8), (1, 4))),
        "lengths": draw_lengths(jax.random.fold_in(seeds[11], 71), 0),
        "routes": draw_routes(jax.random.fold_in(seeds[11], 71), 0),
        "slots": draw_slots(jax.random.fold_in(seeds[11], 71), 0),
        "w_qkv": gaussian(seeds[5], (D, (QH + 2 * KH) * HD), D ** -0.5, 0.125, ((0, 32),)),
        "w_out": gaussian(seeds[6], (QH * HD, D), (QH * HD // 256) ** -0.5, 1.5, ((0, 32),)),
        "w_router": gaussian(seeds[7], (D, EXPERTS), (D // 4) ** -0.5, 0.25, ((0, 32),)),
        "norm_gains": jnp.clip(1.0 + 0.15 * jax.random.normal(seeds[8], (2 * D + 2 * HD,), jnp.float32), 0.25, 1.75).astype(jnp.bfloat16),
        "w_gate_up": gaussian(seeds[9], (EXPERTS, D, 2 * FF), D ** -0.5, 0.125, ((0, 8), (1, 4))),
        "w_down": gaussian(seeds[10], (EXPERTS, FF, D), (FF // 8) ** -0.5, 0.625, ((0, 8), (2, 4))),
    }


@jax.custom_vjp
def low(v):
    return lax.optimization_barrier(v.astype(jnp.bfloat16)).astype(jnp.float32)

@jax.custom_vjp
def reduced_backward(v):
    return v

def low_keep(v):
    return (low(v), None)

def low_pass(kept, grad):
    return (grad,)

def back_keep(v):
    return (v, None)

def back_low(kept, grad):
    return (low(grad),)
low.defvjp(low_keep, low_pass)
reduced_backward.defvjp(back_keep, back_low)
EPSILON = 1e-06
THETA = 1000000.0
MASKED = -1e+30
HIGHEST = lax.Precision.HIGHEST

def rms_norm(values, gain):
    return values * lax.rsqrt(lax.optimization_barrier(jnp.mean(values * values, axis=-1, keepdims=True)) + EPSILON) * gain

def rotate(values, cosine, sine):
    half_dim = values.shape[-1] // 2
    first_half = values[..., :half_dim]
    second_half = values[..., half_dim:]
    return jnp.concatenate([first_half * cosine - second_half * sine, second_half * cosine + first_half * sine], axis=-1)

def matrix_product(form, left, right):
    return jnp.einsum(form, left, right, precision=HIGHEST, preferred_element_type=jnp.float32)

def reference(tokens, cotangent, lengths, routes, slots, w_qkv, w_out, w_router, norm_gains, w_gate_up, w_down):
    seq_count, seq_total, width = tokens.shape
    tok_total = seq_count * seq_total
    block_count = tok_total // TOK_DEV
    expert_count = w_router.shape[1]
    all_slots = expert_count * block_count * CAP
    valid = jnp.arange(seq_total, dtype=jnp.int32)[None, :] < lengths[:, None]
    block_index = (jnp.arange(tok_total, dtype=jnp.int32) // TOK_DEV).reshape(seq_count, seq_total, 1)
    flat_pos = jnp.where(slots >= 0, (routes * block_count + block_index) * CAP + slots, all_slots).reshape(-1).astype(jnp.int32)
    owner = jnp.full((all_slots,), tok_total * TOPK, jnp.int32).at[flat_pos].set(jnp.arange(tok_total * TOPK, dtype=jnp.int32), mode='drop')
    owner_token = owner // TOPK
    frequency = THETA ** (-jnp.arange(HD // 2, dtype=jnp.float32) / (HD // 2))
    angles = jnp.arange(seq_total, dtype=jnp.float32)[:, None] * frequency[None, :]
    cosine = jnp.cos(angles)[:, None, :]
    sine = jnp.sin(angles)[:, None, :]
    scale = HD ** (-0.5)
    key_index = jnp.arange(seq_total, dtype=jnp.int32)
    causal = key_index[None, :] <= key_index[:, None]

    def attend(pieces):
        query, keys, values, length = pieces
        grouped = query.reshape(seq_total, KH, QH // KH, HD)
        scores = matrix_product('qkgd,pkd->kgqp', grouped, keys) * scale
        allowed = causal & (key_index[None, :] < length)
        scores = reduced_backward(jnp.where(allowed, scores, MASKED))
        probs = jax.nn.softmax(scores, axis=-1)
        mixed_tokens = matrix_product('kgqp,pkd->qkgd', low(probs), values)
        return mixed_tokens.reshape(seq_total, QH * HD)

    def expert(pieces):
        rows, gate_up_one, down_one = pieces
        gate_up = reduced_backward(matrix_product('rd,df->rf', rows, gate_up_one))
        hidden = low(reduced_backward(jax.nn.silu(gate_up[:, :FF]) * gate_up[:, FF:]))
        return low(reduced_backward(matrix_product('rf,fd->rd', hidden, down_one)))

    def forward(layer_inputs, query_key_value_weight, output_weight, routing_weight, gains, gate_up_weight, down_weight):
        gain_attn = gains[:width]
        gain_ffn = gains[width:2 * width]
        gain_query = gains[2 * width:2 * width + HD]
        gain_key = gains[2 * width + HD:]
        attention_reduced = low(rms_norm(layer_inputs, gain_attn))
        projected_rows = reduced_backward(matrix_product('qhv,vr->qhr', attention_reduced, query_key_value_weight))
        query = rms_norm(projected_rows[..., :QH * HD].reshape(seq_count, seq_total, QH, HD), gain_query)
        keys = rms_norm(projected_rows[..., QH * HD:(QH + KH) * HD].reshape(seq_count, seq_total, KH, HD), gain_key)
        values = projected_rows[..., (QH + KH) * HD:].reshape(seq_count, seq_total, KH, HD)
        query = reduced_backward(low(rotate(query, cosine, sine)))
        keys = reduced_backward(low(rotate(keys, cosine, sine)))
        values = reduced_backward(low(values))
        mixed_tokens = lax.map(jax.checkpoint(attend), (query, keys, values, lengths))
        mixed_tokens = low(reduced_backward(mixed_tokens))
        residual_stream = layer_inputs + reduced_backward(matrix_product('pzy,ym->pzm', mixed_tokens, output_weight))
        feedforward_reduced = low(rms_norm(residual_stream, gain_ffn))
        router_scores = reduced_backward(matrix_product('qhv,vr->qhr', feedforward_reduced, routing_weight))
        gate_prob = jax.nn.softmax(jnp.take_along_axis(router_scores, routes, axis=-1), axis=-1)
        flat_rows = feedforward_reduced.reshape(tok_total, width)
        expert_in = reduced_backward(jnp.take(flat_rows, owner_token, axis=0, mode='fill', fill_value=0.0))
        expert_in = expert_in.reshape(expert_count, block_count * CAP, width)
        expert_out = lax.map(jax.checkpoint(expert), (expert_in, gate_up_weight, down_weight))
        token_out = jnp.take(expert_out.reshape(all_slots, width), flat_pos, axis=0, mode='fill', fill_value=0.0)
        token_out = token_out.reshape(seq_count, seq_total, TOPK, width)
        moe_out = lax.optimization_barrier(jnp.sum(gate_prob[..., None] * token_out, axis=2))
        return jnp.where(valid[..., None], residual_stream + moe_out, 0.0)
    floats = tuple((arr.astype(jnp.float32) for arr in (tokens, w_qkv, w_out, w_router, norm_gains, w_gate_up, w_down)))
    result, pullback = jax.vjp(forward, *floats)
    grads = pullback(cotangent.astype(jnp.float32))
    return (result.astype(jnp.bfloat16), grads[0], grads[1], grads[2], grads[3], grads[4], grads[5], grads[6])
```

```python
import functools

import jax
import jax.numpy as jnp
from jax import lax
from jax.experimental import pallas as pl
from jax.experimental.pallas import tpu as pltpu
from jax.sharding import PartitionSpec as P

QH = 32
KH = 4
HD = 128
FF = 768
TOPK = 8
EPSILON = 1e-06
THETA = 1000000.0
MASKED = -1e30
AHEAD = 2
BF = jnp.bfloat16
F32 = jnp.float32
MESH = pl.DeviceIdType.MESH
ANY = pl.BlockSpec(memory_space=pl.ANY)
VM = pl.BlockSpec(memory_space=pltpu.VMEM)
DMA = pltpu.SemaphoreType.DMA

def exchange_kernel(axes, sizes, dims, *refs):
    count = len(dims)
    sources, results = refs[:count], refs[count : 2 * count]
    send_sem, recv_sem, own_sem = refs[2 * count :]
    total = 1
    me = 0
    for axis, size in zip(axes, sizes):
        total *= size
        me = me * size + lax.axis_index(axis)

    def place(index):
        if len(axes) == 1:
            return {axes[0]: index}
        return {axes[0]: index // sizes[1], axes[1]: index % sizes[1]}

    def block(ref, dim, index):
        return ref.at[index] if dim == 0 else ref.at[:, index]

    barrier = pltpu.get_barrier_semaphore()
    for step in range(1, total):
        pl.semaphore_signal(
            barrier, inc=1, device_id=place(lax.rem(me + step, total)), device_id_type=MESH
        )
    own = [
        pltpu.make_async_copy(
            block(sources[i], dims[i][0], me), block(results[i], dims[i][1], me), own_sem.at[i]
        )
        for i in range(count)
    ]
    for copy in own:
        copy.start()
    pl.semaphore_wait(barrier, total - 1)
    sends = []
    for step in range(1, total):
        target = lax.rem(me + step, total)
        for i in range(count):
            copy = pltpu.make_async_remote_copy(
                src_ref=block(sources[i], dims[i][0], target),
                dst_ref=block(results[i], dims[i][1], me),
                send_sem=send_sem.at[i, step],
                recv_sem=recv_sem.at[i, step],
                device_id=place(target),
                device_id_type=MESH,
            )
            copy.start()
            sends.append(copy)
    for copy in own:
        copy.wait()
    for copy in sends:
        copy.wait()


def exchange(arrays, axes, sizes, collective_id, dims=None):
    count = len(arrays)
    dims = dims or ((0, 0),) * count
    total = 1
    for size in sizes:
        total *= size
    outs = []
    for array, (before, after) in zip(arrays, dims):
        shape = list(array.shape)
        if before != after:
            shape[0], shape[1] = shape[1], shape[0]
        outs.append(jax.ShapeDtypeStruct(tuple(shape), array.dtype))
    return pl.pallas_call(
        functools.partial(exchange_kernel, axes, sizes, dims),
        out_shape=outs,
        in_specs=[ANY] * count,
        out_specs=[ANY] * count,
        scratch_shapes=[DMA((count, total)), DMA((count, total)), DMA((count,))],
        compiler_params=pltpu.CompilerParams(collective_id=collective_id, has_side_effects=True),
        name=f"exchange_{collective_id}",
    )(*arrays)


def entry_kernel(
    S, F, tok_ref, table_ref, wqkv_ref, wout_ref, small_ref,
    tok_out, table_out, wq_out, wo_out, small_out,
    tok_send, tok_recv, tab_send, tab_recv, wq_zsend, wq_zrecv,
    pl_send, pl_recv, sib_send, sib_recv, sm_send, sm_recv, own_sem,
):
    s = lax.axis_index("seq")
    f = lax.axis_index("fsdp")
    N = S * F
    chips = F // 2
    me = s * F + f
    other = f + 1 - 2 * lax.rem(f, 2)
    rows = tok_ref.shape[0]
    chunks = tok_recv.shape[1]
    span = rows // chunks

    def place(index):
        return {"seq": index // F, "fsdp": index % F}

    barrier = pltpu.get_barrier_semaphore()
    for step in range(1, N):
        pl.semaphore_signal(
            barrier, inc=1, device_id=place(lax.rem(me + step, N)), device_id_type=MESH
        )
    kv = KH * HD // S
    q_width = QH * HD // S
    starts = (0, q_width * S, (q_width + kv) * S)
    widths = (q_width, kv, kv)
    offsets = (0, q_width, q_width + kv)

    def columns(z, p):
        return pl.ds(pl.multiple_of(starts[p] + z * widths[p], 128), widths[p])

    own = [
        pltpu.make_async_copy(tok_ref, tok_out.at[s], own_sem.at[0]),
        pltpu.make_async_copy(table_ref, table_out.at[s], own_sem.at[1]),
        pltpu.make_async_copy(wout_ref, wo_out.at[f], own_sem.at[2]),
        pltpu.make_async_copy(small_ref, small_out.at[me], own_sem.at[3]),
    ]
    for p in range(3):
        own.append(
            pltpu.make_async_copy(
                wqkv_ref.at[:, columns(s, p)],
                wq_out.at[s, f, :, pl.ds(offsets[p], widths[p])],
                own_sem.at[4 + p],
            )
        )
    for copy in own:
        copy.start()
    pl.semaphore_wait(barrier, N - 1)

    def remote(src, dst, send_sem, recv_sem, where):
        return pltpu.make_async_remote_copy(
            src_ref=src, dst_ref=dst, send_sem=send_sem, recv_sem=recv_sem,
            device_id=where, device_id_type=MESH,
        )


    def go(copy):
        copy.start()

    wq_line = []
    for step in range(1, S):
        target = lax.rem(s + step, S)
        for p in range(3):
            copy = remote(
                wqkv_ref.at[:, columns(target, p)],
                wq_out.at[s, f, :, pl.ds(offsets[p], widths[p])],
                wq_zsend.at[step, p], wq_zrecv.at[step, p], {"seq": target},
            )
            copy.start()
            wq_line.append(copy)
        go(remote(table_ref, table_out.at[s], tab_send.at[step], tab_recv.at[step], {"seq": target}))

    def tok_copy(block, c, way, hop):
        here = tok_out.at[block, pl.ds(c * span, span)]
        src = tok_ref.at[pl.ds(c * span, span)] if hop == 1 else here
        return remote(
            src, here, tok_send.at[way, c, hop], tok_recv.at[way, c, hop],
            {"seq": s + 1 if way == 0 else s - 1},
        )

    for c in range(chunks):
        @pl.when(s < S - 1)
        def _():
            tok_copy(s, c, 0, 1).start()

        @pl.when(s > 0)
        def _():
            tok_copy(s, c, 1, 1).start()

    def plane_block(slot, owner):
        if slot == S:
            return wo_out.at[owner]
        return wq_out.at[lax.rem(s - slot + S, S), owner]

    def spread(slot):
        block = plane_block(slot, f)
        for step in range(1, chips):
            go(remote(block, block, pl_send.at[slot, step], pl_recv.at[slot, step],
                      {"fsdp": lax.rem(f + 2 * step, F)}))
        go(remote(block, block, sib_send.at[slot, 0], sib_recv.at[slot, 0], {"fsdp": other}))

    def forward(slot):
        for step in range(1, chips):
            block = plane_block(slot, lax.rem(f - 2 * step + F, F))
            remote(block, block, pl_send.at[slot, step], pl_recv.at[slot, step],
                   {"fsdp": other}).wait_recv()
            go(remote(block, block, sib_send.at[slot, step], sib_recv.at[slot, step],
                      {"fsdp": other}))

    for step in range(1, N):
        target = lax.rem(me + step, N)
        go(remote(small_ref, small_out.at[me], sm_send.at[step], sm_recv.at[step], place(target)))
    for copy in own:
        copy.wait()
    spread(0)
    spread(S)

    def relay(hop):
        for c in range(chunks):
            @pl.when(s >= hop)
            def _():
                tok_copy(s - hop, c, 0, hop).wait_recv()
                if hop < S - 1:
                    @pl.when(s < S - 1)
                    def _():
                        tok_copy(s - hop, c, 0, hop + 1).start()

            @pl.when(s < S - hop)
            def _():
                tok_copy(s + hop, c, 1, hop).wait_recv()
                if hop < S - 1:
                    @pl.when(s > 0)
                    def _():
                        tok_copy(s + hop, c, 1, hop + 1).start()

    relay(1)
    for step in range(1, S):
        for p in range(3):
            wq_line[(step - 1) * 3 + p].wait()
        spread(step)
    for hop in range(2, S):
        relay(hop)
    for slot in range(S + 1):
        forward(slot)
    for hop in range(1, S):
        for c in range(chunks):
            @pl.when((s < S - 1) & (s >= hop - 1))
            def _():
                tok_copy(s, c, 0, hop).wait_send()

            @pl.when((s > 0) & (s <= S - hop))
            def _():
                tok_copy(s, c, 1, hop).wait_send()
    for slot in range(S + 1):
        for step in range(1, chips):
            block = plane_block(slot, f)
            remote(block, block, pl_send.at[slot, step], pl_recv.at[slot, step],
                   {"fsdp": other}).wait_send()
        for step in range(chips):
            block = plane_block(slot, lax.rem(other - 2 * step + F, F))
            remote(block, block, sib_send.at[slot, step], sib_recv.at[slot, step],
                   {"fsdp": other}).wait()
    for step in range(1, S):
        target = lax.rem(s + step, S)
        remote(table_ref, table_out.at[s], tab_send.at[step], tab_recv.at[step], {"seq": target}).wait()
    for step in range(1, N):
        target = lax.rem(me + step, N)
        remote(small_ref, small_out.at[me], sm_send.at[step], sm_recv.at[step], place(target)).wait()


def entry(tokens, table, w_qkv, w_out, small, S, F, collective_id, chunks=4):
    own_width = w_qkv.shape[1] // S
    N = S * F
    return pl.pallas_call(
        functools.partial(entry_kernel, S, F),
        out_shape=[
            jax.ShapeDtypeStruct((S,) + tokens.shape, tokens.dtype),
            jax.ShapeDtypeStruct((S,) + table.shape, table.dtype),
            jax.ShapeDtypeStruct((S, F, w_qkv.shape[0], own_width), w_qkv.dtype),
            jax.ShapeDtypeStruct((F,) + w_out.shape, w_out.dtype),
            jax.ShapeDtypeStruct((N,) + small.shape, small.dtype),
        ],
        in_specs=[ANY] * 5,
        out_specs=[ANY] * 5,
        scratch_shapes=[
            DMA((2, chunks, S)), DMA((2, chunks, S)), DMA((S,)), DMA((S,)),
            DMA((S, 3)), DMA((S, 3)), DMA((S + 1, F // 2)), DMA((S + 1, F // 2)),
            DMA((S + 1, F // 2)), DMA((S + 1, F // 2)), DMA((N,)), DMA((N,)), DMA((7,)),
        ],
        compiler_params=pltpu.CompilerParams(collective_id=collective_id, has_side_effects=True),
        name="entry",
    )(tokens, table, w_qkv, w_out, small)


def line_kernel(S, chunks, mode, *refs):
    if mode == "ffn":
        part, base, gain, resid_out, all_out, from_left, from_right, stage = refs[:8]
        sems = refs[8:]
    elif mode == "grad":
        part, base, gain, resid, add, grad_out, gain_out, all_out, from_left, from_right, stage = refs[:11]
        sems = refs[11:]
    else:
        part, sum_out, from_left, from_right = refs[:4]
        sems = refs[4:]
    rs_send, rs_recv = sems[:2]
    if mode != "sum":
        ag_send, ag_recv, own_sem = sems[2:]
    s = lax.axis_index("seq")
    rows = part.shape[1]
    span = rows // chunks
    barrier = pltpu.get_barrier_semaphore()

    @pl.when(s > 0)
    def _():
        pl.semaphore_signal(barrier, inc=1, device_id={"seq": s - 1}, device_id_type=MESH)

    @pl.when(s < S - 1)
    def _():
        pl.semaphore_signal(barrier, inc=1, device_id={"seq": s + 1}, device_id_type=MESH)

    @pl.when((s > 0) & (s < S - 1))
    def _():
        pl.semaphore_wait(barrier, 2)

    @pl.when((s == 0) | (s == S - 1))
    def _():
        pl.semaphore_wait(barrier, 1)

    def at(c):
        return pl.ds(c * span, span)

    def rs_copy(d, c, way, src):
        buffer = from_left if way == 0 else from_right
        return pltpu.make_async_remote_copy(
            src_ref=src.at[d, at(c)], dst_ref=buffer.at[d, at(c)],
            send_sem=rs_send.at[way, d, c], recv_sem=rs_recv.at[way, d, c],
            device_id={"seq": s + 1 if way == 0 else s - 1}, device_id_type=MESH,
        )

    def ag_copy(block, c, way, hop):
        src = stage.at[at(c)] if hop == 1 else all_out.at[block, at(c)]
        return pltpu.make_async_remote_copy(
            src_ref=src, dst_ref=all_out.at[block, at(c)],
            send_sem=ag_send.at[way, c, hop], recv_sem=ag_recv.at[way, c, hop],
            device_id={"seq": s + 1 if way == 0 else s - 1}, device_id_type=MESH,
        )

    def final_step(c):
        @pl.when(s > 0)
        def _():
            rs_copy(s, c, 0, part).wait_recv()

        @pl.when(s < S - 1)
        def _():
            rs_copy(s, c, 1, part).wait_recv()

        total = part[s, at(c)].astype(F32)
        total = total + jnp.where(s > 0, from_left[s, at(c)].astype(F32), 0.0)
        total = total + jnp.where(s < S - 1, from_right[s, at(c)].astype(F32), 0.0)
        if mode == "sum":
            sum_out[at(c), :] = total
            return
        if mode == "ffn":
            value = base[at(c), :].astype(F32) + total
            resid_out[at(c), :] = value
            factor = lax.rsqrt(jnp.mean(value * value, axis=-1, keepdims=True) + EPSILON)
            low = (value * factor * gain[...]).astype(BF)
        else:
            upstream = total + add[at(c), :]
            value = resid[at(c), :]
            factor = lax.rsqrt(jnp.mean(value * value, axis=-1, keepdims=True) + EPSILON)
            normed = value * factor
            scaled = upstream * gain[...]
            inner = jnp.mean(scaled * normed, axis=-1, keepdims=True)
            result = base[at(c), :] + factor * (scaled - normed * inner)
            grad_out[at(c), :] = result
            gained = jnp.sum(upstream * normed, axis=0, keepdims=True)
            gain_out[...] = gained if c == 0 else gain_out[...] + gained
            low = result.astype(BF)
        stage[at(c), :] = low
        pltpu.make_async_copy(stage.at[at(c)], all_out.at[s, at(c)], own_sem.at[c]).start()

        @pl.when(s < S - 1)
        def _():
            ag_copy(s, c, 0, 1).start()

        @pl.when(s > 0)
        def _():
            ag_copy(s, c, 1, 1).start()

    def relay_step(c, hop):
        @pl.when(s >= hop)
        def _():
            ag_copy(s - hop, c, 0, hop).wait_recv()
            if hop < S - 1:
                @pl.when(s < S - 1)
                def _():
                    ag_copy(s - hop, c, 0, hop + 1).start()

        @pl.when(s < S - hop)
        def _():
            ag_copy(s + hop, c, 1, hop).wait_recv()
            if hop < S - 1:
                @pl.when(s > 0)
                def _():
                    ag_copy(s + hop, c, 1, hop + 1).start()

    def end_step(c):
        for d in range(S - 1, 0, -1):
            @pl.when((s == 0) & (d > s))
            def _():
                rs_copy(d, c, 0, part).start()
        for d in range(S - 1):
            @pl.when((s == S - 1) & (d < s))
            def _():
                rs_copy(d, c, 1, part).start()

    ahead = min(chunks, AHEAD if mode != "sum" else chunks)
    for c in range(ahead):
        end_step(c)

    def middle_step(c):
        for d in range(S - 1, 0, -1):
            @pl.when((s > 0) & (d > s))
            def _():
                rs_copy(d, c, 0, part).wait_recv()
                total = from_left[d, at(c)].astype(F32) + part[d, at(c)].astype(F32)
                from_left[d, at(c)] = total.astype(BF)
                rs_copy(d, c, 0, from_left).start()
        for d in range(S - 1):
            @pl.when((s < S - 1) & (d < s))
            def _():
                rs_copy(d, c, 1, part).wait_recv()
                total = from_right[d, at(c)].astype(F32) + part[d, at(c)].astype(F32)
                from_right[d, at(c)] = total.astype(BF)
                rs_copy(d, c, 1, from_right).start()

    hops = S - 1 if mode != "sum" else 0
    for t in range(chunks + 1 + hops):
        if t < chunks:
            middle_step(t)
        if t + ahead < chunks:
            end_step(t + ahead)
        if 0 <= t - 1 < chunks:
            final_step(t - 1)
        for hop in range(1, hops + 1):
            if 0 <= t - 1 - hop < chunks:
                relay_step(t - 1 - hop, hop)

    for c in range(chunks):
        for d in range(S - 1, 0, -1):
            @pl.when(d > s)
            def _():
                rs_copy(d, c, 0, part).wait_send()
        for d in range(S - 1):
            @pl.when(d < s)
            def _():
                rs_copy(d, c, 1, part).wait_send()
        if mode != "sum":
            pltpu.make_async_copy(stage.at[at(c)], all_out.at[s, at(c)], own_sem.at[c]).wait()
            for hop in range(1, S):
                @pl.when((s < S - 1) & (s >= hop - 1))
                def _():
                    ag_copy(s, c, 0, hop).wait_send()

                @pl.when((s > 0) & (s <= S - hop))
                def _():
                    ag_copy(s, c, 1, hop).wait_send()


def line(mode, S, part, others, collective_id, chunks=8):
    _, rows, width = part.shape
    full = jax.ShapeDtypeStruct((rows, width), F32)
    everyone = jax.ShapeDtypeStruct((S, rows, width), BF)
    recv = [pltpu.VMEM((S, rows, width), BF), pltpu.VMEM((S, rows, width), BF)]
    sems = [DMA((2, S, chunks)), DMA((2, S, chunks))]
    if mode == "ffn":
        outs, specs = [full, everyone], [VM, ANY]
    elif mode == "grad":
        outs, specs = [full, jax.ShapeDtypeStruct((1, width), F32), everyone], [VM, VM, ANY]
    else:
        outs, specs = [full], [VM]
    if mode != "sum":
        recv.append(pltpu.VMEM((rows, width), BF))
        sems += [DMA((2, chunks, S)), DMA((2, chunks, S)), DMA((chunks,))]
    return pl.pallas_call(
        functools.partial(line_kernel, S, chunks, mode),
        out_shape=outs,
        in_specs=[VM] * (1 + len(others)),
        out_specs=specs,
        scratch_shapes=recv + sems,
        compiler_params=pltpu.CompilerParams(collective_id=collective_id, has_side_effects=True, vmem_limit_bytes=56 << 20),
        name=f"line_{mode}",
    )(part, *others)


def turn(values, cosine, sine):
    return values * cosine + pltpu.roll(values, HD // 2, 1) * sine


def softmax_block(query, keys, first_row, length, scale):
    scores = lax.dot_general(query, keys, (((1,), (1,)), ((), ())), preferred_element_type=F32) * scale
    row = first_row + lax.broadcasted_iota(jnp.int32, scores.shape, 0)
    column = lax.broadcasted_iota(jnp.int32, scores.shape, 1)
    scores = jnp.where((column <= row) & (column < length), scores, MASKED)
    peak = jnp.max(scores, axis=-1, keepdims=True)
    weights = jnp.exp(scores - peak)
    return weights * (1.0 / jnp.sum(weights, axis=-1, keepdims=True))


def attend_kernel(heads, blocks, length_ref, proj_ref, cos_ref, sin_ref, gains_ref, low_ref, out_ref, k_all, v_all):
    step = pl.program_id(0)
    rows = proj_ref.shape[0]
    length = length_ref[0]
    cosine = cos_ref[...]
    sine = sin_ref[...]
    q_gain = gains_ref[0:1, :]
    k_gain = gains_ref[1:2, :]
    scale = HD ** (-0.5)

    def normed(raw, gain):
        factor = lax.rsqrt(jnp.mean(raw * raw, axis=-1, keepdims=True) + EPSILON)
        return turn(raw * factor * gain, cosine, sine).astype(BF)

    key = normed(proj_ref[:, heads * HD : (heads + 1) * HD], k_gain)
    value = proj_ref[:, (heads + 1) * HD :].astype(BF)
    low_ref[:, heads * HD : (heads + 1) * HD] = key
    low_ref[:, (heads + 1) * HD :] = value
    here = pl.ds(pl.multiple_of(step * rows, rows), rows)
    k_all[here, :] = key
    v_all[here, :] = value
    for block in range(blocks):
        @pl.when(step == block)
        def _():
            width = (block + 1) * rows

            @pl.loop(0, heads)
            def _(h):
                column = pl.ds(pl.multiple_of(h * HD, HD), HD)
                query = normed(proj_ref[:, column], q_gain)
                low_ref[:, column] = query
                probs = softmax_block(query, k_all[:width, :], block * rows, length, scale)
                mixed = jnp.dot(probs.astype(BF), v_all[:width, :], preferred_element_type=F32)
                out_ref[:, column] = mixed.astype(BF)


def attend(length, projected, cosine, sine, gains, heads, blocks=4):
    total, width = projected.shape
    rows = total // blocks
    return pl.pallas_call(
        functools.partial(attend_kernel, heads, blocks),
        grid=(blocks,),
        out_shape=[
            jax.ShapeDtypeStruct((total, width), BF),
            jax.ShapeDtypeStruct((total, heads * HD), BF),
        ],
        in_specs=[
            pl.BlockSpec(memory_space=pltpu.SMEM),
            pl.BlockSpec((rows, width), lambda i: (i, 0)),
            pl.BlockSpec((rows, HD), lambda i: (i, 0)),
            pl.BlockSpec((rows, HD), lambda i: (i, 0)),
            pl.BlockSpec((2, HD), lambda i: (0, 0)),
        ],
        out_specs=[
            pl.BlockSpec((rows, width), lambda i: (i, 0)),
            pl.BlockSpec((rows, heads * HD), lambda i: (i, 0)),
        ],
        scratch_shapes=[pltpu.VMEM((total, HD), BF), pltpu.VMEM((total, HD), BF)],
        compiler_params=pltpu.CompilerParams(vmem_limit_bytes=56 << 20),
        cost_estimate=pl.CostEstimate(flops=4 * heads * total * total * HD, bytes_accessed=total * width * 8, transcendentals=heads * total * total),
        name="attend",
    )(length, projected, cosine, sine, gains)


def attend_back_kernel(heads, blocks, length_ref, proj_ref, low_ref, kv_ref, grad_ref, cos_ref, sin_ref, gains_ref,
                       out_ref, gains_out, gk_all, gv_all):
    step = pl.program_id(0)
    rows = proj_ref.shape[0]
    length = length_ref[0]
    cosine = cos_ref[...]
    sine = sin_ref[...]
    q_gain = gains_ref[0:1, :]
    k_gain = gains_ref[1:2, :]
    scale = HD ** (-0.5)
    block_at = blocks - 1 - step

    def back(raw, gain, grad):
        grad = turn(grad, cosine, -sine)
        factor = lax.rsqrt(jnp.mean(raw * raw, axis=-1, keepdims=True) + EPSILON)
        unit = raw * factor
        scaled = grad * gain
        inner = jnp.mean(scaled * unit, axis=-1, keepdims=True)
        return factor * (scaled - unit * inner), jnp.sum(grad * unit, axis=0, keepdims=True)

    @pl.when(step == 0)
    def _():
        gk_all[...] = jnp.zeros_like(gk_all)
        gv_all[...] = jnp.zeros_like(gv_all)
        gains_out[...] = jnp.zeros_like(gains_out)

    for block in range(blocks):
        @pl.when(block_at == block)
        def _():
            width = (block + 1) * rows
            keys = kv_ref[:width, :HD]
            values = kv_ref[:width, HD:]

            @pl.loop(0, heads)
            def _(h):
                column = pl.ds(pl.multiple_of(h * HD, HD), HD)
                query = low_ref[:, column]
                grad_o = grad_ref[:, column]
                probs = softmax_block(query, keys, block * rows, length, scale)
                grad_p = lax.dot_general(grad_o, values, (((1,), (1,)), ((), ())), preferred_element_type=F32)
                inner = jnp.sum(probs * grad_p, axis=-1, keepdims=True)
                grad_s = (probs * (grad_p - inner)).astype(BF)
                grad_q = jnp.dot(grad_s, keys, preferred_element_type=F32) * scale
                gk_all[:width, :] += lax.dot_general(
                    grad_s, query, (((0,), (0,)), ((), ())), preferred_element_type=F32
                )
                gv_all[:width, :] += lax.dot_general(
                    probs.astype(BF), grad_o, (((0,), (0,)), ((), ())), preferred_element_type=F32
                )
                grad_raw, gained = back(proj_ref[:, column], q_gain, grad_q.astype(BF).astype(F32))
                out_ref[:, column] = grad_raw.astype(BF)
                gains_out[0:1, :] += gained

    here = pl.ds(pl.multiple_of(block_at * rows, rows), rows)
    grad_k = (gk_all[here, :] * scale).astype(BF).astype(F32)
    grad_raw, gained = back(proj_ref[:, heads * HD : (heads + 1) * HD], k_gain, grad_k)
    out_ref[:, heads * HD : (heads + 1) * HD] = grad_raw.astype(BF)
    out_ref[:, (heads + 1) * HD :] = gv_all[here, :].astype(BF)
    gains_out[1:2, :] += gained


def attend_back(length, projected, low, grad_o, cosine, sine, gains, heads, blocks=4):
    total, width = projected.shape
    rows = total // blocks
    return pl.pallas_call(
        functools.partial(attend_back_kernel, heads, blocks),
        grid=(blocks,),
        out_shape=[
            jax.ShapeDtypeStruct((total, width), BF),
            jax.ShapeDtypeStruct((2, HD), F32),
        ],
        in_specs=[
            pl.BlockSpec(memory_space=pltpu.SMEM),
            pl.BlockSpec((rows, width), lambda i: (blocks - 1 - i, 0)),
            pl.BlockSpec((rows, heads * HD), lambda i: (blocks - 1 - i, 0)),
            pl.BlockSpec((total, 2 * HD), lambda i: (0, heads // 2)),
            pl.BlockSpec((rows, heads * HD), lambda i: (blocks - 1 - i, 0)),
            pl.BlockSpec((rows, HD), lambda i: (blocks - 1 - i, 0)),
            pl.BlockSpec((rows, HD), lambda i: (blocks - 1 - i, 0)),
            pl.BlockSpec((2, HD), lambda i: (0, 0)),
        ],
        out_specs=[
            pl.BlockSpec((rows, width), lambda i: (blocks - 1 - i, 0)),
            pl.BlockSpec((2, HD), lambda i: (0, 0)),
        ],
        scratch_shapes=[pltpu.VMEM((total, HD), F32), pltpu.VMEM((total, HD), F32)],
        compiler_params=pltpu.CompilerParams(vmem_limit_bytes=56 << 20),
        cost_estimate=pl.CostEstimate(flops=10 * heads * total * total * HD, bytes_accessed=total * width * 10, transcendentals=heads * total * total),
        name="attend_back",
    )(length, projected, low, low, grad_o, cosine, sine, gains)


def rms_factor(values):
    return lax.rsqrt(jnp.mean(values * values, axis=-1, keepdims=True) + EPSILON)


def dot(left, right):
    return jnp.dot(left, right, preferred_element_type=F32)


def mm(form, left, right):
    return jnp.einsum(form, left, right, preferred_element_type=F32)


def whole_columns(blocks):
    parts, rows, _ = blocks.shape
    q_width = QH * HD // parts
    kv_width = KH * HD // parts
    moved = blocks.transpose(1, 0, 2)
    return jnp.concatenate(
        [
            moved[..., :q_width].reshape(rows, -1),
            moved[..., q_width : q_width + kv_width].reshape(rows, -1),
            moved[..., q_width + kv_width :].reshape(rows, -1),
        ],
        axis=-1,
    )


def lanes(flat, lead):
    width = flat.shape[-1]
    rows = -(-width // 2048) * 16
    return jnp.pad(flat, ((0, 0), (0, rows * 128 - width))).reshape(lead, rows, 128)


def per_device(
    tokens, cotangent, lengths, routes, slots, w_qkv, w_out, w_router, norm_gains, w_gate_up, w_down
):
    tok_count = tokens.shape[1]
    width = tokens.shape[2]
    S = lax.axis_size("seq")
    F = lax.axis_size("fsdp")
    N = S * F
    local_experts = w_gate_up.shape[0]
    own_experts = local_experts // S
    expert_count = w_router.shape[1]
    capacity = tok_count * TOPK * 5 // (4 * expert_count)
    heads = QH // S
    seq_total = tok_count * S
    q_width = heads * HD
    own_width = q_width + 2 * HD
    seq_at = lax.axis_index("seq")
    w_rows = w_qkv.shape[0]
    small = norm_gains.shape[0]
    router_size = w_router.size
    part_width = w_gate_up.shape[1]
    down_width = w_down.shape[2]
    assert KH == S and local_experts % S == 0

    small_send = lanes(jnp.concatenate([w_router.reshape(-1), norm_gains])[None], 1)[0]
    table = jnp.concatenate([routes[0].T, slots[0].T])
    tok_all, table_all, w_proj, out_own, small_all = entry(
        tokens[0], table, w_qkv, w_out, small_send, S, F, 1
    )
    w_proj = w_proj.reshape(width, own_width)
    out_own = out_own.reshape(q_width, width)
    small_flat = small_all.reshape(N, -1)
    full_router = small_flat[:, :router_size].reshape(width, expert_count)
    gain_values = small_flat[:, router_size : router_size + small].reshape(-1).astype(F32)
    gain_attn = gain_values[:width]
    gain_ffn = gain_values[width : 2 * width][None]
    gain_heads = gain_values[2 * width :].reshape(2, HD)

    def over_seq(step, block):
        pairs = [(i, (i + step) % S) for i in range(S)]
        return lax.ppermute(block, "seq", pairs)

    held = lax.optimization_barrier((w_gate_up, w_down, cotangent, small_all))
    late_gate_up, late_down, late_cot, _ = held
    gate_up_w = jnp.zeros((own_experts, width, 2 * FF), BF)
    down_w = jnp.zeros((own_experts, FF, width), BF)
    for step in range(S):
        target = lax.rem(seq_at + step, S)
        source = lax.rem(seq_at - step + S, S)
        up_block = lax.dynamic_slice_in_dim(late_gate_up, target * own_experts, own_experts, 0)
        down_block = lax.dynamic_slice_in_dim(late_down, target * own_experts, own_experts, 0)
        if step:
            up_block = over_seq(step, up_block)
            down_block = over_seq(step, down_block)
        gate_up_w = lax.dynamic_update_slice_in_dim(gate_up_w, up_block, source * part_width, 1)
        down_w = lax.dynamic_update_slice_in_dim(down_w, down_block, source * down_width, 2)
    cot_all = lax.all_gather(late_cot[0], "seq", axis=0, tiled=False)

    inputs_all = tok_all.reshape(seq_total, width).astype(F32)
    attn_low = (inputs_all * rms_factor(inputs_all) * gain_attn).astype(BF)
    projected = dot(attn_low, w_proj)
    positions = jnp.arange(seq_total, dtype=jnp.int32)
    frequency = THETA ** (-jnp.arange(HD // 2, dtype=F32) / (HD // 2))
    angles = positions.astype(F32)[:, None] * frequency[None, :]
    cosine = jnp.concatenate([jnp.cos(angles)] * 2, axis=-1)
    sine = jnp.concatenate([-jnp.sin(angles), jnp.sin(angles)], axis=-1)
    qkv_low, o_low = attend(lengths, projected, cosine, sine, gain_heads, heads)
    o_part = dot(o_low, out_own).astype(BF).reshape(S, tok_count, width)
    residual, ffn_all = line("ffn", S, o_part, [tokens[0], gain_ffn], 2)
    ffn_low = lax.dynamic_index_in_dim(ffn_all, seq_at, 0, keepdims=False)

    route_rows = routes[0]
    slot_rows = slots[0]
    expert_ids = jnp.arange(expert_count, dtype=jnp.int32)
    slot_ids = jnp.arange(capacity, dtype=jnp.int32)
    router_scores = dot(ffn_low, full_router)
    picked = route_rows[:, :, None] == expert_ids[None, None, :]
    selected = jnp.sum(jnp.where(picked, router_scores[:, None, :], 0.0), axis=-1)
    gate_prob = jax.nn.softmax(selected, axis=-1)
    gate_table = jnp.sum(jnp.where(picked, gate_prob[:, :, None], 0.0), axis=1).T
    hit = table[None, :TOPK] == expert_ids[:, None, None]
    own_slots = jnp.max(jnp.where(hit, table[None, TOPK:], -1), axis=1)
    gate_slots = jnp.sum(
        jnp.where(
            own_slots[:, None, :] == slot_ids[None, :, None], gate_table[:, None, :], 0.0
        ),
        axis=-1,
    )
    by_device = (F, S, own_experts, capacity)

    def to_devices(values):
        return lanes(values.reshape(by_device).transpose(1, 0, 2, 3).reshape(N, -1), N)

    (gate_got,) = exchange([to_devices(gate_slots)], ("seq", "fsdp"), (S, F), 3)
    row_gate = gate_got.reshape(S, F, -1)[:, :, : own_experts * capacity]
    row_gate = row_gate.transpose(1, 0, 2).reshape(F, S, own_experts, capacity, 1)

    plane = (
        jnp.arange(F, dtype=jnp.int32)[:, None] * local_experts
        + seq_at * own_experts
        + jnp.arange(own_experts, dtype=jnp.int32)[None, :]
    ).reshape(-1)
    hit = table_all[:, None, :TOPK] == plane[None, :, None, None]
    plane_slots = jnp.max(jnp.where(hit, table_all[:, None, TOPK:], -1), axis=2)
    one_hot = plane_slots[:, :, None, :] == slot_ids[None, None, :, None]
    select = one_hot.astype(BF).reshape(S, F * own_experts * capacity, tok_count)
    grouped = (S, F, own_experts * capacity, width)
    shape5 = (F, S, own_experts, capacity, width)

    cot_rows = mm("brt,btd->brd", select, cot_all).astype(BF).reshape(grouped)
    g_rows = lax.all_to_all(
        cot_rows.transpose(1, 0, 2, 3), "fsdp", split_axis=0, concat_axis=0, tiled=True
    ).reshape(shape5)
    ffn_rows = mm("brt,btd->brd", select, ffn_all).astype(BF).reshape(grouped)
    (x_rows,) = exchange([ffn_rows], ("fsdp",), (F,), 4, ((1, 0),))
    x_rows = x_rows.reshape(shape5)

    gate_up = mm("asjcd,jdf->asjcf", x_rows, gate_up_w)
    gate_part = gate_up[..., :FF]
    up_part = gate_up[..., FF:]
    hidden_low = (jax.nn.silu(gate_part) * up_part).astype(BF)
    expert_out = mm("asjch,jhd->asjcd", hidden_low, down_w).astype(BF)
    out_wide = expert_out.astype(F32)
    g_wide = g_rows.astype(F32)
    grad_prob_rows = jnp.sum(out_wide * g_wide, axis=-1)
    moe_rows = (row_gate * out_wide).astype(BF)
    grad_eo_low = (row_gate * g_wide).astype(BF)

    grad_hidden_low = mm("asjcd,jhd->asjch", grad_eo_low, down_w).astype(BF)
    grad_hidden = lax.optimization_barrier(grad_hidden_low).astype(F32)
    sigmoid_gate = jax.nn.sigmoid(gate_part)
    grad_gate = grad_hidden * up_part * sigmoid_gate * (1.0 + gate_part * (1.0 - sigmoid_gate))
    grad_up = grad_hidden * gate_part * sigmoid_gate
    grad_gu_low = jnp.concatenate([grad_gate, grad_up], axis=-1).astype(BF)
    grad_rows = mm("asjcf,jdf->asjcd", grad_gu_low, gate_up_w).astype(BF)
    up_term = mm("asjcd,asjcf->jdf", x_rows, grad_gu_low).astype(BF)
    down_term = mm("asjch,asjcd->jhd", hidden_low, grad_eo_low).astype(BF)
    grad_gate_up = jnp.zeros(w_gate_up.shape, F32)
    grad_down = jnp.zeros(w_down.shape, F32)
    for step in range(S):
        target = lax.rem(seq_at + step, S)
        source = lax.rem(seq_at - step + S, S)
        up_block = lax.dynamic_slice_in_dim(up_term, target * part_width, part_width, 1)
        down_block = lax.dynamic_slice_in_dim(down_term, target * down_width, down_width, 2)
        if step:
            up_block = over_seq(step, up_block)
            down_block = over_seq(step, down_block)
        grad_gate_up = lax.dynamic_update_slice_in_dim(
            grad_gate_up, up_block.astype(F32), source * own_experts, 0
        )
        grad_down = lax.dynamic_update_slice_in_dim(
            grad_down, down_block.astype(F32), source * own_experts, 0
        )

    prob_send = grad_prob_rows.reshape(F, S, -1).transpose(1, 0, 2).reshape(N, -1)
    (prob_got,) = exchange([lanes(prob_send, N)], ("seq", "fsdp"), (S, F), 5)
    prob_slots = prob_got.reshape(S, F, -1)[:, :, : own_experts * capacity]
    prob_slots = prob_slots.reshape(S, F, own_experts, capacity).transpose(1, 0, 2, 3)
    prob_slots = prob_slots.reshape(expert_count, capacity)

    back_layout = grad_rows.reshape(F, S, own_experts * capacity, width)
    (grad_back,) = exchange([back_layout], ("fsdp",), (F,), 6, ((0, 1),))
    grad_part = mm("brt,brd->btd", select, grad_back.reshape(S, -1, width)).astype(BF)

    prob_of_route = jnp.einsum(
        "tke,ec->tkc", picked.astype(F32), prob_slots, precision=lax.Precision.HIGHEST
    )
    at_slot = slot_rows[:, :, None] == slot_ids[None, None, :]
    grad_prob = jnp.sum(jnp.where(at_slot, prob_of_route, 0.0), axis=-1)
    grad_selected = gate_prob * (grad_prob - jnp.sum(gate_prob * grad_prob, axis=-1, keepdims=True))
    grad_logits = jnp.sum(jnp.where(picked, grad_selected[:, :, None], 0.0), axis=1).astype(BF)
    grad_ffn_add = mm("te,de->td", grad_logits, full_router)
    grad_router_part = mm("td,te->de", ffn_low, grad_logits)
    valid = (seq_at * tok_count + jnp.arange(tok_count, dtype=jnp.int32)) < lengths[0]
    grad_final = jnp.where(valid[:, None], cotangent[0].astype(F32), 0.0)
    grad_residual, grad_gain_ffn, grad_attn_low = line(
        "grad", S, grad_part, [grad_final, gain_ffn, residual, grad_ffn_add], 7
    )
    grad_attn_low = grad_attn_low.reshape(seq_total, width)

    moe_late, _ = lax.optimization_barrier((moe_rows, grad_residual))
    moe_back = lax.all_to_all(
        moe_late.reshape(F, S, own_experts * capacity, width),
        "fsdp", split_axis=0, concat_axis=0, tiled=True,
    ).transpose(1, 0, 2, 3)
    moe_part = mm("brt,brd->btd", select, moe_back.reshape(S, -1, width)).astype(BF)
    moe_out = lax.psum_scatter(moe_part, "seq", scatter_dimension=0, tiled=False)
    final = jnp.where(valid[:, None], residual + moe_out.astype(F32), 0.0)

    grad_o_low = mm("td,ed->te", grad_attn_low, out_own).astype(BF)
    grad_out_part = mm("te,td->ed", o_low, grad_attn_low).astype(BF)
    grad_out = lax.psum_scatter(grad_out_part, "fsdp", scatter_dimension=0, tiled=True).astype(F32)
    grad_proj, grad_gain_heads = attend_back(
        lengths, projected, qkv_low, grad_o_low, cosine, sine, gain_heads, heads
    )
    grad_qkv_part = mm("td,te->de", attn_low, grad_proj).astype(BF).reshape(S, F, w_rows, own_width)
    grad_qkv_part = grad_qkv_part.transpose(1, 0, 2, 3).reshape(width, own_width)
    grad_qkv_own = lax.psum_scatter(grad_qkv_part, "fsdp", scatter_dimension=0, tiled=True)
    grad_qkv_own = grad_qkv_own.reshape(S, w_rows, own_width)
    attn_part = mm("te,de->td", grad_proj, w_proj).astype(BF).reshape(S, tok_count, width)
    (grad_attn_norm,) = line("sum", S, attn_part, [], 8)
    layer_inputs = tokens[0].astype(F32)
    factor = rms_factor(layer_inputs)
    normed = layer_inputs * factor
    scaled = grad_attn_norm * gain_attn
    inner = jnp.mean(scaled * normed, axis=-1, keepdims=True)
    grad_inputs = grad_residual + factor * (scaled - normed * inner)
    grad_gain_attn = jnp.sum(grad_attn_norm * normed, axis=0)
    (grad_qkv_got,) = exchange([grad_qkv_own], ("seq",), (S,), 9)
    grad_qkv = whole_columns(grad_qkv_got).astype(F32)

    gain_part = jnp.concatenate([grad_gain_attn, grad_gain_ffn[0], grad_gain_heads.reshape(-1)])
    small_part = jnp.concatenate(
        [grad_router_part.reshape(N, -1), gain_part.reshape(N, -1)], axis=1
    )
    (small_got,) = exchange([lanes(small_part, N)], ("seq", "fsdp"), (S, F), 10)
    small_sum = jnp.sum(small_got, axis=0).reshape(-1)
    grad_router = small_sum[:router_size].reshape(w_router.shape)
    grad_gains = small_sum[router_size : router_size + small]
    return (
        final.astype(BF)[None],
        grad_inputs[None],
        grad_qkv,
        grad_out,
        grad_router,
        grad_gains,
        grad_gate_up,
        grad_down,
    )


def solution(mesh):
    in_specs = (
        P("fsdp", "seq", None),
        P("fsdp", "seq", None),
        P("fsdp"),
        P("fsdp", "seq", None),
        P("fsdp", "seq", None),
        P(("seq", "fsdp"), None),
        P(("seq", "fsdp"), None),
        P(("seq", "fsdp"), None),
        P(("seq", "fsdp")),
        P("fsdp", "seq", None),
        P("fsdp", None, "seq"),
    )
    out_specs = (
        P("fsdp", "seq", None),
        P("fsdp", "seq", None),
        P(("seq", "fsdp"), None),
        P(("seq", "fsdp"), None),
        P(("seq", "fsdp"), None),
        P(("seq", "fsdp")),
        P("fsdp", "seq", None),
        P("fsdp", None, "seq"),
    )
    return jax.shard_map(
        per_device, mesh=mesh, in_specs=in_specs, out_specs=out_specs, check_vma=False
    )
```

```python
import functools

import jax
import jax.numpy as jnp
from jax import lax
from jax.experimental import pallas as pl
from jax.experimental.pallas import tpu as pltpu
from jax.sharding import PartitionSpec as P

QH = 32
KH = 4
HD = 128
FF = 768
TOPK = 8
EPSILON = 1e-06
THETA = 1000000.0
MASKED = -1e30
AHEAD = 2
BF = jnp.bfloat16
F32 = jnp.float32
MESH = pl.DeviceIdType.MESH
ANY = pl.BlockSpec(memory_space=pl.ANY)
VM = pl.BlockSpec(memory_space=pltpu.VMEM)
DMA = pltpu.SemaphoreType.DMA
EVERY = ("seq", "fsdp")

def index_of(sizes, axes):
    at = 0
    for axis in axes:
        at = at * sizes[axis] + lax.axis_index(axis)
    return at


def count_of(sizes, axes):
    number = 1
    for axis in axes:
        number *= sizes[axis]
    return number


def place_of(sizes, axes, at):
    if len(axes) == 1:
        return {axes[0]: at}
    return {axes[0]: at // sizes[axes[1]], axes[1]: at % sizes[axes[1]]}


def greet(sizes):
    total = count_of(sizes, EVERY)
    me = index_of(sizes, EVERY)
    barrier = pltpu.get_barrier_semaphore()
    for step in range(1, total):
        pl.semaphore_signal(
            barrier, inc=1, device_id=place_of(sizes, EVERY, lax.rem(me + step, total)),
            device_id_type=MESH,
        )
    return lambda: pl.semaphore_wait(barrier, total - 1)


def block_of(ref, dim, at, total):
    if dim == "columns":
        width = ref.shape[-1] // total
        return ref.at[:, :, pl.ds(pl.multiple_of(at * width, 128), width)]
    return ref.at[at] if dim == 0 else ref.at[:, at]


class Blocks:
    def __init__(self, sizes, specs, sources, results, sems):
        self.own, self.away = [], []
        if not specs:
            return
        send_sem, recv_sem, own_sem = sems
        for i, (axes, before, after) in enumerate(specs):
            me = index_of(sizes, axes)
            total = count_of(sizes, axes)
            self.own.append(
                pltpu.make_async_copy(
                    block_of(sources[i], before, me, total),
                    block_of(results[i], after, me, total),
                    own_sem.at[i],
                )
            )
            for step in range(1, total):
                target = lax.rem(me + step, total)
                self.away.append(
                    pltpu.make_async_remote_copy(
                        src_ref=block_of(sources[i], before, target, total),
                        dst_ref=block_of(results[i], after, me, total),
                        send_sem=send_sem.at[i, step],
                        recv_sem=recv_sem.at[i, step],
                        device_id=place_of(sizes, axes, target),
                        device_id_type=MESH,
                    )
                )

    def start(self):
        for copy in self.own + self.away:
            copy.start()

    def wait(self):
        for copy in self.own + self.away:
            copy.wait()


def block_sems(sizes, specs):
    if not specs:
        return []
    total = max(count_of(sizes, axes) for axes, _, _ in specs)
    return [DMA((len(specs), total)), DMA((len(specs), total)), DMA((len(specs),))]


def block_outs(sizes, arrays, specs):
    outs = []
    for array, (axes, before, after) in zip(arrays, specs):
        shape = list(array.shape)
        total = count_of(sizes, axes)
        if before == "columns":
            shape = [total, shape[0], shape[1], shape[2] // total]
        elif after == "columns":
            shape = [shape[1], shape[2], shape[3] * total]
        elif before != after:
            shape[0], shape[1] = shape[1], shape[0]
        outs.append(jax.ShapeDtypeStruct(tuple(shape), array.dtype))
    return outs


def exchange_kernel(sizes, specs, *refs):
    count = len(specs)
    met = greet(sizes)
    blocks = Blocks(sizes, specs, refs[:count], refs[count : 2 * count], refs[2 * count :])
    met()
    blocks.start()
    blocks.wait()


def exchange(arrays, specs, sizes, collective_id):
    count = len(arrays)
    return pl.pallas_call(
        functools.partial(exchange_kernel, sizes, specs),
        out_shape=block_outs(sizes, arrays, specs),
        in_specs=[ANY] * count,
        out_specs=[ANY] * count,
        scratch_shapes=block_sems(sizes, specs),
        compiler_params=pltpu.CompilerParams(collective_id=collective_id, has_side_effects=True),
        name=f"exchange_{collective_id}",
    )(*arrays)


def entry_kernel(
    sizes, tok_ref, cot_ref, table_ref, wqkv_ref, wout_ref, small_ref,
    tok_out, cot_out, table_out, wq_out, wo_out, small_out,
    tok_send, tok_recv, tab_send, tab_recv, wq_zsend, wq_zrecv,
    pl_send, pl_recv, sib_send, sib_recv, sm_send, sm_recv, own_sem,
):
    S, F = sizes["seq"], sizes["fsdp"]
    s = lax.axis_index("seq")
    f = lax.axis_index("fsdp")
    N = S * F
    chips = F // 2
    me = s * F + f
    other = f + 1 - 2 * lax.rem(f, 2)
    rows = tok_ref.shape[0]
    chunks = tok_recv.shape[2]
    span = rows // chunks
    met = greet(sizes)
    kv = KH * HD // S
    q_width = QH * HD // S
    starts = (0, q_width * S, (q_width + kv) * S)
    widths = (q_width, kv, kv)
    offsets = (0, q_width, q_width + kv)

    def columns(z, p):
        return pl.ds(pl.multiple_of(starts[p] + z * widths[p], 128), widths[p])

    own = [
        pltpu.make_async_copy(tok_ref, tok_out.at[s], own_sem.at[0]),
        pltpu.make_async_copy(table_ref, table_out.at[s], own_sem.at[1]),
        pltpu.make_async_copy(wout_ref, wo_out.at[f], own_sem.at[2]),
        pltpu.make_async_copy(small_ref, small_out.at[me], own_sem.at[3]),
        pltpu.make_async_copy(cot_ref, cot_out.at[s], own_sem.at[4]),
    ]
    for p in range(3):
        own.append(
            pltpu.make_async_copy(
                wqkv_ref.at[:, columns(s, p)],
                wq_out.at[s, f, :, pl.ds(offsets[p], widths[p])],
                own_sem.at[5 + p],
            )
        )
    for copy in own:
        copy.start()
    met()

    def remote(src, dst, send_sem, recv_sem, where):
        return pltpu.make_async_remote_copy(
            src_ref=src, dst_ref=dst, send_sem=send_sem, recv_sem=recv_sem,
            device_id=where, device_id_type=MESH,
        )

    wq_line = []
    tables = []
    for step in range(1, S):
        target = lax.rem(s + step, S)
        for p in range(3):
            copy = remote(
                wqkv_ref.at[:, columns(target, p)],
                wq_out.at[s, f, :, pl.ds(offsets[p], widths[p])],
                wq_zsend.at[step, p], wq_zrecv.at[step, p], {"seq": target},
            )
            copy.start()
            wq_line.append(copy)
        copy = remote(
            table_ref, table_out.at[s], tab_send.at[step], tab_recv.at[step], {"seq": target}
        )
        copy.start()
        tables.append(copy)

    def along(a, block, c, way, hop):
        source, result = ((tok_ref, tok_out), (cot_ref, cot_out))[a]
        here = result.at[block, pl.ds(c * span, span)]
        src = source.at[pl.ds(c * span, span)] if hop == 1 else here
        return remote(
            src, here, tok_send.at[a, way, c, hop], tok_recv.at[a, way, c, hop],
            {"seq": s + 1 if way == 0 else s - 1},
        )

    def depart(a):
        for c in range(chunks):
            @pl.when(s < S - 1)
            def _():
                along(a, s, c, 0, 1).start()

            @pl.when(s > 0)
            def _():
                along(a, s, c, 1, 1).start()

    def relay(a, hop):
        for c in range(chunks):
            @pl.when(s >= hop)
            def _():
                along(a, s - hop, c, 0, hop).wait_recv()
                if hop < S - 1:
                    @pl.when(s < S - 1)
                    def _():
                        along(a, s - hop, c, 0, hop + 1).start()

            @pl.when(s < S - hop)
            def _():
                along(a, s + hop, c, 1, hop).wait_recv()
                if hop < S - 1:
                    @pl.when(s > 0)
                    def _():
                        along(a, s + hop, c, 1, hop + 1).start()

    depart(0)

    def plane_block(slot, owner):
        if slot == S:
            return wo_out.at[owner]
        return wq_out.at[lax.rem(s - slot + S, S), owner]

    def to_chip(slot, step):
        block = plane_block(slot, f)
        return remote(block, block, pl_send.at[slot, step], pl_recv.at[slot, step],
                      {"fsdp": lax.rem(f + 2 * step, F)})

    def to_other(slot, step):
        block = plane_block(slot, lax.rem(f - 2 * step + F, F))
        return remote(block, block, sib_send.at[slot, step], sib_recv.at[slot, step],
                      {"fsdp": other})

    def spread(slot):
        for step in range(1, chips):
            to_chip(slot, step).start()
        to_other(slot, 0).start()

    def forward(slot):
        for step in range(1, chips):
            to_chip(slot, step).wait_recv()
            to_other(slot, step).start()

    smalls = []
    for step in range(1, N):
        target = lax.rem(me + step, N)
        copy = remote(small_ref, small_out.at[me], sm_send.at[step], sm_recv.at[step],
                      place_of(sizes, EVERY, target))
        copy.start()
        smalls.append(copy)
    for copy in own:
        copy.wait()
    spread(0)
    spread(S)
    relay(0, 1)
    depart(1)
    for step in range(1, S):
        for p in range(3):
            wq_line[(step - 1) * 3 + p].wait()
        spread(step)
    for hop in range(2, S):
        relay(0, hop)
        relay(1, hop - 1)
    for slot in range(S + 1):
        forward(slot)
    relay(1, S - 1)
    for a in range(2):
        for hop in range(1, S):
            for c in range(chunks):
                @pl.when((s < S - 1) & (s >= hop - 1))
                def _():
                    along(a, s, c, 0, hop).wait_send()

                @pl.when((s > 0) & (s <= S - hop))
                def _():
                    along(a, s, c, 1, hop).wait_send()
    for slot in range(S + 1):
        for step in range(1, chips):
            to_chip(slot, step).wait_send()
        for step in range(chips):
            to_other(slot, step).wait_send()
            block = plane_block(slot, lax.rem(other - 2 * step + F, F))
            remote(block, block, sib_send.at[slot, step], sib_recv.at[slot, step],
                   {"fsdp": other}).wait_recv()
    for copy in tables + smalls:
        copy.wait()


def entry(tokens, cotangent, table, w_qkv, w_out, small, sizes, collective_id, chunks=4):
    S, F = sizes["seq"], sizes["fsdp"]
    own_width = w_qkv.shape[1] // S
    N = S * F
    line_out = jax.ShapeDtypeStruct((S,) + tokens.shape, tokens.dtype)
    return pl.pallas_call(
        functools.partial(entry_kernel, sizes),
        out_shape=[
            line_out,
            line_out,
            jax.ShapeDtypeStruct((S,) + table.shape, table.dtype),
            jax.ShapeDtypeStruct((S, F, w_qkv.shape[0], own_width), w_qkv.dtype),
            jax.ShapeDtypeStruct((F,) + w_out.shape, w_out.dtype),
            jax.ShapeDtypeStruct((N,) + small.shape, small.dtype),
        ],
        in_specs=[ANY] * 6,
        out_specs=[ANY] * 6,
        scratch_shapes=[
            DMA((2, 2, chunks, S)), DMA((2, 2, chunks, S)), DMA((S,)), DMA((S,)),
            DMA((S, 3)), DMA((S, 3)), DMA((S + 1, F // 2)), DMA((S + 1, F // 2)),
            DMA((S + 1, F // 2)), DMA((S + 1, F // 2)), DMA((N,)), DMA((N,)), DMA((8,)),
        ],
        compiler_params=pltpu.CompilerParams(collective_id=collective_id, has_side_effects=True),
        name="entry",
    )(tokens, cotangent, table, w_qkv, w_out, small)


def line_kernel(sizes, chunks, mode, parts, extra, *refs):
    S = sizes["seq"]
    count = len(extra)
    names = {
        "ffn": (["base", "gain"], ["resid_out", "all_out"]),
        "grad": (["base", "gain", "resid", "add"], ["grad_out", "gain_out", "all_out"]),
        "sum": ([], ["sum_out"]),
    }[mode]
    refs = list(refs)

    def take(number):
        taken, refs[:number] = refs[:number], []
        return taken

    part_refs = take(parts)
    given = dict(zip(names[0], take(len(names[0]))))
    sources = take(count)
    given.update(zip(names[1], take(len(names[1]))))
    results = take(count)
    from_left, from_right = take(2)
    gather = mode != "sum"
    if gather:
        (stage,) = take(1)
    rs_send, rs_recv = take(2)
    if gather:
        ag_send, ag_recv, own_sem = take(3)
        all_out = given["all_out"]
    s = lax.axis_index("seq")
    rows = part_refs[0].shape[1]
    span = rows // chunks
    met = greet(sizes)
    blocks = Blocks(sizes, extra, sources, results, refs)
    met()

    def at(c):
        return pl.ds((c % chunks) * span, span)

    def mine(d, c):
        return part_refs[c // chunks].at[d, at(c)]

    def landed(way, d, c):
        return (from_left, from_right)[way].at[c // chunks, d, at(c)]

    def rs_copy(d, c, way, src):
        return pltpu.make_async_remote_copy(
            src_ref=src, dst_ref=landed(way, d, c),
            send_sem=rs_send.at[way, d, c], recv_sem=rs_recv.at[way, d, c],
            device_id={"seq": s + 1 if way == 0 else s - 1}, device_id_type=MESH,
        )

    def ag_copy(block, c, way, hop):
        src = stage.at[at(c)] if hop == 1 else all_out.at[block, at(c)]
        return pltpu.make_async_remote_copy(
            src_ref=src, dst_ref=all_out.at[block, at(c)],
            send_sem=ag_send.at[way, c, hop], recv_sem=ag_recv.at[way, c, hop],
            device_id={"seq": s + 1 if way == 0 else s - 1}, device_id_type=MESH,
        )

    def end_step(c):
        for d in range(S - 1, 0, -1):
            @pl.when((s == 0) & (d > s))
            def _():
                rs_copy(d, c, 0, mine(d, c)).start()
        for d in range(S - 1):
            @pl.when((s == S - 1) & (d < s))
            def _():
                rs_copy(d, c, 1, mine(d, c)).start()

    def middle_step(c):
        for way in range(2):
            order = range(S - 1, 0, -1) if way == 0 else range(S - 1)
            for d in order:
                inside = (s > 0) & (d > s) if way == 0 else (s < S - 1) & (d < s)

                @pl.when(inside)
                def _():
                    buffer = landed(way, d, c)
                    rs_copy(d, c, way, buffer).wait_recv()
                    total = buffer[...].astype(F32) + mine(d, c)[...].astype(F32)
                    buffer[...] = total.astype(BF)
                    rs_copy(d, c, way, buffer).start()

    def final_step(c):
        @pl.when(s > 0)
        def _():
            rs_copy(s, c, 0, mine(s, c)).wait_recv()

        @pl.when(s < S - 1)
        def _():
            rs_copy(s, c, 1, mine(s, c)).wait_recv()

        total = mine(s, c)[...].astype(F32)
        total = total + jnp.where(s > 0, landed(0, s, c)[...].astype(F32), 0.0)
        total = total + jnp.where(s < S - 1, landed(1, s, c)[...].astype(F32), 0.0)
        if mode == "sum":
            given["sum_out"][c // chunks, at(c), :] = total
            return
        if mode == "ffn":
            value = given["base"][at(c), :].astype(F32) + total
            given["resid_out"][at(c), :] = value
            factor = lax.rsqrt(jnp.mean(value * value, axis=-1, keepdims=True) + EPSILON)
            low = (value * factor * given["gain"][...]).astype(BF)
        else:
            upstream = total + given["add"][at(c), :]
            value = given["resid"][at(c), :]
            factor = lax.rsqrt(jnp.mean(value * value, axis=-1, keepdims=True) + EPSILON)
            normed = value * factor
            scaled = upstream * given["gain"][...]
            inner = jnp.mean(scaled * normed, axis=-1, keepdims=True)
            result = given["base"][at(c), :] + factor * (scaled - normed * inner)
            given["grad_out"][at(c), :] = result
            gained = jnp.sum(upstream * normed, axis=0, keepdims=True)
            gain_out = given["gain_out"]
            gain_out[...] = gained if c == 0 else gain_out[...] + gained
            low = result.astype(BF)
        stage[at(c), :] = low
        pltpu.make_async_copy(stage.at[at(c)], all_out.at[s, at(c)], own_sem.at[c]).start()

        @pl.when(s < S - 1)
        def _():
            ag_copy(s, c, 0, 1).start()

        @pl.when(s > 0)
        def _():
            ag_copy(s, c, 1, 1).start()

    def relay_step(c, hop):
        @pl.when(s >= hop)
        def _():
            ag_copy(s - hop, c, 0, hop).wait_recv()
            if hop < S - 1:
                @pl.when(s < S - 1)
                def _():
                    ag_copy(s - hop, c, 0, hop + 1).start()

        @pl.when(s < S - hop)
        def _():
            ag_copy(s + hop, c, 1, hop).wait_recv()
            if hop < S - 1:
                @pl.when(s > 0)
                def _():
                    ag_copy(s + hop, c, 1, hop + 1).start()

    steps = chunks * parts
    ahead = min(steps, AHEAD if gather else steps)
    for c in range(ahead):
        end_step(c)
    blocks.start()
    hops = S - 1 if gather else 0
    for t in range(steps + 1 + hops):
        if t < steps:
            middle_step(t)
        if t + ahead < steps:
            end_step(t + ahead)
        if 0 <= t - 1 < steps:
            final_step(t - 1)
        for hop in range(1, hops + 1):
            if 0 <= t - 1 - hop < steps:
                relay_step(t - 1 - hop, hop)

    for c in range(steps):
        for d in range(S - 1, 0, -1):
            @pl.when(d > s)
            def _():
                rs_copy(d, c, 0, mine(d, c)).wait_send()
        for d in range(S - 1):
            @pl.when(d < s)
            def _():
                rs_copy(d, c, 1, mine(d, c)).wait_send()
        if gather:
            pltpu.make_async_copy(stage.at[at(c)], all_out.at[s, at(c)], own_sem.at[c]).wait()
            for hop in range(1, S):
                @pl.when((s < S - 1) & (s >= hop - 1))
                def _():
                    ag_copy(s, c, 0, hop).wait_send()

                @pl.when((s > 0) & (s <= S - hop))
                def _():
                    ag_copy(s, c, 1, hop).wait_send()
    blocks.wait()


def line(mode, sizes, parts, others, extras, specs, collective_id, chunks=8):
    S = sizes["seq"]
    _, rows, width = parts[0].shape
    full = jax.ShapeDtypeStruct((rows, width), F32)
    everyone = jax.ShapeDtypeStruct((S, rows, width), BF)
    steps = chunks * len(parts)
    scratch = [pltpu.VMEM((len(parts), S, rows, width), BF)] * 2
    sems = [DMA((2, S, steps)), DMA((2, S, steps))]
    if mode == "ffn":
        outs, out_specs = [full, everyone], [VM, ANY]
    elif mode == "grad":
        outs, out_specs = [full, jax.ShapeDtypeStruct((1, width), F32), everyone], [VM, VM, ANY]
    else:
        outs, out_specs = [jax.ShapeDtypeStruct((len(parts), rows, width), F32)], [VM]
    if mode != "sum":
        scratch.append(pltpu.VMEM((rows, width), BF))
        sems += [DMA((2, chunks, S)), DMA((2, chunks, S)), DMA((chunks,))]
    return pl.pallas_call(
        functools.partial(line_kernel, sizes, chunks, mode, len(parts), specs),
        out_shape=outs + block_outs(sizes, extras, specs),
        in_specs=[VM] * (len(parts) + len(others)) + [ANY] * len(extras),
        out_specs=out_specs + [ANY] * len(extras),
        scratch_shapes=scratch + sems + block_sems(sizes, specs),
        compiler_params=pltpu.CompilerParams(
            collective_id=collective_id, has_side_effects=True, vmem_limit_bytes=56 << 20
        ),
        name=f"line_{mode}",
    )(*parts, *others, *extras)


def turn(values, cosine, sine):
    return values * cosine + pltpu.roll(values, HD // 2, 1) * sine


def softmax_block(query, keys, first_row, length, scale):
    scores = lax.dot_general(query, keys, (((1,), (1,)), ((), ())), preferred_element_type=F32) * scale
    row = first_row + lax.broadcasted_iota(jnp.int32, scores.shape, 0)
    column = lax.broadcasted_iota(jnp.int32, scores.shape, 1)
    scores = jnp.where((column <= row) & (column < length), scores, MASKED)
    peak = jnp.max(scores, axis=-1, keepdims=True)
    weights = jnp.exp(scores - peak)
    return weights * (1.0 / jnp.sum(weights, axis=-1, keepdims=True))


def attend_kernel(heads, blocks, length_ref, proj_ref, cos_ref, sin_ref, gains_ref, low_ref, out_ref, k_all, v_all):
    step = pl.program_id(0)
    rows = proj_ref.shape[0]
    length = length_ref[0]
    cosine = cos_ref[...]
    sine = sin_ref[...]
    q_gain = gains_ref[0:1, :]
    k_gain = gains_ref[1:2, :]
    scale = HD ** (-0.5)

    def normed(raw, gain):
        factor = lax.rsqrt(jnp.mean(raw * raw, axis=-1, keepdims=True) + EPSILON)
        return turn(raw * factor * gain, cosine, sine).astype(BF)

    key = normed(proj_ref[:, heads * HD : (heads + 1) * HD], k_gain)
    value = proj_ref[:, (heads + 1) * HD :].astype(BF)
    low_ref[:, heads * HD : (heads + 1) * HD] = key
    low_ref[:, (heads + 1) * HD :] = value
    here = pl.ds(pl.multiple_of(step * rows, rows), rows)
    k_all[here, :] = key
    v_all[here, :] = value
    for block in range(blocks):
        @pl.when(step == block)
        def _():
            width = (block + 1) * rows

            @pl.loop(0, heads)
            def _(h):
                column = pl.ds(pl.multiple_of(h * HD, HD), HD)
                query = normed(proj_ref[:, column], q_gain)
                low_ref[:, column] = query
                probs = softmax_block(query, k_all[:width, :], block * rows, length, scale)
                mixed = jnp.dot(probs.astype(BF), v_all[:width, :], preferred_element_type=F32)
                out_ref[:, column] = mixed.astype(BF)


def attend(length, projected, cosine, sine, gains, heads, blocks=4):
    total, width = projected.shape
    rows = total // blocks
    return pl.pallas_call(
        functools.partial(attend_kernel, heads, blocks),
        grid=(blocks,),
        out_shape=[
            jax.ShapeDtypeStruct((total, width), BF),
            jax.ShapeDtypeStruct((total, heads * HD), BF),
        ],
        in_specs=[
            pl.BlockSpec(memory_space=pltpu.SMEM),
            pl.BlockSpec((rows, width), lambda i: (i, 0)),
            pl.BlockSpec((rows, HD), lambda i: (i, 0)),
            pl.BlockSpec((rows, HD), lambda i: (i, 0)),
            pl.BlockSpec((2, HD), lambda i: (0, 0)),
        ],
        out_specs=[
            pl.BlockSpec((rows, width), lambda i: (i, 0)),
            pl.BlockSpec((rows, heads * HD), lambda i: (i, 0)),
        ],
        scratch_shapes=[pltpu.VMEM((total, HD), BF), pltpu.VMEM((total, HD), BF)],
        compiler_params=pltpu.CompilerParams(vmem_limit_bytes=56 << 20),
        cost_estimate=pl.CostEstimate(flops=4 * heads * total * total * HD, bytes_accessed=total * width * 8, transcendentals=heads * total * total),
        name="attend",
    )(length, projected, cosine, sine, gains)


def attend_back_kernel(heads, blocks, length_ref, proj_ref, low_ref, kv_ref, grad_ref, cos_ref, sin_ref, gains_ref,
                       out_ref, gains_out, gk_all, gv_all):
    step = pl.program_id(0)
    rows = proj_ref.shape[0]
    length = length_ref[0]
    cosine = cos_ref[...]
    sine = sin_ref[...]
    q_gain = gains_ref[0:1, :]
    k_gain = gains_ref[1:2, :]
    scale = HD ** (-0.5)
    block_at = blocks - 1 - step

    def back(raw, gain, grad):
        grad = turn(grad, cosine, -sine)
        factor = lax.rsqrt(jnp.mean(raw * raw, axis=-1, keepdims=True) + EPSILON)
        unit = raw * factor
        scaled = grad * gain
        inner = jnp.mean(scaled * unit, axis=-1, keepdims=True)
        return factor * (scaled - unit * inner), jnp.sum(grad * unit, axis=0, keepdims=True)

    @pl.when(step == 0)
    def _():
        gk_all[...] = jnp.zeros_like(gk_all)
        gv_all[...] = jnp.zeros_like(gv_all)
        gains_out[...] = jnp.zeros_like(gains_out)

    for block in range(blocks):
        @pl.when(block_at == block)
        def _():
            width = (block + 1) * rows
            keys = kv_ref[:width, :HD]
            values = kv_ref[:width, HD:]

            @pl.loop(0, heads)
            def _(h):
                column = pl.ds(pl.multiple_of(h * HD, HD), HD)
                query = low_ref[:, column]
                grad_o = grad_ref[:, column]
                probs = softmax_block(query, keys, block * rows, length, scale)
                grad_p = lax.dot_general(grad_o, values, (((1,), (1,)), ((), ())), preferred_element_type=F32)
                inner = jnp.sum(probs * grad_p, axis=-1, keepdims=True)
                grad_s = (probs * (grad_p - inner)).astype(BF)
                grad_q = jnp.dot(grad_s, keys, preferred_element_type=F32) * scale
                gk_all[:width, :] += lax.dot_general(
                    grad_s, query, (((0,), (0,)), ((), ())), preferred_element_type=F32
                )
                gv_all[:width, :] += lax.dot_general(
                    probs.astype(BF), grad_o, (((0,), (0,)), ((), ())), preferred_element_type=F32
                )
                grad_raw, gained = back(proj_ref[:, column], q_gain, grad_q.astype(BF).astype(F32))
                out_ref[:, column] = grad_raw.astype(BF)
                gains_out[0:1, :] += gained

    here = pl.ds(pl.multiple_of(block_at * rows, rows), rows)
    grad_k = (gk_all[here, :] * scale).astype(BF).astype(F32)
    grad_raw, gained = back(proj_ref[:, heads * HD : (heads + 1) * HD], k_gain, grad_k)
    out_ref[:, heads * HD : (heads + 1) * HD] = grad_raw.astype(BF)
    out_ref[:, (heads + 1) * HD :] = gv_all[here, :].astype(BF)
    gains_out[1:2, :] += gained


def attend_back(length, projected, low, grad_o, cosine, sine, gains, heads, blocks=4):
    total, width = projected.shape
    rows = total // blocks
    return pl.pallas_call(
        functools.partial(attend_back_kernel, heads, blocks),
        grid=(blocks,),
        out_shape=[
            jax.ShapeDtypeStruct((total, width), BF),
            jax.ShapeDtypeStruct((2, HD), F32),
        ],
        in_specs=[
            pl.BlockSpec(memory_space=pltpu.SMEM),
            pl.BlockSpec((rows, width), lambda i: (blocks - 1 - i, 0)),
            pl.BlockSpec((rows, heads * HD), lambda i: (blocks - 1 - i, 0)),
            pl.BlockSpec((total, 2 * HD), lambda i: (0, heads // 2)),
            pl.BlockSpec((rows, heads * HD), lambda i: (blocks - 1 - i, 0)),
            pl.BlockSpec((rows, HD), lambda i: (blocks - 1 - i, 0)),
            pl.BlockSpec((rows, HD), lambda i: (blocks - 1 - i, 0)),
            pl.BlockSpec((2, HD), lambda i: (0, 0)),
        ],
        out_specs=[
            pl.BlockSpec((rows, width), lambda i: (blocks - 1 - i, 0)),
            pl.BlockSpec((2, HD), lambda i: (0, 0)),
        ],
        scratch_shapes=[pltpu.VMEM((total, HD), F32), pltpu.VMEM((total, HD), F32)],
        compiler_params=pltpu.CompilerParams(vmem_limit_bytes=56 << 20),
        cost_estimate=pl.CostEstimate(flops=10 * heads * total * total * HD, bytes_accessed=total * width * 10, transcendentals=heads * total * total),
        name="attend_back",
    )(length, projected, low, low, grad_o, cosine, sine, gains)


def rms_factor(values):
    return lax.rsqrt(jnp.mean(values * values, axis=-1, keepdims=True) + EPSILON)


def dot(left, right):
    return jnp.dot(left, right, preferred_element_type=F32)


def mm(form, left, right):
    return jnp.einsum(form, left, right, preferred_element_type=F32)


def whole_columns(blocks):
    parts, rows, _ = blocks.shape
    q_width = QH * HD // parts
    kv_width = KH * HD // parts
    moved = blocks.transpose(1, 0, 2)
    return jnp.concatenate(
        [
            moved[..., :q_width].reshape(rows, -1),
            moved[..., q_width : q_width + kv_width].reshape(rows, -1),
            moved[..., q_width + kv_width :].reshape(rows, -1),
        ],
        axis=-1,
    )


def lanes(flat, lead):
    width = flat.shape[-1]
    rows = -(-width // 2048) * 16
    return jnp.pad(flat, ((0, 0), (0, rows * 128 - width))).reshape(lead, rows, 128)


def per_device(
    tokens, cotangent, lengths, routes, slots, w_qkv, w_out, w_router, norm_gains, w_gate_up, w_down
):
    tok_count = tokens.shape[1]
    width = tokens.shape[2]
    S = lax.axis_size("seq")
    F = lax.axis_size("fsdp")
    N = S * F
    sizes = {"seq": S, "fsdp": F}
    local_experts = w_gate_up.shape[0]
    own_experts = local_experts // S
    expert_count = w_router.shape[1]
    capacity = tok_count * TOPK * 5 // (4 * expert_count)
    heads = QH // S
    seq_total = tok_count * S
    q_width = heads * HD
    own_width = q_width + 2 * HD
    seq_at = lax.axis_index("seq")
    w_rows = w_qkv.shape[0]
    small = norm_gains.shape[0]
    router_size = w_router.size
    part_width = w_gate_up.shape[1]
    down_width = w_down.shape[2]
    assert KH == S and local_experts % S == 0

    small_send = lanes(jnp.concatenate([w_router.reshape(-1), norm_gains])[None], 1)[0]
    table = jnp.concatenate([routes[0].T, slots[0].T])
    tok_all, cot_all, table_all, w_proj, out_own, small_all = entry(
        tokens[0], cotangent[0], table, w_qkv, w_out, small_send, sizes, 1
    )
    w_proj = w_proj.reshape(width, own_width)
    out_own = out_own.reshape(q_width, width)
    small_flat = small_all.reshape(N, -1)
    full_router = small_flat[:, :router_size].reshape(width, expert_count)
    gain_values = small_flat[:, router_size : router_size + small].reshape(-1).astype(F32)
    gain_attn = gain_values[:width]
    gain_ffn = gain_values[width : 2 * width][None]
    gain_heads = gain_values[2 * width :].reshape(2, HD)

    inputs_all = tok_all.reshape(seq_total, width).astype(F32)
    attn_low = (inputs_all * rms_factor(inputs_all) * gain_attn).astype(BF)
    projected = dot(attn_low, w_proj)
    positions = jnp.arange(seq_total, dtype=jnp.int32)
    frequency = THETA ** (-jnp.arange(HD // 2, dtype=F32) / (HD // 2))
    angles = positions.astype(F32)[:, None] * frequency[None, :]
    cosine = jnp.concatenate([jnp.cos(angles)] * 2, axis=-1)
    sine = jnp.concatenate([-jnp.sin(angles), jnp.sin(angles)], axis=-1)
    qkv_low, o_low = attend(lengths, projected, cosine, sine, gain_heads, heads)
    o_part = dot(o_low, out_own).astype(BF).reshape(S, tok_count, width)

    expert_ids = jnp.arange(expert_count, dtype=jnp.int32)
    slot_ids = jnp.arange(capacity, dtype=jnp.int32)
    plane = (
        jnp.arange(F, dtype=jnp.int32)[:, None] * local_experts
        + seq_at * own_experts
        + jnp.arange(own_experts, dtype=jnp.int32)[None, :]
    ).reshape(-1)
    hit = table_all[:, None, :TOPK] == plane[None, :, None, None]
    plane_slots = jnp.max(jnp.where(hit, table_all[:, None, TOPK:], -1), axis=2)
    one_hot = plane_slots[:, :, None, :] == slot_ids[None, None, :, None]
    select = one_hot.astype(BF).reshape(S, F * own_experts * capacity, tok_count)
    grouped = (S, F, own_experts * capacity, width)
    shape5 = (F, S, own_experts, capacity, width)

    cot_rows = mm("brt,btd->brd", select, cot_all).astype(BF).reshape(grouped)
    residual, ffn_all, g_rows, down_w = line(
        "ffn", sizes, [o_part], [tokens[0], gain_ffn],
        [cot_rows, w_down.reshape((S, own_experts) + w_down.shape[1:])],
        ((("fsdp",), 1, 0), (("seq",), 0, "columns")), 2,
    )
    g_rows = g_rows.reshape(shape5)
    ffn_low = lax.dynamic_index_in_dim(ffn_all, seq_at, 0, keepdims=False)

    route_rows = routes[0]
    slot_rows = slots[0]
    router_scores = dot(ffn_low, full_router)
    picked = route_rows[:, :, None] == expert_ids[None, None, :]
    selected = jnp.sum(jnp.where(picked, router_scores[:, None, :], 0.0), axis=-1)
    gate_prob = jax.nn.softmax(selected, axis=-1)
    gate_table = jnp.sum(jnp.where(picked, gate_prob[:, :, None], 0.0), axis=1).T
    hit = table[None, :TOPK] == expert_ids[:, None, None]
    own_slots = jnp.max(jnp.where(hit, table[None, TOPK:], -1), axis=1)
    gate_slots = jnp.sum(
        jnp.where(
            own_slots[:, None, :] == slot_ids[None, :, None], gate_table[:, None, :], 0.0
        ),
        axis=-1,
    )
    by_device = (F, S, own_experts, capacity)

    def to_devices(values):
        return lanes(values.reshape(by_device).transpose(1, 0, 2, 3).reshape(N, -1), N)

    gate_send = to_devices(gate_slots)

    ffn_rows = mm("brt,btd->brd", select, ffn_all).astype(BF).reshape(grouped)
    x_rows, gate_up_w, gate_got = exchange(
        [ffn_rows, w_gate_up.reshape((S, own_experts) + w_gate_up.shape[1:]), gate_send],
        ((("fsdp",), 1, 0), (("seq",), 0, 0), (EVERY, 0, 0)), sizes, 4,
    )
    gate_up_w = gate_up_w.transpose(1, 0, 2, 3).reshape(own_experts, width, 2 * FF)
    x_rows = x_rows.reshape(shape5)
    row_gate = gate_got.reshape(S, F, -1)[:, :, : own_experts * capacity]
    row_gate = row_gate.transpose(1, 0, 2).reshape(F, S, own_experts, capacity, 1)

    gate_up = mm("asjcd,jdf->asjcf", x_rows, gate_up_w)
    gate_part = gate_up[..., :FF]
    up_part = gate_up[..., FF:]
    hidden_low = (jax.nn.silu(gate_part) * up_part).astype(BF)
    expert_out = mm("asjch,jhd->asjcd", hidden_low, down_w).astype(BF)
    out_wide = expert_out.astype(F32)
    g_wide = g_rows.astype(F32)
    grad_prob_rows = jnp.sum(out_wide * g_wide, axis=-1)
    moe_rows = (row_gate * out_wide).astype(BF)
    grad_eo_low = (row_gate * g_wide).astype(BF)

    grad_hidden_low = mm("asjcd,jhd->asjch", grad_eo_low, down_w).astype(BF)
    grad_hidden = lax.optimization_barrier(grad_hidden_low).astype(F32)
    sigmoid_gate = jax.nn.sigmoid(gate_part)
    grad_gate = grad_hidden * up_part * sigmoid_gate * (1.0 + gate_part * (1.0 - sigmoid_gate))
    grad_up = grad_hidden * gate_part * sigmoid_gate
    grad_gu_low = jnp.concatenate([grad_gate, grad_up], axis=-1).astype(BF)
    grad_rows = mm("asjcf,jdf->asjcd", grad_gu_low, gate_up_w).astype(BF)
    up_term = mm("asjcd,asjcf->jdf", x_rows, grad_gu_low).astype(BF)
    down_term = mm("asjch,asjcd->jhd", hidden_low, grad_eo_low).astype(BF)
    prob_send = grad_prob_rows.reshape(F, S, -1).transpose(1, 0, 2).reshape(N, -1)
    back_layout = grad_rows.reshape(F, S, own_experts * capacity, width)
    up_blocks = up_term.reshape(own_experts, S, part_width, 2 * FF).transpose(1, 0, 2, 3)
    grad_back, up_got, prob_got = exchange(
        [back_layout, up_blocks, lanes(prob_send, N)],
        ((("fsdp",), 0, 1), (("seq",), 0, 0), (EVERY, 0, 0)), sizes, 6,
    )
    grad_gate_up = up_got.reshape(w_gate_up.shape).astype(F32)
    prob_slots = prob_got.reshape(S, F, -1)[:, :, : own_experts * capacity]
    prob_slots = prob_slots.reshape(S, F, own_experts, capacity).transpose(1, 0, 2, 3)
    prob_slots = prob_slots.reshape(expert_count, capacity)

    grad_part = mm("brt,brd->btd", select, grad_back.reshape(S, -1, width)).astype(BF)

    prob_of_route = jnp.einsum(
        "tke,ec->tkc", picked.astype(F32), prob_slots, precision=lax.Precision.HIGHEST
    )
    at_slot = slot_rows[:, :, None] == slot_ids[None, None, :]
    grad_prob = jnp.sum(jnp.where(at_slot, prob_of_route, 0.0), axis=-1)
    grad_selected = gate_prob * (grad_prob - jnp.sum(gate_prob * grad_prob, axis=-1, keepdims=True))
    grad_logits = jnp.sum(jnp.where(picked, grad_selected[:, :, None], 0.0), axis=1).astype(BF)
    grad_ffn_add = mm("te,de->td", grad_logits, full_router)
    grad_router_part = mm("td,te->de", ffn_low, grad_logits)
    valid = (seq_at * tok_count + jnp.arange(tok_count, dtype=jnp.int32)) < lengths[0]
    grad_final = jnp.where(valid[:, None], cotangent[0].astype(F32), 0.0)
    grad_residual, grad_gain_ffn, grad_attn_low, moe_back, down_got = line(
        "grad", sizes, [grad_part], [grad_final, gain_ffn, residual, grad_ffn_add],
        [moe_rows.reshape(F, S, own_experts * capacity, width), down_term],
        ((("fsdp",), 0, 1), (("seq",), "columns", 0)), 7,
    )
    grad_down = down_got.reshape(w_down.shape).astype(F32)
    grad_attn_low = grad_attn_low.reshape(seq_total, width)

    grad_o_low = mm("td,ed->te", grad_attn_low, out_own).astype(BF)
    grad_out_part = mm("te,td->ed", o_low, grad_attn_low).astype(BF)
    grad_proj, grad_gain_heads = attend_back(
        lengths, projected, qkv_low, grad_o_low, cosine, sine, gain_heads, heads
    )
    grad_qkv_part = mm("td,te->de", attn_low, grad_proj).astype(BF).reshape(S, F, w_rows, own_width)
    attn_part = mm("te,de->td", grad_proj, w_proj).astype(BF).reshape(S, tok_count, width)
    moe_part = mm("brt,brd->btd", select, moe_back.reshape(S, -1, width)).astype(BF)
    sums, grad_out_got, grad_qkv_plane = line(
        "sum", sizes, [attn_part, moe_part], [],
        [grad_out_part.reshape(F, -1, width), grad_qkv_part],
        ((("fsdp",), 0, 0), (("fsdp",), 1, 0)), 8,
    )
    grad_attn_norm, moe_out = sums[0], sums[1]
    final = jnp.where(valid[:, None], residual + moe_out, 0.0)
    grad_out = jnp.sum(grad_out_got.astype(F32), axis=0)
    grad_qkv_own = jnp.sum(grad_qkv_plane.astype(F32), axis=0)
    layer_inputs = tokens[0].astype(F32)
    factor = rms_factor(layer_inputs)
    normed = layer_inputs * factor
    scaled = grad_attn_norm * gain_attn
    inner = jnp.mean(scaled * normed, axis=-1, keepdims=True)
    grad_inputs = grad_residual + factor * (scaled - normed * inner)
    grad_gain_attn = jnp.sum(grad_attn_norm * normed, axis=0)

    gain_part = jnp.concatenate([grad_gain_attn, grad_gain_ffn[0], grad_gain_heads.reshape(-1)])
    small_part = jnp.concatenate(
        [grad_router_part.reshape(N, -1), gain_part.reshape(N, -1)], axis=1
    )
    small_got, grad_qkv_got = exchange(
        [lanes(small_part, N), grad_qkv_own], ((EVERY, 0, 0), (("seq",), 0, 0)), sizes, 10
    )
    grad_qkv = whole_columns(grad_qkv_got)
    small_sum = jnp.sum(small_got, axis=0).reshape(-1)
    grad_router = small_sum[:router_size].reshape(w_router.shape)
    grad_gains = small_sum[router_size : router_size + small]
    return (
        final.astype(BF)[None],
        grad_inputs[None],
        grad_qkv,
        grad_out,
        grad_router,
        grad_gains,
        grad_gate_up,
        grad_down,
    )


def solution(mesh):
    in_specs = (
        P("fsdp", "seq", None),
        P("fsdp", "seq", None),
        P("fsdp"),
        P("fsdp", "seq", None),
        P("fsdp", "seq", None),
        P(("seq", "fsdp"), None),
        P(("seq", "fsdp"), None),
        P(("seq", "fsdp"), None),
        P(("seq", "fsdp")),
        P("fsdp", "seq", None),
        P("fsdp", None, "seq"),
    )
    out_specs = (
        P("fsdp", "seq", None),
        P("fsdp", "seq", None),
        P(("seq", "fsdp"), None),
        P(("seq", "fsdp"), None),
        P(("seq", "fsdp"), None),
        P(("seq", "fsdp")),
        P("fsdp", "seq", None),
        P("fsdp", None, "seq"),
    )
    return jax.shard_map(
        per_device, mesh=mesh, in_specs=in_specs, out_specs=out_specs, check_vma=False
    )
```

```python
import functools

import jax
import jax.numpy as jnp
from jax import lax
from jax.experimental import pallas as pl
from jax.experimental.pallas import tpu as pltpu
from jax.sharding import PartitionSpec as P

QH = 32
KH = 4
HD = 128
FF = 768
TOPK = 8
EPSILON = 1e-06
THETA = 1000000.0
MASKED = -1e30
AHEAD = 2
BF = jnp.bfloat16
F32 = jnp.float32
MESH = pl.DeviceIdType.MESH
ANY = pl.BlockSpec(memory_space=pl.ANY)
VM = pl.BlockSpec(memory_space=pltpu.VMEM)
DMA = pltpu.SemaphoreType.DMA
EVERY = ("seq", "fsdp")

def index_of(sizes, axes):
    at = 0
    for axis in axes:
        at = at * sizes[axis] + lax.axis_index(axis)
    return at


def count_of(sizes, axes):
    number = 1
    for axis in axes:
        number *= sizes[axis]
    return number


def place_of(sizes, axes, at):
    if len(axes) == 1:
        return {axes[0]: at}
    return {axes[0]: at // sizes[axes[1]], axes[1]: at % sizes[axes[1]]}


def greet(sizes):
    total = count_of(sizes, EVERY)
    me = index_of(sizes, EVERY)
    barrier = pltpu.get_barrier_semaphore()
    for step in range(1, total):
        pl.semaphore_signal(
            barrier, inc=1, device_id=place_of(sizes, EVERY, lax.rem(me + step, total)),
            device_id_type=MESH,
        )
    return lambda: pl.semaphore_wait(barrier, total - 1)


def block_of(ref, dim, at, total):
    if dim == "columns":
        width = ref.shape[-1] // total
        return ref.at[:, :, pl.ds(pl.multiple_of(at * width, 128), width)]
    return ref.at[at] if dim == 0 else ref.at[:, at]


class Blocks:
    def __init__(self, sizes, specs, sources, results, sems):
        self.own, self.away = [], []
        if not specs:
            return
        send_sem, recv_sem, own_sem, *stages = sems
        for i, (axes, before, after) in enumerate(specs):
            me = index_of(sizes, axes)
            total = count_of(sizes, axes)
            source = block_of(sources[i], before, me, total)
            result = block_of(results[i], after, me, total)
            self.own.append(
                (
                    pltpu.make_async_copy(source, stages[i], own_sem.at[i, 0]),
                    pltpu.make_async_copy(stages[i], result, own_sem.at[i, 1]),
                )
            )
            for step in range(1, total):
                target = lax.rem(me + step, total)
                self.away.append(
                    pltpu.make_async_remote_copy(
                        src_ref=block_of(sources[i], before, target, total),
                        dst_ref=block_of(results[i], after, me, total),
                        send_sem=send_sem.at[i, step],
                        recv_sem=recv_sem.at[i, step],
                        device_id=place_of(sizes, axes, target),
                        device_id_type=MESH,
                    )
                )

    def start(self):
        for copy in self.away:
            copy.start()
        for inward, _ in self.own:
            inward.start()

    def wait(self):
        for inward, outward in self.own:
            inward.wait()
            outward.start()
        for _, outward in self.own:
            outward.wait()
        for copy in self.away:
            copy.wait()


def block_scratch(sizes, arrays, specs):
    if not specs:
        return []
    total = max(count_of(sizes, axes) for axes, _, _ in specs)
    stages = []
    for array, (axes, before, after) in zip(arrays, specs):
        shape = list(array.shape)
        if before == "columns":
            shape[-1] //= count_of(sizes, axes)
        else:
            del shape[before]
        stages.append(pltpu.VMEM(tuple(shape), array.dtype))
    count = len(specs)
    return [DMA((count, total)), DMA((count, total)), DMA((count, 2))] + stages


def block_outs(sizes, arrays, specs):
    outs = []
    for array, (axes, before, after) in zip(arrays, specs):
        shape = list(array.shape)
        total = count_of(sizes, axes)
        if before == "columns":
            shape = [total, shape[0], shape[1], shape[2] // total]
        elif after == "columns":
            shape = [shape[1], shape[2], shape[3] * total]
        elif before != after:
            shape[0], shape[1] = shape[1], shape[0]
        outs.append(jax.ShapeDtypeStruct(tuple(shape), array.dtype))
    return outs


def exchange_kernel(sizes, specs, *refs):
    count = len(specs)
    met = greet(sizes)
    blocks = Blocks(sizes, specs, refs[:count], refs[count : 2 * count], refs[2 * count :])
    met()
    blocks.start()
    blocks.wait()


def exchange(arrays, specs, sizes, collective_id):
    count = len(arrays)
    return pl.pallas_call(
        functools.partial(exchange_kernel, sizes, specs),
        out_shape=block_outs(sizes, arrays, specs),
        in_specs=[ANY] * count,
        out_specs=[ANY] * count,
        scratch_shapes=block_scratch(sizes, arrays, specs),
        compiler_params=pltpu.CompilerParams(collective_id=collective_id, has_side_effects=True),
        name=f"exchange_{collective_id}",
    )(*arrays)


def entry_kernel(
    sizes, tok_ref, cot_ref, table_ref, wqkv_ref, wout_ref, small_ref,
    tok_out, cot_out, table_out, wq_out, wo_out, small_out,
    tok_send, tok_recv, tab_send, tab_recv, wq_zsend, wq_zrecv,
    pl_send, pl_recv, sib_send, sib_recv, sm_send, sm_recv, own_sem, *stages,
):
    S, F = sizes["seq"], sizes["fsdp"]
    s = lax.axis_index("seq")
    f = lax.axis_index("fsdp")
    N = S * F
    chips = F // 2
    me = s * F + f
    other = f + 1 - 2 * lax.rem(f, 2)
    rows = tok_ref.shape[0]
    chunks = tok_recv.shape[2]
    span = rows // chunks
    met = greet(sizes)
    kv = KH * HD // S
    q_width = QH * HD // S
    starts = (0, q_width * S, (q_width + kv) * S)
    widths = (q_width, kv, kv)
    offsets = (0, q_width, q_width + kv)

    def columns(z, p):
        return pl.ds(pl.multiple_of(starts[p] + z * widths[p], 128), widths[p])

    pairs = [
        (wqkv_ref.at[:, columns(s, p)], wq_out.at[s, f, :, pl.ds(offsets[p], widths[p])])
        for p in range(3)
    ] + [
        (wout_ref, wo_out.at[f]),
        (tok_ref, tok_out.at[s]),
        (cot_ref, cot_out.at[s]),
        (table_ref, table_out.at[s]),
        (small_ref, small_out.at[me]),
    ]
    inward = [
        pltpu.make_async_copy(source, stages[i], own_sem.at[i, 0])
        for i, (source, _) in enumerate(pairs)
    ]
    outward = [
        pltpu.make_async_copy(stages[i], result, own_sem.at[i, 1])
        for i, (_, result) in enumerate(pairs)
    ]
    for copy in inward:
        copy.start()
    met()

    def remote(src, dst, send_sem, recv_sem, where):
        return pltpu.make_async_remote_copy(
            src_ref=src, dst_ref=dst, send_sem=send_sem, recv_sem=recv_sem,
            device_id=where, device_id_type=MESH,
        )

    wq_line = []
    tables = []
    for step in range(1, S):
        target = lax.rem(s + step, S)
        for p in range(3):
            copy = remote(
                wqkv_ref.at[:, columns(target, p)],
                wq_out.at[s, f, :, pl.ds(offsets[p], widths[p])],
                wq_zsend.at[step, p], wq_zrecv.at[step, p], {"seq": target},
            )
            copy.start()
            wq_line.append(copy)
        copy = remote(
            table_ref, table_out.at[s], tab_send.at[step], tab_recv.at[step], {"seq": target}
        )
        copy.start()
        tables.append(copy)

    def along(a, block, c, way, hop):
        source, result = ((tok_ref, tok_out), (cot_ref, cot_out))[a]
        here = result.at[block, pl.ds(c * span, span)]
        src = source.at[pl.ds(c * span, span)] if hop == 1 else here
        return remote(
            src, here, tok_send.at[a, way, c, hop], tok_recv.at[a, way, c, hop],
            {"seq": s + 1 if way == 0 else s - 1},
        )

    def depart(a):
        for c in range(chunks):
            @pl.when(s < S - 1)
            def _():
                along(a, s, c, 0, 1).start()

            @pl.when(s > 0)
            def _():
                along(a, s, c, 1, 1).start()

    def relay(a, hop):
        for c in range(chunks):
            @pl.when(s >= hop)
            def _():
                along(a, s - hop, c, 0, hop).wait_recv()
                if hop < S - 1:
                    @pl.when(s < S - 1)
                    def _():
                        along(a, s - hop, c, 0, hop + 1).start()

            @pl.when(s < S - hop)
            def _():
                along(a, s + hop, c, 1, hop).wait_recv()
                if hop < S - 1:
                    @pl.when(s > 0)
                    def _():
                        along(a, s + hop, c, 1, hop + 1).start()

    depart(0)

    def plane_block(slot, owner):
        if slot == S:
            return wo_out.at[owner]
        return wq_out.at[lax.rem(s - slot + S, S), owner]

    def to_chip(slot, step):
        block = plane_block(slot, f)
        return remote(block, block, pl_send.at[slot, step], pl_recv.at[slot, step],
                      {"fsdp": lax.rem(f + 2 * step, F)})

    def to_other(slot, step):
        block = plane_block(slot, lax.rem(f - 2 * step + F, F))
        return remote(block, block, sib_send.at[slot, step], sib_recv.at[slot, step],
                      {"fsdp": other})

    def spread(slot):
        for step in range(1, chips):
            to_chip(slot, step).start()
        to_other(slot, 0).start()

    def forward(slot):
        for step in range(1, chips):
            to_chip(slot, step).wait_recv()
            to_other(slot, step).start()

    smalls = []
    for step in range(1, N):
        target = lax.rem(me + step, N)
        copy = remote(small_ref, small_out.at[me], sm_send.at[step], sm_recv.at[step],
                      place_of(sizes, EVERY, target))
        copy.start()
        smalls.append(copy)
    for i, copy in enumerate(inward):
        copy.wait()
        outward[i].start()
    for copy in outward[:3]:
        copy.wait()
    spread(0)
    outward[3].wait()
    spread(S)
    relay(0, 1)
    depart(1)
    for step in range(1, S):
        for p in range(3):
            wq_line[(step - 1) * 3 + p].wait()
        spread(step)
    for hop in range(2, S):
        relay(0, hop)
        relay(1, hop - 1)
    for slot in range(S + 1):
        forward(slot)
    relay(1, S - 1)
    for a in range(2):
        for hop in range(1, S):
            for c in range(chunks):
                @pl.when((s < S - 1) & (s >= hop - 1))
                def _():
                    along(a, s, c, 0, hop).wait_send()

                @pl.when((s > 0) & (s <= S - hop))
                def _():
                    along(a, s, c, 1, hop).wait_send()
    for copy in outward[4:]:
        copy.wait()
    for slot in range(S + 1):
        for step in range(1, chips):
            to_chip(slot, step).wait_send()
        for step in range(chips):
            to_other(slot, step).wait_send()
            block = plane_block(slot, lax.rem(other - 2 * step + F, F))
            remote(block, block, sib_send.at[slot, step], sib_recv.at[slot, step],
                   {"fsdp": other}).wait_recv()
    for copy in tables + smalls:
        copy.wait()


def entry(tokens, cotangent, table, w_qkv, w_out, small, sizes, collective_id, chunks=4):
    S, F = sizes["seq"], sizes["fsdp"]
    own_width = w_qkv.shape[1] // S
    N = S * F
    line_out = jax.ShapeDtypeStruct((S,) + tokens.shape, tokens.dtype)
    q_width, kv = QH * HD // S, KH * HD // S
    stages = [
        pltpu.VMEM(shape, dtype)
        for shape, dtype in [
            ((w_qkv.shape[0], q_width), BF),
            ((w_qkv.shape[0], kv), BF),
            ((w_qkv.shape[0], kv), BF),
            (w_out.shape, BF),
            (tokens.shape, BF),
            (cotangent.shape, BF),
            (table.shape, table.dtype),
            (small.shape, BF),
        ]
    ]
    return pl.pallas_call(
        functools.partial(entry_kernel, sizes),
        out_shape=[
            line_out,
            line_out,
            jax.ShapeDtypeStruct((S,) + table.shape, table.dtype),
            jax.ShapeDtypeStruct((S, F, w_qkv.shape[0], own_width), w_qkv.dtype),
            jax.ShapeDtypeStruct((F,) + w_out.shape, w_out.dtype),
            jax.ShapeDtypeStruct((N,) + small.shape, small.dtype),
        ],
        in_specs=[ANY] * 6,
        out_specs=[ANY] * 6,
        scratch_shapes=[
            DMA((2, 2, chunks, S)), DMA((2, 2, chunks, S)), DMA((S,)), DMA((S,)),
            DMA((S, 3)), DMA((S, 3)), DMA((S + 1, F // 2)), DMA((S + 1, F // 2)),
            DMA((S + 1, F // 2)), DMA((S + 1, F // 2)), DMA((N,)), DMA((N,)), DMA((8, 2)),
        ] + stages,
        compiler_params=pltpu.CompilerParams(collective_id=collective_id, has_side_effects=True),
        name="entry",
    )(tokens, cotangent, table, w_qkv, w_out, small)


def line_kernel(sizes, chunks, mode, parts, extra, *refs):
    S = sizes["seq"]
    count = len(extra)
    names = {
        "ffn": (["base", "gain"], ["resid_out", "all_out"]),
        "grad": (["base", "gain", "resid", "add"], ["grad_out", "gain_out", "all_out"]),
        "sum": ([], ["sum_out"]),
    }[mode]
    refs = list(refs)

    def take(number):
        taken, refs[:number] = refs[:number], []
        return taken

    part_refs = take(parts)
    given = dict(zip(names[0], take(len(names[0]))))
    sources = take(count)
    given.update(zip(names[1], take(len(names[1]))))
    results = take(count)
    from_left, from_right = take(2)
    gather = mode != "sum"
    if gather:
        (stage,) = take(1)
    rs_send, rs_recv = take(2)
    if gather:
        ag_send, ag_recv, own_sem = take(3)
        all_out = given["all_out"]
    s = lax.axis_index("seq")
    rows = part_refs[0].shape[1]
    span = rows // chunks
    met = greet(sizes)
    blocks = Blocks(sizes, extra, sources, results, refs)
    met()

    def at(c):
        return pl.ds((c % chunks) * span, span)

    def mine(d, c):
        return part_refs[c // chunks].at[d, at(c)]

    def landed(way, d, c):
        return (from_left, from_right)[way].at[c // chunks, d, at(c)]

    def rs_copy(d, c, way, src):
        return pltpu.make_async_remote_copy(
            src_ref=src, dst_ref=landed(way, d, c),
            send_sem=rs_send.at[way, d, c], recv_sem=rs_recv.at[way, d, c],
            device_id={"seq": s + 1 if way == 0 else s - 1}, device_id_type=MESH,
        )

    def ag_copy(block, c, way, hop):
        src = stage.at[at(c)] if hop == 1 else all_out.at[block, at(c)]
        return pltpu.make_async_remote_copy(
            src_ref=src, dst_ref=all_out.at[block, at(c)],
            send_sem=ag_send.at[way, c, hop], recv_sem=ag_recv.at[way, c, hop],
            device_id={"seq": s + 1 if way == 0 else s - 1}, device_id_type=MESH,
        )

    def end_step(c):
        for d in range(S - 1, 0, -1):
            @pl.when((s == 0) & (d > s))
            def _():
                rs_copy(d, c, 0, mine(d, c)).start()
        for d in range(S - 1):
            @pl.when((s == S - 1) & (d < s))
            def _():
                rs_copy(d, c, 1, mine(d, c)).start()

    def middle_step(c):
        for way in range(2):
            order = range(S - 1, 0, -1) if way == 0 else range(S - 1)
            for d in order:
                inside = (s > 0) & (d > s) if way == 0 else (s < S - 1) & (d < s)

                @pl.when(inside)
                def _():
                    buffer = landed(way, d, c)
                    rs_copy(d, c, way, buffer).wait_recv()
                    total = buffer[...].astype(F32) + mine(d, c)[...].astype(F32)
                    buffer[...] = total.astype(BF)
                    rs_copy(d, c, way, buffer).start()

    def final_step(c):
        @pl.when(s > 0)
        def _():
            rs_copy(s, c, 0, mine(s, c)).wait_recv()

        @pl.when(s < S - 1)
        def _():
            rs_copy(s, c, 1, mine(s, c)).wait_recv()

        total = mine(s, c)[...].astype(F32)
        total = total + jnp.where(s > 0, landed(0, s, c)[...].astype(F32), 0.0)
        total = total + jnp.where(s < S - 1, landed(1, s, c)[...].astype(F32), 0.0)
        if mode == "sum":
            given["sum_out"][c // chunks, at(c), :] = total
            return
        if mode == "ffn":
            value = given["base"][at(c), :].astype(F32) + total
            given["resid_out"][at(c), :] = value
            factor = lax.rsqrt(jnp.mean(value * value, axis=-1, keepdims=True) + EPSILON)
            low = (value * factor * given["gain"][...]).astype(BF)
        else:
            upstream = total + given["add"][at(c), :]
            value = given["resid"][at(c), :]
            factor = lax.rsqrt(jnp.mean(value * value, axis=-1, keepdims=True) + EPSILON)
            normed = value * factor
            scaled = upstream * given["gain"][...]
            inner = jnp.mean(scaled * normed, axis=-1, keepdims=True)
            result = given["base"][at(c), :] + factor * (scaled - normed * inner)
            given["grad_out"][at(c), :] = result
            gained = jnp.sum(upstream * normed, axis=0, keepdims=True)
            gain_out = given["gain_out"]
            gain_out[...] = gained if c == 0 else gain_out[...] + gained
            low = result.astype(BF)
        stage[at(c), :] = low
        pltpu.make_async_copy(stage.at[at(c)], all_out.at[s, at(c)], own_sem.at[c]).start()

        @pl.when(s < S - 1)
        def _():
            ag_copy(s, c, 0, 1).start()

        @pl.when(s > 0)
        def _():
            ag_copy(s, c, 1, 1).start()

    def relay_step(c, hop):
        @pl.when(s >= hop)
        def _():
            ag_copy(s - hop, c, 0, hop).wait_recv()
            if hop < S - 1:
                @pl.when(s < S - 1)
                def _():
                    ag_copy(s - hop, c, 0, hop + 1).start()

        @pl.when(s < S - hop)
        def _():
            ag_copy(s + hop, c, 1, hop).wait_recv()
            if hop < S - 1:
                @pl.when(s > 0)
                def _():
                    ag_copy(s + hop, c, 1, hop + 1).start()

    steps = chunks * parts
    ahead = min(steps, AHEAD if gather else steps)
    for c in range(ahead):
        end_step(c)
    blocks.start()
    hops = S - 1 if gather else 0
    for t in range(steps + 1 + hops):
        if t < steps:
            middle_step(t)
        if t + ahead < steps:
            end_step(t + ahead)
        if 0 <= t - 1 < steps:
            final_step(t - 1)
        for hop in range(1, hops + 1):
            if 0 <= t - 1 - hop < steps:
                relay_step(t - 1 - hop, hop)

    for c in range(steps):
        for d in range(S - 1, 0, -1):
            @pl.when(d > s)
            def _():
                rs_copy(d, c, 0, mine(d, c)).wait_send()
        for d in range(S - 1):
            @pl.when(d < s)
            def _():
                rs_copy(d, c, 1, mine(d, c)).wait_send()
        if gather:
            pltpu.make_async_copy(stage.at[at(c)], all_out.at[s, at(c)], own_sem.at[c]).wait()
            for hop in range(1, S):
                @pl.when((s < S - 1) & (s >= hop - 1))
                def _():
                    ag_copy(s, c, 0, hop).wait_send()

                @pl.when((s > 0) & (s <= S - hop))
                def _():
                    ag_copy(s, c, 1, hop).wait_send()
    blocks.wait()


def line(mode, sizes, parts, others, extras, specs, collective_id, chunks=8):
    S = sizes["seq"]
    _, rows, width = parts[0].shape
    full = jax.ShapeDtypeStruct((rows, width), F32)
    everyone = jax.ShapeDtypeStruct((S, rows, width), BF)
    steps = chunks * len(parts)
    scratch = [pltpu.VMEM((len(parts), S, rows, width), BF)] * 2
    sems = [DMA((2, S, steps)), DMA((2, S, steps))]
    if mode == "ffn":
        outs, out_specs = [full, everyone], [VM, ANY]
    elif mode == "grad":
        outs, out_specs = [full, jax.ShapeDtypeStruct((1, width), F32), everyone], [VM, VM, ANY]
    else:
        outs, out_specs = [jax.ShapeDtypeStruct((len(parts), rows, width), F32)], [VM]
    if mode != "sum":
        scratch.append(pltpu.VMEM((rows, width), BF))
        sems += [DMA((2, chunks, S)), DMA((2, chunks, S)), DMA((chunks,))]
    return pl.pallas_call(
        functools.partial(line_kernel, sizes, chunks, mode, len(parts), specs),
        out_shape=outs + block_outs(sizes, extras, specs),
        in_specs=[VM] * (len(parts) + len(others)) + [ANY] * len(extras),
        out_specs=out_specs + [ANY] * len(extras),
        scratch_shapes=scratch + sems + block_scratch(sizes, extras, specs),
        compiler_params=pltpu.CompilerParams(
            collective_id=collective_id, has_side_effects=True, vmem_limit_bytes=56 << 20
        ),
        name=f"line_{mode}",
    )(*parts, *others, *extras)


def turn(values, cosine, sine):
    return values * cosine + pltpu.roll(values, HD // 2, 1) * sine


def softmax_block(query, keys, first_row, length, scale):
    scores = lax.dot_general(
        query, keys, (((1,), (1,)), ((), ())), preferred_element_type=F32
    ) * scale
    row = first_row + lax.broadcasted_iota(jnp.int32, scores.shape, 0)
    column = lax.broadcasted_iota(jnp.int32, scores.shape, 1)
    scores = jnp.where((column <= row) & (column < length), scores, MASKED)
    peak = jnp.max(scores, axis=-1, keepdims=True)
    weights = jnp.exp(scores - peak)
    return weights * (1.0 / jnp.sum(weights, axis=-1, keepdims=True))


def tiles(width, step, body):
    @pl.loop(0, width // step)
    def _(n):
        body(pl.ds(pl.multiple_of(n * step, step), step))


def attend_kernel(sizes, heads, blocks, specs, *refs):
    count = len(specs)
    length_ref, tok_ref, gain_ref, wq_ref, cos_ref, sin_ref, gains_ref, wo_ref = refs[:8]
    sources = refs[8 : 8 + count]
    attn_ref, proj_ref, low_ref, out_ref, part_ref = refs[8 + count : 13 + count]
    results = refs[13 + count : 13 + 2 * count]
    k_all, v_all, *sems = refs[13 + 2 * count :]
    step = pl.program_id(0)

    @pl.when(step == 0)
    def _():
        greet(sizes)()
        Blocks(sizes, specs, sources, results, sems).start()

    rows, width = proj_ref.shape
    length = length_ref[0]
    cosine = cos_ref[...]
    sine = sin_ref[...]
    q_gain = gains_ref[0:1, :]
    k_gain = gains_ref[1:2, :]
    scale = HD ** (-0.5)
    value = tok_ref[...].astype(F32)
    factor = lax.rsqrt(jnp.mean(value * value, axis=-1, keepdims=True) + EPSILON)
    attn_ref[...] = (value * factor * gain_ref[...]).astype(BF)

    def project(at):
        proj_ref[:, at] = jnp.dot(attn_ref[...], wq_ref[:, at], preferred_element_type=F32)

    tiles(width, 256, project)

    def normed(raw, gain):
        factor = lax.rsqrt(jnp.mean(raw * raw, axis=-1, keepdims=True) + EPSILON)
        return turn(raw * factor * gain, cosine, sine).astype(BF)

    key = normed(proj_ref[:, heads * HD : (heads + 1) * HD], k_gain)
    value_low = proj_ref[:, (heads + 1) * HD :].astype(BF)
    low_ref[:, heads * HD : (heads + 1) * HD] = key
    low_ref[:, (heads + 1) * HD :] = value_low
    here = pl.ds(pl.multiple_of(step * rows, rows), rows)
    k_all[here, :] = key
    v_all[here, :] = value_low
    for block in range(blocks):
        @pl.when(step == block)
        def _():
            reach = (block + 1) * rows

            def one(column):
                query = normed(proj_ref[:, column], q_gain)
                low_ref[:, column] = query
                probs = softmax_block(query, k_all[:reach, :], block * rows, length, scale)
                mixed = jnp.dot(probs.astype(BF), v_all[:reach, :], preferred_element_type=F32)
                out_ref[:, column] = mixed.astype(BF)

            tiles(heads * HD, HD, one)

    def leave(at):
        part_ref[:, at] = jnp.dot(
            out_ref[...], wo_ref[:, at], preferred_element_type=F32
        ).astype(BF)

    tiles(part_ref.shape[1], 256, leave)

    @pl.when(step == blocks - 1)
    def _():
        Blocks(sizes, specs, sources, results, sems).wait()


def attend(
    length, tokens, gain, w_proj, cosine, sine, gains, w_out, heads, extras, specs, sizes,
    collective_id, blocks=4,
):
    total, width = tokens.shape
    own_width = w_proj.shape[1]
    rows = total // blocks
    q_width = heads * HD

    def by_rows(columns):
        return pl.BlockSpec((rows, columns), lambda i: (i, 0))

    def whole(array):
        return pl.BlockSpec(array.shape, lambda i: (0, 0), pipeline_mode=pl.Buffered(1))

    return pl.pallas_call(
        functools.partial(attend_kernel, sizes, heads, blocks, specs),
        grid=(blocks,),
        out_shape=[
            jax.ShapeDtypeStruct((total, width), BF),
            jax.ShapeDtypeStruct((total, own_width), F32),
            jax.ShapeDtypeStruct((total, own_width), BF),
            jax.ShapeDtypeStruct((total, q_width), BF),
            jax.ShapeDtypeStruct((total, width), BF),
        ] + block_outs(sizes, extras, specs),
        in_specs=[
            pl.BlockSpec(memory_space=pltpu.SMEM),
            by_rows(width),
            whole(gain),
            whole(w_proj),
            by_rows(HD),
            by_rows(HD),
            whole(gains),
            whole(w_out),
        ] + [ANY] * len(extras),
        out_specs=[by_rows(width), by_rows(own_width), by_rows(own_width), by_rows(q_width), by_rows(width)]
        + [ANY] * len(extras),
        scratch_shapes=[pltpu.VMEM((total, HD), BF), pltpu.VMEM((total, HD), BF)]
        + block_scratch(sizes, extras, specs),
        compiler_params=pltpu.CompilerParams(
            collective_id=collective_id, has_side_effects=True, vmem_limit_bytes=58 << 20
        ),
        name="attend",
    )(length, tokens, gain, w_proj, cosine, sine, gains, w_out, *extras)


def attend_back_kernel(sizes, heads, blocks, specs, *refs):
    count = len(specs)
    length_ref, proj_ref, low_ref, kv_ref, grad_ref, wo_ref, wq_ref, cos_ref, sin_ref, gains_ref = refs[:10]
    sources = refs[10 : 10 + count]
    out_ref, part_ref, gains_out = refs[10 + count : 13 + count]
    results = refs[13 + count : 13 + 2 * count]
    gk_all, gv_all, go_ref, *sems = refs[13 + 2 * count :]
    step = pl.program_id(0)
    rows = proj_ref.shape[0]
    length = length_ref[0]
    cosine = cos_ref[...]
    sine = sin_ref[...]
    q_gain = gains_ref[0:1, :]
    k_gain = gains_ref[1:2, :]
    scale = HD ** (-0.5)
    block_at = blocks - 1 - step

    def back(raw, gain, grad):
        grad = turn(grad, cosine, -sine)
        factor = lax.rsqrt(jnp.mean(raw * raw, axis=-1, keepdims=True) + EPSILON)
        unit = raw * factor
        scaled = grad * gain
        inner = jnp.mean(scaled * unit, axis=-1, keepdims=True)
        return factor * (scaled - unit * inner), jnp.sum(grad * unit, axis=0, keepdims=True)

    @pl.when(step == 0)
    def _():
        greet(sizes)()
        Blocks(sizes, specs, sources, results, sems).start()
        gk_all[...] = jnp.zeros_like(gk_all)
        gv_all[...] = jnp.zeros_like(gv_all)
        gains_out[...] = jnp.zeros_like(gains_out)

    def arrive(at):
        go_ref[:, at] = lax.dot_general(
            grad_ref[...], wo_ref[at, :], (((1,), (1,)), ((), ())), preferred_element_type=F32
        ).astype(BF)

    tiles(heads * HD, 256, arrive)
    for block in range(blocks):
        @pl.when(block_at == block)
        def _():
            reach = (block + 1) * rows
            keys = kv_ref[:reach, :HD]
            values = kv_ref[:reach, HD:]

            def one(column):
                query = low_ref[:, column]
                grad_o = go_ref[:, column]
                probs = softmax_block(query, keys, block * rows, length, scale)
                grad_p = lax.dot_general(
                    grad_o, values, (((1,), (1,)), ((), ())), preferred_element_type=F32
                )
                inner = jnp.sum(probs * grad_p, axis=-1, keepdims=True)
                grad_s = (probs * (grad_p - inner)).astype(BF)
                grad_q = jnp.dot(grad_s, keys, preferred_element_type=F32) * scale
                gk_all[:reach, :] += lax.dot_general(
                    grad_s, query, (((0,), (0,)), ((), ())), preferred_element_type=F32
                )
                gv_all[:reach, :] += lax.dot_general(
                    probs.astype(BF), grad_o, (((0,), (0,)), ((), ())), preferred_element_type=F32
                )
                grad_raw, gained = back(proj_ref[:, column], q_gain, grad_q.astype(BF).astype(F32))
                out_ref[:, column] = grad_raw.astype(BF)
                gains_out[0:1, :] += gained

            tiles(heads * HD, HD, one)

    here = pl.ds(pl.multiple_of(block_at * rows, rows), rows)
    grad_k = (gk_all[here, :] * scale).astype(BF).astype(F32)
    grad_raw, gained = back(proj_ref[:, heads * HD : (heads + 1) * HD], k_gain, grad_k)
    out_ref[:, heads * HD : (heads + 1) * HD] = grad_raw.astype(BF)
    out_ref[:, (heads + 1) * HD :] = gv_all[here, :].astype(BF)
    gains_out[1:2, :] += gained

    def leave(at):
        part_ref[:, at] = lax.dot_general(
            out_ref[...], wq_ref[at, :], (((1,), (1,)), ((), ())), preferred_element_type=F32
        ).astype(BF)

    tiles(part_ref.shape[1], 256, leave)

    @pl.when(step == blocks - 1)
    def _():
        Blocks(sizes, specs, sources, results, sems).wait()


def attend_back(
    length, projected, low, grad, w_out, w_proj, cosine, sine, gains, heads, extras, specs, sizes,
    collective_id, blocks=4,
):
    total, own_width = projected.shape
    width = w_out.shape[1]
    rows = total // blocks
    q_width = heads * HD

    def by_rows(columns):
        return pl.BlockSpec((rows, columns), lambda i: (blocks - 1 - i, 0))

    def whole(array):
        return pl.BlockSpec(array.shape, lambda i: (0, 0), pipeline_mode=pl.Buffered(1))

    return pl.pallas_call(
        functools.partial(attend_back_kernel, sizes, heads, blocks, specs),
        grid=(blocks,),
        out_shape=[
            jax.ShapeDtypeStruct((total, own_width), BF),
            jax.ShapeDtypeStruct((total, width), BF),
            jax.ShapeDtypeStruct((2, HD), F32),
        ] + block_outs(sizes, extras, specs),
        in_specs=[
            pl.BlockSpec(memory_space=pltpu.SMEM),
            by_rows(own_width),
            by_rows(q_width),
            pl.BlockSpec((total, 2 * HD), lambda i: (0, heads // 2)),
            by_rows(width),
            whole(w_out),
            whole(w_proj),
            by_rows(HD),
            by_rows(HD),
            whole(gains),
        ] + [ANY] * len(extras),
        out_specs=[by_rows(own_width), by_rows(width), pl.BlockSpec((2, HD), lambda i: (0, 0))]
        + [ANY] * len(extras),
        scratch_shapes=[
            pltpu.VMEM((total, HD), F32),
            pltpu.VMEM((total, HD), F32),
            pltpu.VMEM((rows, q_width), BF),
        ] + block_scratch(sizes, extras, specs),
        compiler_params=pltpu.CompilerParams(
            collective_id=collective_id, has_side_effects=True, vmem_limit_bytes=58 << 20
        ),
        name="attend_back",
    )(length, projected, low, low, grad, w_out, w_proj, cosine, sine, gains, *extras)


def rms_factor(values):
    return lax.rsqrt(jnp.mean(values * values, axis=-1, keepdims=True) + EPSILON)


def dot(left, right):
    return jnp.dot(left, right, preferred_element_type=F32)


def mm(form, left, right):
    return jnp.einsum(form, left, right, preferred_element_type=F32)


def whole_columns(blocks):
    parts, rows, _ = blocks.shape
    q_width = QH * HD // parts
    kv_width = KH * HD // parts
    moved = blocks.transpose(1, 0, 2)
    return jnp.concatenate(
        [
            moved[..., :q_width].reshape(rows, -1),
            moved[..., q_width : q_width + kv_width].reshape(rows, -1),
            moved[..., q_width + kv_width :].reshape(rows, -1),
        ],
        axis=-1,
    )


def lanes(flat, lead):
    width = flat.shape[-1]
    rows = -(-width // 2048) * 16
    return jnp.pad(flat, ((0, 0), (0, rows * 128 - width))).reshape(lead, rows, 128)


def per_device(
    tokens, cotangent, lengths, routes, slots, w_qkv, w_out, w_router, norm_gains, w_gate_up, w_down
):
    tok_count = tokens.shape[1]
    width = tokens.shape[2]
    S = lax.axis_size("seq")
    F = lax.axis_size("fsdp")
    N = S * F
    sizes = {"seq": S, "fsdp": F}
    local_experts = w_gate_up.shape[0]
    own_experts = local_experts // S
    expert_count = w_router.shape[1]
    capacity = tok_count * TOPK * 5 // (4 * expert_count)
    heads = QH // S
    seq_total = tok_count * S
    q_width = heads * HD
    own_width = q_width + 2 * HD
    seq_at = lax.axis_index("seq")
    w_rows = w_qkv.shape[0]
    small = norm_gains.shape[0]
    router_size = w_router.size
    part_width = w_gate_up.shape[1]
    down_width = w_down.shape[2]
    assert KH == S and local_experts % S == 0

    small_send = lanes(jnp.concatenate([w_router.reshape(-1), norm_gains])[None], 1)[0]
    table = jnp.concatenate([routes[0].T, slots[0].T])
    tok_all, cot_all, table_all, w_proj, out_own, small_all = entry(
        tokens[0], cotangent[0], table, w_qkv, w_out, small_send, sizes, 1
    )
    w_proj = w_proj.reshape(width, own_width)
    out_own = out_own.reshape(q_width, width)
    small_flat = small_all.reshape(N, -1)
    full_router = small_flat[:, :router_size].reshape(width, expert_count)
    gain_values = small_flat[:, router_size : router_size + small].reshape(-1).astype(F32)
    gain_attn = gain_values[:width]
    gain_ffn = gain_values[width : 2 * width][None]
    gain_heads = gain_values[2 * width :].reshape(2, HD)

    positions = jnp.arange(seq_total, dtype=jnp.int32)
    frequency = THETA ** (-jnp.arange(HD // 2, dtype=F32) / (HD // 2))
    angles = positions.astype(F32)[:, None] * frequency[None, :]
    cosine = jnp.concatenate([jnp.cos(angles)] * 2, axis=-1)
    sine = jnp.concatenate([-jnp.sin(angles), jnp.sin(angles)], axis=-1)
    attn_low, projected, qkv_low, o_low, o_part, down_w = attend(
        lengths, tok_all.reshape(seq_total, width), gain_attn[None], w_proj, cosine, sine,
        gain_heads, out_own, heads, [w_down.reshape((S, own_experts) + w_down.shape[1:])],
        ((("seq",), 0, "columns"),), sizes, 3,
    )
    o_part = o_part.reshape(S, tok_count, width)

    expert_ids = jnp.arange(expert_count, dtype=jnp.int32)
    slot_ids = jnp.arange(capacity, dtype=jnp.int32)
    plane = (
        jnp.arange(F, dtype=jnp.int32)[:, None] * local_experts
        + seq_at * own_experts
        + jnp.arange(own_experts, dtype=jnp.int32)[None, :]
    ).reshape(-1)
    hit = table_all[:, None, :TOPK] == plane[None, :, None, None]
    plane_slots = jnp.max(jnp.where(hit, table_all[:, None, TOPK:], -1), axis=2)
    one_hot = plane_slots[:, :, None, :] == slot_ids[None, None, :, None]
    select = one_hot.astype(BF).reshape(S, F * own_experts * capacity, tok_count)
    grouped = (S, F, own_experts * capacity, width)
    shape5 = (F, S, own_experts, capacity, width)

    cot_rows = mm("brt,btd->brd", select, cot_all).astype(BF).reshape(grouped)
    residual, ffn_all, g_rows = line(
        "ffn", sizes, [o_part], [tokens[0], gain_ffn], [cot_rows], ((("fsdp",), 1, 0),), 2
    )
    g_rows = g_rows.reshape(shape5)
    ffn_low = lax.dynamic_index_in_dim(ffn_all, seq_at, 0, keepdims=False)

    route_rows = routes[0]
    slot_rows = slots[0]
    router_scores = dot(ffn_low, full_router)
    picked = route_rows[:, :, None] == expert_ids[None, None, :]
    selected = jnp.sum(jnp.where(picked, router_scores[:, None, :], 0.0), axis=-1)
    gate_prob = jax.nn.softmax(selected, axis=-1)
    gate_table = jnp.sum(jnp.where(picked, gate_prob[:, :, None], 0.0), axis=1).T
    hit = table[None, :TOPK] == expert_ids[:, None, None]
    own_slots = jnp.max(jnp.where(hit, table[None, TOPK:], -1), axis=1)
    gate_slots = jnp.sum(
        jnp.where(
            own_slots[:, None, :] == slot_ids[None, :, None], gate_table[:, None, :], 0.0
        ),
        axis=-1,
    )
    by_device = (F, S, own_experts, capacity)

    def to_devices(values):
        return lanes(values.reshape(by_device).transpose(1, 0, 2, 3).reshape(N, -1), N)

    gate_send = to_devices(gate_slots)

    ffn_rows = mm("brt,btd->brd", select, ffn_all).astype(BF).reshape(grouped)
    x_rows, gate_up_w, gate_got = exchange(
        [ffn_rows, w_gate_up.reshape((S, own_experts) + w_gate_up.shape[1:]), gate_send],
        ((("fsdp",), 1, 0), (("seq",), 0, 0), (EVERY, 0, 0)), sizes, 4,
    )
    gate_up_w = gate_up_w.transpose(1, 0, 2, 3).reshape(own_experts, width, 2 * FF)
    x_rows = x_rows.reshape(shape5)
    row_gate = gate_got.reshape(S, F, -1)[:, :, : own_experts * capacity]
    row_gate = row_gate.transpose(1, 0, 2).reshape(F, S, own_experts, capacity, 1)

    gate_up = mm("asjcd,jdf->asjcf", x_rows, gate_up_w)
    gate_part = gate_up[..., :FF]
    up_part = gate_up[..., FF:]
    hidden_low = (jax.nn.silu(gate_part) * up_part).astype(BF)
    expert_out = mm("asjch,jhd->asjcd", hidden_low, down_w).astype(BF)
    out_wide = expert_out.astype(F32)
    g_wide = g_rows.astype(F32)
    grad_prob_rows = jnp.sum(out_wide * g_wide, axis=-1)
    moe_rows = (row_gate * out_wide).astype(BF)
    grad_eo_low = (row_gate * g_wide).astype(BF)

    grad_hidden_low = mm("asjcd,jhd->asjch", grad_eo_low, down_w).astype(BF)
    grad_hidden = lax.optimization_barrier(grad_hidden_low).astype(F32)
    sigmoid_gate = jax.nn.sigmoid(gate_part)
    grad_gate = grad_hidden * up_part * sigmoid_gate * (1.0 + gate_part * (1.0 - sigmoid_gate))
    grad_up = grad_hidden * gate_part * sigmoid_gate
    grad_gu_low = jnp.concatenate([grad_gate, grad_up], axis=-1).astype(BF)
    grad_rows = mm("asjcf,jdf->asjcd", grad_gu_low, gate_up_w).astype(BF)
    up_term = mm("asjcd,asjcf->jdf", x_rows, grad_gu_low).astype(BF)
    down_term = mm("asjch,asjcd->jhd", hidden_low, grad_eo_low).astype(BF)
    prob_send = grad_prob_rows.reshape(F, S, -1).transpose(1, 0, 2).reshape(N, -1)
    back_layout = grad_rows.reshape(F, S, own_experts * capacity, width)
    up_blocks = up_term.reshape(own_experts, S, part_width, 2 * FF).transpose(1, 0, 2, 3)
    grad_back, up_got, prob_got = exchange(
        [back_layout, up_blocks, lanes(prob_send, N)],
        ((("fsdp",), 0, 1), (("seq",), 0, 0), (EVERY, 0, 0)), sizes, 6,
    )
    grad_gate_up = up_got.reshape(w_gate_up.shape).astype(F32)
    prob_slots = prob_got.reshape(S, F, -1)[:, :, : own_experts * capacity]
    prob_slots = prob_slots.reshape(S, F, own_experts, capacity).transpose(1, 0, 2, 3)
    prob_slots = prob_slots.reshape(expert_count, capacity)

    grad_part = mm("brt,brd->btd", select, grad_back.reshape(S, -1, width)).astype(BF)

    prob_of_route = jnp.einsum(
        "tke,ec->tkc", picked.astype(F32), prob_slots, precision=lax.Precision.HIGHEST
    )
    at_slot = slot_rows[:, :, None] == slot_ids[None, None, :]
    grad_prob = jnp.sum(jnp.where(at_slot, prob_of_route, 0.0), axis=-1)
    grad_selected = gate_prob * (grad_prob - jnp.sum(gate_prob * grad_prob, axis=-1, keepdims=True))
    grad_logits = jnp.sum(jnp.where(picked, grad_selected[:, :, None], 0.0), axis=1).astype(BF)
    grad_ffn_add = mm("te,de->td", grad_logits, full_router)
    grad_router_part = mm("td,te->de", ffn_low, grad_logits)
    valid = (seq_at * tok_count + jnp.arange(tok_count, dtype=jnp.int32)) < lengths[0]
    grad_final = jnp.where(valid[:, None], cotangent[0].astype(F32), 0.0)
    grad_residual, grad_gain_ffn, grad_attn_low, moe_back = line(
        "grad", sizes, [grad_part], [grad_final, gain_ffn, residual, grad_ffn_add],
        [moe_rows.reshape(F, S, own_experts * capacity, width)], ((("fsdp",), 0, 1),), 7,
    )
    grad_attn_low = grad_attn_low.reshape(seq_total, width)

    grad_proj, attn_part, grad_gain_heads, down_got = attend_back(
        lengths, projected, qkv_low, grad_attn_low, out_own, w_proj, cosine, sine, gain_heads,
        heads, [down_term], ((("seq",), "columns", 0),), sizes, 9,
    )
    grad_down = down_got.reshape(w_down.shape).astype(F32)
    attn_part = attn_part.reshape(S, tok_count, width)
    grad_out_part = mm("te,td->ed", o_low, grad_attn_low).astype(BF)
    grad_qkv_part = mm("td,te->de", attn_low, grad_proj).astype(BF).reshape(S, F, w_rows, own_width)
    moe_part = mm("brt,brd->btd", select, moe_back.reshape(S, -1, width)).astype(BF)
    sums, grad_out_got, grad_qkv_plane = line(
        "sum", sizes, [attn_part, moe_part], [],
        [grad_out_part.reshape(F, -1, width), grad_qkv_part],
        ((("fsdp",), 0, 0), (("fsdp",), 1, 0)), 8,
    )
    grad_attn_norm, moe_out = sums[0], sums[1]
    final = jnp.where(valid[:, None], residual + moe_out, 0.0)
    grad_out = jnp.sum(grad_out_got.astype(F32), axis=0)
    grad_qkv_own = jnp.sum(grad_qkv_plane.astype(F32), axis=0).astype(BF)
    layer_inputs = tokens[0].astype(F32)
    factor = rms_factor(layer_inputs)
    normed = layer_inputs * factor
    scaled = grad_attn_norm * gain_attn
    inner = jnp.mean(scaled * normed, axis=-1, keepdims=True)
    grad_inputs = grad_residual + factor * (scaled - normed * inner)
    grad_gain_attn = jnp.sum(grad_attn_norm * normed, axis=0)

    gain_part = jnp.concatenate([grad_gain_attn, grad_gain_ffn[0], grad_gain_heads.reshape(-1)])
    small_part = jnp.concatenate(
        [grad_router_part.reshape(N, -1), gain_part.reshape(N, -1)], axis=1
    )
    small_got, grad_qkv_got = exchange(
        [lanes(small_part, N), grad_qkv_own], ((EVERY, 0, 0), (("seq",), 0, 0)), sizes, 10
    )
    grad_qkv = whole_columns(grad_qkv_got).astype(F32)
    small_sum = jnp.sum(small_got, axis=0).reshape(-1)
    grad_router = small_sum[:router_size].reshape(w_router.shape)
    grad_gains = small_sum[router_size : router_size + small]
    return (
        final.astype(BF)[None],
        grad_inputs[None],
        grad_qkv,
        grad_out,
        grad_router,
        grad_gains,
        grad_gate_up,
        grad_down,
    )


def solution(mesh):
    in_specs = (
        P("fsdp", "seq", None),
        P("fsdp", "seq", None),
        P("fsdp"),
        P("fsdp", "seq", None),
        P("fsdp", "seq", None),
        P(("seq", "fsdp"), None),
        P(("seq", "fsdp"), None),
        P(("seq", "fsdp"), None),
        P(("seq", "fsdp")),
        P("fsdp", "seq", None),
        P("fsdp", None, "seq"),
    )
    out_specs = (
        P("fsdp", "seq", None),
        P("fsdp", "seq", None),
        P(("seq", "fsdp"), None),
        P(("seq", "fsdp"), None),
        P(("seq", "fsdp"), None),
        P(("seq", "fsdp")),
        P("fsdp", "seq", None),
        P("fsdp", None, "seq"),
    )
    return jax.shard_map(
        per_device, mesh=mesh, in_specs=in_specs, out_specs=out_specs, check_vma=False
    )
```

```python
import functools

import jax
import jax.numpy as jnp
from jax import lax
from jax.experimental import pallas as pl
from jax.experimental.pallas import tpu as pltpu
from jax.sharding import PartitionSpec as P

QH = 32
KH = 4
HD = 128
FF = 768
TOPK = 8
EPSILON = 1e-06
THETA = 1000000.0
MASKED = -1e30
AHEAD = 2
BF = jnp.bfloat16
F32 = jnp.float32
MESH = pl.DeviceIdType.MESH
ANY = pl.BlockSpec(memory_space=pl.ANY)
VM = pl.BlockSpec(memory_space=pltpu.VMEM)
DMA = pltpu.SemaphoreType.DMA
EVERY = ("seq", "fsdp")

def index_of(sizes, axes):
    at = 0
    for axis in axes:
        at = at * sizes[axis] + lax.axis_index(axis)
    return at


def count_of(sizes, axes):
    number = 1
    for axis in axes:
        number *= sizes[axis]
    return number


def place_of(sizes, axes, at):
    if len(axes) == 1:
        return {axes[0]: at}
    return {axes[0]: at // sizes[axes[1]], axes[1]: at % sizes[axes[1]]}


def greet(sizes):
    total = count_of(sizes, EVERY)
    me = index_of(sizes, EVERY)
    barrier = pltpu.get_barrier_semaphore()
    for step in range(1, total):
        pl.semaphore_signal(
            barrier, inc=1, device_id=place_of(sizes, EVERY, lax.rem(me + step, total)),
            device_id_type=MESH,
        )
    return lambda: pl.semaphore_wait(barrier, total - 1)


def block_of(ref, dim, at, total):
    if dim is None:
        return ref
    if dim == "columns":
        width = ref.shape[-1] // total
        return ref.at[:, :, pl.ds(pl.multiple_of(at * width, 128), width)]
    return ref.at[at] if dim == 0 else ref.at[:, at]


class Blocks:
    def __init__(self, sizes, specs, sources, results, sems):
        self.own, self.away = [], []
        if not specs:
            return
        send_sem, recv_sem, own_sem, *stages = sems
        for i, (axes, before, after) in enumerate(specs):
            me = index_of(sizes, axes)
            total = count_of(sizes, axes)
            source = block_of(sources[i], before, me, total)
            result = block_of(results[i], after, me, total)
            self.own.append(
                (
                    pltpu.make_async_copy(source, stages[i], own_sem.at[i, 0]),
                    pltpu.make_async_copy(stages[i], result, own_sem.at[i, 1]),
                )
            )
            for step in range(1, total):
                target = lax.rem(me + step, total)
                self.away.append(
                    pltpu.make_async_remote_copy(
                        src_ref=block_of(sources[i], before, target, total),
                        dst_ref=block_of(results[i], after, me, total),
                        send_sem=send_sem.at[i, step],
                        recv_sem=recv_sem.at[i, step],
                        device_id=place_of(sizes, axes, target),
                        device_id_type=MESH,
                    )
                )

    def start(self):
        for copy in self.away:
            copy.start()
        for inward, _ in self.own:
            inward.start()

    def wait(self):
        for inward, outward in self.own:
            inward.wait()
            outward.start()
        for _, outward in self.own:
            outward.wait()
        for copy in self.away:
            copy.wait()


def block_scratch(sizes, arrays, specs):
    if not specs:
        return []
    total = max(count_of(sizes, axes) for axes, _, _ in specs)
    stages = []
    for array, (axes, before, after) in zip(arrays, specs):
        shape = list(array.shape)
        if before == "columns":
            shape[-1] //= count_of(sizes, axes)
        elif before is not None:
            del shape[before]
        stages.append(pltpu.VMEM(tuple(shape), array.dtype))
    count = len(specs)
    return [DMA((count, total)), DMA((count, total)), DMA((count, 2))] + stages


def block_outs(sizes, arrays, specs):
    outs = []
    for array, (axes, before, after) in zip(arrays, specs):
        shape = list(array.shape)
        total = count_of(sizes, axes)
        if before is None:
            shape = [total] + shape
        elif before == "columns":
            shape = [total, shape[0], shape[1], shape[2] // total]
        elif after == "columns":
            shape = [shape[1], shape[2], shape[3] * total]
        elif before != after:
            shape[0], shape[1] = shape[1], shape[0]
        outs.append(jax.ShapeDtypeStruct(tuple(shape), array.dtype))
    return outs


def exchange_kernel(sizes, specs, *refs):
    count = len(specs)
    met = greet(sizes)
    blocks = Blocks(sizes, specs, refs[:count], refs[count : 2 * count], refs[2 * count :])
    met()
    blocks.start()
    blocks.wait()


def exchange(arrays, specs, sizes, collective_id):
    count = len(arrays)
    return pl.pallas_call(
        functools.partial(exchange_kernel, sizes, specs),
        out_shape=block_outs(sizes, arrays, specs),
        in_specs=[ANY] * count,
        out_specs=[ANY] * count,
        scratch_shapes=block_scratch(sizes, arrays, specs),
        compiler_params=pltpu.CompilerParams(collective_id=collective_id, has_side_effects=True),
        name=f"exchange_{collective_id}",
    )(*arrays)


def entry_kernel(
    sizes, tok_ref, cot_ref, table_ref, wqkv_ref, wout_ref, small_ref,
    tok_out, cot_out, table_out, wq_out, wo_out, small_out,
    tok_send, tok_recv, tab_send, tab_recv, wq_zsend, wq_zrecv,
    pl_send, pl_recv, sib_send, sib_recv, sm_send, sm_recv, own_sem, *stages,
):
    S, F = sizes["seq"], sizes["fsdp"]
    s = lax.axis_index("seq")
    f = lax.axis_index("fsdp")
    N = S * F
    chips = F // 2
    me = s * F + f
    other = f + 1 - 2 * lax.rem(f, 2)
    rows = tok_ref.shape[0]
    chunks = tok_recv.shape[2]
    span = rows // chunks
    met = greet(sizes)
    kv = KH * HD // S
    q_width = QH * HD // S
    starts = (0, q_width * S, (q_width + kv) * S)
    widths = (q_width, kv, kv)
    offsets = (0, q_width, q_width + kv)

    def columns(z, p):
        return pl.ds(pl.multiple_of(starts[p] + z * widths[p], 128), widths[p])

    pairs = [
        (wqkv_ref.at[:, columns(s, p)], wq_out.at[s, f, :, pl.ds(offsets[p], widths[p])])
        for p in range(3)
    ] + [
        (wout_ref, wo_out.at[f]),
        (tok_ref, tok_out.at[s]),
        (cot_ref, cot_out.at[s]),
        (table_ref, table_out.at[s]),
        (small_ref, small_out.at[me]),
    ]
    inward = [
        pltpu.make_async_copy(source, stages[i], own_sem.at[i, 0])
        for i, (source, _) in enumerate(pairs)
    ]
    outward = [
        pltpu.make_async_copy(stages[i], result, own_sem.at[i, 1])
        for i, (_, result) in enumerate(pairs)
    ]
    for copy in inward:
        copy.start()
    met()

    def remote(src, dst, send_sem, recv_sem, where):
        return pltpu.make_async_remote_copy(
            src_ref=src, dst_ref=dst, send_sem=send_sem, recv_sem=recv_sem,
            device_id=where, device_id_type=MESH,
        )

    wq_line = []
    tables = []
    for step in range(1, S):
        target = lax.rem(s + step, S)
        for p in range(3):
            copy = remote(
                wqkv_ref.at[:, columns(target, p)],
                wq_out.at[s, f, :, pl.ds(offsets[p], widths[p])],
                wq_zsend.at[step, p], wq_zrecv.at[step, p], {"seq": target},
            )
            copy.start()
            wq_line.append(copy)
        copy = remote(
            table_ref, table_out.at[s], tab_send.at[step], tab_recv.at[step], {"seq": target}
        )
        copy.start()
        tables.append(copy)

    def along(a, block, c, way, hop):
        source, result = ((tok_ref, tok_out), (cot_ref, cot_out))[a]
        here = result.at[block, pl.ds(c * span, span)]
        src = source.at[pl.ds(c * span, span)] if hop == 1 else here
        return remote(
            src, here, tok_send.at[a, way, c, hop], tok_recv.at[a, way, c, hop],
            {"seq": s + 1 if way == 0 else s - 1},
        )

    def depart(a):
        for c in range(chunks):
            @pl.when(s < S - 1)
            def _():
                along(a, s, c, 0, 1).start()

            @pl.when(s > 0)
            def _():
                along(a, s, c, 1, 1).start()

    def relay(a, hop):
        for c in range(chunks):
            @pl.when(s >= hop)
            def _():
                along(a, s - hop, c, 0, hop).wait_recv()
                if hop < S - 1:
                    @pl.when(s < S - 1)
                    def _():
                        along(a, s - hop, c, 0, hop + 1).start()

            @pl.when(s < S - hop)
            def _():
                along(a, s + hop, c, 1, hop).wait_recv()
                if hop < S - 1:
                    @pl.when(s > 0)
                    def _():
                        along(a, s + hop, c, 1, hop + 1).start()

    depart(0)

    def plane_block(slot, owner):
        if slot == S:
            return wo_out.at[owner]
        return wq_out.at[lax.rem(s - slot + S, S), owner]

    def to_chip(slot, step):
        block = plane_block(slot, f)
        return remote(block, block, pl_send.at[slot, step], pl_recv.at[slot, step],
                      {"fsdp": lax.rem(f + 2 * step, F)})

    def to_other(slot, step):
        block = plane_block(slot, lax.rem(f - 2 * step + F, F))
        return remote(block, block, sib_send.at[slot, step], sib_recv.at[slot, step],
                      {"fsdp": other})

    def spread(slot):
        for step in range(1, chips):
            to_chip(slot, step).start()
        to_other(slot, 0).start()

    def forward(slot):
        for step in range(1, chips):
            to_chip(slot, step).wait_recv()
            to_other(slot, step).start()

    smalls = []
    for step in range(1, N):
        target = lax.rem(me + step, N)
        copy = remote(small_ref, small_out.at[me], sm_send.at[step], sm_recv.at[step],
                      place_of(sizes, EVERY, target))
        copy.start()
        smalls.append(copy)
    for i, copy in enumerate(inward):
        copy.wait()
        outward[i].start()
    for copy in outward[:3]:
        copy.wait()
    spread(0)
    outward[3].wait()
    spread(S)
    relay(0, 1)
    depart(1)
    for step in range(1, S):
        for p in range(3):
            wq_line[(step - 1) * 3 + p].wait()
        spread(step)
    for hop in range(2, S):
        relay(0, hop)
        relay(1, hop - 1)
    for slot in range(S + 1):
        forward(slot)
    relay(1, S - 1)
    for a in range(2):
        for hop in range(1, S):
            for c in range(chunks):
                @pl.when((s < S - 1) & (s >= hop - 1))
                def _():
                    along(a, s, c, 0, hop).wait_send()

                @pl.when((s > 0) & (s <= S - hop))
                def _():
                    along(a, s, c, 1, hop).wait_send()
    for copy in outward[4:]:
        copy.wait()
    for slot in range(S + 1):
        for step in range(1, chips):
            to_chip(slot, step).wait_send()
        for step in range(chips):
            to_other(slot, step).wait_send()
            block = plane_block(slot, lax.rem(other - 2 * step + F, F))
            remote(block, block, sib_send.at[slot, step], sib_recv.at[slot, step],
                   {"fsdp": other}).wait_recv()
    for copy in tables + smalls:
        copy.wait()


def entry(tokens, cotangent, table, w_qkv, w_out, small, sizes, collective_id, chunks=4):
    S, F = sizes["seq"], sizes["fsdp"]
    own_width = w_qkv.shape[1] // S
    N = S * F
    line_out = jax.ShapeDtypeStruct((S,) + tokens.shape, tokens.dtype)
    q_width, kv = QH * HD // S, KH * HD // S
    stages = [
        pltpu.VMEM(shape, dtype)
        for shape, dtype in [
            ((w_qkv.shape[0], q_width), BF),
            ((w_qkv.shape[0], kv), BF),
            ((w_qkv.shape[0], kv), BF),
            (w_out.shape, BF),
            (tokens.shape, BF),
            (cotangent.shape, BF),
            (table.shape, table.dtype),
            (small.shape, BF),
        ]
    ]
    return pl.pallas_call(
        functools.partial(entry_kernel, sizes),
        out_shape=[
            line_out,
            line_out,
            jax.ShapeDtypeStruct((S,) + table.shape, table.dtype),
            jax.ShapeDtypeStruct((S, F, w_qkv.shape[0], own_width), w_qkv.dtype),
            jax.ShapeDtypeStruct((F,) + w_out.shape, w_out.dtype),
            jax.ShapeDtypeStruct((N,) + small.shape, small.dtype),
        ],
        in_specs=[ANY] * 6,
        out_specs=[ANY] * 6,
        scratch_shapes=[
            DMA((2, 2, chunks, S)), DMA((2, 2, chunks, S)), DMA((S,)), DMA((S,)),
            DMA((S, 3)), DMA((S, 3)), DMA((S + 1, F // 2)), DMA((S + 1, F // 2)),
            DMA((S + 1, F // 2)), DMA((S + 1, F // 2)), DMA((N,)), DMA((N,)), DMA((8, 2)),
        ] + stages,
        compiler_params=pltpu.CompilerParams(collective_id=collective_id, has_side_effects=True),
        name="entry",
    )(tokens, cotangent, table, w_qkv, w_out, small)


class Widen:
    def __init__(self, pairs, sems, buffers):
        self.jobs = []
        for i, (source, result) in enumerate(pairs):
            narrow, wide = buffers[2 * i], buffers[2 * i + 1]
            for j in range(source.shape[0]):
                self.jobs.append(
                    (
                        pltpu.make_async_copy(source.at[j], narrow.at[j % 2], sems.at[i, 0, j % 2]),
                        pltpu.make_async_copy(wide.at[j % 2], result.at[j], sems.at[i, 1, j % 2]),
                        narrow.at[j % 2],
                        wide.at[j % 2],
                        j,
                        source.shape[0],
                    )
                )
        self.done = 0

    def start(self):
        for inward, _, _, _, j, _ in self.jobs:
            if j < 2:
                inward.start()

    def turn(self):
        if self.done == len(self.jobs):
            return
        at = self.done
        inward, outward, narrow, wide, j, number = self.jobs[at]
        inward.wait()
        if j >= 2:
            self.jobs[at - 2][1].wait()
        wide[...] = narrow[...].astype(F32)
        outward.start()
        if j + 2 < number:
            self.jobs[at + 2][0].start()
        self.done += 1

    def wait(self):
        while self.done < len(self.jobs):
            self.turn()
        for _, outward, _, _, j, number in self.jobs:
            if j >= number - 2:
                outward.wait()


def widen_scratch(arrays):
    if not arrays:
        return []
    scratch = [DMA((len(arrays), 2, 2))]
    for array in arrays:
        shape = (2,) + array.shape[1:]
        scratch += [pltpu.VMEM(shape, BF), pltpu.VMEM(shape, F32)]
    return scratch


def grads_kernel(sizes, specs, *refs):
    S = sizes["seq"]
    count = len(specs)
    sources, (x_any, gu_any, ph_any, g_any) = refs[:count], refs[count : count + 4]
    results, (up_out, down_out) = refs[count + 4 : 2 * count + 4], refs[2 * count + 4 : 2 * count + 6]
    x_ref, gu_ref, ph_ref, g_ref, up_stage, down_stage, in_sem, up_send, up_recv, out_sem, *sems = refs[2 * count + 6 :]
    s = lax.axis_index("seq")
    inward = [
        pltpu.make_async_copy(source, target, in_sem.at[i])
        for i, (source, target) in enumerate(
            ((x_any, x_ref), (gu_any, gu_ref), (ph_any, ph_ref), (g_any, g_ref))
        )
    ]
    met = greet(sizes)
    for copy in inward:
        copy.start()
    blocks = Blocks(sizes, specs, sources, results, sems)
    met()
    blocks.start()
    inward[0].wait()
    inward[1].wait()
    part = up_stage.shape[1]
    over_rows = (((0,), (0,)), ((), ()))
    sent = []
    for turn_at in range(1, S + 1):
        target = lax.rem(s + turn_at, S)
        mine = pl.ds(pl.multiple_of(target * part, 128), part)
        block = up_stage.at[turn_at - 1]

        def one(at):
            block[:, at] = lax.dot_general(
                x_ref[:, mine], gu_ref[:, at], over_rows, preferred_element_type=F32
            ).astype(BF)

        tiles(gu_ref.shape[1], 256, one)
        if turn_at < S:
            copy = pltpu.make_async_remote_copy(
                src_ref=block, dst_ref=up_out.at[s],
                send_sem=up_send.at[turn_at], recv_sem=up_recv.at[turn_at],
                device_id={"seq": target}, device_id_type=MESH,
            )
        else:
            copy = pltpu.make_async_copy(block, up_out.at[s], out_sem.at[0])
        copy.start()
        sent.append(copy)
    inward[2].wait()
    inward[3].wait()

    def one_down(at):
        down_stage[:, at] = lax.dot_general(
            ph_ref[...], g_ref[:, at], over_rows, preferred_element_type=F32
        ).astype(BF)

    tiles(g_ref.shape[1], 256, one_down)
    copy = pltpu.make_async_copy(down_stage, down_out, out_sem.at[1])
    copy.start()
    sent.append(copy)
    blocks.wait()
    for copy in sent:
        copy.wait()


def grads(arrays, specs, rows, grad_gu, hidden, grad_out, sizes, collective_id):
    S = sizes["seq"]
    part = rows.shape[1] // S
    up_block = (part, grad_gu.shape[1])
    down = (hidden.shape[1], grad_out.shape[1])
    inner = [rows, grad_gu, hidden, grad_out]
    return pl.pallas_call(
        functools.partial(grads_kernel, sizes, specs),
        out_shape=block_outs(sizes, arrays, specs)
        + [jax.ShapeDtypeStruct((S,) + up_block, BF), jax.ShapeDtypeStruct(down, BF)],
        in_specs=[ANY] * (len(arrays) + 4),
        out_specs=[ANY] * (len(arrays) + 2),
        scratch_shapes=[pltpu.VMEM(array.shape, BF) for array in inner]
        + [pltpu.VMEM((S,) + up_block, BF), pltpu.VMEM(down, BF)]
        + [DMA((4,)), DMA((S,)), DMA((S,)), DMA((2,))]
        + block_scratch(sizes, arrays, specs),
        compiler_params=pltpu.CompilerParams(
            collective_id=collective_id, has_side_effects=True, vmem_limit_bytes=60 << 20
        ),
        name="grads",
    )(*arrays, *inner)


def line_kernel(sizes, chunks, mode, parts, extra, widened, *refs):
    S, F = sizes["seq"], sizes["fsdp"]
    count = len(extra)
    names = {
        "ffn": (["base", "gain"], ["resid_out", "all_out"]),
        "grad": (["base", "gain", "resid", "add"], ["grad_out", "gain_out", "all_out"]),
        "last": (
            ["base", "gain", "resid", "inputs", "length", "gout", "gqkv"],
            ["grad_out", "low_out", "gains_all", "gout_out", "gqkv_out"],
        ),
    }[mode]
    refs = list(refs)

    def take(number):
        taken, refs[:number] = refs[:number], []
        return taken

    part_refs = take(parts)
    given = dict(zip(names[0], take(len(names[0]))))
    sources = take(count)
    narrow = take(widened)
    given.update(zip(names[1], take(len(names[1]))))
    results = take(count)
    wide = take(widened)
    from_left, from_right = take(2)
    gather = mode != "last"
    if gather:
        stage, rs_send, rs_recv, ag_send, ag_recv, own_sem = take(6)
        all_out = given["all_out"]
    else:
        gain_sum, gain_stage, gain_send, gain_recv, gain_own = take(5)
        plane_gout, plane_gqkv, gqkv_stage, gqkv_line, line_send, line_recv = take(6)
        plane_sems = take(5)
        rs_send, rs_recv = take(2)
    s = lax.axis_index("seq")
    f = lax.axis_index("fsdp")
    me = s * F + f
    N = S * F
    rows = part_refs[0].shape[1]
    span = rows // chunks
    met = greet(sizes)
    widen = Widen(list(zip(narrow, wide)), refs[0], refs[1:]) if widened else None
    del refs[: (1 + 2 * widened) if widened else 0]
    blocks = Blocks(sizes, extra, sources, results, refs)
    if widen:
        widen.start()
    met()

    def at(c):
        return pl.ds((c % chunks) * span, span)

    def mine(d, c):
        return part_refs[c // chunks].at[d, at(c)]

    def landed(way, d, c):
        return (from_left, from_right)[way].at[c // chunks, d, at(c)]

    def rs_copy(d, c, way, src):
        return pltpu.make_async_remote_copy(
            src_ref=src, dst_ref=landed(way, d, c),
            send_sem=rs_send.at[way, d, c], recv_sem=rs_recv.at[way, d, c],
            device_id={"seq": s + 1 if way == 0 else s - 1}, device_id_type=MESH,
        )

    def ag_copy(block, c, way, hop):
        src = stage.at[at(c)] if hop == 1 else all_out.at[block, at(c)]
        return pltpu.make_async_remote_copy(
            src_ref=src, dst_ref=all_out.at[block, at(c)],
            send_sem=ag_send.at[way, c, hop], recv_sem=ag_recv.at[way, c, hop],
            device_id={"seq": s + 1 if way == 0 else s - 1}, device_id_type=MESH,
        )

    def end_step(c):
        for d in range(S - 1, 0, -1):
            @pl.when((s == 0) & (d > s))
            def _():
                rs_copy(d, c, 0, mine(d, c)).start()
        for d in range(S - 1):
            @pl.when((s == S - 1) & (d < s))
            def _():
                rs_copy(d, c, 1, mine(d, c)).start()

    def middle_step(c):
        for way in range(2):
            order = range(S - 1, 0, -1) if way == 0 else range(S - 1)
            for d in order:
                inside = (s > 0) & (d > s) if way == 0 else (s < S - 1) & (d < s)

                @pl.when(inside)
                def _():
                    buffer = landed(way, d, c)
                    rs_copy(d, c, way, buffer).wait_recv()
                    total = buffer[...].astype(F32) + mine(d, c)[...].astype(F32)
                    buffer[...] = total.astype(BF)
                    rs_copy(d, c, way, buffer).start()

    def final_step(c):
        @pl.when(s > 0)
        def _():
            rs_copy(s, c, 0, mine(s, c)).wait_recv()

        @pl.when(s < S - 1)
        def _():
            rs_copy(s, c, 1, mine(s, c)).wait_recv()

        total = mine(s, c)[...].astype(F32)
        total = total + jnp.where(s > 0, landed(0, s, c)[...].astype(F32), 0.0)
        total = total + jnp.where(s < S - 1, landed(1, s, c)[...].astype(F32), 0.0)
        if mode == "last":
            if c >= chunks:
                row = s * rows + (c % chunks) * span + lax.broadcasted_iota(jnp.int32, total.shape, 0)
                value = given["resid"][at(c), :] + total
                given["low_out"][at(c), :] = jnp.where(row < given["length"][0], value, 0.0).astype(BF)
                return
            value = given["inputs"][at(c), :].astype(F32)
            factor = lax.rsqrt(jnp.mean(value * value, axis=-1, keepdims=True) + EPSILON)
            normed = value * factor
            scaled = total * given["gain"][...]
            inner = jnp.mean(scaled * normed, axis=-1, keepdims=True)
            given["grad_out"][at(c), :] = given["base"][at(c), :] + factor * (scaled - normed * inner)
            gained = jnp.sum(total * normed, axis=0, keepdims=True)
            gain_sum[...] = gained if c == 0 else gain_sum[...] + gained
            if c == chunks - 1:
                send_gains()
            return
        if mode == "ffn":
            value = given["base"][at(c), :].astype(F32) + total
            given["resid_out"][at(c), :] = value
            factor = lax.rsqrt(jnp.mean(value * value, axis=-1, keepdims=True) + EPSILON)
            low = (value * factor * given["gain"][...]).astype(BF)
        else:
            upstream = total + given["add"][at(c), :]
            value = given["resid"][at(c), :]
            factor = lax.rsqrt(jnp.mean(value * value, axis=-1, keepdims=True) + EPSILON)
            normed = value * factor
            scaled = upstream * given["gain"][...]
            inner = jnp.mean(scaled * normed, axis=-1, keepdims=True)
            result = given["base"][at(c), :] + factor * (scaled - normed * inner)
            given["grad_out"][at(c), :] = result
            gained = jnp.sum(upstream * normed, axis=0, keepdims=True)
            gain_out = given["gain_out"]
            gain_out[...] = gained if c == 0 else gain_out[...] + gained
            low = result.astype(BF)
        stage[at(c), :] = low
        pltpu.make_async_copy(stage.at[at(c)], all_out.at[s, at(c)], own_sem.at[c]).start()

        @pl.when(s < S - 1)
        def _():
            ag_copy(s, c, 0, 1).start()

        @pl.when(s > 0)
        def _():
            ag_copy(s, c, 1, 1).start()

    def gain_copy(step):
        return pltpu.make_async_remote_copy(
            src_ref=gain_stage, dst_ref=given["gains_all"].at[me],
            send_sem=gain_send.at[step], recv_sem=gain_recv.at[step],
            device_id=place_of(sizes, EVERY, lax.rem(me + step, N)), device_id_type=MESH,
        )

    def own_gains():
        return pltpu.make_async_copy(gain_stage, given["gains_all"].at[me], gain_own.at[0])

    def send_gains():
        for j in range(gain_stage.shape[0]):
            gain_stage[j : j + 1, :] = gain_sum[:, j * 128 : (j + 1) * 128]
        own_gains().start()
        for step in range(1, N):
            gain_copy(step).start()

    plane = None
    if mode == "last":
        plane = Blocks(
            sizes, ((("fsdp",), 0, 0), (("fsdp",), 1, 0)), [given["gout"], given["gqkv"]],
            [plane_gout, plane_gqkv], plane_sems,
        )

    def line_copy(step):
        return pltpu.make_async_remote_copy(
            src_ref=gqkv_stage.at[lax.rem(s + step, S)], dst_ref=gqkv_line.at[s],
            send_sem=line_send.at[step], recv_sem=line_recv.at[step],
            device_id={"seq": lax.rem(s + step, S)}, device_id_type=MESH,
        )

    def plane_step():
        plane.wait()
        for z in range(S):
            total = plane_gqkv[0, z].astype(F32)
            for owner in range(1, F):
                total = total + plane_gqkv[owner, z].astype(F32)
            gqkv_stage[z] = total.astype(BF)
        for step in range(1, S):
            line_copy(step).start()
        gqkv_line[s] = gqkv_stage[s]
        half = plane_gout.shape[1] // 2
        for part_at in range(2):
            own = pl.ds(part_at * half, half)
            total = plane_gout[0, own].astype(F32)
            for owner in range(1, F):
                total = total + plane_gout[owner, own].astype(F32)
            given["gout_out"][own, :] = total

    def columns_step():
        for step in range(1, S):
            line_copy(step).wait()
        result = given["gqkv_out"]
        q_width, kv = QH * HD // S, KH * HD // S
        for z in range(S):
            block = gqkv_line[z].astype(F32)
            result[:, z * q_width : (z + 1) * q_width] = block[:, :q_width]
            key_at = S * q_width + z * kv
            result[:, key_at : key_at + kv] = block[:, q_width : q_width + kv]
            value_at = S * (q_width + kv) + z * kv
            result[:, value_at : value_at + kv] = block[:, q_width + kv :]

    def relay_step(c, hop):
        @pl.when(s >= hop)
        def _():
            ag_copy(s - hop, c, 0, hop).wait_recv()
            if hop < S - 1:
                @pl.when(s < S - 1)
                def _():
                    ag_copy(s - hop, c, 0, hop + 1).start()

        @pl.when(s < S - hop)
        def _():
            ag_copy(s + hop, c, 1, hop).wait_recv()
            if hop < S - 1:
                @pl.when(s > 0)
                def _():
                    ag_copy(s + hop, c, 1, hop + 1).start()

    steps = chunks * parts
    ahead = min(steps, AHEAD if gather else steps)
    for c in range(ahead):
        end_step(c)
    blocks.start()
    if plane:
        plane.start()
    hops = S - 1 if gather else 0
    plane_at = steps - 3
    for t in range(steps + 1 + hops):
        if t < steps:
            middle_step(t)
        if t + ahead < steps:
            end_step(t + ahead)
        if 0 <= t - 1 < steps:
            final_step(t - 1)
        for hop in range(1, hops + 1):
            if 0 <= t - 1 - hop < steps:
                relay_step(t - 1 - hop, hop)
        if widen:
            widen.turn()
        if plane and t == plane_at:
            plane_step()

    for c in range(steps):
        for d in range(S - 1, 0, -1):
            @pl.when(d > s)
            def _():
                rs_copy(d, c, 0, mine(d, c)).wait_send()
        for d in range(S - 1):
            @pl.when(d < s)
            def _():
                rs_copy(d, c, 1, mine(d, c)).wait_send()
        if gather:
            pltpu.make_async_copy(stage.at[at(c)], all_out.at[s, at(c)], own_sem.at[c]).wait()
            for hop in range(1, S):
                @pl.when((s < S - 1) & (s >= hop - 1))
                def _():
                    ag_copy(s, c, 0, hop).wait_send()

                @pl.when((s > 0) & (s <= S - hop))
                def _():
                    ag_copy(s, c, 1, hop).wait_send()
    if mode == "last":
        columns_step()
        own_gains().wait()
        for step in range(1, N):
            gain_copy(step).wait()
    if widen:
        widen.wait()
    blocks.wait()


def line(mode, sizes, parts, others, extras, specs, collective_id, chunks=8, widened=()):
    S = sizes["seq"]
    _, rows, width = parts[0].shape
    full = jax.ShapeDtypeStruct((rows, width), F32)
    everyone = jax.ShapeDtypeStruct((S, rows, width), BF)
    steps = chunks * len(parts)
    scratch = [pltpu.VMEM((len(parts), S, rows, width), BF)] * 2
    in_specs = [VM] * (len(parts) + len(others))
    sems = [DMA((2, S, steps)), DMA((2, S, steps))]
    if mode == "ffn":
        outs, out_specs = [full, everyone], [VM, ANY]
    elif mode == "grad":
        outs, out_specs = [full, jax.ShapeDtypeStruct((1, width), F32), everyone], [VM, VM, ANY]
    else:
        gout, gqkv = others[-2:]
        owned = gqkv.shape[2:]
        outs = [
            full,
            jax.ShapeDtypeStruct((rows, width), BF),
            jax.ShapeDtypeStruct((S * sizes["fsdp"], width // 128, 128), F32),
            jax.ShapeDtypeStruct(gout.shape[1:], F32),
            jax.ShapeDtypeStruct((owned[0], owned[1] * S), F32),
        ]
        out_specs = [VM, VM, ANY, VM, VM]
        N = S * sizes["fsdp"]
        scratch += [pltpu.VMEM((1, width), F32), pltpu.VMEM((width // 128, 128), F32)]
        scratch += [DMA((N,)), DMA((N,)), DMA((1,))]
        scratch += [
            pltpu.VMEM(gout.shape, BF),
            pltpu.VMEM((sizes["fsdp"], S) + owned, BF),
            pltpu.VMEM((S,) + owned, BF),
            pltpu.VMEM((S,) + owned, BF),
            DMA((S,)),
            DMA((S,)),
        ]
        scratch += block_scratch(sizes, [gout, gqkv], ((("fsdp",), 0, 0), (("fsdp",), 1, 0)))
        in_specs[-2:] = [ANY, ANY]
        in_specs[-3] = pl.BlockSpec(memory_space=pltpu.SMEM)
    if mode != "last":
        scratch.append(pltpu.VMEM((rows, width), BF))
        sems += [DMA((2, chunks, S)), DMA((2, chunks, S)), DMA((chunks,))]
    return pl.pallas_call(
        functools.partial(line_kernel, sizes, chunks, mode, len(parts), specs, len(widened)),
        out_shape=outs
        + block_outs(sizes, extras, specs)
        + [jax.ShapeDtypeStruct(array.shape, F32) for array in widened],
        in_specs=in_specs + [ANY] * (len(extras) + len(widened)),
        out_specs=out_specs + [ANY] * (len(extras) + len(widened)),
        scratch_shapes=scratch + sems + widen_scratch(widened) + block_scratch(sizes, extras, specs),
        compiler_params=pltpu.CompilerParams(
            collective_id=collective_id, has_side_effects=True, vmem_limit_bytes=56 << 20
        ),
        name=f"line_{mode}",
    )(*parts, *others, *extras, *widened)


def turn(values, cosine, sine):
    return values * cosine + pltpu.roll(values, HD // 2, 1) * sine


def softmax_block(query, keys, first_row, length, scale):
    scores = lax.dot_general(
        query, keys, (((1,), (1,)), ((), ())), preferred_element_type=F32
    ) * scale
    row = first_row + lax.broadcasted_iota(jnp.int32, scores.shape, 0)
    column = lax.broadcasted_iota(jnp.int32, scores.shape, 1)
    scores = jnp.where((column <= row) & (column < length), scores, MASKED)
    peak = jnp.max(scores, axis=-1, keepdims=True)
    weights = jnp.exp(scores - peak)
    return weights * (1.0 / jnp.sum(weights, axis=-1, keepdims=True))


def tiles(width, step, body):
    @pl.loop(0, width // step)
    def _(n):
        body(pl.ds(pl.multiple_of(n * step, step), step))


def attend_kernel(sizes, heads, blocks, specs, *refs):
    count = len(specs)
    length_ref, tok_ref, gain_ref, wq_ref, cos_ref, sin_ref, gains_ref, wo_ref = refs[:8]
    sources = refs[8 : 8 + count]
    attn_ref, proj_ref, low_ref, out_ref, part_ref = refs[8 + count : 13 + count]
    results = refs[13 + count : 13 + 2 * count]
    k_all, v_all, *sems = refs[13 + 2 * count :]
    step = pl.program_id(0)

    @pl.when(step == 0)
    def _():
        greet(sizes)()
        Blocks(sizes, specs, sources, results, sems).start()

    rows, width = proj_ref.shape
    length = length_ref[0]
    cosine = cos_ref[...]
    sine = sin_ref[...]
    q_gain = gains_ref[0:1, :]
    k_gain = gains_ref[1:2, :]
    scale = HD ** (-0.5)
    value = tok_ref[...].astype(F32)
    factor = lax.rsqrt(jnp.mean(value * value, axis=-1, keepdims=True) + EPSILON)
    attn_ref[...] = (value * factor * gain_ref[...]).astype(BF)

    def project(at):
        proj_ref[:, at] = jnp.dot(attn_ref[...], wq_ref[:, at], preferred_element_type=F32)

    tiles(width, 256, project)

    def normed(raw, gain):
        factor = lax.rsqrt(jnp.mean(raw * raw, axis=-1, keepdims=True) + EPSILON)
        return turn(raw * factor * gain, cosine, sine).astype(BF)

    key = normed(proj_ref[:, heads * HD : (heads + 1) * HD], k_gain)
    value_low = proj_ref[:, (heads + 1) * HD :].astype(BF)
    low_ref[:, heads * HD : (heads + 1) * HD] = key
    low_ref[:, (heads + 1) * HD :] = value_low
    here = pl.ds(pl.multiple_of(step * rows, rows), rows)
    k_all[here, :] = key
    v_all[here, :] = value_low
    for block in range(blocks):
        @pl.when(step == block)
        def _():
            reach = (block + 1) * rows

            def one(column):
                query = normed(proj_ref[:, column], q_gain)
                low_ref[:, column] = query
                probs = softmax_block(query, k_all[:reach, :], block * rows, length, scale)
                mixed = jnp.dot(probs.astype(BF), v_all[:reach, :], preferred_element_type=F32)
                out_ref[:, column] = mixed.astype(BF)

            tiles(heads * HD, HD, one)

    def leave(at):
        part_ref[:, at] = jnp.dot(
            out_ref[...], wo_ref[:, at], preferred_element_type=F32
        ).astype(BF)

    tiles(part_ref.shape[1], 256, leave)

    @pl.when(step == blocks - 1)
    def _():
        Blocks(sizes, specs, sources, results, sems).wait()


def attend(
    length, tokens, gain, w_proj, cosine, sine, gains, w_out, heads, extras, specs, sizes,
    collective_id, blocks=4,
):
    total, width = tokens.shape
    own_width = w_proj.shape[1]
    rows = total // blocks
    q_width = heads * HD

    def by_rows(columns):
        return pl.BlockSpec((rows, columns), lambda i: (i, 0))

    def whole(array):
        return pl.BlockSpec(array.shape, lambda i: (0, 0), pipeline_mode=pl.Buffered(1))

    return pl.pallas_call(
        functools.partial(attend_kernel, sizes, heads, blocks, specs),
        grid=(blocks,),
        out_shape=[
            jax.ShapeDtypeStruct((total, width), BF),
            jax.ShapeDtypeStruct((total, own_width), F32),
            jax.ShapeDtypeStruct((total, own_width), BF),
            jax.ShapeDtypeStruct((total, q_width), BF),
            jax.ShapeDtypeStruct((total, width), BF),
        ] + block_outs(sizes, extras, specs),
        in_specs=[
            pl.BlockSpec(memory_space=pltpu.SMEM),
            by_rows(width),
            whole(gain),
            whole(w_proj),
            by_rows(HD),
            by_rows(HD),
            whole(gains),
            whole(w_out),
        ] + [ANY] * len(extras),
        out_specs=[by_rows(width), by_rows(own_width), by_rows(own_width), by_rows(q_width), by_rows(width)]
        + [ANY] * len(extras),
        scratch_shapes=[pltpu.VMEM((total, HD), BF), pltpu.VMEM((total, HD), BF)]
        + block_scratch(sizes, extras, specs),
        compiler_params=pltpu.CompilerParams(
            collective_id=collective_id, has_side_effects=True, vmem_limit_bytes=58 << 20
        ),
        name="attend",
    )(length, tokens, gain, w_proj, cosine, sine, gains, w_out, *extras)


def attend_back_kernel(sizes, heads, blocks, specs, *refs):
    count = len(specs)
    length_ref, proj_ref, low_ref, kv_ref, grad_ref, wo_ref, wq_ref, cos_ref, sin_ref, gains_ref = refs[:10]
    sources = refs[10 : 10 + count]
    out_ref, part_ref, gains_out = refs[10 + count : 13 + count]
    results = refs[13 + count : 13 + 2 * count]
    gk_all, gv_all, go_ref, *sems = refs[13 + 2 * count :]
    step = pl.program_id(0)
    rows = proj_ref.shape[0]
    length = length_ref[0]
    cosine = cos_ref[...]
    sine = sin_ref[...]
    q_gain = gains_ref[0:1, :]
    k_gain = gains_ref[1:2, :]
    scale = HD ** (-0.5)
    block_at = blocks - 1 - step

    def back(raw, gain, grad):
        grad = turn(grad, cosine, -sine)
        factor = lax.rsqrt(jnp.mean(raw * raw, axis=-1, keepdims=True) + EPSILON)
        unit = raw * factor
        scaled = grad * gain
        inner = jnp.mean(scaled * unit, axis=-1, keepdims=True)
        return factor * (scaled - unit * inner), jnp.sum(grad * unit, axis=0, keepdims=True)

    @pl.when(step == 0)
    def _():
        greet(sizes)()
        Blocks(sizes, specs, sources, results, sems).start()
        gk_all[...] = jnp.zeros_like(gk_all)
        gv_all[...] = jnp.zeros_like(gv_all)
        gains_out[...] = jnp.zeros_like(gains_out)

    def arrive(at):
        go_ref[:, at] = lax.dot_general(
            grad_ref[...], wo_ref[at, :], (((1,), (1,)), ((), ())), preferred_element_type=F32
        ).astype(BF)

    tiles(heads * HD, 256, arrive)
    for block in range(blocks):
        @pl.when(block_at == block)
        def _():
            reach = (block + 1) * rows
            keys = kv_ref[:reach, :HD]
            values = kv_ref[:reach, HD:]

            def one(column):
                query = low_ref[:, column]
                grad_o = go_ref[:, column]
                probs = softmax_block(query, keys, block * rows, length, scale)
                grad_p = lax.dot_general(
                    grad_o, values, (((1,), (1,)), ((), ())), preferred_element_type=F32
                )
                inner = jnp.sum(probs * grad_p, axis=-1, keepdims=True)
                grad_s = (probs * (grad_p - inner)).astype(BF)
                grad_q = jnp.dot(grad_s, keys, preferred_element_type=F32) * scale
                gk_all[:reach, :] += lax.dot_general(
                    grad_s, query, (((0,), (0,)), ((), ())), preferred_element_type=F32
                )
                gv_all[:reach, :] += lax.dot_general(
                    probs.astype(BF), grad_o, (((0,), (0,)), ((), ())), preferred_element_type=F32
                )
                grad_raw, gained = back(proj_ref[:, column], q_gain, grad_q.astype(BF).astype(F32))
                out_ref[:, column] = grad_raw.astype(BF)
                gains_out[0:1, :] += gained

            tiles(heads * HD, HD, one)

    here = pl.ds(pl.multiple_of(block_at * rows, rows), rows)
    grad_k = (gk_all[here, :] * scale).astype(BF).astype(F32)
    grad_raw, gained = back(proj_ref[:, heads * HD : (heads + 1) * HD], k_gain, grad_k)
    out_ref[:, heads * HD : (heads + 1) * HD] = grad_raw.astype(BF)
    out_ref[:, (heads + 1) * HD :] = gv_all[here, :].astype(BF)
    gains_out[1:2, :] += gained

    def leave(at):
        part_ref[:, at] = lax.dot_general(
            out_ref[...], wq_ref[at, :], (((1,), (1,)), ((), ())), preferred_element_type=F32
        ).astype(BF)

    tiles(part_ref.shape[1], 256, leave)

    @pl.when(step == blocks - 1)
    def _():
        Blocks(sizes, specs, sources, results, sems).wait()


def attend_back(
    length, projected, low, grad, w_out, w_proj, cosine, sine, gains, heads, extras, specs, sizes,
    collective_id, blocks=4,
):
    total, own_width = projected.shape
    width = w_out.shape[1]
    rows = total // blocks
    q_width = heads * HD

    def by_rows(columns):
        return pl.BlockSpec((rows, columns), lambda i: (blocks - 1 - i, 0))

    def whole(array):
        return pl.BlockSpec(array.shape, lambda i: (0, 0), pipeline_mode=pl.Buffered(1))

    return pl.pallas_call(
        functools.partial(attend_back_kernel, sizes, heads, blocks, specs),
        grid=(blocks,),
        out_shape=[
            jax.ShapeDtypeStruct((total, own_width), BF),
            jax.ShapeDtypeStruct((total, width), BF),
            jax.ShapeDtypeStruct((2, HD), F32),
        ] + block_outs(sizes, extras, specs),
        in_specs=[
            pl.BlockSpec(memory_space=pltpu.SMEM),
            by_rows(own_width),
            by_rows(q_width),
            pl.BlockSpec((total, 2 * HD), lambda i: (0, heads // 2)),
            by_rows(width),
            whole(w_out),
            whole(w_proj),
            by_rows(HD),
            by_rows(HD),
            whole(gains),
        ] + [ANY] * len(extras),
        out_specs=[by_rows(own_width), by_rows(width), pl.BlockSpec((2, HD), lambda i: (0, 0))]
        + [ANY] * len(extras),
        scratch_shapes=[
            pltpu.VMEM((total, HD), F32),
            pltpu.VMEM((total, HD), F32),
            pltpu.VMEM((rows, q_width), BF),
        ] + block_scratch(sizes, extras, specs),
        compiler_params=pltpu.CompilerParams(
            collective_id=collective_id, has_side_effects=True, vmem_limit_bytes=58 << 20
        ),
        name="attend_back",
    )(length, projected, low, low, grad, w_out, w_proj, cosine, sine, gains, *extras)


def rms_factor(values):
    return lax.rsqrt(jnp.mean(values * values, axis=-1, keepdims=True) + EPSILON)


def dot(left, right):
    return jnp.dot(left, right, preferred_element_type=F32)


def mm(form, left, right):
    return jnp.einsum(form, left, right, preferred_element_type=F32)


def whole_columns(blocks):
    parts, rows, _ = blocks.shape
    q_width = QH * HD // parts
    kv_width = KH * HD // parts
    moved = blocks.transpose(1, 0, 2)
    return jnp.concatenate(
        [
            moved[..., :q_width].reshape(rows, -1),
            moved[..., q_width : q_width + kv_width].reshape(rows, -1),
            moved[..., q_width + kv_width :].reshape(rows, -1),
        ],
        axis=-1,
    )


def lanes(flat, lead):
    width = flat.shape[-1]
    rows = -(-width // 2048) * 16
    return jnp.pad(flat, ((0, 0), (0, rows * 128 - width))).reshape(lead, rows, 128)


def per_device(
    tokens, cotangent, lengths, routes, slots, w_qkv, w_out, w_router, norm_gains, w_gate_up, w_down
):
    tok_count = tokens.shape[1]
    width = tokens.shape[2]
    S = lax.axis_size("seq")
    F = lax.axis_size("fsdp")
    N = S * F
    sizes = {"seq": S, "fsdp": F}
    local_experts = w_gate_up.shape[0]
    own_experts = local_experts // S
    expert_count = w_router.shape[1]
    capacity = tok_count * TOPK * 5 // (4 * expert_count)
    heads = QH // S
    seq_total = tok_count * S
    q_width = heads * HD
    own_width = q_width + 2 * HD
    seq_at = lax.axis_index("seq")
    w_rows = w_qkv.shape[0]
    small = norm_gains.shape[0]
    router_size = w_router.size
    part_width = w_gate_up.shape[1]
    down_width = w_down.shape[2]
    assert KH == S and local_experts % S == 0

    small_send = lanes(jnp.concatenate([w_router.reshape(-1), norm_gains])[None], 1)[0]
    table = jnp.concatenate([routes[0].T, slots[0].T])
    tok_all, cot_all, table_all, w_proj, out_own, small_all = entry(
        tokens[0], cotangent[0], table, w_qkv, w_out, small_send, sizes, 1
    )
    w_proj = w_proj.reshape(width, own_width)
    out_own = out_own.reshape(q_width, width)
    small_flat = small_all.reshape(N, -1)
    full_router = small_flat[:, :router_size].reshape(width, expert_count)
    gain_values = small_flat[:, router_size : router_size + small].reshape(-1).astype(F32)
    gain_attn = gain_values[:width]
    gain_ffn = gain_values[width : 2 * width][None]
    gain_heads = gain_values[2 * width :].reshape(2, HD)

    positions = jnp.arange(seq_total, dtype=jnp.int32)
    frequency = THETA ** (-jnp.arange(HD // 2, dtype=F32) / (HD // 2))
    angles = positions.astype(F32)[:, None] * frequency[None, :]
    cosine = jnp.concatenate([jnp.cos(angles)] * 2, axis=-1)
    sine = jnp.concatenate([-jnp.sin(angles), jnp.sin(angles)], axis=-1)
    attn_low, projected, qkv_low, o_low, o_part, down_w = attend(
        lengths, tok_all.reshape(seq_total, width), gain_attn[None], w_proj, cosine, sine,
        gain_heads, out_own, heads, [w_down.reshape((S, own_experts) + w_down.shape[1:])],
        ((("seq",), 0, "columns"),), sizes, 3,
    )
    o_part = o_part.reshape(S, tok_count, width)

    expert_ids = jnp.arange(expert_count, dtype=jnp.int32)
    slot_ids = jnp.arange(capacity, dtype=jnp.int32)
    plane = (
        jnp.arange(F, dtype=jnp.int32)[:, None] * local_experts
        + seq_at * own_experts
        + jnp.arange(own_experts, dtype=jnp.int32)[None, :]
    ).reshape(-1)
    hit = table_all[:, None, :TOPK] == plane[None, :, None, None]
    plane_slots = jnp.max(jnp.where(hit, table_all[:, None, TOPK:], -1), axis=2)
    one_hot = plane_slots[:, :, None, :] == slot_ids[None, None, :, None]
    select = one_hot.astype(BF).reshape(S, F * own_experts * capacity, tok_count)
    grouped = (S, F, own_experts * capacity, width)
    shape5 = (F, S, own_experts, capacity, width)

    cot_rows = mm("brt,btd->brd", select, cot_all).astype(BF).reshape(grouped)
    residual, ffn_all, g_rows = line(
        "ffn", sizes, [o_part], [tokens[0], gain_ffn], [cot_rows], ((("fsdp",), 1, 0),), 2
    )
    g_rows = g_rows.reshape(shape5)
    ffn_low = lax.dynamic_index_in_dim(ffn_all, seq_at, 0, keepdims=False)

    route_rows = routes[0]
    slot_rows = slots[0]
    router_scores = dot(ffn_low, full_router)
    picked = route_rows[:, :, None] == expert_ids[None, None, :]
    selected = jnp.sum(jnp.where(picked, router_scores[:, None, :], 0.0), axis=-1)
    gate_prob = jax.nn.softmax(selected, axis=-1)
    gate_table = jnp.sum(jnp.where(picked, gate_prob[:, :, None], 0.0), axis=1).T
    hit = table[None, :TOPK] == expert_ids[:, None, None]
    own_slots = jnp.max(jnp.where(hit, table[None, TOPK:], -1), axis=1)
    gate_slots = jnp.sum(
        jnp.where(
            own_slots[:, None, :] == slot_ids[None, :, None], gate_table[:, None, :], 0.0
        ),
        axis=-1,
    )
    by_device = (F, S, own_experts, capacity)

    def to_devices(values):
        return lanes(values.reshape(by_device).transpose(1, 0, 2, 3).reshape(N, -1), N)

    gate_send = to_devices(gate_slots)

    ffn_rows = mm("brt,btd->brd", select, ffn_all).astype(BF).reshape(grouped)
    x_rows, gate_up_w, gate_got = exchange(
        [ffn_rows, w_gate_up.reshape((S, own_experts) + w_gate_up.shape[1:]), gate_send],
        ((("fsdp",), 1, 0), (("seq",), 0, 0), (EVERY, 0, 0)), sizes, 4,
    )
    gate_up_w = gate_up_w.transpose(1, 0, 2, 3).reshape(own_experts, width, 2 * FF)
    x_rows = x_rows.reshape(shape5)
    row_gate = gate_got.reshape(S, F, -1)[:, :, : own_experts * capacity]
    row_gate = row_gate.transpose(1, 0, 2).reshape(F, S, own_experts, capacity, 1)

    gate_up = mm("asjcd,jdf->asjcf", x_rows, gate_up_w)
    gate_part = gate_up[..., :FF]
    up_part = gate_up[..., FF:]
    hidden_low = (jax.nn.silu(gate_part) * up_part).astype(BF)
    expert_out = mm("asjch,jhd->asjcd", hidden_low, down_w).astype(BF)
    out_wide = expert_out.astype(F32)
    grad_prob_rows = jnp.sum(out_wide * g_rows.astype(F32), axis=-1)
    moe_rows = (row_gate * out_wide).astype(BF)

    through_down = mm("asjcd,jhd->asjch", g_rows, down_w)
    grad_hidden = lax.optimization_barrier((row_gate * through_down).astype(BF)).astype(F32)
    gated_hidden = (row_gate * hidden_low.astype(F32)).astype(BF)
    sigmoid_gate = jax.nn.sigmoid(gate_part)
    grad_gate = grad_hidden * up_part * sigmoid_gate * (1.0 + gate_part * (1.0 - sigmoid_gate))
    grad_up = grad_hidden * gate_part * sigmoid_gate
    grad_gu_low = jnp.concatenate([grad_gate, grad_up], axis=-1).astype(BF)
    grad_rows = mm("asjcf,jdf->asjcd", grad_gu_low, gate_up_w).astype(BF)
    prob_send = grad_prob_rows.reshape(F, S, -1).transpose(1, 0, 2).reshape(N, -1)
    back_layout = grad_rows.reshape(F, S, own_experts * capacity, width)
    back_blocks = [back_layout, lanes(prob_send, N)]
    back_specs = ((("fsdp",), 0, 1), (EVERY, 0, 0))
    if own_experts == 1:
        grad_back, prob_got, up_got, down_term = grads(
            back_blocks, back_specs, x_rows.reshape(-1, width), grad_gu_low.reshape(-1, 2 * FF),
            gated_hidden.reshape(-1, FF), g_rows.reshape(-1, width), sizes, 6,
        )
        down_term = down_term[None]
    else:
        up_term = mm("asjcd,asjcf->jdf", x_rows, grad_gu_low).astype(BF)
        down_term = mm("asjch,asjcd->jhd", gated_hidden, g_rows).astype(BF)
        up_blocks = up_term.reshape(own_experts, S, part_width, 2 * FF).transpose(1, 0, 2, 3)
        grad_back, prob_got, up_got = exchange(
            back_blocks + [up_blocks], back_specs + ((("seq",), 0, 0),), sizes, 6
        )
    up_got = up_got.reshape(w_gate_up.shape)
    prob_slots = prob_got.reshape(S, F, -1)[:, :, : own_experts * capacity]
    prob_slots = prob_slots.reshape(S, F, own_experts, capacity).transpose(1, 0, 2, 3)
    prob_slots = prob_slots.reshape(expert_count, capacity)

    grad_part = mm("brt,brd->btd", select, grad_back.reshape(S, -1, width)).astype(BF)

    prob_of_route = jnp.einsum(
        "tke,ec->tkc", picked.astype(F32), prob_slots, precision=lax.Precision.HIGHEST
    )
    at_slot = slot_rows[:, :, None] == slot_ids[None, None, :]
    grad_prob = jnp.sum(jnp.where(at_slot, prob_of_route, 0.0), axis=-1)
    grad_selected = gate_prob * (grad_prob - jnp.sum(gate_prob * grad_prob, axis=-1, keepdims=True))
    grad_logits = jnp.sum(jnp.where(picked, grad_selected[:, :, None], 0.0), axis=1).astype(BF)
    grad_ffn_add = mm("te,de->td", grad_logits, full_router)
    grad_router_part = mm("td,te->de", ffn_low, grad_logits)
    valid = (seq_at * tok_count + jnp.arange(tok_count, dtype=jnp.int32)) < lengths[0]
    grad_final = jnp.where(valid[:, None], cotangent[0].astype(F32), 0.0)
    grad_residual, grad_gain_ffn, grad_attn_low, moe_back, grad_gate_up = line(
        "grad", sizes, [grad_part], [grad_final, gain_ffn, residual, grad_ffn_add],
        [moe_rows.reshape(F, S, own_experts * capacity, width)], ((("fsdp",), 0, 1),), 7,
        widened=(up_got,),
    )
    grad_attn_low = grad_attn_low.reshape(seq_total, width)

    grad_proj, attn_part, grad_gain_heads, down_got = attend_back(
        lengths, projected, qkv_low, grad_attn_low, out_own, w_proj, cosine, sine, gain_heads,
        heads, [down_term], ((("seq",), "columns", 0),), sizes, 9,
    )
    attn_part = attn_part.reshape(S, tok_count, width)
    grad_out_part = mm("te,td->ed", o_low, grad_attn_low).astype(BF)
    grad_qkv_part = mm("td,te->de", attn_low, grad_proj).astype(BF).reshape(S, F, w_rows, own_width)
    moe_part = mm("brt,brd->btd", select, moe_back.reshape(S, -1, width)).astype(BF)
    router_blocks = lanes(grad_router_part.reshape(N, -1), N)
    early_gains = lanes(jnp.concatenate([grad_gain_ffn[0], grad_gain_heads.reshape(-1)])[None], 1)[0]
    (
        grad_inputs, final, late_gains, grad_out, grad_qkv, router_got, gains_got, grad_down
    ) = line(
        "last", sizes, [attn_part, moe_part],
        [
            grad_residual, gain_attn[None], residual, tokens[0], lengths,
            grad_out_part.reshape(F, -1, width), grad_qkv_part,
        ],
        [router_blocks, early_gains], ((EVERY, 0, 0), (EVERY, None, 0)), 8,
        widened=(down_got.reshape(w_down.shape),),
    )
    grad_router = jnp.sum(router_got, axis=0).reshape(-1)[:router_size].reshape(w_router.shape)
    gain_sum = jnp.concatenate(
        [
            jnp.sum(late_gains, axis=0).reshape(-1),
            jnp.sum(gains_got, axis=0).reshape(-1)[: width + 2 * HD],
        ]
    )
    device_at = seq_at * F + lax.axis_index("fsdp")
    grad_gains = lax.dynamic_slice_in_dim(gain_sum, device_at * small, small, 0)
    return (
        final[None],
        grad_inputs[None],
        grad_qkv,
        grad_out,
        grad_router,
        grad_gains,
        grad_gate_up,
        grad_down,
    )


def solution(mesh):
    in_specs = (
        P("fsdp", "seq", None),
        P("fsdp", "seq", None),
        P("fsdp"),
        P("fsdp", "seq", None),
        P("fsdp", "seq", None),
        P(("seq", "fsdp"), None),
        P(("seq", "fsdp"), None),
        P(("seq", "fsdp"), None),
        P(("seq", "fsdp")),
        P("fsdp", "seq", None),
        P("fsdp", None, "seq"),
    )
    out_specs = (
        P("fsdp", "seq", None),
        P("fsdp", "seq", None),
        P(("seq", "fsdp"), None),
        P(("seq", "fsdp"), None),
        P(("seq", "fsdp"), None),
        P(("seq", "fsdp")),
        P("fsdp", "seq", None),
        P("fsdp", None, "seq"),
    )
    return jax.shard_map(
        per_device, mesh=mesh, in_specs=in_specs, out_specs=out_specs, check_vma=False
    )
```

```python
import functools

import jax
import jax.numpy as jnp
from jax import lax
from jax.experimental import pallas as pl
from jax.experimental.pallas import tpu as pltpu
from jax.sharding import PartitionSpec as P

QH = 32
KH = 4
HD = 128
FF = 768
TOPK = 8
EPSILON = 1e-06
THETA = 1000000.0
MASKED = -1e30
AHEAD = 1
BF = jnp.bfloat16
F32 = jnp.float32
MESH = pl.DeviceIdType.MESH
ANY = pl.BlockSpec(memory_space=pl.ANY)
VM = pl.BlockSpec(memory_space=pltpu.VMEM)
DMA = pltpu.SemaphoreType.DMA
EVERY = ("seq", "fsdp")

def index_of(sizes, axes):
    at = 0
    for axis in axes:
        at = at * sizes[axis] + lax.axis_index(axis)
    return at


def count_of(sizes, axes):
    number = 1
    for axis in axes:
        number *= sizes[axis]
    return number


def place_of(sizes, axes, at):
    if len(axes) == 1:
        return {axes[0]: at}
    return {axes[0]: at // sizes[axes[1]], axes[1]: at % sizes[axes[1]]}


def greet(sizes):
    total = count_of(sizes, EVERY)
    me = index_of(sizes, EVERY)
    barrier = pltpu.get_barrier_semaphore()
    for step in range(1, total):
        pl.semaphore_signal(
            barrier, inc=1, device_id=place_of(sizes, EVERY, lax.rem(me + step, total)),
            device_id_type=MESH,
        )
    return lambda: pl.semaphore_wait(barrier, total - 1)


def block_of(ref, dim, at, total):
    if dim is None:
        return ref
    if dim == "columns":
        width = ref.shape[-1] // total
        return ref.at[:, :, pl.ds(pl.multiple_of(at * width, 128), width)]
    return ref.at[at] if dim == 0 else ref.at[:, at]


class Blocks:
    def __init__(self, sizes, specs, sources, results, sems):
        self.own, self.parted = [], []
        if not specs:
            return
        send_sem, recv_sem, own_sem, *stages = sems
        for i, (axes, before, after) in enumerate(specs):
            me = index_of(sizes, axes)
            total = count_of(sizes, axes)
            source = block_of(sources[i], before, me, total)
            result = block_of(results[i], after, me, total)
            self.own.append(
                (
                    pltpu.make_async_copy(source, stages[i], own_sem.at[i, 0]),
                    pltpu.make_async_copy(stages[i], result, own_sem.at[i, 1]),
                )
            )
            self.parted.append([])
            for step in range(1, total):
                target = lax.rem(me + step, total)
                self.parted[-1].append(
                    pltpu.make_async_remote_copy(
                        src_ref=block_of(sources[i], before, target, total),
                        dst_ref=block_of(results[i], after, me, total),
                        send_sem=send_sem.at[i, step],
                        recv_sem=recv_sem.at[i, step],
                        device_id=place_of(sizes, axes, target),
                        device_id_type=MESH,
                    )
                )

    def start(self):
        for copies in self.parted:
            for copy in copies:
                copy.start()
        for inward, _ in self.own:
            inward.start()

    def wait(self):
        for i in range(len(self.own)):
            self.wait_one(i)

    def wait_one(self, i):
        inward, outward = self.own[i]
        inward.wait()
        outward.start()
        outward.wait()
        for copy in self.parted[i]:
            copy.wait()


def block_scratch(sizes, arrays, specs):
    if not specs:
        return []
    total = max(count_of(sizes, axes) for axes, _, _ in specs)
    stages = []
    for array, (axes, before, after) in zip(arrays, specs):
        shape = list(array.shape)
        if before == "columns":
            shape[-1] //= count_of(sizes, axes)
        elif before is not None:
            del shape[before]
        stages.append(pltpu.VMEM(tuple(shape), array.dtype))
    count = len(specs)
    return [DMA((count, total)), DMA((count, total)), DMA((count, 2))] + stages


def block_outs(sizes, arrays, specs):
    outs = []
    for array, (axes, before, after) in zip(arrays, specs):
        shape = list(array.shape)
        total = count_of(sizes, axes)
        if before is None:
            shape = [total] + shape
        elif before == "columns":
            shape = [total, shape[0], shape[1], shape[2] // total]
        elif after == "columns":
            shape = [shape[1], shape[2], shape[3] * total]
        elif before != after:
            shape[0], shape[1] = shape[1], shape[0]
        outs.append(jax.ShapeDtypeStruct(tuple(shape), array.dtype))
    return outs


def exchange_kernel(sizes, specs, *refs):
    count = len(specs)
    met = greet(sizes)
    blocks = Blocks(sizes, specs, refs[:count], refs[count : 2 * count], refs[2 * count :])
    met()
    blocks.start()
    blocks.wait()


def exchange(arrays, specs, sizes, collective_id):
    count = len(arrays)
    return pl.pallas_call(
        functools.partial(exchange_kernel, sizes, specs),
        out_shape=block_outs(sizes, arrays, specs),
        in_specs=[ANY] * count,
        out_specs=[ANY] * count,
        scratch_shapes=block_scratch(sizes, arrays, specs),
        compiler_params=pltpu.CompilerParams(collective_id=collective_id, has_side_effects=True),
        name=f"exchange_{collective_id}",
    )(*arrays)


def entry_kernel(
    sizes, tok_ref, cot_ref, table_ref, wqkv_ref, wout_ref, small_ref,
    tok_out, cot_out, table_out, wq_out, wo_out, small_out,
    tok_send, tok_recv, tab_send, tab_recv, wq_zsend, wq_zrecv,
    pl_send, pl_recv, sib_send, sib_recv, sm_send, sm_recv, own_sem, *stages,
):
    S, F = sizes["seq"], sizes["fsdp"]
    s = lax.axis_index("seq")
    f = lax.axis_index("fsdp")
    N = S * F
    chips = F // 2
    me = s * F + f
    other = f + 1 - 2 * lax.rem(f, 2)
    rows = tok_ref.shape[0]
    chunks = tok_recv.shape[2]
    span = rows // chunks
    met = greet(sizes)
    kv = KH * HD // S
    q_width = QH * HD // S
    starts = (0, q_width * S, (q_width + kv) * S)
    widths = (q_width, kv, kv)
    offsets = (0, q_width, q_width + kv)

    def columns(z, p):
        return pl.ds(pl.multiple_of(starts[p] + z * widths[p], 128), widths[p])

    pairs = [
        (wqkv_ref.at[:, columns(s, p)], wq_out.at[s, f, :, pl.ds(offsets[p], widths[p])])
        for p in range(3)
    ] + [
        (wout_ref, wo_out.at[f]),
        (tok_ref, tok_out.at[s]),
        (cot_ref, cot_out.at[s]),
        (table_ref, table_out.at[s]),
        (small_ref, small_out.at[me]),
    ]
    inward = [
        pltpu.make_async_copy(source, stages[i], own_sem.at[i, 0])
        for i, (source, _) in enumerate(pairs)
    ]
    outward = [
        pltpu.make_async_copy(stages[i], result, own_sem.at[i, 1])
        for i, (_, result) in enumerate(pairs)
    ]
    for copy in inward:
        copy.start()
    met()

    def remote(src, dst, send_sem, recv_sem, where):
        return pltpu.make_async_remote_copy(
            src_ref=src, dst_ref=dst, send_sem=send_sem, recv_sem=recv_sem,
            device_id=where, device_id_type=MESH,
        )

    wq_line = []
    tables = []
    for step in range(1, S):
        target = lax.rem(s + step, S)
        for p in range(3):
            copy = remote(
                wqkv_ref.at[:, columns(target, p)],
                wq_out.at[s, f, :, pl.ds(offsets[p], widths[p])],
                wq_zsend.at[step, p], wq_zrecv.at[step, p], {"seq": target},
            )
            copy.start()
            wq_line.append(copy)
        copy = remote(
            table_ref, table_out.at[s], tab_send.at[step], tab_recv.at[step], {"seq": target}
        )
        copy.start()
        tables.append(copy)

    def along(a, block, c, way, hop):
        source, result = ((tok_ref, tok_out), (cot_ref, cot_out))[a]
        here = result.at[block, pl.ds(c * span, span)]
        src = source.at[pl.ds(c * span, span)] if hop == 1 else here
        return remote(
            src, here, tok_send.at[a, way, c, hop], tok_recv.at[a, way, c, hop],
            {"seq": s + 1 if way == 0 else s - 1},
        )

    def depart(a):
        for c in range(chunks):
            @pl.when(s < S - 1)
            def _():
                along(a, s, c, 0, 1).start()

            @pl.when(s > 0)
            def _():
                along(a, s, c, 1, 1).start()

    def relay(a, hop):
        for c in range(chunks):
            @pl.when(s >= hop)
            def _():
                along(a, s - hop, c, 0, hop).wait_recv()
                if hop < S - 1:
                    @pl.when(s < S - 1)
                    def _():
                        along(a, s - hop, c, 0, hop + 1).start()

            @pl.when(s < S - hop)
            def _():
                along(a, s + hop, c, 1, hop).wait_recv()
                if hop < S - 1:
                    @pl.when(s > 0)
                    def _():
                        along(a, s + hop, c, 1, hop + 1).start()

    depart(0)

    def plane_block(slot, owner):
        if slot == S:
            return wo_out.at[owner]
        return wq_out.at[lax.rem(s - slot + S, S), owner]

    def to_chip(slot, step):
        block = plane_block(slot, f)
        return remote(block, block, pl_send.at[slot, step], pl_recv.at[slot, step],
                      {"fsdp": lax.rem(f + 2 * step, F)})

    def to_other(slot, step):
        block = plane_block(slot, lax.rem(f - 2 * step + F, F))
        return remote(block, block, sib_send.at[slot, step], sib_recv.at[slot, step],
                      {"fsdp": other})

    def spread(slot):
        for step in range(1, chips):
            to_chip(slot, step).start()
        to_other(slot, 0).start()

    def forward(slot):
        for step in range(1, chips):
            to_chip(slot, step).wait_recv()
            to_other(slot, step).start()

    smalls = []
    for step in range(1, N):
        target = lax.rem(me + step, N)
        copy = remote(small_ref, small_out.at[me], sm_send.at[step], sm_recv.at[step],
                      place_of(sizes, EVERY, target))
        copy.start()
        smalls.append(copy)
    for i, copy in enumerate(inward):
        copy.wait()
        outward[i].start()
    for copy in outward[:3]:
        copy.wait()
    spread(0)
    outward[3].wait()
    spread(S)
    relay(0, 1)
    depart(1)
    for step in range(1, S):
        for p in range(3):
            wq_line[(step - 1) * 3 + p].wait()
        spread(step)
    for hop in range(2, S):
        relay(0, hop)
        relay(1, hop - 1)
    for slot in range(S + 1):
        forward(slot)
    relay(1, S - 1)
    for a in range(2):
        for hop in range(1, S):
            for c in range(chunks):
                @pl.when((s < S - 1) & (s >= hop - 1))
                def _():
                    along(a, s, c, 0, hop).wait_send()

                @pl.when((s > 0) & (s <= S - hop))
                def _():
                    along(a, s, c, 1, hop).wait_send()
    for copy in outward[4:]:
        copy.wait()
    for slot in range(S + 1):
        for step in range(1, chips):
            to_chip(slot, step).wait_send()
        for step in range(chips):
            to_other(slot, step).wait_send()
            block = plane_block(slot, lax.rem(other - 2 * step + F, F))
            remote(block, block, sib_send.at[slot, step], sib_recv.at[slot, step],
                   {"fsdp": other}).wait_recv()
    for copy in tables + smalls:
        copy.wait()


def entry(tokens, cotangent, table, w_qkv, w_out, small, sizes, collective_id, chunks=4):
    S, F = sizes["seq"], sizes["fsdp"]
    own_width = w_qkv.shape[1] // S
    N = S * F
    line_out = jax.ShapeDtypeStruct((S,) + tokens.shape, tokens.dtype)
    q_width, kv = QH * HD // S, KH * HD // S
    stages = [
        pltpu.VMEM(shape, dtype)
        for shape, dtype in [
            ((w_qkv.shape[0], q_width), BF),
            ((w_qkv.shape[0], kv), BF),
            ((w_qkv.shape[0], kv), BF),
            (w_out.shape, BF),
            (tokens.shape, BF),
            (cotangent.shape, BF),
            (table.shape, table.dtype),
            (small.shape, BF),
        ]
    ]
    return pl.pallas_call(
        functools.partial(entry_kernel, sizes),
        out_shape=[
            line_out,
            line_out,
            jax.ShapeDtypeStruct((S,) + table.shape, table.dtype),
            jax.ShapeDtypeStruct((S, F, w_qkv.shape[0], own_width), w_qkv.dtype),
            jax.ShapeDtypeStruct((F,) + w_out.shape, w_out.dtype),
            jax.ShapeDtypeStruct((N,) + small.shape, small.dtype),
        ],
        in_specs=[ANY] * 6,
        out_specs=[ANY] * 6,
        scratch_shapes=[
            DMA((2, 2, chunks, S)), DMA((2, 2, chunks, S)), DMA((S,)), DMA((S,)),
            DMA((S, 3)), DMA((S, 3)), DMA((S + 1, F // 2)), DMA((S + 1, F // 2)),
            DMA((S + 1, F // 2)), DMA((S + 1, F // 2)), DMA((N,)), DMA((N,)), DMA((8, 2)),
        ] + stages,
        compiler_params=pltpu.CompilerParams(collective_id=collective_id, has_side_effects=True),
        name="entry",
    )(tokens, cotangent, table, w_qkv, w_out, small)


class Widen:
    def __init__(self, pairs, sems, buffers):
        self.jobs = []
        for i, (source, result) in enumerate(pairs):
            narrow, wide = buffers[2 * i], buffers[2 * i + 1]
            for j in range(source.shape[0]):
                self.jobs.append(
                    (
                        pltpu.make_async_copy(source.at[j], narrow.at[j % 2], sems.at[i, 0, j % 2]),
                        pltpu.make_async_copy(wide.at[j % 2], result.at[j], sems.at[i, 1, j % 2]),
                        narrow.at[j % 2],
                        wide.at[j % 2],
                        j,
                        source.shape[0],
                    )
                )
        self.done = 0

    def start(self):
        for inward, _, _, _, j, _ in self.jobs:
            if j < 2:
                inward.start()

    def turn(self):
        if self.done == len(self.jobs):
            return
        at = self.done
        inward, outward, narrow, wide, j, number = self.jobs[at]
        inward.wait()
        if j >= 2:
            self.jobs[at - 2][1].wait()
        wide[...] = narrow[...].astype(F32)
        outward.start()
        if j + 2 < number:
            self.jobs[at + 2][0].start()
        self.done += 1

    def wait(self):
        while self.done < len(self.jobs):
            self.turn()
        for _, outward, _, _, j, number in self.jobs:
            if j >= number - 2:
                outward.wait()


def widen_scratch(arrays):
    if not arrays:
        return []
    scratch = [DMA((len(arrays), 2, 2))]
    for array in arrays:
        shape = (2,) + array.shape[1:]
        scratch += [pltpu.VMEM(shape, BF), pltpu.VMEM(shape, F32)]
    return scratch


def grads_kernel(sizes, specs, combined, *refs):
    S = sizes["seq"]
    count = len(specs)
    refs = list(refs)

    def take(number):
        taken, refs[:number] = refs[:number], []
        return taken

    sources, (x_any, gu_any, ph_any, g_any) = take(count), take(4)
    combine = take(1) if combined else None
    results, (up_out, down_out) = take(count), take(2)
    part_out = take(1) if combined else None
    x_ref, gu_ref, ph_ref, g_ref, up_stage, down_stage = take(6)
    in_sem, up_send, up_recv, out_sem, back_sem, *sems = refs
    s = lax.axis_index("seq")
    inward = [
        pltpu.make_async_copy(source, target, in_sem.at[i])
        for i, (source, target) in enumerate(
            ((x_any, x_ref), (gu_any, gu_ref), (ph_any, ph_ref), (g_any, g_ref))
        )
    ]
    met = greet(sizes)
    for copy in inward:
        copy.start()
    blocks = Blocks(sizes, specs, sources, results, sems)
    met()
    blocks.start()
    inward[0].wait()
    inward[1].wait()
    part = up_stage.shape[1]
    over_rows = (((0,), (0,)), ((), ()))
    sent = []
    for turn_at in range(1, S + 1):
        target = lax.rem(s + turn_at, S)
        mine = pl.ds(pl.multiple_of(target * part, 128), part)
        block = up_stage.at[turn_at - 1]

        def one(at):
            block[:, at] = lax.dot_general(
                x_ref[:, mine], gu_ref[:, at], over_rows, preferred_element_type=F32
            ).astype(BF)

        tiles(gu_ref.shape[1], 256, one)
        if turn_at < S:
            copy = pltpu.make_async_remote_copy(
                src_ref=block, dst_ref=up_out.at[s],
                send_sem=up_send.at[turn_at], recv_sem=up_recv.at[turn_at],
                device_id={"seq": target}, device_id_type=MESH,
            )
        else:
            copy = pltpu.make_async_copy(block, up_out.at[s], out_sem.at[0])
        copy.start()
        sent.append(copy)
    inward[2].wait()
    inward[3].wait()

    def one_down(at):
        down_stage[:, at] = lax.dot_general(
            ph_ref[...], g_ref[:, at], over_rows, preferred_element_type=F32
        ).astype(BF)

    tiles(g_ref.shape[1], 256, one_down)
    copy = pltpu.make_async_copy(down_stage, down_out, out_sem.at[1])
    copy.start()
    sent.append(copy)
    blocks.wait_one(0)
    if combined:
        back = results[0]
        groups, slots = back.shape[1], back.shape[2]
        pieces = []
        for block_at in range(S):
            for group in range(groups):
                row = pl.ds((block_at * groups + group) * slots, slots)
                pieces.append(
                    pltpu.make_async_copy(
                        back.at[block_at, group], x_ref.at[row], back_sem.at[block_at, group]
                    )
                )
                pieces[-1].start()
        for copy in pieces:
            copy.wait()
        reach = groups * slots
        for block_at in range(S):

            def one_part(at):
                part_out[0][block_at, :, at] = lax.dot_general(
                    combine[0][block_at], x_ref[block_at * reach : (block_at + 1) * reach, at],
                    over_rows, preferred_element_type=F32,
                ).astype(BF)

            tiles(part_out[0].shape[2], 512, one_part)
    for i in range(1, count):
        blocks.wait_one(i)
    for copy in sent:
        copy.wait()


def grads(arrays, specs, rows, grad_gu, hidden, grad_out, select, sizes, collective_id):
    S = sizes["seq"]
    combined = select is not None
    groups = arrays[0].shape[0]
    part = rows.shape[1] // S
    up_block = (part, grad_gu.shape[1])
    down = (hidden.shape[1], grad_out.shape[1])
    inner = [rows, grad_gu, hidden, grad_out]
    return pl.pallas_call(
        functools.partial(grads_kernel, sizes, specs, combined),
        out_shape=block_outs(sizes, arrays, specs)
        + [jax.ShapeDtypeStruct((S,) + up_block, BF), jax.ShapeDtypeStruct(down, BF)]
        + ([jax.ShapeDtypeStruct((S, select.shape[2], rows.shape[1]), BF)] if combined else []),
        in_specs=[ANY] * (len(arrays) + 4) + [VM] * combined,
        out_specs=[ANY] * (len(arrays) + 2) + [VM] * combined,
        scratch_shapes=[pltpu.VMEM(array.shape, BF) for array in inner]
        + [pltpu.VMEM((S,) + up_block, BF), pltpu.VMEM(down, BF)]
        + [DMA((4,)), DMA((S,)), DMA((S,)), DMA((2,)), DMA((S, groups))]
        + block_scratch(sizes, arrays, specs),
        compiler_params=pltpu.CompilerParams(
            collective_id=collective_id, has_side_effects=True, vmem_limit_bytes=60 << 20
        ),
        name="grads",
    )(*arrays, *inner, *([select] if combined else []))


def dispatch_kernel(sizes, specs, *refs):
    S, F = sizes["seq"], sizes["fsdp"]
    count = len(specs)
    refs = list(refs)

    def take(number):
        taken, refs[:number] = refs[:number], []
        return taken

    sources = take(count)
    tok_any, g_any, down_any, select_ref = take(4)
    results = take(count)
    rows_out, through_out = take(2)
    tok_ref, rows_ref, g_ref, down_ref, through_ref, row_send, row_recv, own_sem, in_sem, out_sem, *sems = refs
    f = lax.axis_index("fsdp")
    slots = rows_out.shape[2]
    met = greet(sizes)
    inward = [pltpu.make_async_copy(tok_any.at[b], tok_ref.at[b], in_sem.at[b]) for b in range(S)]
    inward.append(pltpu.make_async_copy(down_any, down_ref, in_sem.at[S]))
    inward.append(pltpu.make_async_copy(g_any, g_ref, in_sem.at[S + 1]))
    for copy in inward:
        copy.start()
    blocks = Blocks(sizes, specs, sources, results, sems)
    met()
    sent = []
    for b in range(S):
        inward[b].wait()

        def one(at):
            rows_ref[b, :, at] = jnp.dot(
                select_ref[b], tok_ref[b, :, at], preferred_element_type=F32
            ).astype(BF)

        tiles(rows_ref.shape[2], 512, one)
        for step in range(1, F):
            target = lax.rem(f + step, F)
            copy = pltpu.make_async_remote_copy(
                src_ref=rows_ref.at[b, pl.ds(pl.multiple_of(target * slots, 16), slots)],
                dst_ref=rows_out.at[f, b],
                send_sem=row_send.at[b, step], recv_sem=row_recv.at[b, step],
                device_id={"fsdp": target}, device_id_type=MESH,
            )
            copy.start()
            sent.append(copy)
        copy = pltpu.make_async_copy(
            rows_ref.at[b, pl.ds(pl.multiple_of(f * slots, 16), slots)], rows_out.at[f, b], own_sem.at[b]
        )
        copy.start()
        sent.append(copy)
        if b == 0:
            blocks.start()
    inward[S].wait()
    inward[S + 1].wait()
    span = through_ref.shape[1]
    outward = []
    for n in range(g_ref.shape[0] // span):
        if n >= 2:
            outward[n - 2].wait()
        own = pl.ds(n * span, span)

        def one_through(at):
            through_ref[n % 2, :, at] = lax.dot_general(
                g_ref[own, :], down_ref[at, :], (((1,), (1,)), ((), ())), preferred_element_type=F32
            )

        tiles(through_ref.shape[2], 256, one_through)
        outward.append(pltpu.make_async_copy(through_ref.at[n % 2], through_out.at[own], out_sem.at[n % 2]))
        outward[-1].start()
    for copy in outward[-2:]:
        copy.wait()
    blocks.wait()
    for copy in sent:
        copy.wait()


def dispatch(arrays, specs, tokens, grads_in, w_down, select, sizes, collective_id):
    S, F = sizes["seq"], sizes["fsdp"]
    slots = select.shape[1] // F
    width = tokens.shape[2]
    count = grads_in.shape[0]
    hidden = w_down.shape[0]
    span = 512
    return pl.pallas_call(
        functools.partial(dispatch_kernel, sizes, specs),
        out_shape=block_outs(sizes, arrays, specs)
        + [
            jax.ShapeDtypeStruct((F, S, slots, width), BF),
            jax.ShapeDtypeStruct((count, hidden), F32),
        ],
        in_specs=[ANY] * (len(arrays) + 3) + [VM],
        out_specs=[ANY] * (len(arrays) + 2),
        scratch_shapes=[
            pltpu.VMEM(tokens.shape, BF),
            pltpu.VMEM((S, select.shape[1], width), BF),
            pltpu.VMEM(grads_in.shape, BF),
            pltpu.VMEM(w_down.shape, BF),
            pltpu.VMEM((2, span, hidden), F32),
            DMA((S, F)), DMA((S, F)), DMA((S,)), DMA((S + 2,)), DMA((2,)),
        ] + block_scratch(sizes, arrays, specs),
        compiler_params=pltpu.CompilerParams(
            collective_id=collective_id, has_side_effects=True, vmem_limit_bytes=58 << 20
        ),
        name="dispatch",
    )(*arrays, tokens, grads_in, w_down, select)


def expert_kernel(
    x_ref, gate_ref, through_ref, g_ref, up_w, down_w,
    moe_ref, back_ref, gu_ref, gated_ref, prob_ref, hidden_ref,
):
    hidden = hidden_ref.shape[1]
    width = x_ref.shape[1]
    row_gate = gate_ref[...]
    for at in range(0, hidden, 256):
        low = slice(at, at + 256)
        high = slice(hidden + at, hidden + at + 256)
        gate = jnp.dot(x_ref[...], up_w[:, low], preferred_element_type=F32)
        up = jnp.dot(x_ref[...], up_w[:, high], preferred_element_type=F32)
        sigmoid = jax.nn.sigmoid(gate)
        silu = gate * sigmoid
        value = (silu * up).astype(BF)
        hidden_ref[:, low] = value
        gated_ref[:, low] = (row_gate * value.astype(F32)).astype(BF)
        grad = (row_gate * through_ref[:, low]).astype(BF).astype(F32)
        gu_ref[:, low] = (grad * up * sigmoid * (1.0 + gate * (1.0 - sigmoid))).astype(BF)
        gu_ref[:, high] = (grad * silu).astype(BF)
    prob = jnp.zeros_like(row_gate)
    for at in range(0, width, 256):
        here = slice(at, at + 256)
        out = jnp.dot(hidden_ref[...], down_w[:, here], preferred_element_type=F32)
        out = out.astype(BF).astype(F32)
        moe_ref[:, here] = (row_gate * out).astype(BF)
        prob = prob + jnp.sum(out * g_ref[:, here].astype(F32), axis=-1, keepdims=True)
        back_ref[:, here] = lax.dot_general(
            gu_ref[...], up_w[here, :], (((1,), (1,)), ((), ())), preferred_element_type=F32
        ).astype(BF)
    prob_ref[...] = prob


def expert(x, row_gate, through, g, up_w, down_w, steps):
    count, width = x.shape
    hidden = down_w.shape[0]
    rows = count // steps

    def by_rows(columns):
        return pl.BlockSpec((rows, columns), lambda i: (i, 0))

    def whole(array):
        return pl.BlockSpec(array.shape, lambda i: (0, 0), pipeline_mode=pl.Buffered(1))

    return pl.pallas_call(
        expert_kernel,
        grid=(steps,),
        out_shape=[
            jax.ShapeDtypeStruct((count, width), BF),
            jax.ShapeDtypeStruct((count, width), BF),
            jax.ShapeDtypeStruct((count, 2 * hidden), BF),
            jax.ShapeDtypeStruct((count, hidden), BF),
            jax.ShapeDtypeStruct((count, 1), F32),
        ],
        in_specs=[by_rows(width), by_rows(1), by_rows(hidden), by_rows(width), whole(up_w), whole(down_w)],
        out_specs=[by_rows(width), by_rows(width), by_rows(2 * hidden), by_rows(hidden), by_rows(1)],
        scratch_shapes=[pltpu.VMEM((rows, hidden), BF)],
        compiler_params=pltpu.CompilerParams(vmem_limit_bytes=60 << 20),
        name="expert",
    )(x, row_gate, through, g, up_w, down_w)


def line_kernel(sizes, chunks, mode, parts, extra, widened, *refs):
    S, F = sizes["seq"], sizes["fsdp"]
    count = len(extra)
    names = {
        "ffn": (["base", "gain"], ["resid_out", "all_out"]),
        "grad": (["base", "gain", "resid", "add"], ["grad_out", "gain_out", "all_out"]),
        "last": (
            ["base", "gain", "resid", "inputs", "length", "gout", "gqkv"],
            ["grad_out", "low_out", "gains_all", "gout_out", "gqkv_out"],
        ),
    }[mode]
    refs = list(refs)

    def take(number):
        taken, refs[:number] = refs[:number], []
        return taken

    part_refs = take(parts)
    given = dict(zip(names[0], take(len(names[0]))))
    sources = take(count)
    narrow = take(widened)
    given.update(zip(names[1], take(len(names[1]))))
    results = take(count)
    wide = take(widened)
    from_left, from_right = take(2)
    gather = mode != "last"
    if gather:
        stage, rs_send, rs_recv, ag_send, ag_recv, own_sem = take(6)
        all_out = given["all_out"]
    else:
        gain_sum, gain_stage, gain_send, gain_recv, gain_own = take(5)
        plane_gout, plane_gqkv, gqkv_stage, gqkv_line, line_send, line_recv = take(6)
        plane_sems = take(5)
        rs_send, rs_recv = take(2)
    s = lax.axis_index("seq")
    f = lax.axis_index("fsdp")
    me = s * F + f
    N = S * F
    rows = part_refs[0].shape[1]
    span = rows // chunks
    met = greet(sizes)
    widen = Widen(list(zip(narrow, wide)), refs[0], refs[1:]) if widened else None
    del refs[: (1 + 2 * widened) if widened else 0]
    blocks = Blocks(sizes, extra, sources, results, refs)
    if widen:
        widen.start()
    met()

    def at(c):
        return pl.ds((c % chunks) * span, span)

    def mine(d, c):
        return part_refs[c // chunks].at[d, at(c)]

    def landed(way, d, c):
        return (from_left, from_right)[way].at[c // chunks, d, at(c)]

    def rs_copy(d, c, way, src):
        return pltpu.make_async_remote_copy(
            src_ref=src, dst_ref=landed(way, d, c),
            send_sem=rs_send.at[way, d, c], recv_sem=rs_recv.at[way, d, c],
            device_id={"seq": s + 1 if way == 0 else s - 1}, device_id_type=MESH,
        )

    def ag_copy(block, c, way, hop):
        src = stage.at[at(c)] if hop == 1 else all_out.at[block, at(c)]
        return pltpu.make_async_remote_copy(
            src_ref=src, dst_ref=all_out.at[block, at(c)],
            send_sem=ag_send.at[way, c, hop], recv_sem=ag_recv.at[way, c, hop],
            device_id={"seq": s + 1 if way == 0 else s - 1}, device_id_type=MESH,
        )

    def end_step(c):
        for d in range(S - 1, 0, -1):
            @pl.when((s == 0) & (d > s))
            def _():
                rs_copy(d, c, 0, mine(d, c)).start()
        for d in range(S - 1):
            @pl.when((s == S - 1) & (d < s))
            def _():
                rs_copy(d, c, 1, mine(d, c)).start()

    def middle_step(c):
        for way in range(2):
            order = range(S - 1, 0, -1) if way == 0 else range(S - 1)
            for d in order:
                inside = (s > 0) & (d > s) if way == 0 else (s < S - 1) & (d < s)

                @pl.when(inside)
                def _():
                    buffer = landed(way, d, c)
                    rs_copy(d, c, way, buffer).wait_recv()
                    total = buffer[...].astype(F32) + mine(d, c)[...].astype(F32)
                    buffer[...] = total.astype(BF)
                    rs_copy(d, c, way, buffer).start()

    def final_step(c):
        @pl.when(s > 0)
        def _():
            rs_copy(s, c, 0, mine(s, c)).wait_recv()

        @pl.when(s < S - 1)
        def _():
            rs_copy(s, c, 1, mine(s, c)).wait_recv()

        total = mine(s, c)[...].astype(F32)
        total = total + jnp.where(s > 0, landed(0, s, c)[...].astype(F32), 0.0)
        total = total + jnp.where(s < S - 1, landed(1, s, c)[...].astype(F32), 0.0)
        if mode == "last":
            if c >= chunks:
                row = s * rows + (c % chunks) * span + lax.broadcasted_iota(jnp.int32, total.shape, 0)
                value = given["resid"][at(c), :] + total
                given["low_out"][at(c), :] = jnp.where(row < given["length"][0], value, 0.0).astype(BF)
                return
            value = given["inputs"][at(c), :].astype(F32)
            factor = lax.rsqrt(jnp.mean(value * value, axis=-1, keepdims=True) + EPSILON)
            normed = value * factor
            scaled = total * given["gain"][...]
            inner = jnp.mean(scaled * normed, axis=-1, keepdims=True)
            given["grad_out"][at(c), :] = given["base"][at(c), :] + factor * (scaled - normed * inner)
            gained = jnp.sum(total * normed, axis=0, keepdims=True)
            gain_sum[...] = gained if c == 0 else gain_sum[...] + gained
            if c == chunks - 1:
                send_gains()
            return
        if mode == "ffn":
            value = given["base"][at(c), :].astype(F32) + total
            given["resid_out"][at(c), :] = value
            factor = lax.rsqrt(jnp.mean(value * value, axis=-1, keepdims=True) + EPSILON)
            low = (value * factor * given["gain"][...]).astype(BF)
        else:
            upstream = total + given["add"][at(c), :]
            value = given["resid"][at(c), :]
            factor = lax.rsqrt(jnp.mean(value * value, axis=-1, keepdims=True) + EPSILON)
            normed = value * factor
            scaled = upstream * given["gain"][...]
            inner = jnp.mean(scaled * normed, axis=-1, keepdims=True)
            result = given["base"][at(c), :] + factor * (scaled - normed * inner)
            given["grad_out"][at(c), :] = result
            gained = jnp.sum(upstream * normed, axis=0, keepdims=True)
            gain_out = given["gain_out"]
            gain_out[...] = gained if c == 0 else gain_out[...] + gained
            low = result.astype(BF)
        stage[at(c), :] = low
        pltpu.make_async_copy(stage.at[at(c)], all_out.at[s, at(c)], own_sem.at[c]).start()

        @pl.when(s < S - 1)
        def _():
            ag_copy(s, c, 0, 1).start()

        @pl.when(s > 0)
        def _():
            ag_copy(s, c, 1, 1).start()

    def gain_copy(step):
        return pltpu.make_async_remote_copy(
            src_ref=gain_stage, dst_ref=given["gains_all"].at[me],
            send_sem=gain_send.at[step], recv_sem=gain_recv.at[step],
            device_id=place_of(sizes, EVERY, lax.rem(me + step, N)), device_id_type=MESH,
        )

    def own_gains():
        return pltpu.make_async_copy(gain_stage, given["gains_all"].at[me], gain_own.at[0])

    def send_gains():
        for j in range(gain_stage.shape[0]):
            gain_stage[j : j + 1, :] = gain_sum[:, j * 128 : (j + 1) * 128]
        own_gains().start()
        for step in range(1, N):
            gain_copy(step).start()

    plane = None
    if mode == "last":
        plane = Blocks(
            sizes, ((("fsdp",), 0, 0), (("fsdp",), 1, 0)), [given["gout"], given["gqkv"]],
            [plane_gout, plane_gqkv], plane_sems,
        )

    def line_copy(step):
        return pltpu.make_async_remote_copy(
            src_ref=gqkv_stage.at[lax.rem(s + step, S)], dst_ref=gqkv_line.at[s],
            send_sem=line_send.at[step], recv_sem=line_recv.at[step],
            device_id={"seq": lax.rem(s + step, S)}, device_id_type=MESH,
        )

    def plane_step():
        plane.wait()
        for z in range(S):
            total = plane_gqkv[0, z].astype(F32)
            for owner in range(1, F):
                total = total + plane_gqkv[owner, z].astype(F32)
            gqkv_stage[z] = total.astype(BF)
        for step in range(1, S):
            line_copy(step).start()
        gqkv_line[s] = gqkv_stage[s]
        half = plane_gout.shape[1] // 2
        for part_at in range(2):
            own = pl.ds(part_at * half, half)
            total = plane_gout[0, own].astype(F32)
            for owner in range(1, F):
                total = total + plane_gout[owner, own].astype(F32)
            given["gout_out"][own, :] = total

    def columns_step():
        for step in range(1, S):
            line_copy(step).wait()
        result = given["gqkv_out"]
        q_width, kv = QH * HD // S, KH * HD // S
        for z in range(S):
            block = gqkv_line[z].astype(F32)
            result[:, z * q_width : (z + 1) * q_width] = block[:, :q_width]
            key_at = S * q_width + z * kv
            result[:, key_at : key_at + kv] = block[:, q_width : q_width + kv]
            value_at = S * (q_width + kv) + z * kv
            result[:, value_at : value_at + kv] = block[:, q_width + kv :]

    def relay_step(c, hop):
        @pl.when(s >= hop)
        def _():
            ag_copy(s - hop, c, 0, hop).wait_recv()
            if hop < S - 1:
                @pl.when(s < S - 1)
                def _():
                    ag_copy(s - hop, c, 0, hop + 1).start()

        @pl.when(s < S - hop)
        def _():
            ag_copy(s + hop, c, 1, hop).wait_recv()
            if hop < S - 1:
                @pl.when(s > 0)
                def _():
                    ag_copy(s + hop, c, 1, hop + 1).start()

    steps = chunks * parts
    ahead = min(steps, AHEAD if gather else steps)
    for c in range(ahead):
        end_step(c)
    blocks.start()
    if plane:
        plane.start()
    hops = S - 1 if gather else 0
    plane_at = steps - 3
    for t in range(steps + 1 + hops):
        if t < steps:
            middle_step(t)
        if t + ahead < steps:
            end_step(t + ahead)
        if 0 <= t - 1 < steps:
            final_step(t - 1)
        for hop in range(1, hops + 1):
            if 0 <= t - 1 - hop < steps:
                relay_step(t - 1 - hop, hop)
        if widen:
            widen.turn()
        if plane and t == plane_at:
            plane_step()

    for c in range(steps):
        for d in range(S - 1, 0, -1):
            @pl.when(d > s)
            def _():
                rs_copy(d, c, 0, mine(d, c)).wait_send()
        for d in range(S - 1):
            @pl.when(d < s)
            def _():
                rs_copy(d, c, 1, mine(d, c)).wait_send()
        if gather:
            pltpu.make_async_copy(stage.at[at(c)], all_out.at[s, at(c)], own_sem.at[c]).wait()
            for hop in range(1, S):
                @pl.when((s < S - 1) & (s >= hop - 1))
                def _():
                    ag_copy(s, c, 0, hop).wait_send()

                @pl.when((s > 0) & (s <= S - hop))
                def _():
                    ag_copy(s, c, 1, hop).wait_send()
    if mode == "last":
        columns_step()
        own_gains().wait()
        for step in range(1, N):
            gain_copy(step).wait()
    if widen:
        widen.wait()
    blocks.wait()


def line(mode, sizes, parts, others, extras, specs, collective_id, chunks=8, widened=()):
    S = sizes["seq"]
    _, rows, width = parts[0].shape
    full = jax.ShapeDtypeStruct((rows, width), F32)
    everyone = jax.ShapeDtypeStruct((S, rows, width), BF)
    steps = chunks * len(parts)
    scratch = [pltpu.VMEM((len(parts), S, rows, width), BF)] * 2
    in_specs = [VM] * (len(parts) + len(others))
    sems = [DMA((2, S, steps)), DMA((2, S, steps))]
    if mode == "ffn":
        outs, out_specs = [full, everyone], [VM, ANY]
    elif mode == "grad":
        outs, out_specs = [full, jax.ShapeDtypeStruct((1, width), F32), everyone], [VM, VM, ANY]
    else:
        gout, gqkv = others[-2:]
        owned = gqkv.shape[2:]
        outs = [
            full,
            jax.ShapeDtypeStruct((rows, width), BF),
            jax.ShapeDtypeStruct((S * sizes["fsdp"], width // 128, 128), F32),
            jax.ShapeDtypeStruct(gout.shape[1:], F32),
            jax.ShapeDtypeStruct((owned[0], owned[1] * S), F32),
        ]
        out_specs = [VM, VM, ANY, VM, VM]
        N = S * sizes["fsdp"]
        scratch += [pltpu.VMEM((1, width), F32), pltpu.VMEM((width // 128, 128), F32)]
        scratch += [DMA((N,)), DMA((N,)), DMA((1,))]
        scratch += [
            pltpu.VMEM(gout.shape, BF),
            pltpu.VMEM((sizes["fsdp"], S) + owned, BF),
            pltpu.VMEM((S,) + owned, BF),
            pltpu.VMEM((S,) + owned, BF),
            DMA((S,)),
            DMA((S,)),
        ]
        scratch += block_scratch(sizes, [gout, gqkv], ((("fsdp",), 0, 0), (("fsdp",), 1, 0)))
        in_specs[-2:] = [ANY, ANY]
        in_specs[-3] = pl.BlockSpec(memory_space=pltpu.SMEM)
    if mode != "last":
        scratch.append(pltpu.VMEM((rows, width), BF))
        sems += [DMA((2, chunks, S)), DMA((2, chunks, S)), DMA((chunks,))]
    return pl.pallas_call(
        functools.partial(line_kernel, sizes, chunks, mode, len(parts), specs, len(widened)),
        out_shape=outs
        + block_outs(sizes, extras, specs)
        + [jax.ShapeDtypeStruct(array.shape, F32) for array in widened],
        in_specs=in_specs + [ANY] * (len(extras) + len(widened)),
        out_specs=out_specs + [ANY] * (len(extras) + len(widened)),
        scratch_shapes=scratch + sems + widen_scratch(widened) + block_scratch(sizes, extras, specs),
        compiler_params=pltpu.CompilerParams(
            collective_id=collective_id, has_side_effects=True, vmem_limit_bytes=56 << 20
        ),
        name=f"line_{mode}",
    )(*parts, *others, *extras, *widened)


def turn(values, cosine, sine):
    return values * cosine + pltpu.roll(values, HD // 2, 1) * sine


def softmax_block(query, keys, first_row, length, scale):
    scores = lax.dot_general(
        query, keys, (((1,), (1,)), ((), ())), preferred_element_type=F32
    ) * scale
    row = first_row + lax.broadcasted_iota(jnp.int32, scores.shape, 0)
    column = lax.broadcasted_iota(jnp.int32, scores.shape, 1)
    scores = jnp.where((column <= row) & (column < length), scores, MASKED)
    peak = jnp.max(scores, axis=-1, keepdims=True)
    weights = jnp.exp(scores - peak)
    return weights * (1.0 / jnp.sum(weights, axis=-1, keepdims=True))


def tiles(width, step, body):
    @pl.loop(0, width // step)
    def _(n):
        body(pl.ds(pl.multiple_of(n * step, step), step))


def attend_kernel(sizes, heads, blocks, specs, *refs):
    count = len(specs)
    length_ref, tok_ref, gain_ref, wq_ref, cos_ref, sin_ref, gains_ref, wo_ref = refs[:8]
    sources = refs[8 : 8 + count]
    attn_ref, proj_ref, low_ref, out_ref, part_ref = refs[8 + count : 13 + count]
    results = refs[13 + count : 13 + 2 * count]
    k_all, v_all, *sems = refs[13 + 2 * count :]
    step = pl.program_id(0)

    @pl.when(step == 0)
    def _():
        greet(sizes)()
        Blocks(sizes, specs, sources, results, sems).start()

    rows, width = proj_ref.shape
    length = length_ref[0]
    cosine = cos_ref[...]
    sine = sin_ref[...]
    q_gain = gains_ref[0:1, :]
    k_gain = gains_ref[1:2, :]
    scale = HD ** (-0.5)
    value = tok_ref[...].astype(F32)
    factor = lax.rsqrt(jnp.mean(value * value, axis=-1, keepdims=True) + EPSILON)
    attn_ref[...] = (value * factor * gain_ref[...]).astype(BF)

    def project(at):
        proj_ref[:, at] = jnp.dot(attn_ref[...], wq_ref[:, at], preferred_element_type=F32)

    tiles(width, 256, project)

    def normed(raw, gain):
        factor = lax.rsqrt(jnp.mean(raw * raw, axis=-1, keepdims=True) + EPSILON)
        return turn(raw * factor * gain, cosine, sine).astype(BF)

    key = normed(proj_ref[:, heads * HD : (heads + 1) * HD], k_gain)
    value_low = proj_ref[:, (heads + 1) * HD :].astype(BF)
    low_ref[:, heads * HD : (heads + 1) * HD] = key
    low_ref[:, (heads + 1) * HD :] = value_low
    here = pl.ds(pl.multiple_of(step * rows, rows), rows)
    k_all[here, :] = key
    v_all[here, :] = value_low
    for block in range(blocks):
        @pl.when(step == block)
        def _():
            reach = (block + 1) * rows

            def one(column):
                query = normed(proj_ref[:, column], q_gain)
                low_ref[:, column] = query
                probs = softmax_block(query, k_all[:reach, :], block * rows, length, scale)
                mixed = jnp.dot(probs.astype(BF), v_all[:reach, :], preferred_element_type=F32)
                out_ref[:, column] = mixed.astype(BF)

            tiles(heads * HD, HD, one)

    def leave(at):
        part_ref[:, at] = jnp.dot(
            out_ref[...], wo_ref[:, at], preferred_element_type=F32
        ).astype(BF)

    tiles(part_ref.shape[1], 256, leave)

    @pl.when(step == blocks - 1)
    def _():
        Blocks(sizes, specs, sources, results, sems).wait()


def attend(
    length, tokens, gain, w_proj, cosine, sine, gains, w_out, heads, extras, specs, sizes,
    collective_id, blocks=4,
):
    total, width = tokens.shape
    own_width = w_proj.shape[1]
    rows = total // blocks
    q_width = heads * HD

    def by_rows(columns):
        return pl.BlockSpec((rows, columns), lambda i: (i, 0))

    def whole(array):
        return pl.BlockSpec(array.shape, lambda i: (0, 0), pipeline_mode=pl.Buffered(1))

    return pl.pallas_call(
        functools.partial(attend_kernel, sizes, heads, blocks, specs),
        grid=(blocks,),
        out_shape=[
            jax.ShapeDtypeStruct((total, width), BF),
            jax.ShapeDtypeStruct((total, own_width), F32),
            jax.ShapeDtypeStruct((total, own_width), BF),
            jax.ShapeDtypeStruct((total, q_width), BF),
            jax.ShapeDtypeStruct((total, width), BF),
        ] + block_outs(sizes, extras, specs),
        in_specs=[
            pl.BlockSpec(memory_space=pltpu.SMEM),
            by_rows(width),
            whole(gain),
            whole(w_proj),
            by_rows(HD),
            by_rows(HD),
            whole(gains),
            whole(w_out),
        ] + [ANY] * len(extras),
        out_specs=[by_rows(width), by_rows(own_width), by_rows(own_width), by_rows(q_width), by_rows(width)]
        + [ANY] * len(extras),
        scratch_shapes=[pltpu.VMEM((total, HD), BF), pltpu.VMEM((total, HD), BF)]
        + block_scratch(sizes, extras, specs),
        compiler_params=pltpu.CompilerParams(
            collective_id=collective_id, has_side_effects=True, vmem_limit_bytes=58 << 20
        ),
        name="attend",
    )(length, tokens, gain, w_proj, cosine, sine, gains, w_out, *extras)


def attend_back_kernel(sizes, heads, blocks, specs, *refs):
    count = len(specs)
    length_ref, proj_ref, low_ref, kv_ref, grad_ref, wo_ref, wq_ref, cos_ref, sin_ref, gains_ref = refs[:10]
    sources = refs[10 : 10 + count]
    out_ref, part_ref, gains_out = refs[10 + count : 13 + count]
    results = refs[13 + count : 13 + 2 * count]
    gk_all, gv_all, go_ref, *sems = refs[13 + 2 * count :]
    step = pl.program_id(0)
    rows = proj_ref.shape[0]
    length = length_ref[0]
    cosine = cos_ref[...]
    sine = sin_ref[...]
    q_gain = gains_ref[0:1, :]
    k_gain = gains_ref[1:2, :]
    scale = HD ** (-0.5)
    block_at = blocks - 1 - step

    def back(raw, gain, grad):
        grad = turn(grad, cosine, -sine)
        factor = lax.rsqrt(jnp.mean(raw * raw, axis=-1, keepdims=True) + EPSILON)
        unit = raw * factor
        scaled = grad * gain
        inner = jnp.mean(scaled * unit, axis=-1, keepdims=True)
        return factor * (scaled - unit * inner), jnp.sum(grad * unit, axis=0, keepdims=True)

    @pl.when(step == 0)
    def _():
        greet(sizes)()
        Blocks(sizes, specs, sources, results, sems).start()
        gk_all[...] = jnp.zeros_like(gk_all)
        gv_all[...] = jnp.zeros_like(gv_all)
        gains_out[...] = jnp.zeros_like(gains_out)

    def arrive(at):
        go_ref[:, at] = lax.dot_general(
            grad_ref[...], wo_ref[at, :], (((1,), (1,)), ((), ())), preferred_element_type=F32
        ).astype(BF)

    tiles(heads * HD, 256, arrive)
    for block in range(blocks):
        @pl.when(block_at == block)
        def _():
            reach = (block + 1) * rows
            keys = kv_ref[:reach, :HD]
            values = kv_ref[:reach, HD:]

            def one(column):
                query = low_ref[:, column]
                grad_o = go_ref[:, column]
                probs = softmax_block(query, keys, block * rows, length, scale)
                grad_p = lax.dot_general(
                    grad_o, values, (((1,), (1,)), ((), ())), preferred_element_type=F32
                )
                inner = jnp.sum(probs * grad_p, axis=-1, keepdims=True)
                grad_s = (probs * (grad_p - inner)).astype(BF)
                grad_q = jnp.dot(grad_s, keys, preferred_element_type=F32) * scale
                gk_all[:reach, :] += lax.dot_general(
                    grad_s, query, (((0,), (0,)), ((), ())), preferred_element_type=F32
                )
                gv_all[:reach, :] += lax.dot_general(
                    probs.astype(BF), grad_o, (((0,), (0,)), ((), ())), preferred_element_type=F32
                )
                grad_raw, gained = back(proj_ref[:, column], q_gain, grad_q.astype(BF).astype(F32))
                out_ref[:, column] = grad_raw.astype(BF)
                gains_out[0:1, :] += gained

            tiles(heads * HD, HD, one)

    here = pl.ds(pl.multiple_of(block_at * rows, rows), rows)
    grad_k = (gk_all[here, :] * scale).astype(BF).astype(F32)
    grad_raw, gained = back(proj_ref[:, heads * HD : (heads + 1) * HD], k_gain, grad_k)
    out_ref[:, heads * HD : (heads + 1) * HD] = grad_raw.astype(BF)
    out_ref[:, (heads + 1) * HD :] = gv_all[here, :].astype(BF)
    gains_out[1:2, :] += gained

    def leave(at):
        part_ref[:, at] = lax.dot_general(
            out_ref[...], wq_ref[at, :], (((1,), (1,)), ((), ())), preferred_element_type=F32
        ).astype(BF)

    tiles(part_ref.shape[1], 256, leave)

    @pl.when(step == blocks - 1)
    def _():
        Blocks(sizes, specs, sources, results, sems).wait()


def attend_back(
    length, projected, low, grad, w_out, w_proj, cosine, sine, gains, heads, extras, specs, sizes,
    collective_id, blocks=4,
):
    total, own_width = projected.shape
    width = w_out.shape[1]
    rows = total // blocks
    q_width = heads * HD

    def by_rows(columns):
        return pl.BlockSpec((rows, columns), lambda i: (blocks - 1 - i, 0))

    def whole(array):
        return pl.BlockSpec(array.shape, lambda i: (0, 0), pipeline_mode=pl.Buffered(1))

    return pl.pallas_call(
        functools.partial(attend_back_kernel, sizes, heads, blocks, specs),
        grid=(blocks,),
        out_shape=[
            jax.ShapeDtypeStruct((total, own_width), BF),
            jax.ShapeDtypeStruct((total, width), BF),
            jax.ShapeDtypeStruct((2, HD), F32),
        ] + block_outs(sizes, extras, specs),
        in_specs=[
            pl.BlockSpec(memory_space=pltpu.SMEM),
            by_rows(own_width),
            by_rows(q_width),
            pl.BlockSpec((total, 2 * HD), lambda i: (0, heads // 2)),
            by_rows(width),
            whole(w_out),
            whole(w_proj),
            by_rows(HD),
            by_rows(HD),
            whole(gains),
        ] + [ANY] * len(extras),
        out_specs=[by_rows(own_width), by_rows(width), pl.BlockSpec((2, HD), lambda i: (0, 0))]
        + [ANY] * len(extras),
        scratch_shapes=[
            pltpu.VMEM((total, HD), F32),
            pltpu.VMEM((total, HD), F32),
            pltpu.VMEM((rows, q_width), BF),
        ] + block_scratch(sizes, extras, specs),
        compiler_params=pltpu.CompilerParams(
            collective_id=collective_id, has_side_effects=True, vmem_limit_bytes=58 << 20
        ),
        name="attend_back",
    )(length, projected, low, low, grad, w_out, w_proj, cosine, sine, gains, *extras)


def rms_factor(values):
    return lax.rsqrt(jnp.mean(values * values, axis=-1, keepdims=True) + EPSILON)


def dot(left, right):
    return jnp.dot(left, right, preferred_element_type=F32)


def mm(form, left, right):
    return jnp.einsum(form, left, right, preferred_element_type=F32)


def whole_columns(blocks):
    parts, rows, _ = blocks.shape
    q_width = QH * HD // parts
    kv_width = KH * HD // parts
    moved = blocks.transpose(1, 0, 2)
    return jnp.concatenate(
        [
            moved[..., :q_width].reshape(rows, -1),
            moved[..., q_width : q_width + kv_width].reshape(rows, -1),
            moved[..., q_width + kv_width :].reshape(rows, -1),
        ],
        axis=-1,
    )


def lanes(flat, lead):
    width = flat.shape[-1]
    rows = -(-width // 2048) * 16
    return jnp.pad(flat, ((0, 0), (0, rows * 128 - width))).reshape(lead, rows, 128)


def per_device(
    tokens, cotangent, lengths, routes, slots, w_qkv, w_out, w_router, norm_gains, w_gate_up, w_down
):
    tok_count = tokens.shape[1]
    width = tokens.shape[2]
    S = lax.axis_size("seq")
    F = lax.axis_size("fsdp")
    N = S * F
    sizes = {"seq": S, "fsdp": F}
    local_experts = w_gate_up.shape[0]
    own_experts = local_experts // S
    expert_count = w_router.shape[1]
    capacity = tok_count * TOPK * 5 // (4 * expert_count)
    heads = QH // S
    seq_total = tok_count * S
    q_width = heads * HD
    own_width = q_width + 2 * HD
    seq_at = lax.axis_index("seq")
    w_rows = w_qkv.shape[0]
    small = norm_gains.shape[0]
    router_size = w_router.size
    part_width = w_gate_up.shape[1]
    down_width = w_down.shape[2]
    assert KH == S and own_experts == 1

    small_send = lanes(jnp.concatenate([w_router.reshape(-1), norm_gains])[None], 1)[0]
    table = jnp.concatenate([routes[0].T, slots[0].T])
    tok_all, cot_all, table_all, w_proj, out_own, small_all = entry(
        tokens[0], cotangent[0], table, w_qkv, w_out, small_send, sizes, 1
    )
    w_proj = w_proj.reshape(width, own_width)
    out_own = out_own.reshape(q_width, width)
    small_flat = small_all.reshape(N, -1)
    full_router = small_flat[:, :router_size].reshape(width, expert_count)
    gain_values = small_flat[:, router_size : router_size + small].reshape(-1).astype(F32)
    gain_attn = gain_values[:width]
    gain_ffn = gain_values[width : 2 * width][None]
    gain_heads = gain_values[2 * width :].reshape(2, HD)

    positions = jnp.arange(seq_total, dtype=jnp.int32)
    frequency = THETA ** (-jnp.arange(HD // 2, dtype=F32) / (HD // 2))
    angles = positions.astype(F32)[:, None] * frequency[None, :]
    cosine = jnp.concatenate([jnp.cos(angles)] * 2, axis=-1)
    sine = jnp.concatenate([-jnp.sin(angles), jnp.sin(angles)], axis=-1)
    attn_low, projected, qkv_low, o_low, o_part, down_w = attend(
        lengths, tok_all.reshape(seq_total, width), gain_attn[None], w_proj, cosine, sine,
        gain_heads, out_own, heads, [w_down.reshape((S, own_experts) + w_down.shape[1:])],
        ((("seq",), 0, "columns"),), sizes, 3,
    )
    o_part = o_part.reshape(S, tok_count, width)

    expert_ids = jnp.arange(expert_count, dtype=jnp.int32)
    slot_ids = jnp.arange(capacity, dtype=jnp.int32)
    plane = (
        jnp.arange(F, dtype=jnp.int32)[:, None] * local_experts
        + seq_at * own_experts
        + jnp.arange(own_experts, dtype=jnp.int32)[None, :]
    ).reshape(-1)
    hit = table_all[:, None, :TOPK] == plane[None, :, None, None]
    plane_slots = jnp.max(jnp.where(hit, table_all[:, None, TOPK:], -1), axis=2)
    one_hot = plane_slots[:, :, None, :] == slot_ids[None, None, :, None]
    select = one_hot.astype(BF).reshape(S, F * own_experts * capacity, tok_count)
    grouped = (S, F, own_experts * capacity, width)

    cot_rows = mm("brt,btd->brd", select, cot_all).astype(BF).reshape(grouped)
    residual, ffn_all, g_rows = line(
        "ffn", sizes, [o_part], [tokens[0], gain_ffn], [cot_rows], ((("fsdp",), 1, 0),), 2
    )
    ffn_low = lax.dynamic_index_in_dim(ffn_all, seq_at, 0, keepdims=False)

    route_rows = routes[0]
    slot_rows = slots[0]
    router_scores = dot(ffn_low, full_router)
    picked = route_rows[:, :, None] == expert_ids[None, None, :]
    selected = jnp.sum(jnp.where(picked, router_scores[:, None, :], 0.0), axis=-1)
    gate_prob = jax.nn.softmax(selected, axis=-1)
    gate_table = jnp.sum(jnp.where(picked, gate_prob[:, :, None], 0.0), axis=1).T
    hit = table[None, :TOPK] == expert_ids[:, None, None]
    own_slots = jnp.max(jnp.where(hit, table[None, TOPK:], -1), axis=1)
    gate_slots = jnp.sum(
        jnp.where(
            own_slots[:, None, :] == slot_ids[None, :, None], gate_table[:, None, :], 0.0
        ),
        axis=-1,
    )
    by_device = (F, S, own_experts, capacity)

    def to_devices(values):
        return lanes(values.reshape(by_device).transpose(1, 0, 2, 3).reshape(N, -1), N)

    gate_send = to_devices(gate_slots)

    up_blocks = w_gate_up.reshape((S, own_experts) + w_gate_up.shape[1:])
    side_specs = ((("seq",), 0, 0), (EVERY, 0, 0))
    g_flat = g_rows.reshape(-1, width)
    fused = capacity % 16 == 0
    if fused:
        gate_up_w, gate_got, x_rows, through = dispatch(
            [up_blocks, gate_send], side_specs, ffn_all, g_flat, down_w[0], select, sizes, 4
        )
    else:
        ffn_rows = mm("brt,btd->brd", select, ffn_all).astype(BF).reshape(grouped)
        gate_up_w, gate_got, x_rows = exchange(
            [up_blocks, gate_send, ffn_rows], side_specs + ((("fsdp",), 1, 0),), sizes, 4
        )
        through = mm("rd,hd->rh", g_flat, down_w[0])
    row_gate = gate_got.reshape(S, F, -1)[:, :, :capacity].transpose(1, 0, 2).reshape(-1, 1)
    x_flat = x_rows.reshape(-1, width)
    moe_rows, grad_rows, grad_gu_low, gated_hidden, prob_rows = expert(
        x_flat, row_gate, through, g_flat, gate_up_w.reshape(width, 2 * FF), down_w[0], 5
    )
    prob_send = prob_rows.reshape(F, S, -1).transpose(1, 0, 2).reshape(N, -1)
    back_blocks = [grad_rows.reshape(F, S, capacity, width), lanes(prob_send, N)]
    grad_back, prob_got, up_got, down_term, *grad_part = grads(
        back_blocks, ((("fsdp",), 0, 1), (EVERY, 0, 0)), x_flat, grad_gu_low, gated_hidden, g_flat,
        select if fused else None, sizes, 6,
    )
    if fused:
        (grad_part,) = grad_part
    else:
        grad_part = mm("brt,brd->btd", select, grad_back.reshape(S, -1, width)).astype(BF)
    grad_gate_up = up_got.reshape(w_gate_up.shape).astype(F32)
    prob_slots = prob_got.reshape(S, F, -1)[:, :, :capacity].transpose(1, 0, 2)
    prob_slots = prob_slots.reshape(expert_count, capacity)


    prob_of_route = jnp.einsum(
        "tke,ec->tkc", picked.astype(F32), prob_slots, precision=lax.Precision.HIGHEST
    )
    at_slot = slot_rows[:, :, None] == slot_ids[None, None, :]
    grad_prob = jnp.sum(jnp.where(at_slot, prob_of_route, 0.0), axis=-1)
    grad_selected = gate_prob * (grad_prob - jnp.sum(gate_prob * grad_prob, axis=-1, keepdims=True))
    grad_logits = jnp.sum(jnp.where(picked, grad_selected[:, :, None], 0.0), axis=1).astype(BF)
    grad_ffn_add = mm("te,de->td", grad_logits, full_router)
    grad_router_part = mm("td,te->de", ffn_low, grad_logits)
    valid = (seq_at * tok_count + jnp.arange(tok_count, dtype=jnp.int32)) < lengths[0]
    grad_final = jnp.where(valid[:, None], cotangent[0].astype(F32), 0.0)
    grad_residual, grad_gain_ffn, grad_attn_low, moe_back = line(
        "grad", sizes, [grad_part], [grad_final, gain_ffn, residual, grad_ffn_add],
        [moe_rows.reshape(F, S, capacity, width)], ((("fsdp",), 0, 1),), 7,
    )
    grad_attn_low = grad_attn_low.reshape(seq_total, width)

    grad_proj, attn_part, grad_gain_heads, down_got = attend_back(
        lengths, projected, qkv_low, grad_attn_low, out_own, w_proj, cosine, sine, gain_heads,
        heads, [down_term[None]], ((("seq",), "columns", 0),), sizes, 9,
    )
    attn_part = attn_part.reshape(S, tok_count, width)
    grad_out_part = mm("te,td->ed", o_low, grad_attn_low).astype(BF)
    grad_qkv_part = mm("td,te->de", attn_low, grad_proj).astype(BF).reshape(S, F, w_rows, own_width)
    moe_part = mm("brt,brd->btd", select, moe_back.reshape(S, -1, width)).astype(BF)
    early_gains = jnp.concatenate(
        [jnp.zeros((width,), F32), grad_gain_ffn[0], grad_gain_heads.reshape(-1)]
    )
    small_blocks = jnp.concatenate(
        [grad_router_part.reshape(N, -1), early_gains.reshape(N, -1)], axis=1
    )
    small_rows = -(-small_blocks.shape[1] // 1024) * 8
    small_blocks = jnp.pad(small_blocks, ((0, 0), (0, small_rows * 128 - small_blocks.shape[1])))
    small_blocks = small_blocks.reshape(N, small_rows, 128)
    (
        grad_inputs, final, late_gains, grad_out, grad_qkv, small_got
    ) = line(
        "last", sizes, [attn_part, moe_part],
        [
            grad_residual, gain_attn[None], residual, tokens[0], lengths,
            grad_out_part.reshape(F, -1, width), grad_qkv_part,
        ],
        [small_blocks], ((EVERY, 0, 0),), 8,
    )
    grad_down = down_got.reshape(w_down.shape).astype(F32)
    small_sum = jnp.sum(small_got, axis=0).reshape(-1)
    grad_router = small_sum[:router_size].reshape(w_router.shape)
    late_sum = jnp.concatenate(
        [jnp.sum(late_gains, axis=0).reshape(-1), jnp.zeros((width + 2 * HD,), F32)]
    )
    device_at = seq_at * F + lax.axis_index("fsdp")
    grad_gains = small_sum[router_size : router_size + small] + lax.dynamic_slice_in_dim(
        late_sum, device_at * small, small, 0
    )
    return (
        final[None],
        grad_inputs[None],
        grad_qkv,
        grad_out,
        grad_router,
        grad_gains,
        grad_gate_up,
        grad_down,
    )


def solution(mesh):
    in_specs = (
        P("fsdp", "seq", None),
        P("fsdp", "seq", None),
        P("fsdp"),
        P("fsdp", "seq", None),
        P("fsdp", "seq", None),
        P(("seq", "fsdp"), None),
        P(("seq", "fsdp"), None),
        P(("seq", "fsdp"), None),
        P(("seq", "fsdp")),
        P("fsdp", "seq", None),
        P("fsdp", None, "seq"),
    )
    out_specs = (
        P("fsdp", "seq", None),
        P("fsdp", "seq", None),
        P(("seq", "fsdp"), None),
        P(("seq", "fsdp"), None),
        P(("seq", "fsdp"), None),
        P(("seq", "fsdp")),
        P("fsdp", "seq", None),
        P("fsdp", None, "seq"),
    )
    return jax.shard_map(
        per_device, mesh=mesh, in_specs=in_specs, out_specs=out_specs, check_vma=False
    )
```

```python
import functools

import jax
import jax.numpy as jnp
from jax import lax
from jax.experimental import pallas as pl
from jax.experimental.pallas import tpu as pltpu
from jax.sharding import PartitionSpec as P

QH = 32
KH = 4
HD = 128
FF = 768
TOPK = 8
EPSILON = 1e-06
THETA = 1000000.0
MASKED = -1e30
AHEAD = 1
CHUNKS = 16
BF = jnp.bfloat16
F32 = jnp.float32
MESH = pl.DeviceIdType.MESH
ANY = pl.BlockSpec(memory_space=pl.ANY)
VM = pl.BlockSpec(memory_space=pltpu.VMEM)
DMA = pltpu.SemaphoreType.DMA
EVERY = ("seq", "fsdp")

def index_of(sizes, axes):
    at = 0
    for axis in axes:
        at = at * sizes[axis] + lax.axis_index(axis)
    return at


def count_of(sizes, axes):
    number = 1
    for axis in axes:
        number *= sizes[axis]
    return number


def place_of(sizes, axes, at):
    if len(axes) == 1:
        return {axes[0]: at}
    return {axes[0]: at // sizes[axes[1]], axes[1]: at % sizes[axes[1]]}


def greet(sizes):
    total = count_of(sizes, EVERY)
    me = index_of(sizes, EVERY)
    barrier = pltpu.get_barrier_semaphore()
    for step in range(1, total):
        pl.semaphore_signal(
            barrier, inc=1, device_id=place_of(sizes, EVERY, lax.rem(me + step, total)),
            device_id_type=MESH,
        )
    return lambda: pl.semaphore_wait(barrier, total - 1)


def block_of(ref, dim, at, total):
    if dim is None:
        return ref
    if dim == "columns":
        width = ref.shape[-1] // total
        return ref.at[:, :, pl.ds(pl.multiple_of(at * width, 128), width)]
    return ref.at[at] if dim == 0 else ref.at[:, at]


class Blocks:
    def __init__(self, sizes, specs, sources, results, sems):
        self.own, self.parted = [], []
        if not specs:
            return
        send_sem, recv_sem, own_sem, *stages = sems
        for i, (axes, before, after) in enumerate(specs):
            me = index_of(sizes, axes)
            total = count_of(sizes, axes)
            source = block_of(sources[i], before, me, total)
            result = block_of(results[i], after, me, total)
            self.own.append(
                (
                    pltpu.make_async_copy(source, stages[i], own_sem.at[i, 0]),
                    pltpu.make_async_copy(stages[i], result, own_sem.at[i, 1]),
                )
            )
            self.parted.append([])
            for step in range(1, total):
                target = lax.rem(me + step, total)
                self.parted[-1].append(
                    pltpu.make_async_remote_copy(
                        src_ref=block_of(sources[i], before, target, total),
                        dst_ref=block_of(results[i], after, me, total),
                        send_sem=send_sem.at[i, step],
                        recv_sem=recv_sem.at[i, step],
                        device_id=place_of(sizes, axes, target),
                        device_id_type=MESH,
                    )
                )

    def start(self):
        for copies in self.parted:
            for copy in copies:
                copy.start()
        for inward, _ in self.own:
            inward.start()

    def wait(self):
        for i in range(len(self.own)):
            self.wait_one(i)

    def wait_one(self, i):
        inward, outward = self.own[i]
        inward.wait()
        outward.start()
        outward.wait()
        for copy in self.parted[i]:
            copy.wait()


def block_scratch(sizes, arrays, specs):
    if not specs:
        return []
    total = max(count_of(sizes, axes) for axes, _, _ in specs)
    stages = []
    for array, (axes, before, after) in zip(arrays, specs):
        shape = list(array.shape)
        if before == "columns":
            shape[-1] //= count_of(sizes, axes)
        elif before is not None:
            del shape[before]
        stages.append(pltpu.VMEM(tuple(shape), array.dtype))
    count = len(specs)
    return [DMA((count, total)), DMA((count, total)), DMA((count, 2))] + stages


def block_outs(sizes, arrays, specs):
    outs = []
    for array, (axes, before, after) in zip(arrays, specs):
        shape = list(array.shape)
        total = count_of(sizes, axes)
        if before is None:
            shape = [total] + shape
        elif before == "columns":
            shape = [total, shape[0], shape[1], shape[2] // total]
        elif after == "columns":
            shape = [shape[1], shape[2], shape[3] * total]
        elif before != after:
            shape[0], shape[1] = shape[1], shape[0]
        outs.append(jax.ShapeDtypeStruct(tuple(shape), array.dtype))
    return outs


def exchange_kernel(sizes, specs, *refs):
    count = len(specs)
    met = greet(sizes)
    blocks = Blocks(sizes, specs, refs[:count], refs[count : 2 * count], refs[2 * count :])
    met()
    blocks.start()
    blocks.wait()


def exchange(arrays, specs, sizes, collective_id):
    count = len(arrays)
    return pl.pallas_call(
        functools.partial(exchange_kernel, sizes, specs),
        out_shape=block_outs(sizes, arrays, specs),
        in_specs=[ANY] * count,
        out_specs=[ANY] * count,
        scratch_shapes=block_scratch(sizes, arrays, specs),
        compiler_params=pltpu.CompilerParams(collective_id=collective_id, has_side_effects=True),
        name=f"exchange_{collective_id}",
    )(*arrays)


def entry_kernel(
    sizes, tok_ref, cot_ref, table_ref, wqkv_ref, wout_ref, small_ref,
    tok_out, cot_out, table_out, wq_out, wo_out, small_out,
    tok_send, tok_recv, tab_send, tab_recv, wq_zsend, wq_zrecv,
    pl_send, pl_recv, sib_send, sib_recv, sm_send, sm_recv, own_sem, *stages,
):
    S, F = sizes["seq"], sizes["fsdp"]
    s = lax.axis_index("seq")
    f = lax.axis_index("fsdp")
    N = S * F
    chips = F // 2
    me = s * F + f
    other = f + 1 - 2 * lax.rem(f, 2)
    rows = tok_ref.shape[0]
    chunks = tok_recv.shape[2]
    span = rows // chunks
    met = greet(sizes)
    kv = KH * HD // S
    q_width = QH * HD // S
    starts = (0, q_width * S, (q_width + kv) * S)
    widths = (q_width, kv, kv)
    offsets = (0, q_width, q_width + kv)

    def columns(z, p):
        return pl.ds(pl.multiple_of(starts[p] + z * widths[p], 128), widths[p])

    pairs = [
        (wqkv_ref.at[:, columns(s, p)], wq_out.at[s, f, :, pl.ds(offsets[p], widths[p])])
        for p in range(3)
    ] + [
        (wout_ref, wo_out.at[f]),
        (tok_ref, tok_out.at[s]),
        (cot_ref, cot_out.at[s]),
        (table_ref, table_out.at[s]),
        (small_ref, small_out.at[me]),
    ]
    inward = [
        pltpu.make_async_copy(source, stages[i], own_sem.at[i, 0])
        for i, (source, _) in enumerate(pairs)
    ]
    outward = [
        pltpu.make_async_copy(stages[i], result, own_sem.at[i, 1])
        for i, (_, result) in enumerate(pairs)
    ]
    for copy in inward:
        copy.start()
    met()

    def remote(src, dst, send_sem, recv_sem, where):
        return pltpu.make_async_remote_copy(
            src_ref=src, dst_ref=dst, send_sem=send_sem, recv_sem=recv_sem,
            device_id=where, device_id_type=MESH,
        )

    wq_line = []
    tables = []
    for step in range(1, S):
        target = lax.rem(s + step, S)
        for p in range(3):
            copy = remote(
                wqkv_ref.at[:, columns(target, p)],
                wq_out.at[s, f, :, pl.ds(offsets[p], widths[p])],
                wq_zsend.at[step, p], wq_zrecv.at[step, p], {"seq": target},
            )
            copy.start()
            wq_line.append(copy)
        copy = remote(
            table_ref, table_out.at[s], tab_send.at[step], tab_recv.at[step], {"seq": target}
        )
        copy.start()
        tables.append(copy)

    def along(a, block, c, way, hop):
        source, result = ((tok_ref, tok_out), (cot_ref, cot_out))[a]
        here = result.at[block, pl.ds(c * span, span)]
        src = source.at[pl.ds(c * span, span)] if hop == 1 else here
        return remote(
            src, here, tok_send.at[a, way, c, hop], tok_recv.at[a, way, c, hop],
            {"seq": s + 1 if way == 0 else s - 1},
        )

    def depart(a):
        for c in range(chunks):
            @pl.when(s < S - 1)
            def _():
                along(a, s, c, 0, 1).start()

            @pl.when(s > 0)
            def _():
                along(a, s, c, 1, 1).start()

    def relay(a, hop):
        for c in range(chunks):
            @pl.when(s >= hop)
            def _():
                along(a, s - hop, c, 0, hop).wait_recv()
                if hop < S - 1:
                    @pl.when(s < S - 1)
                    def _():
                        along(a, s - hop, c, 0, hop + 1).start()

            @pl.when(s < S - hop)
            def _():
                along(a, s + hop, c, 1, hop).wait_recv()
                if hop < S - 1:
                    @pl.when(s > 0)
                    def _():
                        along(a, s + hop, c, 1, hop + 1).start()

    depart(0)

    def plane_block(slot, owner):
        if slot == S:
            return wo_out.at[owner]
        return wq_out.at[lax.rem(s - slot + S, S), owner]

    def to_chip(slot, step):
        block = plane_block(slot, f)
        return remote(block, block, pl_send.at[slot, step], pl_recv.at[slot, step],
                      {"fsdp": lax.rem(f + 2 * step, F)})

    def to_other(slot, step):
        block = plane_block(slot, lax.rem(f - 2 * step + F, F))
        return remote(block, block, sib_send.at[slot, step], sib_recv.at[slot, step],
                      {"fsdp": other})

    def spread(slot):
        for step in range(1, chips):
            to_chip(slot, step).start()
        to_other(slot, 0).start()

    def forward(slot):
        for step in range(1, chips):
            to_chip(slot, step).wait_recv()
            to_other(slot, step).start()

    smalls = []
    for step in range(1, N):
        target = lax.rem(me + step, N)
        copy = remote(small_ref, small_out.at[me], sm_send.at[step], sm_recv.at[step],
                      place_of(sizes, EVERY, target))
        copy.start()
        smalls.append(copy)
    for i, copy in enumerate(inward):
        copy.wait()
        outward[i].start()
    for copy in outward[:3]:
        copy.wait()
    spread(0)
    outward[3].wait()
    spread(S)
    relay(0, 1)
    depart(1)
    for step in range(1, S):
        for p in range(3):
            wq_line[(step - 1) * 3 + p].wait()
        spread(step)
    for hop in range(2, S):
        relay(0, hop)
        relay(1, hop - 1)
    for slot in range(S + 1):
        forward(slot)
    relay(1, S - 1)
    for a in range(2):
        for hop in range(1, S):
            for c in range(chunks):
                @pl.when((s < S - 1) & (s >= hop - 1))
                def _():
                    along(a, s, c, 0, hop).wait_send()

                @pl.when((s > 0) & (s <= S - hop))
                def _():
                    along(a, s, c, 1, hop).wait_send()
    for copy in outward[4:]:
        copy.wait()
    for slot in range(S + 1):
        for step in range(1, chips):
            to_chip(slot, step).wait_send()
        for step in range(chips):
            to_other(slot, step).wait_send()
            block = plane_block(slot, lax.rem(other - 2 * step + F, F))
            remote(block, block, sib_send.at[slot, step], sib_recv.at[slot, step],
                   {"fsdp": other}).wait_recv()
    for copy in tables + smalls:
        copy.wait()


def entry(tokens, cotangent, table, w_qkv, w_out, small, sizes, collective_id, chunks=4):
    S, F = sizes["seq"], sizes["fsdp"]
    own_width = w_qkv.shape[1] // S
    N = S * F
    line_out = jax.ShapeDtypeStruct((S,) + tokens.shape, tokens.dtype)
    q_width, kv = QH * HD // S, KH * HD // S
    stages = [
        pltpu.VMEM(shape, dtype)
        for shape, dtype in [
            ((w_qkv.shape[0], q_width), BF),
            ((w_qkv.shape[0], kv), BF),
            ((w_qkv.shape[0], kv), BF),
            (w_out.shape, BF),
            (tokens.shape, BF),
            (cotangent.shape, BF),
            (table.shape, table.dtype),
            (small.shape, BF),
        ]
    ]
    return pl.pallas_call(
        functools.partial(entry_kernel, sizes),
        out_shape=[
            line_out,
            line_out,
            jax.ShapeDtypeStruct((S,) + table.shape, table.dtype),
            jax.ShapeDtypeStruct((S, F, w_qkv.shape[0], own_width), w_qkv.dtype),
            jax.ShapeDtypeStruct((F,) + w_out.shape, w_out.dtype),
            jax.ShapeDtypeStruct((N,) + small.shape, small.dtype),
        ],
        in_specs=[ANY] * 6,
        out_specs=[ANY] * 6,
        scratch_shapes=[
            DMA((2, 2, chunks, S)), DMA((2, 2, chunks, S)), DMA((S,)), DMA((S,)),
            DMA((S, 3)), DMA((S, 3)), DMA((S + 1, F // 2)), DMA((S + 1, F // 2)),
            DMA((S + 1, F // 2)), DMA((S + 1, F // 2)), DMA((N,)), DMA((N,)), DMA((8, 2)),
        ] + stages,
        compiler_params=pltpu.CompilerParams(collective_id=collective_id, has_side_effects=True),
        name="entry",
    )(tokens, cotangent, table, w_qkv, w_out, small)


def grads_kernel(sizes, specs, combined, *refs):
    S = sizes["seq"]
    count = len(specs)
    refs = list(refs)

    def take(number):
        taken, refs[:number] = refs[:number], []
        return taken

    sources, (x_any, gu_any, ph_any, g_any) = take(count), take(4)
    combine = take(1) if combined else None
    results, (up_out, down_out) = take(count), take(2)
    part_out = take(1) if combined else None
    x_ref, gu_ref, ph_ref, g_ref, up_stage, down_stage = take(6)
    in_sem, up_send, up_recv, out_sem, back_sem, *sems = refs
    s = lax.axis_index("seq")
    inward = [
        pltpu.make_async_copy(source, target, in_sem.at[i])
        for i, (source, target) in enumerate(
            ((x_any, x_ref), (gu_any, gu_ref), (ph_any, ph_ref), (g_any, g_ref))
        )
    ]
    met = greet(sizes)
    for copy in inward:
        copy.start()
    blocks = Blocks(sizes, specs, sources, results, sems)
    met()
    blocks.start()
    inward[0].wait()
    inward[1].wait()
    part = up_stage.shape[1]
    over_rows = (((0,), (0,)), ((), ()))
    sent = []
    for turn_at in range(1, S + 1):
        target = lax.rem(s + turn_at, S)
        mine = pl.ds(pl.multiple_of(target * part, 128), part)
        block = up_stage.at[turn_at - 1]

        def one(at):
            block[:, at] = lax.dot_general(
                x_ref[:, mine], gu_ref[:, at], over_rows, preferred_element_type=F32
            ).astype(BF)

        tiles(gu_ref.shape[1], 256, one)
        if turn_at < S:
            copy = pltpu.make_async_remote_copy(
                src_ref=block, dst_ref=up_out.at[s],
                send_sem=up_send.at[turn_at], recv_sem=up_recv.at[turn_at],
                device_id={"seq": target}, device_id_type=MESH,
            )
        else:
            copy = pltpu.make_async_copy(block, up_out.at[s], out_sem.at[0])
        copy.start()
        sent.append(copy)
    inward[2].wait()
    inward[3].wait()

    def one_down(at):
        down_stage[:, at] = lax.dot_general(
            ph_ref[...], g_ref[:, at], over_rows, preferred_element_type=F32
        ).astype(BF)

    tiles(g_ref.shape[1], 256, one_down)
    copy = pltpu.make_async_copy(down_stage, down_out, out_sem.at[1])
    copy.start()
    sent.append(copy)
    blocks.wait_one(0)
    if combined:
        back = results[0]
        groups, slots = back.shape[1], back.shape[2]
        pieces = []
        for block_at in range(S):
            for group in range(groups):
                row = pl.ds((block_at * groups + group) * slots, slots)
                pieces.append(
                    pltpu.make_async_copy(
                        back.at[block_at, group], x_ref.at[row], back_sem.at[block_at, group]
                    )
                )
                pieces[-1].start()
        for copy in pieces:
            copy.wait()
        reach = groups * slots
        for block_at in range(S):

            def one_part(at):
                part_out[0][block_at, :, at] = lax.dot_general(
                    combine[0][block_at], x_ref[block_at * reach : (block_at + 1) * reach, at],
                    over_rows, preferred_element_type=F32,
                ).astype(BF)

            tiles(part_out[0].shape[2], 512, one_part)
    for i in range(1, count):
        blocks.wait_one(i)
    for copy in sent:
        copy.wait()


def grads(arrays, specs, rows, grad_gu, hidden, grad_out, select, sizes, collective_id):
    S = sizes["seq"]
    combined = select is not None
    groups = arrays[0].shape[0]
    part = rows.shape[1] // S
    up_block = (part, grad_gu.shape[1])
    down = (hidden.shape[1], grad_out.shape[1])
    inner = [rows, grad_gu, hidden, grad_out]
    return pl.pallas_call(
        functools.partial(grads_kernel, sizes, specs, combined),
        out_shape=block_outs(sizes, arrays, specs)
        + [jax.ShapeDtypeStruct((S,) + up_block, BF), jax.ShapeDtypeStruct(down, BF)]
        + ([jax.ShapeDtypeStruct((S, select.shape[2], rows.shape[1]), BF)] if combined else []),
        in_specs=[ANY] * (len(arrays) + 4) + [VM] * combined,
        out_specs=[ANY] * (len(arrays) + 2) + [VM] * combined,
        scratch_shapes=[pltpu.VMEM(array.shape, BF) for array in inner]
        + [pltpu.VMEM((S,) + up_block, BF), pltpu.VMEM(down, BF)]
        + [DMA((4,)), DMA((S,)), DMA((S,)), DMA((2,)), DMA((S, groups))]
        + block_scratch(sizes, arrays, specs),
        compiler_params=pltpu.CompilerParams(
            collective_id=collective_id, has_side_effects=True, vmem_limit_bytes=60 << 20
        ),
        name="grads",
    )(*arrays, *inner, *([select] if combined else []))


def dispatch_kernel(sizes, specs, *refs):
    S, F = sizes["seq"], sizes["fsdp"]
    count = len(specs)
    refs = list(refs)

    def take(number):
        taken, refs[:number] = refs[:number], []
        return taken

    sources = take(count)
    tok_any, g_any, down_any, select_ref = take(4)
    results = take(count)
    rows_out, through_out = take(2)
    tok_ref, rows_ref, g_ref, down_ref, through_ref, row_send, row_recv, own_sem, in_sem, out_sem, *sems = refs
    f = lax.axis_index("fsdp")
    slots = rows_out.shape[2]
    met = greet(sizes)
    inward = [pltpu.make_async_copy(tok_any.at[b], tok_ref.at[b], in_sem.at[b]) for b in range(S)]
    inward.append(pltpu.make_async_copy(down_any, down_ref, in_sem.at[S]))
    inward.append(pltpu.make_async_copy(g_any, g_ref, in_sem.at[S + 1]))
    for copy in inward:
        copy.start()
    blocks = Blocks(sizes, specs, sources, results, sems)
    met()
    sent = []
    for b in range(S):
        inward[b].wait()

        def one(at):
            rows_ref[b, :, at] = jnp.dot(
                select_ref[b], tok_ref[b, :, at], preferred_element_type=F32
            ).astype(BF)

        tiles(rows_ref.shape[2], 512, one)
        for step in range(1, F):
            target = lax.rem(f + step, F)
            copy = pltpu.make_async_remote_copy(
                src_ref=rows_ref.at[b, pl.ds(pl.multiple_of(target * slots, 16), slots)],
                dst_ref=rows_out.at[f, b],
                send_sem=row_send.at[b, step], recv_sem=row_recv.at[b, step],
                device_id={"fsdp": target}, device_id_type=MESH,
            )
            copy.start()
            sent.append(copy)
        copy = pltpu.make_async_copy(
            rows_ref.at[b, pl.ds(pl.multiple_of(f * slots, 16), slots)], rows_out.at[f, b], own_sem.at[b]
        )
        copy.start()
        sent.append(copy)
        if b == 0:
            blocks.start()
    inward[S].wait()
    inward[S + 1].wait()
    span = through_ref.shape[1]
    outward = []
    for n in range(g_ref.shape[0] // span):
        if n >= 2:
            outward[n - 2].wait()
        own = pl.ds(n * span, span)

        def one_through(at):
            through_ref[n % 2, :, at] = lax.dot_general(
                g_ref[own, :], down_ref[at, :], (((1,), (1,)), ((), ())), preferred_element_type=F32
            )

        tiles(through_ref.shape[2], 256, one_through)
        outward.append(pltpu.make_async_copy(through_ref.at[n % 2], through_out.at[own], out_sem.at[n % 2]))
        outward[-1].start()
    for copy in outward[-2:]:
        copy.wait()
    blocks.wait()
    for copy in sent:
        copy.wait()


def dispatch(arrays, specs, tokens, grads_in, w_down, select, sizes, collective_id):
    S, F = sizes["seq"], sizes["fsdp"]
    slots = select.shape[1] // F
    width = tokens.shape[2]
    count = grads_in.shape[0]
    hidden = w_down.shape[0]
    span = 512
    return pl.pallas_call(
        functools.partial(dispatch_kernel, sizes, specs),
        out_shape=block_outs(sizes, arrays, specs)
        + [
            jax.ShapeDtypeStruct((F, S, slots, width), BF),
            jax.ShapeDtypeStruct((count, hidden), F32),
        ],
        in_specs=[ANY] * (len(arrays) + 3) + [VM],
        out_specs=[ANY] * (len(arrays) + 2),
        scratch_shapes=[
            pltpu.VMEM(tokens.shape, BF),
            pltpu.VMEM((S, select.shape[1], width), BF),
            pltpu.VMEM(grads_in.shape, BF),
            pltpu.VMEM(w_down.shape, BF),
            pltpu.VMEM((2, span, hidden), F32),
            DMA((S, F)), DMA((S, F)), DMA((S,)), DMA((S + 2,)), DMA((2,)),
        ] + block_scratch(sizes, arrays, specs),
        compiler_params=pltpu.CompilerParams(
            collective_id=collective_id, has_side_effects=True, vmem_limit_bytes=58 << 20
        ),
        name="dispatch",
    )(*arrays, tokens, grads_in, w_down, select)


def expert_kernel(
    x_ref, gate_ref, through_ref, g_ref, up_w, down_w,
    moe_ref, back_ref, gu_ref, gated_ref, prob_ref, hidden_ref,
):
    hidden = hidden_ref.shape[1]
    width = x_ref.shape[1]
    row_gate = gate_ref[...]
    for at in range(0, hidden, 256):
        low = slice(at, at + 256)
        high = slice(hidden + at, hidden + at + 256)
        gate = jnp.dot(x_ref[...], up_w[:, low], preferred_element_type=F32)
        up = jnp.dot(x_ref[...], up_w[:, high], preferred_element_type=F32)
        sigmoid = jax.nn.sigmoid(gate)
        silu = gate * sigmoid
        value = (silu * up).astype(BF)
        hidden_ref[:, low] = value
        gated_ref[:, low] = (row_gate * value.astype(F32)).astype(BF)
        grad = (row_gate * through_ref[:, low]).astype(BF).astype(F32)
        gu_ref[:, low] = (grad * up * sigmoid * (1.0 + gate * (1.0 - sigmoid))).astype(BF)
        gu_ref[:, high] = (grad * silu).astype(BF)
    prob = jnp.zeros_like(row_gate)
    for at in range(0, width, 256):
        here = slice(at, at + 256)
        out = jnp.dot(hidden_ref[...], down_w[:, here], preferred_element_type=F32)
        out = out.astype(BF).astype(F32)
        moe_ref[:, here] = (row_gate * out).astype(BF)
        prob = prob + jnp.sum(out * g_ref[:, here].astype(F32), axis=-1, keepdims=True)
        back_ref[:, here] = lax.dot_general(
            gu_ref[...], up_w[here, :], (((1,), (1,)), ((), ())), preferred_element_type=F32
        ).astype(BF)
    prob_ref[...] = prob


def expert(x, row_gate, through, g, up_w, down_w, steps):
    count, width = x.shape
    hidden = down_w.shape[0]
    rows = count // steps

    def by_rows(columns):
        return pl.BlockSpec((rows, columns), lambda i: (i, 0))

    def whole(array):
        return pl.BlockSpec(array.shape, lambda i: (0, 0), pipeline_mode=pl.Buffered(1))

    return pl.pallas_call(
        expert_kernel,
        grid=(steps,),
        out_shape=[
            jax.ShapeDtypeStruct((count, width), BF),
            jax.ShapeDtypeStruct((count, width), BF),
            jax.ShapeDtypeStruct((count, 2 * hidden), BF),
            jax.ShapeDtypeStruct((count, hidden), BF),
            jax.ShapeDtypeStruct((count, 1), F32),
        ],
        in_specs=[by_rows(width), by_rows(1), by_rows(hidden), by_rows(width), whole(up_w), whole(down_w)],
        out_specs=[by_rows(width), by_rows(width), by_rows(2 * hidden), by_rows(hidden), by_rows(1)],
        scratch_shapes=[pltpu.VMEM((rows, hidden), BF)],
        compiler_params=pltpu.CompilerParams(vmem_limit_bytes=60 << 20),
        name="expert",
    )(x, row_gate, through, g, up_w, down_w)


def line_kernel(sizes, chunks, mode, extra, *refs):
    S, F = sizes["seq"], sizes["fsdp"]
    count = len(extra)
    names = {
        "ffn": (["base", "gain"], ["resid_out", "all_out"]),
        "grad": (["base", "gain", "resid", "add"], ["grad_out", "gain_out", "all_out"]),
        "last": (
            ["base", "gain", "resid", "inputs", "length", "gout", "gqkv"],
            ["grad_out", "low_out", "gains_all", "gout_out", "gqkv_out"],
        ),
    }[mode]
    refs = list(refs)

    def take(number):
        taken, refs[:number] = refs[:number], []
        return taken

    (part,) = take(1)
    given = dict(zip(names[0], take(len(names[0]))))
    sources = take(count)
    given.update(zip(names[1], take(len(names[1]))))
    results = take(count)
    landings = take(2)
    gather = mode != "last"
    if gather:
        stage, rs_send, rs_recv, ag_send, ag_recv, own_sem = take(6)
        all_out = given["all_out"]
    else:
        gain_sum, gain_stage, gain_send, gain_recv, gain_own = take(5)
        plane_gout, plane_gqkv, gqkv_stage, gqkv_line, line_send, line_recv = take(6)
        plane_sems = take(5)
        rs_send, rs_recv = take(2)
    s = lax.axis_index("seq")
    f = lax.axis_index("fsdp")
    me = s * F + f
    N = S * F
    steps = chunks * part.shape[0]
    rows = part.shape[2]
    span = rows // chunks
    met = greet(sizes)
    blocks = Blocks(sizes, extra, sources, results, refs)
    met()
    if mode == "grad":
        given["gain_out"][...] = jnp.zeros_like(given["gain_out"])
    if mode == "last":
        gain_sum[...] = jnp.zeros_like(gain_sum)

    def at(c):
        return pl.ds(pl.multiple_of((c % chunks) * span, span), span)

    def mine(d, c):
        return part.at[c // chunks, d, at(c)]

    def landed(way, d, c):
        return landings[way].at[c // chunks, d, at(c)]

    def rs_copy(d, c, way, src):
        return pltpu.make_async_remote_copy(
            src_ref=src, dst_ref=landed(way, d, c),
            send_sem=rs_send.at[way, d, c], recv_sem=rs_recv.at[way, d, c],
            device_id={"seq": s + 1 if way == 0 else s - 1}, device_id_type=MESH,
        )

    def ag_copy(block, c, way, hop):
        src = stage.at[at(c)] if hop == 1 else all_out.at[block, at(c)]
        return pltpu.make_async_remote_copy(
            src_ref=src, dst_ref=all_out.at[block, at(c)],
            send_sem=ag_send.at[way, c, hop], recv_sem=ag_recv.at[way, c, hop],
            device_id={"seq": s + 1 if way == 0 else s - 1}, device_id_type=MESH,
        )

    def end_step(c):
        @pl.when(s == 0)
        def _():
            for d in range(S - 1, 0, -1):
                rs_copy(d, c, 0, mine(d, c)).start()

        @pl.when(s == S - 1)
        def _():
            for d in range(S - 1):
                rs_copy(d, c, 1, mine(d, c)).start()

    def middle_step(way, c):
        for d in range(S - 1, 0, -1) if way == 0 else range(S - 1):
            @pl.when(d > s if way == 0 else d < s)
            def _():
                buffer = landed(way, d, c)
                rs_copy(d, c, way, buffer).wait_recv()
                total = buffer[...].astype(F32) + mine(d, c)[...].astype(F32)
                buffer[...] = total.astype(BF)
                rs_copy(d, c, way, buffer).start()

    def final_step(c):
        @pl.when(s > 0)
        def _():
            rs_copy(s, c, 0, mine(s, c)).wait_recv()

        @pl.when(s < S - 1)
        def _():
            rs_copy(s, c, 1, mine(s, c)).wait_recv()

        total = mine(s, c)[...].astype(F32)
        total = total + jnp.where(s > 0, landed(0, s, c)[...].astype(F32), 0.0)
        total = total + jnp.where(s < S - 1, landed(1, s, c)[...].astype(F32), 0.0)
        if mode == "last":
            @pl.when(c >= chunks)
            def _():
                row = s * rows + (c % chunks) * span
                row = row + lax.broadcasted_iota(jnp.int32, total.shape, 0)
                value = given["resid"][at(c), :] + total
                given["low_out"][at(c), :] = jnp.where(row < given["length"][0], value, 0.0).astype(BF)

            @pl.when(c < chunks)
            def _():
                value = given["inputs"][at(c), :].astype(F32)
                factor = lax.rsqrt(jnp.mean(value * value, axis=-1, keepdims=True) + EPSILON)
                normed = value * factor
                scaled = total * given["gain"][...]
                inner = jnp.mean(scaled * normed, axis=-1, keepdims=True)
                given["grad_out"][at(c), :] = given["base"][at(c), :] + factor * (scaled - normed * inner)
                gain_sum[...] += jnp.sum(total * normed, axis=0, keepdims=True)

            @pl.when(c == chunks - 1)
            def _():
                send_gains()

            return
        if mode == "ffn":
            value = given["base"][at(c), :].astype(F32) + total
            given["resid_out"][at(c), :] = value
            factor = lax.rsqrt(jnp.mean(value * value, axis=-1, keepdims=True) + EPSILON)
            low = (value * factor * given["gain"][...]).astype(BF)
        else:
            upstream = total + given["add"][at(c), :]
            value = given["resid"][at(c), :]
            factor = lax.rsqrt(jnp.mean(value * value, axis=-1, keepdims=True) + EPSILON)
            normed = value * factor
            scaled = upstream * given["gain"][...]
            inner = jnp.mean(scaled * normed, axis=-1, keepdims=True)
            result = given["base"][at(c), :] + factor * (scaled - normed * inner)
            given["grad_out"][at(c), :] = result
            given["gain_out"][...] += jnp.sum(upstream * normed, axis=0, keepdims=True)
            low = result.astype(BF)
        stage[at(c), :] = low
        pltpu.make_async_copy(stage.at[at(c)], all_out.at[s, at(c)], own_sem.at[c]).start()

        @pl.when(s < S - 1)
        def _():
            ag_copy(s, c, 0, 1).start()

        @pl.when(s > 0)
        def _():
            ag_copy(s, c, 1, 1).start()

    def gain_copy(step):
        return pltpu.make_async_remote_copy(
            src_ref=gain_stage, dst_ref=given["gains_all"].at[me],
            send_sem=gain_send.at[step], recv_sem=gain_recv.at[step],
            device_id=place_of(sizes, EVERY, lax.rem(me + step, N)), device_id_type=MESH,
        )

    def own_gains():
        return pltpu.make_async_copy(gain_stage, given["gains_all"].at[me], gain_own.at[0])

    def send_gains():
        for j in range(gain_stage.shape[0]):
            gain_stage[j : j + 1, :] = gain_sum[:, j * 128 : (j + 1) * 128]
        own_gains().start()
        for step in range(1, N):
            gain_copy(step).start()

    plane = None
    if mode == "last":
        plane = Blocks(
            sizes, ((("fsdp",), 0, 0), (("fsdp",), 1, 0)), [given["gout"], given["gqkv"]],
            [plane_gout, plane_gqkv], plane_sems,
        )

    def line_copy(step):
        return pltpu.make_async_remote_copy(
            src_ref=gqkv_stage.at[lax.rem(s + step, S)], dst_ref=gqkv_line.at[s],
            send_sem=line_send.at[step], recv_sem=line_recv.at[step],
            device_id={"seq": lax.rem(s + step, S)}, device_id_type=MESH,
        )

    def plane_step():
        plane.wait_one(1)
        for z in range(S):
            total = plane_gqkv[0, z].astype(F32)
            for owner in range(1, F):
                total = total + plane_gqkv[owner, z].astype(F32)
            gqkv_stage[z] = total.astype(BF)
        for step in range(1, S):
            line_copy(step).start()
        gqkv_line[s] = gqkv_stage[s]

    def rows_step():
        plane.wait_one(0)
        half = plane_gout.shape[1] // 2
        for part_at in range(2):
            own = pl.ds(part_at * half, half)
            total = plane_gout[0, own].astype(F32)
            for owner in range(1, F):
                total = total + plane_gout[owner, own].astype(F32)
            given["gout_out"][own, :] = total

    def columns_step():
        for step in range(1, S):
            line_copy(step).wait()
        result = given["gqkv_out"]
        q_width, kv = QH * HD // S, KH * HD // S
        for z in range(S):
            block = gqkv_line[z].astype(F32)
            result[:, z * q_width : (z + 1) * q_width] = block[:, :q_width]
            key_at = S * q_width + z * kv
            result[:, key_at : key_at + kv] = block[:, q_width : q_width + kv]
            value_at = S * (q_width + kv) + z * kv
            result[:, value_at : value_at + kv] = block[:, q_width + kv :]

    def relay_step(way, hop, c):
        block = s - hop if way == 0 else s + hop
        ag_copy(block, c, way, hop).wait_recv()
        if hop < S - 1:
            @pl.when(s < S - 1 if way == 0 else s > 0)
            def _():
                ag_copy(block, c, way, hop + 1).start()

    def final_lag(z):
        return 1 + jnp.maximum(jnp.maximum(z - 2, S - 3 - z), 0)

    ahead = min(steps, AHEAD if gather else 4)
    for c in range(ahead):
        end_step(c)
    if plane:
        plane.start()
    blocks.start()
    turns = steps + (2 * S - 2 if gather else S)

    def inside(c):
        return (c >= 0) & (c < steps)

    @pl.loop(0, turns)
    def _(t):
        for way in range(2):
            come = t - (s - 1 if way == 0 else S - 2 - s)

            @pl.when(inside(come) & ((s > 0) & (s < S - 1)))
            def _():
                middle_step(way, come)

        @pl.when(inside(t + ahead) & ((s == 0) | (s == S - 1)))
        def _():
            end_step(t + ahead)

        done = t - final_lag(s)

        @pl.when(inside(done))
        def _():
            final_step(done)

        if gather:
            for hop in range(1, S):
                for way in range(2):
                    block = s - hop if way == 0 else s + hop
                    passed = t - final_lag(block) - hop

                    @pl.when(inside(passed) & ((block >= 0) & (block < S)))
                    def _():
                        relay_step(way, hop, passed)
        else:
            @pl.when(t == steps * 13 // 16)
            def _():
                plane_step()

    if plane:
        rows_step()

    @pl.loop(0, steps)
    def _(c):
        for d in range(S - 1, 0, -1):
            @pl.when(d > s)
            def _():
                rs_copy(d, c, 0, mine(d, c)).wait_send()
        for d in range(S - 1):
            @pl.when(d < s)
            def _():
                rs_copy(d, c, 1, mine(d, c)).wait_send()
        if gather:
            pltpu.make_async_copy(stage.at[at(c)], all_out.at[s, at(c)], own_sem.at[c]).wait()
            for hop in range(1, S):
                @pl.when((s < S - 1) & (s >= hop - 1))
                def _():
                    ag_copy(s, c, 0, hop).wait_send()

                @pl.when((s > 0) & (s <= S - hop))
                def _():
                    ag_copy(s, c, 1, hop).wait_send()

    if mode == "last":
        columns_step()
        own_gains().wait()
        for step in range(1, N):
            gain_copy(step).wait()
    blocks.wait()


def line(mode, sizes, part, others, extras, specs, collective_id, chunks=CHUNKS):
    S, F = sizes["seq"], sizes["fsdp"]
    parts, _, rows, width = part.shape
    full = jax.ShapeDtypeStruct((rows, width), F32)
    everyone = jax.ShapeDtypeStruct((S, rows, width), BF)
    steps = chunks * parts
    scratch = [pltpu.VMEM((parts, S, rows, width), BF)] * 2
    in_specs = [VM] * (1 + len(others))
    sems = [DMA((2, S, steps)), DMA((2, S, steps))]
    if mode == "ffn":
        outs, out_specs = [full, everyone], [VM, ANY]
    elif mode == "grad":
        outs, out_specs = [full, jax.ShapeDtypeStruct((1, width), F32), everyone], [VM, VM, ANY]
    else:
        gout, gqkv = others[-2:]
        owned = gqkv.shape[2:]
        outs = [
            full,
            jax.ShapeDtypeStruct((rows, width), BF),
            jax.ShapeDtypeStruct((S * F, width // 128, 128), F32),
            jax.ShapeDtypeStruct(gout.shape[1:], F32),
            jax.ShapeDtypeStruct((owned[0], owned[1] * S), F32),
        ]
        out_specs = [VM, VM, ANY, VM, VM]
        N = S * F
        scratch += [pltpu.VMEM((1, width), F32), pltpu.VMEM((width // 128, 128), F32)]
        scratch += [DMA((N,)), DMA((N,)), DMA((1,))]
        scratch += [
            pltpu.VMEM(gout.shape, BF),
            pltpu.VMEM((F, S) + owned, BF),
            pltpu.VMEM((S,) + owned, BF),
            pltpu.VMEM((S,) + owned, BF),
            DMA((S,)),
            DMA((S,)),
        ]
        scratch += block_scratch(sizes, [gout, gqkv], ((("fsdp",), 0, 0), (("fsdp",), 1, 0)))
        in_specs[-2:] = [ANY, ANY]
        in_specs[-3] = pl.BlockSpec(memory_space=pltpu.SMEM)
    if mode != "last":
        scratch.append(pltpu.VMEM((rows, width), BF))
        sems += [DMA((2, chunks, S)), DMA((2, chunks, S)), DMA((chunks,))]
    return pl.pallas_call(
        functools.partial(line_kernel, sizes, chunks, mode, specs),
        out_shape=outs + block_outs(sizes, extras, specs),
        in_specs=in_specs + [ANY] * len(extras),
        out_specs=out_specs + [ANY] * len(extras),
        scratch_shapes=scratch + sems + block_scratch(sizes, extras, specs),
        compiler_params=pltpu.CompilerParams(
            collective_id=collective_id, has_side_effects=True, vmem_limit_bytes=58 << 20
        ),
        name=f"line_{mode}",
    )(part, *others, *extras)


def turn(values, cosine, sine):
    return values * cosine + pltpu.roll(values, HD // 2, 1) * sine


def softmax_block(query, keys, first_row, length, scale):
    scores = lax.dot_general(
        query, keys, (((1,), (1,)), ((), ())), preferred_element_type=F32
    ) * scale
    row = first_row + lax.broadcasted_iota(jnp.int32, scores.shape, 0)
    column = lax.broadcasted_iota(jnp.int32, scores.shape, 1)
    scores = jnp.where((column <= row) & (column < length), scores, MASKED)
    peak = jnp.max(scores, axis=-1, keepdims=True)
    weights = jnp.exp(scores - peak)
    return weights * (1.0 / jnp.sum(weights, axis=-1, keepdims=True))


def tiles(width, step, body):
    @pl.loop(0, width // step)
    def _(n):
        body(pl.ds(pl.multiple_of(n * step, step), step))


def attend_kernel(sizes, heads, blocks, specs, *refs):
    count = len(specs)
    length_ref, tok_ref, gain_ref, wq_ref, cos_ref, sin_ref, gains_ref, wo_ref = refs[:8]
    select_ref, cot_ref = refs[8:10]
    sources = refs[10 : 10 + count]
    attn_ref, proj_ref, low_ref, out_ref, part_ref, rows_ref = refs[10 + count : 16 + count]
    results = refs[16 + count : 16 + 2 * count]
    k_all, v_all, *sems = refs[16 + 2 * count :]
    step = pl.program_id(0)

    @pl.when(step == 0)
    def _():
        greet(sizes)()
        Blocks(sizes, specs, sources, results, sems).start()

    rows, width = proj_ref.shape
    length = length_ref[0]
    cosine = cos_ref[...]
    sine = sin_ref[...]
    q_gain = gains_ref[0:1, :]
    k_gain = gains_ref[1:2, :]
    scale = HD ** (-0.5)
    value = tok_ref[...].astype(F32)
    factor = lax.rsqrt(jnp.mean(value * value, axis=-1, keepdims=True) + EPSILON)
    attn_ref[...] = (value * factor * gain_ref[...]).astype(BF)

    def project(at):
        proj_ref[:, at] = jnp.dot(attn_ref[...], wq_ref[:, at], preferred_element_type=F32)

    tiles(width, 256, project)

    def normed(raw, gain):
        factor = lax.rsqrt(jnp.mean(raw * raw, axis=-1, keepdims=True) + EPSILON)
        return turn(raw * factor * gain, cosine, sine).astype(BF)

    key = normed(proj_ref[:, heads * HD : (heads + 1) * HD], k_gain)
    value_low = proj_ref[:, (heads + 1) * HD :].astype(BF)
    low_ref[:, heads * HD : (heads + 1) * HD] = key
    low_ref[:, (heads + 1) * HD :] = value_low
    here = pl.ds(pl.multiple_of(step * rows, rows), rows)
    k_all[here, :] = key
    v_all[here, :] = value_low
    for block in range(blocks):
        @pl.when(step == block)
        def _():
            reach = (block + 1) * rows

            def one(column):
                query = normed(proj_ref[:, column], q_gain)
                low_ref[:, column] = query
                probs = softmax_block(query, k_all[:reach, :], block * rows, length, scale)
                mixed = jnp.dot(probs.astype(BF), v_all[:reach, :], preferred_element_type=F32)
                out_ref[:, column] = mixed.astype(BF)

            tiles(heads * HD, HD, one)

    def leave(at):
        part_ref[:, at] = jnp.dot(
            out_ref[...], wo_ref[:, at], preferred_element_type=F32
        ).astype(BF)

    tiles(part_ref.shape[1], 256, leave)

    def pick(at):
        rows_ref[0, :, at] = jnp.dot(
            select_ref[0], cot_ref[0, :, at], preferred_element_type=F32
        ).astype(BF)

    tiles(rows_ref.shape[2], 512, pick)

    @pl.when(step == blocks - 1)
    def _():
        Blocks(sizes, specs, sources, results, sems).wait()


def attend(
    length, tokens, gain, w_proj, cosine, sine, gains, w_out, select, cot, heads, extras, specs,
    sizes, collective_id,
):
    total, width = tokens.shape
    blocks = select.shape[0]
    own_width = w_proj.shape[1]
    rows = total // blocks
    q_width = heads * HD

    def by_rows(columns):
        return pl.BlockSpec((rows, columns), lambda i: (i, 0))

    def by_block(array):
        return pl.BlockSpec((1,) + array.shape[1:], lambda i: (i, 0, 0))

    def whole(array):
        return pl.BlockSpec(array.shape, lambda i: (0, 0), pipeline_mode=pl.Buffered(1))

    return pl.pallas_call(
        functools.partial(attend_kernel, sizes, heads, blocks, specs),
        grid=(blocks,),
        out_shape=[
            jax.ShapeDtypeStruct((total, width), BF),
            jax.ShapeDtypeStruct((total, own_width), F32),
            jax.ShapeDtypeStruct((total, own_width), BF),
            jax.ShapeDtypeStruct((total, q_width), BF),
            jax.ShapeDtypeStruct((total, width), BF),
            jax.ShapeDtypeStruct(select.shape[:2] + (width,), BF),
        ] + block_outs(sizes, extras, specs),
        in_specs=[
            pl.BlockSpec(memory_space=pltpu.SMEM),
            by_rows(width),
            whole(gain),
            whole(w_proj),
            by_rows(HD),
            by_rows(HD),
            whole(gains),
            whole(w_out),
            by_block(select),
            by_block(cot),
        ] + [ANY] * len(extras),
        out_specs=[
            by_rows(width), by_rows(own_width), by_rows(own_width), by_rows(q_width), by_rows(width),
            pl.BlockSpec((1, select.shape[1], width), lambda i: (i, 0, 0)),
        ] + [ANY] * len(extras),
        scratch_shapes=[pltpu.VMEM((total, HD), BF), pltpu.VMEM((total, HD), BF)]
        + block_scratch(sizes, extras, specs),
        compiler_params=pltpu.CompilerParams(
            collective_id=collective_id, has_side_effects=True, vmem_limit_bytes=58 << 20
        ),
        name="attend",
    )(length, tokens, gain, w_proj, cosine, sine, gains, w_out, select, cot, *extras)


def attend_back_kernel(sizes, heads, blocks, specs, *refs):
    count = len(specs)
    length_ref, proj_ref, low_ref, kv_ref, grad_ref, wo_ref, wq_ref, cos_ref, sin_ref, gains_ref = refs[:10]
    select_ref, back_ref, attn_any, o_any, ga_any = refs[10:15]
    sources = refs[15 : 15 + count]
    part_ref, gains_out, gqkv_out, gout_out = refs[15 + count : 19 + count]
    results = refs[19 + count : 19 + 2 * count]
    gk_all, gv_all, go_ref, out_all, attn_all, o_all, ga_all, gqkv_stage, gout_stage, all_sem, out_sem, *sems = refs[
        19 + 2 * count :
    ]
    inward = [
        pltpu.make_async_copy(source, target, all_sem.at[i])
        for i, (source, target) in enumerate(((attn_any, attn_all), (o_any, o_all), (ga_any, ga_all)))
    ]
    step = pl.program_id(0)
    rows = proj_ref.shape[0]
    length = length_ref[0]
    cosine = cos_ref[...]
    sine = sin_ref[...]
    q_gain = gains_ref[0:1, :]
    k_gain = gains_ref[1:2, :]
    scale = HD ** (-0.5)
    block_at = blocks - 1 - step
    here = pl.ds(pl.multiple_of(block_at * rows, rows), rows)

    def back(raw, gain, grad):
        grad = turn(grad, cosine, -sine)
        factor = lax.rsqrt(jnp.mean(raw * raw, axis=-1, keepdims=True) + EPSILON)
        unit = raw * factor
        scaled = grad * gain
        inner = jnp.mean(scaled * unit, axis=-1, keepdims=True)
        return factor * (scaled - unit * inner), jnp.sum(grad * unit, axis=0, keepdims=True)

    @pl.when(step == 0)
    def _():
        greet(sizes)()
        Blocks(sizes, specs, sources, results, sems).start()
        for copy in inward:
            copy.start()
        gk_all[...] = jnp.zeros_like(gk_all)
        gv_all[...] = jnp.zeros_like(gv_all)
        gains_out[...] = jnp.zeros_like(gains_out)

    def arrive(at):
        go_ref[:, at] = lax.dot_general(
            grad_ref[...], wo_ref[at, :], (((1,), (1,)), ((), ())), preferred_element_type=F32
        ).astype(BF)

    tiles(heads * HD, 256, arrive)
    for block in range(blocks):
        @pl.when(block_at == block)
        def _():
            reach = (block + 1) * rows
            keys = kv_ref[:reach, :HD]
            values = kv_ref[:reach, HD:]

            def one(column):
                query = low_ref[:, column]
                grad_o = go_ref[:, column]
                probs = softmax_block(query, keys, block * rows, length, scale)
                grad_p = lax.dot_general(
                    grad_o, values, (((1,), (1,)), ((), ())), preferred_element_type=F32
                )
                inner = jnp.sum(probs * grad_p, axis=-1, keepdims=True)
                grad_s = (probs * (grad_p - inner)).astype(BF)
                grad_q = jnp.dot(grad_s, keys, preferred_element_type=F32) * scale
                gk_all[:reach, :] += lax.dot_general(
                    grad_s, query, (((0,), (0,)), ((), ())), preferred_element_type=F32
                )
                gv_all[:reach, :] += lax.dot_general(
                    probs.astype(BF), grad_o, (((0,), (0,)), ((), ())), preferred_element_type=F32
                )
                grad_raw, gained = back(proj_ref[:, column], q_gain, grad_q.astype(BF).astype(F32))
                out_all[here, column] = grad_raw.astype(BF)
                gains_out[0:1, :] += gained

            tiles(heads * HD, HD, one)

    grad_k = (gk_all[here, :] * scale).astype(BF).astype(F32)
    grad_raw, gained = back(proj_ref[:, heads * HD : (heads + 1) * HD], k_gain, grad_k)
    out_all[here, heads * HD : (heads + 1) * HD] = grad_raw.astype(BF)
    out_all[here, (heads + 1) * HD :] = gv_all[here, :].astype(BF)
    gains_out[1:2, :] += gained

    def leave(at):
        part_ref[0, :, at] = lax.dot_general(
            out_all[here, :], wq_ref[at, :], (((1,), (1,)), ((), ())), preferred_element_type=F32
        ).astype(BF)

    tiles(part_ref.shape[2], 256, leave)
    over_rows = (((0,), (0,)), ((), ()))

    def combine(at):
        part_ref[1, :, at] = lax.dot_general(
            select_ref[0], back_ref[0, :, at], over_rows, preferred_element_type=F32
        ).astype(BF)

    tiles(part_ref.shape[2], 512, combine)

    @pl.when(step == blocks - 1)
    def _():
        for copy in inward:
            copy.wait()
        for i, (left, right, stage, result) in enumerate(
            ((attn_all, out_all, gqkv_stage, gqkv_out), (o_all, ga_all, gout_stage, gout_out))
        ):
            span = stage.shape[1]
            sent = []
            for n in range(left.shape[1] // span):
                if n >= 2:
                    sent[n - 2].wait()
                stage[n % 2] = lax.dot_general(
                    left[:, n * span : (n + 1) * span], right[...], over_rows,
                    preferred_element_type=F32,
                ).astype(BF)
                sent.append(
                    pltpu.make_async_copy(
                        stage.at[n % 2], result.at[pl.ds(n * span, span)], out_sem.at[i, n % 2]
                    )
                )
                sent[-1].start()
            for copy in sent[-2:]:
                copy.wait()
        Blocks(sizes, specs, sources, results, sems).wait()


def attend_back(
    length, projected, low, grad, w_out, w_proj, cosine, sine, gains, select, back, attn_low, o_low,
    heads, extras, specs, sizes, collective_id,
):
    total, own_width = projected.shape
    width = w_out.shape[1]
    blocks = select.shape[0]
    span = 256
    rows = total // blocks
    q_width = heads * HD

    def by_rows(columns):
        return pl.BlockSpec((rows, columns), lambda i: (blocks - 1 - i, 0))

    def by_block(array):
        return pl.BlockSpec((1,) + array.shape[1:], lambda i: (blocks - 1 - i, 0, 0))

    def whole(array):
        return pl.BlockSpec(array.shape, lambda i: (0, 0), pipeline_mode=pl.Buffered(1))

    return pl.pallas_call(
        functools.partial(attend_back_kernel, sizes, heads, blocks, specs),
        grid=(blocks,),
        out_shape=[
            jax.ShapeDtypeStruct((2, total, width), BF),
            jax.ShapeDtypeStruct((2, HD), F32),
            jax.ShapeDtypeStruct((width, own_width), BF),
            jax.ShapeDtypeStruct((q_width, width), BF),
        ] + block_outs(sizes, extras, specs),
        in_specs=[
            pl.BlockSpec(memory_space=pltpu.SMEM),
            by_rows(own_width),
            by_rows(q_width),
            pl.BlockSpec((total, 2 * HD), lambda i: (0, heads // 2)),
            by_rows(width),
            whole(w_out),
            whole(w_proj),
            by_rows(HD),
            by_rows(HD),
            whole(gains),
            by_block(select),
            by_block(back),
        ] + [ANY] * (3 + len(extras)),
        out_specs=[
            pl.BlockSpec((2, rows, width), lambda i: (0, blocks - 1 - i, 0)),
            pl.BlockSpec((2, HD), lambda i: (0, 0)),
        ] + [ANY] * (2 + len(extras)),
        scratch_shapes=[
            pltpu.VMEM((total, HD), F32),
            pltpu.VMEM((total, HD), F32),
            pltpu.VMEM((rows, q_width), BF),
            pltpu.VMEM((total, own_width), BF),
            pltpu.VMEM((total, width), BF),
            pltpu.VMEM((total, q_width), BF),
            pltpu.VMEM((total, width), BF),
            pltpu.VMEM((2, span, own_width), BF),
            pltpu.VMEM((2, span, width), BF),
            DMA((3,)),
            DMA((2, 2)),
        ] + block_scratch(sizes, extras, specs),
        compiler_params=pltpu.CompilerParams(
            collective_id=collective_id, has_side_effects=True, vmem_limit_bytes=58 << 20
        ),
        name="attend_back",
    )(
        length, projected, low, low, grad, w_out, w_proj, cosine, sine, gains, select, back,
        attn_low, o_low, grad, *extras,
    )


def rms_factor(values):
    return lax.rsqrt(jnp.mean(values * values, axis=-1, keepdims=True) + EPSILON)


def dot(left, right):
    return jnp.dot(left, right, preferred_element_type=F32)


def mm(form, left, right):
    return jnp.einsum(form, left, right, preferred_element_type=F32)


def whole_columns(blocks):
    parts, rows, _ = blocks.shape
    q_width = QH * HD // parts
    kv_width = KH * HD // parts
    moved = blocks.transpose(1, 0, 2)
    return jnp.concatenate(
        [
            moved[..., :q_width].reshape(rows, -1),
            moved[..., q_width : q_width + kv_width].reshape(rows, -1),
            moved[..., q_width + kv_width :].reshape(rows, -1),
        ],
        axis=-1,
    )


def lanes(flat, lead):
    width = flat.shape[-1]
    rows = -(-width // 2048) * 16
    return jnp.pad(flat, ((0, 0), (0, rows * 128 - width))).reshape(lead, rows, 128)


def per_device(
    tokens, cotangent, lengths, routes, slots, w_qkv, w_out, w_router, norm_gains, w_gate_up, w_down
):
    tok_count = tokens.shape[1]
    width = tokens.shape[2]
    S = lax.axis_size("seq")
    F = lax.axis_size("fsdp")
    N = S * F
    sizes = {"seq": S, "fsdp": F}
    local_experts = w_gate_up.shape[0]
    own_experts = local_experts // S
    expert_count = w_router.shape[1]
    capacity = tok_count * TOPK * 5 // (4 * expert_count)
    heads = QH // S
    seq_total = tok_count * S
    q_width = heads * HD
    own_width = q_width + 2 * HD
    seq_at = lax.axis_index("seq")
    w_rows = w_qkv.shape[0]
    small = norm_gains.shape[0]
    router_size = w_router.size
    part_width = w_gate_up.shape[1]
    down_width = w_down.shape[2]
    assert KH == S and own_experts == 1

    small_send = lanes(jnp.concatenate([w_router.reshape(-1), norm_gains])[None], 1)[0]
    table = jnp.concatenate([routes[0].T, slots[0].T])
    tok_all, cot_all, table_all, w_proj, out_own, small_all = entry(
        tokens[0], cotangent[0], table, w_qkv, w_out, small_send, sizes, 1
    )
    w_proj = w_proj.reshape(width, own_width)
    out_own = out_own.reshape(q_width, width)
    small_flat = small_all.reshape(N, -1)
    full_router = small_flat[:, :router_size].reshape(width, expert_count)
    gain_values = small_flat[:, router_size : router_size + small].reshape(-1).astype(F32)
    gain_attn = gain_values[:width]
    gain_ffn = gain_values[width : 2 * width][None]
    gain_heads = gain_values[2 * width :].reshape(2, HD)

    positions = jnp.arange(seq_total, dtype=jnp.int32)
    frequency = THETA ** (-jnp.arange(HD // 2, dtype=F32) / (HD // 2))
    angles = positions.astype(F32)[:, None] * frequency[None, :]
    cosine = jnp.concatenate([jnp.cos(angles)] * 2, axis=-1)
    sine = jnp.concatenate([-jnp.sin(angles), jnp.sin(angles)], axis=-1)
    expert_ids = jnp.arange(expert_count, dtype=jnp.int32)
    slot_ids = jnp.arange(capacity, dtype=jnp.int32)
    plane = (
        jnp.arange(F, dtype=jnp.int32)[:, None] * local_experts
        + seq_at * own_experts
        + jnp.arange(own_experts, dtype=jnp.int32)[None, :]
    ).reshape(-1)
    hit = table_all[:, None, :TOPK] == plane[None, :, None, None]
    plane_slots = jnp.max(jnp.where(hit, table_all[:, None, TOPK:], -1), axis=2)
    one_hot = plane_slots[:, :, None, :] == slot_ids[None, None, :, None]
    select = one_hot.astype(BF).reshape(S, F * own_experts * capacity, tok_count)
    grouped = (S, F, own_experts * capacity, width)

    attn_low, projected, qkv_low, o_low, o_part, cot_rows, down_w = attend(
        lengths, tok_all.reshape(seq_total, width), gain_attn[None], w_proj, cosine, sine,
        gain_heads, out_own, select, cot_all, heads, [w_down.reshape((S, own_experts) + w_down.shape[1:])],
        ((("seq",), 0, "columns"),), sizes, 3,
    )
    o_part = o_part.reshape(1, S, tok_count, width)
    cot_rows = cot_rows.reshape(grouped)

    residual, ffn_all, g_rows = line(
        "ffn", sizes, o_part, [tokens[0], gain_ffn], [cot_rows], ((("fsdp",), 1, 0),), 2
    )
    ffn_low = lax.dynamic_index_in_dim(ffn_all, seq_at, 0, keepdims=False)

    route_rows = routes[0]
    slot_rows = slots[0]
    router_scores = dot(ffn_low, full_router)
    picked = route_rows[:, :, None] == expert_ids[None, None, :]
    selected = jnp.sum(jnp.where(picked, router_scores[:, None, :], 0.0), axis=-1)
    gate_prob = jax.nn.softmax(selected, axis=-1)
    gate_table = jnp.sum(jnp.where(picked, gate_prob[:, :, None], 0.0), axis=1).T
    hit = table[None, :TOPK] == expert_ids[:, None, None]
    own_slots = jnp.max(jnp.where(hit, table[None, TOPK:], -1), axis=1)
    gate_slots = jnp.sum(
        jnp.where(
            own_slots[:, None, :] == slot_ids[None, :, None], gate_table[:, None, :], 0.0
        ),
        axis=-1,
    )
    by_device = (F, S, own_experts, capacity)

    def to_devices(values):
        return lanes(values.reshape(by_device).transpose(1, 0, 2, 3).reshape(N, -1), N)

    gate_send = to_devices(gate_slots)

    up_blocks = w_gate_up.reshape((S, own_experts) + w_gate_up.shape[1:])
    side_specs = ((("seq",), 0, 0), (EVERY, 0, 0))
    g_flat = g_rows.reshape(-1, width)
    fused = capacity % 16 == 0
    if fused:
        gate_up_w, gate_got, x_rows, through = dispatch(
            [up_blocks, gate_send], side_specs, ffn_all, g_flat, down_w[0], select, sizes, 4
        )
    else:
        ffn_rows = mm("brt,btd->brd", select, ffn_all).astype(BF).reshape(grouped)
        gate_up_w, gate_got, x_rows = exchange(
            [up_blocks, gate_send, ffn_rows], side_specs + ((("fsdp",), 1, 0),), sizes, 4
        )
        through = mm("rd,hd->rh", g_flat, down_w[0])
    row_gate = gate_got.reshape(S, F, -1)[:, :, :capacity].transpose(1, 0, 2).reshape(-1, 1)
    x_flat = x_rows.reshape(-1, width)
    moe_rows, grad_rows, grad_gu_low, gated_hidden, prob_rows = expert(
        x_flat, row_gate, through, g_flat, gate_up_w.reshape(width, 2 * FF), down_w[0], 5
    )
    prob_send = prob_rows.reshape(F, S, -1).transpose(1, 0, 2).reshape(N, -1)
    back_blocks = [grad_rows.reshape(F, S, capacity, width), lanes(prob_send, N)]
    grad_back, prob_got, up_got, down_term, *grad_part = grads(
        back_blocks, ((("fsdp",), 0, 1), (EVERY, 0, 0)), x_flat, grad_gu_low, gated_hidden, g_flat,
        select if fused else None, sizes, 6,
    )
    if fused:
        (grad_part,) = grad_part
    else:
        grad_part = mm("brt,brd->btd", select, grad_back.reshape(S, -1, width)).astype(BF)
    grad_gate_up = up_got.reshape(w_gate_up.shape).astype(F32)
    prob_slots = prob_got.reshape(S, F, -1)[:, :, :capacity].transpose(1, 0, 2)
    prob_slots = prob_slots.reshape(expert_count, capacity)


    prob_of_route = jnp.einsum(
        "tke,ec->tkc", picked.astype(F32), prob_slots, precision=lax.Precision.HIGHEST
    )
    at_slot = slot_rows[:, :, None] == slot_ids[None, None, :]
    grad_prob = jnp.sum(jnp.where(at_slot, prob_of_route, 0.0), axis=-1)
    grad_selected = gate_prob * (grad_prob - jnp.sum(gate_prob * grad_prob, axis=-1, keepdims=True))
    grad_logits = jnp.sum(jnp.where(picked, grad_selected[:, :, None], 0.0), axis=1).astype(BF)
    grad_ffn_add = mm("te,de->td", grad_logits, full_router)
    grad_router_part = mm("td,te->de", ffn_low, grad_logits)
    valid = (seq_at * tok_count + jnp.arange(tok_count, dtype=jnp.int32)) < lengths[0]
    grad_final = jnp.where(valid[:, None], cotangent[0].astype(F32), 0.0)
    grad_residual, grad_gain_ffn, grad_attn_low, moe_back = line(
        "grad", sizes, grad_part[None], [grad_final, gain_ffn, residual, grad_ffn_add],
        [moe_rows.reshape(F, S, capacity, width)], ((("fsdp",), 0, 1),), 7,
    )
    grad_attn_low = grad_attn_low.reshape(seq_total, width)

    last_parts, grad_gain_heads, grad_qkv_part, grad_out_part, down_got = attend_back(
        lengths, projected, qkv_low, grad_attn_low, out_own, w_proj, cosine, sine, gain_heads,
        select, moe_back.reshape(S, -1, width), attn_low, o_low, heads, [down_term[None]],
        ((("seq",), "columns", 0),), sizes, 9,
    )
    grad_qkv_part = grad_qkv_part.reshape(S, F, w_rows, own_width)
    early_gains = jnp.concatenate(
        [jnp.zeros((width,), F32), grad_gain_ffn[0], grad_gain_heads.reshape(-1)]
    )
    small_blocks = jnp.concatenate(
        [grad_router_part.reshape(N, -1), early_gains.reshape(N, -1)], axis=1
    )
    small_rows = -(-small_blocks.shape[1] // 1024) * 8
    small_blocks = jnp.pad(small_blocks, ((0, 0), (0, small_rows * 128 - small_blocks.shape[1])))
    small_blocks = small_blocks.reshape(N, small_rows, 128)
    (
        grad_inputs, final, late_gains, grad_out, grad_qkv, small_got
    ) = line(
        "last", sizes, last_parts.reshape(2, S, tok_count, width),
        [
            grad_residual, gain_attn[None], residual, tokens[0], lengths,
            grad_out_part.reshape(F, -1, width), grad_qkv_part,
        ],
        [small_blocks], ((EVERY, 0, 0),), 8,
    )
    grad_down = down_got.reshape(w_down.shape).astype(F32)
    small_sum = jnp.sum(small_got, axis=0).reshape(-1)
    grad_router = small_sum[:router_size].reshape(w_router.shape)
    late_sum = jnp.concatenate(
        [jnp.sum(late_gains, axis=0).reshape(-1), jnp.zeros((width + 2 * HD,), F32)]
    )
    device_at = seq_at * F + lax.axis_index("fsdp")
    grad_gains = small_sum[router_size : router_size + small] + lax.dynamic_slice_in_dim(
        late_sum, device_at * small, small, 0
    )
    return (
        final[None],
        grad_inputs[None],
        grad_qkv,
        grad_out,
        grad_router,
        grad_gains,
        grad_gate_up,
        grad_down,
    )


def solution(mesh):
    in_specs = (
        P("fsdp", "seq", None),
        P("fsdp", "seq", None),
        P("fsdp"),
        P("fsdp", "seq", None),
        P("fsdp", "seq", None),
        P(("seq", "fsdp"), None),
        P(("seq", "fsdp"), None),
        P(("seq", "fsdp"), None),
        P(("seq", "fsdp")),
        P("fsdp", "seq", None),
        P("fsdp", None, "seq"),
    )
    out_specs = (
        P("fsdp", "seq", None),
        P("fsdp", "seq", None),
        P(("seq", "fsdp"), None),
        P(("seq", "fsdp"), None),
        P(("seq", "fsdp"), None),
        P(("seq", "fsdp")),
        P("fsdp", "seq", None),
        P("fsdp", None, "seq"),
    )
    return jax.shard_map(
        per_device, mesh=mesh, in_specs=in_specs, out_specs=out_specs, check_vma=False
    )
```

```python
import functools

import jax
import jax.numpy as jnp
from jax import lax
from jax.experimental import pallas as pl
from jax.experimental.pallas import tpu as pltpu
from jax.sharding import PartitionSpec as P

QH = 32
KH = 4
HD = 128
FF = 768
TOPK = 8
EPSILON = 1e-06
THETA = 1000000.0
MASKED = -1e30
AHEAD = 1
CHUNKS = 16
BF = jnp.bfloat16
F32 = jnp.float32
MESH = pl.DeviceIdType.MESH
ANY = pl.BlockSpec(memory_space=pl.ANY)
VM = pl.BlockSpec(memory_space=pltpu.VMEM)
DMA = pltpu.SemaphoreType.DMA
EVERY = ("seq", "fsdp")

def index_of(sizes, axes):
    at = 0
    for axis in axes:
        at = at * sizes[axis] + lax.axis_index(axis)
    return at


def count_of(sizes, axes):
    number = 1
    for axis in axes:
        number *= sizes[axis]
    return number


def place_of(sizes, axes, at):
    if len(axes) == 1:
        return {axes[0]: at}
    return {axes[0]: at // sizes[axes[1]], axes[1]: at % sizes[axes[1]]}


def greet(sizes):
    total = count_of(sizes, EVERY)
    me = index_of(sizes, EVERY)
    barrier = pltpu.get_barrier_semaphore()
    for step in range(1, total):
        pl.semaphore_signal(
            barrier, inc=1, device_id=place_of(sizes, EVERY, lax.rem(me + step, total)),
            device_id_type=MESH,
        )
    return lambda: pl.semaphore_wait(barrier, total - 1)


def block_of(ref, dim, at, total):
    if isinstance(dim, tuple):
        return ref.at[at, pl.ds(*dim)]
    if dim == "columns":
        width = ref.shape[-1] // total
        return ref.at[:, :, pl.ds(pl.multiple_of(at * width, 128), width)]
    return ref.at[at] if dim == 0 else ref.at[:, at]


class Blocks:
    def __init__(self, sizes, specs, sources, results, sems):
        self.own, self.parted = [], []
        if not specs:
            return
        send_sem, recv_sem, own_sem, *stages = sems
        for i, (axes, before, after) in enumerate(specs):
            me = index_of(sizes, axes)
            total = count_of(sizes, axes)
            source = block_of(sources[i], before, me, total)
            result = block_of(results[i], after, me, total)
            self.own.append(
                (
                    pltpu.make_async_copy(source, stages[i], own_sem.at[i, 0]),
                    pltpu.make_async_copy(stages[i], result, own_sem.at[i, 1]),
                )
            )
            self.parted.append([])
            for step in range(1, total):
                target = lax.rem(me + step, total)
                self.parted[-1].append(
                    pltpu.make_async_remote_copy(
                        src_ref=block_of(sources[i], before, target, total),
                        dst_ref=block_of(results[i], after, me, total),
                        send_sem=send_sem.at[i, step],
                        recv_sem=recv_sem.at[i, step],
                        device_id=place_of(sizes, axes, target),
                        device_id_type=MESH,
                    )
                )

    def start(self):
        for copies in self.parted:
            for copy in copies:
                copy.start()
        for inward, _ in self.own:
            inward.start()

    def wait(self):
        for i in range(len(self.own)):
            self.wait_one(i)

    def wait_one(self, i):
        inward, outward = self.own[i]
        inward.wait()
        outward.start()
        outward.wait()
        for copy in self.parted[i]:
            copy.wait()


def block_scratch(sizes, arrays, specs):
    if not specs:
        return []
    total = max(count_of(sizes, axes) for axes, _, _ in specs)
    stages = []
    for array, (axes, before, after) in zip(arrays, specs):
        shape = list(array.shape)
        if before == "columns":
            shape[-1] //= count_of(sizes, axes)
        elif isinstance(before, tuple):
            shape = [before[1]] + shape[2:]
        else:
            del shape[before]
        stages.append(pltpu.VMEM(tuple(shape), array.dtype))
    count = len(specs)
    return [DMA((count, total)), DMA((count, total)), DMA((count, 2))] + stages


def block_outs(sizes, arrays, specs):
    outs = []
    for array, (axes, before, after) in zip(arrays, specs):
        shape = list(array.shape)
        total = count_of(sizes, axes)
        if isinstance(before, tuple):
            shape = [before[1], shape[0]] + shape[2:]
        elif before == "columns":
            shape = [total, shape[0], shape[1], shape[2] // total]
        elif after == "columns":
            shape = [shape[1], shape[2], shape[3] * total]
        elif before != after:
            shape[0], shape[1] = shape[1], shape[0]
        outs.append(jax.ShapeDtypeStruct(tuple(shape), array.dtype))
    return outs


def exchange_kernel(sizes, specs, *refs):
    count = len(specs)
    met = greet(sizes)
    blocks = Blocks(sizes, specs, refs[:count], refs[count : 2 * count], refs[2 * count :])
    met()
    blocks.start()
    blocks.wait()


def exchange(arrays, specs, sizes, collective_id):
    count = len(arrays)
    return pl.pallas_call(
        functools.partial(exchange_kernel, sizes, specs),
        out_shape=block_outs(sizes, arrays, specs),
        in_specs=[ANY] * count,
        out_specs=[ANY] * count,
        scratch_shapes=block_scratch(sizes, arrays, specs),
        compiler_params=pltpu.CompilerParams(collective_id=collective_id, has_side_effects=True),
        name=f"exchange_{collective_id}",
    )(*arrays)


def entry_kernel(
    sizes, tok_ref, cot_ref, table_ref, wqkv_ref, wout_ref, small_ref,
    tok_out, cot_out, table_out, wq_out, wo_out, small_out,
    tok_send, tok_recv, tab_send, tab_recv, wq_zsend, wq_zrecv,
    pl_send, pl_recv, sib_send, sib_recv, sm_send, sm_recv, own_sem, *stages,
):
    S, F = sizes["seq"], sizes["fsdp"]
    s = lax.axis_index("seq")
    f = lax.axis_index("fsdp")
    N = S * F
    chips = F // 2
    me = s * F + f
    other = f + 1 - 2 * lax.rem(f, 2)
    rows = tok_ref.shape[0]
    chunks = tok_recv.shape[2]
    span = rows // chunks
    met = greet(sizes)
    kv = KH * HD // S
    q_width = QH * HD // S
    starts = (0, q_width * S, (q_width + kv) * S)
    widths = (q_width, kv, kv)
    offsets = (0, q_width, q_width + kv)

    def columns(z, p):
        return pl.ds(pl.multiple_of(starts[p] + z * widths[p], 128), widths[p])

    pairs = [
        (wqkv_ref.at[:, columns(s, p)], wq_out.at[s, f, :, pl.ds(offsets[p], widths[p])])
        for p in range(3)
    ] + [
        (wout_ref, wo_out.at[f]),
        (tok_ref, tok_out.at[s]),
        (cot_ref, cot_out.at[s]),
        (table_ref, table_out.at[s]),
        (small_ref, small_out.at[me]),
    ]
    inward = [
        pltpu.make_async_copy(source, stages[i], own_sem.at[i, 0])
        for i, (source, _) in enumerate(pairs)
    ]
    outward = [
        pltpu.make_async_copy(stages[i], result, own_sem.at[i, 1])
        for i, (_, result) in enumerate(pairs)
    ]
    for copy in inward:
        copy.start()
    met()

    def remote(src, dst, send_sem, recv_sem, where):
        return pltpu.make_async_remote_copy(
            src_ref=src, dst_ref=dst, send_sem=send_sem, recv_sem=recv_sem,
            device_id=where, device_id_type=MESH,
        )

    wq_line = []
    tables = []
    for step in range(1, S):
        target = lax.rem(s + step, S)
        for p in range(3):
            copy = remote(
                wqkv_ref.at[:, columns(target, p)],
                wq_out.at[s, f, :, pl.ds(offsets[p], widths[p])],
                wq_zsend.at[step, p], wq_zrecv.at[step, p], {"seq": target},
            )
            copy.start()
            wq_line.append(copy)
        copy = remote(
            table_ref, table_out.at[s], tab_send.at[step], tab_recv.at[step], {"seq": target}
        )
        copy.start()
        tables.append(copy)

    def along(a, block, c, way, hop):
        source, result = ((tok_ref, tok_out), (cot_ref, cot_out))[a]
        here = result.at[block, pl.ds(c * span, span)]
        src = source.at[pl.ds(c * span, span)] if hop == 1 else here
        return remote(
            src, here, tok_send.at[a, way, c, hop], tok_recv.at[a, way, c, hop],
            {"seq": s + 1 if way == 0 else s - 1},
        )

    def depart(a):
        for c in range(chunks):
            @pl.when(s < S - 1)
            def _():
                along(a, s, c, 0, 1).start()

            @pl.when(s > 0)
            def _():
                along(a, s, c, 1, 1).start()

    def relay(a, hop):
        for c in range(chunks):
            @pl.when(s >= hop)
            def _():
                along(a, s - hop, c, 0, hop).wait_recv()
                if hop < S - 1:
                    @pl.when(s < S - 1)
                    def _():
                        along(a, s - hop, c, 0, hop + 1).start()

            @pl.when(s < S - hop)
            def _():
                along(a, s + hop, c, 1, hop).wait_recv()
                if hop < S - 1:
                    @pl.when(s > 0)
                    def _():
                        along(a, s + hop, c, 1, hop + 1).start()

    depart(0)

    def plane_block(slot, owner):
        if slot == S:
            return wo_out.at[owner]
        return wq_out.at[lax.rem(s - slot + S, S), owner]

    def to_chip(slot, step):
        block = plane_block(slot, f)
        return remote(block, block, pl_send.at[slot, step], pl_recv.at[slot, step],
                      {"fsdp": lax.rem(f + 2 * step, F)})

    def to_other(slot, step):
        block = plane_block(slot, lax.rem(f - 2 * step + F, F))
        return remote(block, block, sib_send.at[slot, step], sib_recv.at[slot, step],
                      {"fsdp": other})

    def spread(slot):
        for step in range(1, chips):
            to_chip(slot, step).start()
        to_other(slot, 0).start()

    def forward(slot):
        for step in range(1, chips):
            to_chip(slot, step).wait_recv()
            to_other(slot, step).start()

    smalls = []
    for step in range(1, N):
        target = lax.rem(me + step, N)
        copy = remote(small_ref, small_out.at[me], sm_send.at[step], sm_recv.at[step],
                      place_of(sizes, EVERY, target))
        copy.start()
        smalls.append(copy)
    for i, copy in enumerate(inward):
        copy.wait()
        outward[i].start()
    for copy in outward[:3]:
        copy.wait()
    spread(0)
    outward[3].wait()
    spread(S)
    relay(0, 1)
    depart(1)
    for step in range(1, S):
        for p in range(3):
            wq_line[(step - 1) * 3 + p].wait()
        spread(step)
    for hop in range(2, S):
        relay(0, hop)
        relay(1, hop - 1)
    for slot in range(S + 1):
        forward(slot)
    relay(1, S - 1)
    for a in range(2):
        for hop in range(1, S):
            for c in range(chunks):
                @pl.when((s < S - 1) & (s >= hop - 1))
                def _():
                    along(a, s, c, 0, hop).wait_send()

                @pl.when((s > 0) & (s <= S - hop))
                def _():
                    along(a, s, c, 1, hop).wait_send()
    for copy in outward[4:]:
        copy.wait()
    for slot in range(S + 1):
        for step in range(1, chips):
            to_chip(slot, step).wait_send()
        for step in range(chips):
            to_other(slot, step).wait_send()
            block = plane_block(slot, lax.rem(other - 2 * step + F, F))
            remote(block, block, sib_send.at[slot, step], sib_recv.at[slot, step],
                   {"fsdp": other}).wait_recv()
    for copy in tables + smalls:
        copy.wait()


def entry(tokens, cotangent, table, w_qkv, w_out, small, sizes, collective_id, chunks=4):
    S, F = sizes["seq"], sizes["fsdp"]
    own_width = w_qkv.shape[1] // S
    N = S * F
    line_out = jax.ShapeDtypeStruct((S,) + tokens.shape, tokens.dtype)
    q_width, kv = QH * HD // S, KH * HD // S
    stages = [
        pltpu.VMEM(shape, dtype)
        for shape, dtype in [
            ((w_qkv.shape[0], q_width), BF),
            ((w_qkv.shape[0], kv), BF),
            ((w_qkv.shape[0], kv), BF),
            (w_out.shape, BF),
            (tokens.shape, BF),
            (cotangent.shape, BF),
            (table.shape, table.dtype),
            (small.shape, BF),
        ]
    ]
    return pl.pallas_call(
        functools.partial(entry_kernel, sizes),
        out_shape=[
            line_out,
            line_out,
            jax.ShapeDtypeStruct((S,) + table.shape, table.dtype),
            jax.ShapeDtypeStruct((S, F, w_qkv.shape[0], own_width), w_qkv.dtype),
            jax.ShapeDtypeStruct((F,) + w_out.shape, w_out.dtype),
            jax.ShapeDtypeStruct((N,) + small.shape, small.dtype),
        ],
        in_specs=[ANY] * 6,
        out_specs=[ANY] * 6,
        scratch_shapes=[
            DMA((2, 2, chunks, S)), DMA((2, 2, chunks, S)), DMA((S,)), DMA((S,)),
            DMA((S, 3)), DMA((S, 3)), DMA((S + 1, F // 2)), DMA((S + 1, F // 2)),
            DMA((S + 1, F // 2)), DMA((S + 1, F // 2)), DMA((N,)), DMA((N,)), DMA((8, 2)),
        ] + stages,
        compiler_params=pltpu.CompilerParams(collective_id=collective_id, has_side_effects=True),
        name="entry",
    )(tokens, cotangent, table, w_qkv, w_out, small)


def grads_kernel(sizes, specs, combined, *refs):
    S = sizes["seq"]
    count = len(specs)
    refs = list(refs)

    def take(number):
        taken, refs[:number] = refs[:number], []
        return taken

    sources, (x_any, gu_any, ph_any, g_any) = take(count), take(4)
    combine = take(1) if combined else None
    results, (up_out, down_out) = take(count), take(2)
    part_out = take(1) if combined else None
    x_ref, gu_ref, ph_ref, g_ref, up_stage, down_stage = take(6)
    in_sem, up_send, up_recv, out_sem, back_sem, *sems = refs
    s = lax.axis_index("seq")
    inward = [
        pltpu.make_async_copy(source, target, in_sem.at[i])
        for i, (source, target) in enumerate(
            ((x_any, x_ref), (gu_any, gu_ref), (ph_any, ph_ref), (g_any, g_ref))
        )
    ]
    met = greet(sizes)
    for copy in inward:
        copy.start()
    blocks = Blocks(sizes, specs, sources, results, sems)
    met()
    blocks.start()
    inward[0].wait()
    inward[1].wait()
    part = up_stage.shape[1]
    over_rows = (((0,), (0,)), ((), ()))
    sent = []
    for turn_at in range(1, S + 1):
        target = lax.rem(s + turn_at, S)
        mine = pl.ds(pl.multiple_of(target * part, 128), part)
        block = up_stage.at[turn_at - 1]

        def one(at):
            block[:, at] = lax.dot_general(
                x_ref[:, mine], gu_ref[:, at], over_rows, preferred_element_type=F32
            ).astype(BF)

        tiles(gu_ref.shape[1], 256, one)
        if turn_at < S:
            copy = pltpu.make_async_remote_copy(
                src_ref=block, dst_ref=up_out.at[s],
                send_sem=up_send.at[turn_at], recv_sem=up_recv.at[turn_at],
                device_id={"seq": target}, device_id_type=MESH,
            )
        else:
            copy = pltpu.make_async_copy(block, up_out.at[s], out_sem.at[0])
        copy.start()
        sent.append(copy)
    inward[2].wait()
    inward[3].wait()

    def one_down(at):
        down_stage[:, at] = lax.dot_general(
            ph_ref[...], g_ref[:, at], over_rows, preferred_element_type=F32
        ).astype(BF)

    tiles(g_ref.shape[1], 256, one_down)
    copy = pltpu.make_async_copy(down_stage, down_out, out_sem.at[1])
    copy.start()
    sent.append(copy)
    blocks.wait_one(0)
    if combined:
        back = results[0]
        groups, slots = back.shape[1], back.shape[2]
        pieces = []
        for block_at in range(S):
            for group in range(groups):
                row = pl.ds((block_at * groups + group) * slots, slots)
                pieces.append(
                    pltpu.make_async_copy(
                        back.at[block_at, group], x_ref.at[row], back_sem.at[block_at, group]
                    )
                )
                pieces[-1].start()
        for copy in pieces:
            copy.wait()
        reach = groups * slots
        for block_at in range(S):

            def one_part(at):
                part_out[0][block_at, :, at] = lax.dot_general(
                    combine[0][block_at], x_ref[block_at * reach : (block_at + 1) * reach, at],
                    over_rows, preferred_element_type=F32,
                ).astype(BF)

            tiles(part_out[0].shape[2], 512, one_part)
    for i in range(1, count):
        blocks.wait_one(i)
    for copy in sent:
        copy.wait()


def grads(arrays, specs, rows, grad_gu, hidden, grad_out, select, sizes, collective_id):
    S = sizes["seq"]
    combined = select is not None
    groups = arrays[0].shape[0]
    part = rows.shape[1] // S
    up_block = (part, grad_gu.shape[1])
    down = (hidden.shape[1], grad_out.shape[1])
    inner = [rows, grad_gu, hidden, grad_out]
    return pl.pallas_call(
        functools.partial(grads_kernel, sizes, specs, combined),
        out_shape=block_outs(sizes, arrays, specs)
        + [jax.ShapeDtypeStruct((S,) + up_block, BF), jax.ShapeDtypeStruct(down, BF)]
        + ([jax.ShapeDtypeStruct((S, select.shape[2], rows.shape[1]), BF)] if combined else []),
        in_specs=[ANY] * (len(arrays) + 4) + [VM] * combined,
        out_specs=[ANY] * (len(arrays) + 2) + [VM] * combined,
        scratch_shapes=[pltpu.VMEM(array.shape, BF) for array in inner]
        + [pltpu.VMEM((S,) + up_block, BF), pltpu.VMEM(down, BF)]
        + [DMA((4,)), DMA((S,)), DMA((S,)), DMA((2,)), DMA((S, groups))]
        + block_scratch(sizes, arrays, specs),
        compiler_params=pltpu.CompilerParams(
            collective_id=collective_id, has_side_effects=True, vmem_limit_bytes=60 << 20
        ),
        name="grads",
    )(*arrays, *inner, *([select] if combined else []))


def dispatch_kernel(sizes, specs, parts, *refs):
    S, F = sizes["seq"], sizes["fsdp"]
    count = len(specs)
    refs = list(refs)

    def take(number):
        taken, refs[:number] = refs[:number], []
        return taken

    sources = take(count)
    tok_any, down_any, select_ref = take(3)
    g_parts = take(parts)
    results = take(count)
    rows_out, through_out, g_out = take(3)
    tok_ref, rows_ref, g_ref, down_ref, through_ref, row_send, row_recv, own_sem, in_sem, out_sem, g_sem, *sems = refs
    f = lax.axis_index("fsdp")
    slots = rows_out.shape[2]
    met = greet(sizes)
    inward = [pltpu.make_async_copy(tok_any.at[b], tok_ref.at[b], in_sem.at[b]) for b in range(S)]
    inward.append(pltpu.make_async_copy(down_any, down_ref, in_sem.at[S]))
    b = 0
    for g_any in g_parts:
        for j in range(g_any.shape[1]):
            for group in range(F):
                row = pl.ds((group * S + b) * slots, slots)
                inward.append(
                    pltpu.make_async_copy(g_any.at[group, j], g_ref.at[row], g_sem.at[b, group])
                )
            b += 1
    whole_g = pltpu.make_async_copy(g_ref, g_out, in_sem.at[S + 1])
    for copy in inward:
        copy.start()
    blocks = Blocks(sizes, specs, sources, results, sems)
    met()
    sent = []
    for b in range(S):
        inward[b].wait()

        def one(at):
            rows_ref[b, :, at] = jnp.dot(
                select_ref[b], tok_ref[b, :, at], preferred_element_type=F32
            ).astype(BF)

        tiles(rows_ref.shape[2], 512, one)
        for step in range(1, F):
            target = lax.rem(f + step, F)
            copy = pltpu.make_async_remote_copy(
                src_ref=rows_ref.at[b, pl.ds(pl.multiple_of(target * slots, 16), slots)],
                dst_ref=rows_out.at[f, b],
                send_sem=row_send.at[b, step], recv_sem=row_recv.at[b, step],
                device_id={"fsdp": target}, device_id_type=MESH,
            )
            copy.start()
            sent.append(copy)
        copy = pltpu.make_async_copy(
            rows_ref.at[b, pl.ds(pl.multiple_of(f * slots, 16), slots)], rows_out.at[f, b], own_sem.at[b]
        )
        copy.start()
        sent.append(copy)
        if b == 0:
            blocks.start()
    for copy in inward[S:]:
        copy.wait()
    whole_g.start()
    span = through_ref.shape[1]
    outward = []
    for n in range(g_ref.shape[0] // span):
        if n >= 2:
            outward[n - 2].wait()
        own = pl.ds(n * span, span)

        def one_through(at):
            through_ref[n % 2, :, at] = lax.dot_general(
                g_ref[own, :], down_ref[at, :], (((1,), (1,)), ((), ())), preferred_element_type=F32
            )

        tiles(through_ref.shape[2], 256, one_through)
        outward.append(pltpu.make_async_copy(through_ref.at[n % 2], through_out.at[own], out_sem.at[n % 2]))
        outward[-1].start()
    for copy in outward[-2:]:
        copy.wait()
    whole_g.wait()
    blocks.wait()
    for copy in sent:
        copy.wait()


def dispatch(arrays, specs, tokens, g_parts, w_down, select, sizes, collective_id):
    S, F = sizes["seq"], sizes["fsdp"]
    slots = select.shape[1] // F
    width = tokens.shape[2]
    count = F * S * slots
    hidden = w_down.shape[0]
    span = 512
    return pl.pallas_call(
        functools.partial(dispatch_kernel, sizes, specs, len(g_parts)),
        out_shape=block_outs(sizes, arrays, specs)
        + [
            jax.ShapeDtypeStruct((F, S, slots, width), BF),
            jax.ShapeDtypeStruct((count, hidden), F32),
            jax.ShapeDtypeStruct((count, width), BF),
        ],
        in_specs=[ANY] * (len(arrays) + 2) + [VM] + [ANY] * len(g_parts),
        out_specs=[ANY] * (len(arrays) + 3),
        scratch_shapes=[
            pltpu.VMEM(tokens.shape, BF),
            pltpu.VMEM((S, select.shape[1], width), BF),
            pltpu.VMEM((count, width), BF),
            pltpu.VMEM(w_down.shape, BF),
            pltpu.VMEM((2, span, hidden), F32),
            DMA((S, F)), DMA((S, F)), DMA((S,)), DMA((S + 2,)), DMA((2,)), DMA((S, F)),
        ] + block_scratch(sizes, arrays, specs),
        compiler_params=pltpu.CompilerParams(
            collective_id=collective_id, has_side_effects=True, vmem_limit_bytes=58 << 20
        ),
        name="dispatch",
    )(*arrays, tokens, w_down, select, *g_parts)


def expert_kernel(
    x_ref, gate_ref, through_ref, g_ref, up_w, down_w,
    moe_ref, back_ref, gu_ref, gated_ref, prob_ref, hidden_ref,
):
    hidden = hidden_ref.shape[1]
    width = x_ref.shape[1]
    row_gate = gate_ref[...]
    for at in range(0, hidden, 256):
        low = slice(at, at + 256)
        high = slice(hidden + at, hidden + at + 256)
        gate = jnp.dot(x_ref[...], up_w[:, low], preferred_element_type=F32)
        up = jnp.dot(x_ref[...], up_w[:, high], preferred_element_type=F32)
        sigmoid = jax.nn.sigmoid(gate)
        silu = gate * sigmoid
        value = (silu * up).astype(BF)
        hidden_ref[:, low] = value
        gated_ref[:, low] = (row_gate * value.astype(F32)).astype(BF)
        grad = (row_gate * through_ref[:, low]).astype(BF).astype(F32)
        gu_ref[:, low] = (grad * up * sigmoid * (1.0 + gate * (1.0 - sigmoid))).astype(BF)
        gu_ref[:, high] = (grad * silu).astype(BF)
    prob = jnp.zeros_like(row_gate)
    for at in range(0, width, 256):
        here = slice(at, at + 256)
        out = jnp.dot(hidden_ref[...], down_w[:, here], preferred_element_type=F32)
        out = out.astype(BF).astype(F32)
        moe_ref[:, here] = (row_gate * out).astype(BF)
        prob = prob + jnp.sum(out * g_ref[:, here].astype(F32), axis=-1, keepdims=True)
        back_ref[:, here] = lax.dot_general(
            gu_ref[...], up_w[here, :], (((1,), (1,)), ((), ())), preferred_element_type=F32
        ).astype(BF)
    prob_ref[...] = prob


def expert(x, row_gate, through, g, up_w, down_w, steps):
    count, width = x.shape
    hidden = down_w.shape[0]
    rows = count // steps

    def by_rows(columns):
        return pl.BlockSpec((rows, columns), lambda i: (i, 0))

    def whole(array):
        return pl.BlockSpec(array.shape, lambda i: (0, 0), pipeline_mode=pl.Buffered(1))

    return pl.pallas_call(
        expert_kernel,
        grid=(steps,),
        out_shape=[
            jax.ShapeDtypeStruct((count, width), BF),
            jax.ShapeDtypeStruct((count, width), BF),
            jax.ShapeDtypeStruct((count, 2 * hidden), BF),
            jax.ShapeDtypeStruct((count, hidden), BF),
            jax.ShapeDtypeStruct((count, 1), F32),
        ],
        in_specs=[by_rows(width), by_rows(1), by_rows(hidden), by_rows(width), whole(up_w), whole(down_w)],
        out_specs=[by_rows(width), by_rows(width), by_rows(2 * hidden), by_rows(hidden), by_rows(1)],
        scratch_shapes=[pltpu.VMEM((rows, hidden), BF)],
        compiler_params=pltpu.CompilerParams(vmem_limit_bytes=60 << 20),
        name="expert",
    )(x, row_gate, through, g, up_w, down_w)


def line_kernel(sizes, chunks, mode, extra, *refs):
    S, F = sizes["seq"], sizes["fsdp"]
    count = len(extra)
    names = {
        "ffn": (["base", "gain"], ["resid_out", "all_out"]),
        "grad": (["base", "gain", "resid", "add"], ["grad_out", "gain_out", "all_out"]),
        "last": (
            ["base", "gain", "resid", "inputs", "heads", "length", "gout", "gqkv"],
            ["grad_out", "low_out", "gains_all", "gout_out", "gqkv_out"],
        ),
    }[mode]
    refs = list(refs)

    def take(number):
        taken, refs[:number] = refs[:number], []
        return taken

    (part,) = take(1)
    given = dict(zip(names[0], take(len(names[0]))))
    sources = take(count)
    given.update(zip(names[1], take(len(names[1]))))
    results = take(count)
    landings = take(2)
    gather = mode != "last"
    if gather:
        stage, rs_send, rs_recv, ag_send, ag_recv, own_sem = take(6)
        all_out = given["all_out"]
    else:
        gain_sum, gain_stage, gain_send, gain_recv, gain_own = take(5)
        plane_gout, plane_gqkv, gqkv_stage, gqkv_line, line_send, line_recv = take(6)
        plane_sems = take(5)
        rs_send, rs_recv = take(2)
    s = lax.axis_index("seq")
    f = lax.axis_index("fsdp")
    me = s * F + f
    N = S * F
    steps = chunks * part.shape[0]
    rows = part.shape[2]
    span = rows // chunks
    met = greet(sizes)
    blocks = Blocks(sizes, extra, sources, results, refs)
    met()
    if mode == "grad":
        given["gain_out"][...] = jnp.zeros_like(given["gain_out"])
    if mode == "last":
        gain_sum[...] = jnp.zeros_like(gain_sum)

    def at(c):
        return pl.ds(pl.multiple_of((c % chunks) * span, span), span)

    def mine(d, c):
        return part.at[c // chunks, d, at(c)]

    def landed(way, d, c):
        return landings[way].at[c // chunks, d, at(c)]

    def rs_copy(d, c, way, src):
        return pltpu.make_async_remote_copy(
            src_ref=src, dst_ref=landed(way, d, c),
            send_sem=rs_send.at[way, d, c], recv_sem=rs_recv.at[way, d, c],
            device_id={"seq": s + 1 if way == 0 else s - 1}, device_id_type=MESH,
        )

    def ag_copy(block, c, way, hop):
        src = stage.at[at(c)] if hop == 1 else all_out.at[block, at(c)]
        return pltpu.make_async_remote_copy(
            src_ref=src, dst_ref=all_out.at[block, at(c)],
            send_sem=ag_send.at[way, c, hop], recv_sem=ag_recv.at[way, c, hop],
            device_id={"seq": s + 1 if way == 0 else s - 1}, device_id_type=MESH,
        )

    def end_step(c):
        @pl.when(s == 0)
        def _():
            for d in range(S - 1, 0, -1):
                rs_copy(d, c, 0, mine(d, c)).start()

        @pl.when(s == S - 1)
        def _():
            for d in range(S - 1):
                rs_copy(d, c, 1, mine(d, c)).start()

    def middle_step(way, c):
        for d in range(S - 1, 0, -1) if way == 0 else range(S - 1):
            @pl.when(d > s if way == 0 else d < s)
            def _():
                buffer = landed(way, d, c)
                rs_copy(d, c, way, buffer).wait_recv()
                total = buffer[...].astype(F32) + mine(d, c)[...].astype(F32)
                buffer[...] = total.astype(BF)
                rs_copy(d, c, way, buffer).start()

    def final_step(c):
        @pl.when(s > 0)
        def _():
            rs_copy(s, c, 0, mine(s, c)).wait_recv()

        @pl.when(s < S - 1)
        def _():
            rs_copy(s, c, 1, mine(s, c)).wait_recv()

        total = mine(s, c)[...].astype(F32)
        total = total + jnp.where(s > 0, landed(0, s, c)[...].astype(F32), 0.0)
        total = total + jnp.where(s < S - 1, landed(1, s, c)[...].astype(F32), 0.0)
        if mode == "last":
            @pl.when(c >= chunks)
            def _():
                row = s * rows + (c % chunks) * span
                row = row + lax.broadcasted_iota(jnp.int32, total.shape, 0)
                value = given["resid"][at(c), :] + total
                given["low_out"][at(c), :] = jnp.where(row < given["length"][0], value, 0.0).astype(BF)

            @pl.when(c < chunks)
            def _():
                value = given["inputs"][at(c), :].astype(F32)
                factor = lax.rsqrt(jnp.mean(value * value, axis=-1, keepdims=True) + EPSILON)
                normed = value * factor
                scaled = total * given["gain"][...]
                inner = jnp.mean(scaled * normed, axis=-1, keepdims=True)
                given["grad_out"][at(c), :] = given["base"][at(c), :] + factor * (scaled - normed * inner)
                gain_sum[...] += jnp.sum(total * normed, axis=0, keepdims=True)

            @pl.when(c == chunks - 1)
            def _():
                send_gains()

            return
        if mode == "ffn":
            value = given["base"][at(c), :].astype(F32) + total
            given["resid_out"][at(c), :] = value
            factor = lax.rsqrt(jnp.mean(value * value, axis=-1, keepdims=True) + EPSILON)
            low = (value * factor * given["gain"][...]).astype(BF)
        else:
            upstream = total + given["add"][at(c), :]
            value = given["resid"][at(c), :]
            factor = lax.rsqrt(jnp.mean(value * value, axis=-1, keepdims=True) + EPSILON)
            normed = value * factor
            scaled = upstream * given["gain"][...]
            inner = jnp.mean(scaled * normed, axis=-1, keepdims=True)
            result = given["base"][at(c), :] + factor * (scaled - normed * inner)
            given["grad_out"][at(c), :] = result
            given["gain_out"][...] += jnp.sum(upstream * normed, axis=0, keepdims=True)
            low = result.astype(BF)
        stage[at(c), :] = low
        pltpu.make_async_copy(stage.at[at(c)], all_out.at[s, at(c)], own_sem.at[c]).start()

        @pl.when(s < S - 1)
        def _():
            ag_copy(s, c, 0, 1).start()

        @pl.when(s > 0)
        def _():
            ag_copy(s, c, 1, 1).start()

    def gain_copy(step):
        return pltpu.make_async_remote_copy(
            src_ref=gain_stage, dst_ref=given["gains_all"].at[me],
            send_sem=gain_send.at[step], recv_sem=gain_recv.at[step],
            device_id=place_of(sizes, EVERY, lax.rem(me + step, N)), device_id_type=MESH,
        )

    def own_gains():
        return pltpu.make_async_copy(gain_stage, given["gains_all"].at[me], gain_own.at[0])

    def send_gains():
        number = gain_sum.shape[1] // 128
        for j in range(number):
            gain_stage[j : j + 1, :] = gain_sum[:, j * 128 : (j + 1) * 128]
        gain_stage[number:, :] = given["heads"][...]
        own_gains().start()
        for step in range(1, N):
            gain_copy(step).start()

    plane = None
    if mode == "last":
        plane = Blocks(
            sizes, ((("fsdp",), 0, 0), (("fsdp",), 1, 0)), [given["gout"], given["gqkv"]],
            [plane_gout, plane_gqkv], plane_sems,
        )

    def line_copy(step):
        return pltpu.make_async_remote_copy(
            src_ref=gqkv_stage.at[lax.rem(s + step, S)], dst_ref=gqkv_line.at[s],
            send_sem=line_send.at[step], recv_sem=line_recv.at[step],
            device_id={"seq": lax.rem(s + step, S)}, device_id_type=MESH,
        )

    def plane_step():
        plane.wait_one(1)
        for z in range(S):
            total = plane_gqkv[0, z].astype(F32)
            for owner in range(1, F):
                total = total + plane_gqkv[owner, z].astype(F32)
            gqkv_stage[z] = total.astype(BF)
        for step in range(1, S):
            line_copy(step).start()
        gqkv_line[s] = gqkv_stage[s]

    def rows_step():
        plane.wait_one(0)
        half = plane_gout.shape[1] // 2
        for part_at in range(2):
            own = pl.ds(part_at * half, half)
            total = plane_gout[0, own].astype(F32)
            for owner in range(1, F):
                total = total + plane_gout[owner, own].astype(F32)
            given["gout_out"][own, :] = total

    def columns_step():
        for step in range(1, S):
            line_copy(step).wait()
        result = given["gqkv_out"]
        q_width, kv = QH * HD // S, KH * HD // S
        for z in range(S):
            block = gqkv_line[z].astype(F32)
            result[:, z * q_width : (z + 1) * q_width] = block[:, :q_width]
            key_at = S * q_width + z * kv
            result[:, key_at : key_at + kv] = block[:, q_width : q_width + kv]
            value_at = S * (q_width + kv) + z * kv
            result[:, value_at : value_at + kv] = block[:, q_width + kv :]

    def relay_step(way, hop, c):
        block = s - hop if way == 0 else s + hop
        ag_copy(block, c, way, hop).wait_recv()
        if hop < S - 1:
            @pl.when(s < S - 1 if way == 0 else s > 0)
            def _():
                ag_copy(block, c, way, hop + 1).start()

    def final_lag(z):
        return 1 + jnp.maximum(jnp.maximum(z - 2, S - 3 - z), 0)

    ahead = min(steps, AHEAD if gather else 4)
    for c in range(ahead):
        end_step(c)
    if plane:
        plane.start()
    blocks.start()
    turns = steps + (2 * S - 2 if gather else S)

    def inside(c):
        return (c >= 0) & (c < steps)

    @pl.loop(0, turns)
    def _(t):
        for way in range(2):
            come = t - (s - 1 if way == 0 else S - 2 - s)

            @pl.when(inside(come) & ((s > 0) & (s < S - 1)))
            def _():
                middle_step(way, come)

        @pl.when(inside(t + ahead) & ((s == 0) | (s == S - 1)))
        def _():
            end_step(t + ahead)

        done = t - final_lag(s)

        @pl.when(inside(done))
        def _():
            final_step(done)

        if gather:
            for hop in range(1, S):
                for way in range(2):
                    block = s - hop if way == 0 else s + hop
                    passed = t - final_lag(block) - hop

                    @pl.when(inside(passed) & ((block >= 0) & (block < S)))
                    def _():
                        relay_step(way, hop, passed)
        else:
            @pl.when(t == steps * 13 // 16)
            def _():
                plane_step()

    if plane:
        rows_step()

    @pl.loop(0, steps)
    def _(c):
        for d in range(S - 1, 0, -1):
            @pl.when(d > s)
            def _():
                rs_copy(d, c, 0, mine(d, c)).wait_send()
        for d in range(S - 1):
            @pl.when(d < s)
            def _():
                rs_copy(d, c, 1, mine(d, c)).wait_send()
        if gather:
            pltpu.make_async_copy(stage.at[at(c)], all_out.at[s, at(c)], own_sem.at[c]).wait()
            for hop in range(1, S):
                @pl.when((s < S - 1) & (s >= hop - 1))
                def _():
                    ag_copy(s, c, 0, hop).wait_send()

                @pl.when((s > 0) & (s <= S - hop))
                def _():
                    ag_copy(s, c, 1, hop).wait_send()

    if mode == "last":
        columns_step()
        own_gains().wait()
        for step in range(1, N):
            gain_copy(step).wait()
    blocks.wait()


def line(mode, sizes, part, others, extras, specs, collective_id, chunks=CHUNKS):
    S, F = sizes["seq"], sizes["fsdp"]
    parts, _, rows, width = part.shape
    full = jax.ShapeDtypeStruct((rows, width), F32)
    everyone = jax.ShapeDtypeStruct((S, rows, width), BF)
    steps = chunks * parts
    scratch = [pltpu.VMEM((parts, S, rows, width), BF)] * 2
    in_specs = [VM] * (1 + len(others))
    sems = [DMA((2, S, steps)), DMA((2, S, steps))]
    if mode == "ffn":
        outs, out_specs = [full, everyone], [VM, ANY]
    elif mode == "grad":
        outs, out_specs = [full, jax.ShapeDtypeStruct((1, width), F32), everyone], [VM, VM, ANY]
    else:
        gout, gqkv = others[-2:]
        owned = gqkv.shape[2:]
        outs = [
            full,
            jax.ShapeDtypeStruct((rows, width), BF),
            jax.ShapeDtypeStruct((S * F, width // 128 + 2, 128), F32),
            jax.ShapeDtypeStruct(gout.shape[1:], F32),
            jax.ShapeDtypeStruct((owned[0], owned[1] * S), F32),
        ]
        out_specs = [VM, VM, ANY, VM, VM]
        N = S * F
        scratch += [pltpu.VMEM((1, width), F32), pltpu.VMEM((width // 128 + 2, 128), F32)]
        scratch += [DMA((N,)), DMA((N,)), DMA((1,))]
        scratch += [
            pltpu.VMEM(gout.shape, BF),
            pltpu.VMEM((F, S) + owned, BF),
            pltpu.VMEM((S,) + owned, BF),
            pltpu.VMEM((S,) + owned, BF),
            DMA((S,)),
            DMA((S,)),
        ]
        scratch += block_scratch(sizes, [gout, gqkv], ((("fsdp",), 0, 0), (("fsdp",), 1, 0)))
        in_specs[-2:] = [ANY, ANY]
        in_specs[-3] = pl.BlockSpec(memory_space=pltpu.SMEM)
    if mode != "last":
        scratch.append(pltpu.VMEM((rows, width), BF))
        sems += [DMA((2, chunks, S)), DMA((2, chunks, S)), DMA((chunks,))]
    return pl.pallas_call(
        functools.partial(line_kernel, sizes, chunks, mode, specs),
        out_shape=outs + block_outs(sizes, extras, specs),
        in_specs=in_specs + [ANY] * len(extras),
        out_specs=out_specs + [ANY] * len(extras),
        scratch_shapes=scratch + sems + block_scratch(sizes, extras, specs),
        compiler_params=pltpu.CompilerParams(
            collective_id=collective_id, has_side_effects=True, vmem_limit_bytes=58 << 20
        ),
        name=f"line_{mode}",
    )(part, *others, *extras)


def widen_kernel(*refs):
    half = len(refs) // 2
    for narrow, wide in zip(refs[:half], refs[half:]):
        wide[...] = narrow[...].astype(F32)


def widen(arrays):
    specs = [pl.BlockSpec((1,) + array.shape[1:], lambda i: (i, 0, 0)) for array in arrays]
    return pl.pallas_call(
        widen_kernel,
        grid=(arrays[0].shape[0],),
        out_shape=[jax.ShapeDtypeStruct(array.shape, F32) for array in arrays],
        in_specs=specs,
        out_specs=specs,
        compiler_params=pltpu.CompilerParams(vmem_limit_bytes=40 << 20),
        name="widen",
    )(*arrays)


def turn(values, cosine, sine):
    return values * cosine + pltpu.roll(values, HD // 2, 1) * sine


def softmax_block(query, keys, first_row, length, scale):
    scores = lax.dot_general(
        query, keys, (((1,), (1,)), ((), ())), preferred_element_type=F32
    ) * scale
    row = first_row + lax.broadcasted_iota(jnp.int32, scores.shape, 0)
    column = lax.broadcasted_iota(jnp.int32, scores.shape, 1)
    scores = jnp.where((column <= row) & (column < length), scores, MASKED)
    peak = jnp.max(scores, axis=-1, keepdims=True)
    weights = jnp.exp(scores - peak)
    return weights * (1.0 / jnp.sum(weights, axis=-1, keepdims=True))


def tiles(width, step, body):
    @pl.loop(0, width // step)
    def _(n):
        body(pl.ds(pl.multiple_of(n * step, step), step))


class Rows:
    def __init__(self, sizes, early, source, target, sems):
        F = sizes["fsdp"]
        f = lax.axis_index("fsdp")
        send_sem, recv_sem, own_sem = sems
        self.copies = []
        for b in range(early):
            own = pltpu.make_async_copy(source(b, f), target(b, f), own_sem.at[b])
            self.copies.append([own])
            for step in range(1, F):
                away = lax.rem(f + step, F)
                self.copies[b].append(
                    pltpu.make_async_remote_copy(
                        src_ref=source(b, away), dst_ref=target(b, f),
                        send_sem=send_sem.at[b, step], recv_sem=recv_sem.at[b, step],
                        device_id={"fsdp": away}, device_id_type=MESH,
                    )
                )

    def start(self, b):
        for copy in self.copies[b]:
            copy.start()

    def wait(self, b):
        for copy in self.copies[b]:
            copy.wait()


def row_scratch(sizes, early, slots, width):
    if not early:
        return []
    F = sizes["fsdp"]
    return [pltpu.VMEM((early, F * slots, width), BF), DMA((early, F)), DMA((early, F)), DMA((early,))]


def rows_at(ref, slots):
    return lambda b, i: ref.at[b, pl.ds(pl.multiple_of(i * slots, 16), slots)]


def attend_kernel(sizes, heads, blocks, early, specs, *refs):
    count = len(specs)
    length_ref, tok_ref, gain_ref, wq_ref, cos_ref, sin_ref, gains_ref, wo_ref = refs[:8]
    select_ref, cot_ref = refs[8:10]
    refs = list(refs[10:])

    def take(number):
        taken, refs[:number] = refs[:number], []
        return taken

    first = take(2 if early else 0)
    sources = take(count)
    attn_ref, proj_ref, low_ref, out_ref, part_ref, rows_ref = take(6)
    early_out = take(1 if early else 0)
    results = take(count)
    k_all, v_all = take(2)
    row_refs = take(4 if early else 0)
    sems = refs
    step = pl.program_id(0)

    def early_rows():
        slots = early_out[0].shape[2]
        return Rows(
            sizes, early, rows_at(row_refs[0], slots), lambda b, i: early_out[0].at[i, b], row_refs[1:]
        )

    @pl.when(step == 0)
    def _():
        greet(sizes)()
        Blocks(sizes, specs, sources, results, sems).start()
        if early:
            rows_away = early_rows()
            for b in range(early):

                def pick_first(at):
                    row_refs[0][b, :, at] = jnp.dot(
                        first[0][b], first[1][b, :, at], preferred_element_type=F32
                    ).astype(BF)

                tiles(row_refs[0].shape[2], 512, pick_first)
                rows_away.start(b)

    rows, width = proj_ref.shape
    length = length_ref[0]
    cosine = cos_ref[...]
    sine = sin_ref[...]
    q_gain = gains_ref[0:1, :]
    k_gain = gains_ref[1:2, :]
    scale = HD ** (-0.5)
    value = tok_ref[...].astype(F32)
    factor = lax.rsqrt(jnp.mean(value * value, axis=-1, keepdims=True) + EPSILON)
    attn_ref[...] = (value * factor * gain_ref[...]).astype(BF)

    def project(at):
        proj_ref[:, at] = jnp.dot(attn_ref[...], wq_ref[:, at], preferred_element_type=F32)

    tiles(width, 256, project)

    def normed(raw, gain):
        factor = lax.rsqrt(jnp.mean(raw * raw, axis=-1, keepdims=True) + EPSILON)
        return turn(raw * factor * gain, cosine, sine).astype(BF)

    key = normed(proj_ref[:, heads * HD : (heads + 1) * HD], k_gain)
    value_low = proj_ref[:, (heads + 1) * HD :].astype(BF)
    low_ref[:, heads * HD : (heads + 1) * HD] = key
    low_ref[:, (heads + 1) * HD :] = value_low
    here = pl.ds(pl.multiple_of(step * rows, rows), rows)
    k_all[here, :] = key
    v_all[here, :] = value_low
    for block in range(blocks):
        @pl.when(step == block)
        def _():
            reach = (block + 1) * rows

            def one(column):
                query = normed(proj_ref[:, column], q_gain)
                low_ref[:, column] = query
                probs = softmax_block(query, k_all[:reach, :], block * rows, length, scale)
                mixed = jnp.dot(probs.astype(BF), v_all[:reach, :], preferred_element_type=F32)
                out_ref[:, column] = mixed.astype(BF)

            tiles(heads * HD, HD, one)

    def leave(at):
        part_ref[:, at] = jnp.dot(
            out_ref[...], wo_ref[:, at], preferred_element_type=F32
        ).astype(BF)

    tiles(part_ref.shape[1], 256, leave)

    def pick(at):
        rows_ref[0, :, at] = jnp.dot(
            select_ref[0], cot_ref[0, :, at], preferred_element_type=F32
        ).astype(BF)

    @pl.when(step >= early)
    def _():
        tiles(rows_ref.shape[2], 512, pick)

    @pl.when(step == blocks - 1)
    def _():
        if early:
            rows_away = early_rows()
            for b in range(early):
                rows_away.wait(b)
        Blocks(sizes, specs, sources, results, sems).wait()


def attend(
    length, tokens, gain, w_proj, cosine, sine, gains, w_out, select, cot, heads, early, extras,
    specs, sizes, collective_id,
):
    total, width = tokens.shape
    blocks = select.shape[0]
    F = sizes["fsdp"]
    slots = select.shape[1] // F
    own_width = w_proj.shape[1]
    rows = total // blocks
    q_width = heads * HD

    def by_rows(columns):
        return pl.BlockSpec((rows, columns), lambda i: (i, 0))

    def leading(array):
        return pl.BlockSpec(
            (early,) + array.shape[1:], lambda i: (0, 0, 0), pipeline_mode=pl.Buffered(1)
        )

    def by_block(array):
        return pl.BlockSpec((1,) + array.shape[1:], lambda i: (i, 0, 0))

    def whole(array):
        return pl.BlockSpec(array.shape, lambda i: (0, 0), pipeline_mode=pl.Buffered(1))

    return pl.pallas_call(
        functools.partial(attend_kernel, sizes, heads, blocks, early, specs),
        grid=(blocks,),
        out_shape=[
            jax.ShapeDtypeStruct((total, width), BF),
            jax.ShapeDtypeStruct((total, own_width), F32),
            jax.ShapeDtypeStruct((total, own_width), BF),
            jax.ShapeDtypeStruct((total, q_width), BF),
            jax.ShapeDtypeStruct((total, width), BF),
            jax.ShapeDtypeStruct((blocks - early, select.shape[1], width), BF),
        ]
        + ([jax.ShapeDtypeStruct((F, early, slots, width), BF)] if early else [])
        + block_outs(sizes, extras, specs),
        in_specs=[
            pl.BlockSpec(memory_space=pltpu.SMEM),
            by_rows(width),
            whole(gain),
            whole(w_proj),
            by_rows(HD),
            by_rows(HD),
            whole(gains),
            whole(w_out),
            by_block(select),
            by_block(cot),
        ]
        + ([leading(select), leading(cot)] if early else [])
        + [ANY] * len(extras),
        out_specs=[
            by_rows(width), by_rows(own_width), by_rows(own_width), by_rows(q_width), by_rows(width),
            pl.BlockSpec((1, select.shape[1], width), lambda i: (jnp.maximum(i - early, 0), 0, 0)),
        ] + [ANY] * (len(extras) + (1 if early else 0)),
        scratch_shapes=[pltpu.VMEM((total, HD), BF), pltpu.VMEM((total, HD), BF)]
        + row_scratch(sizes, early, slots, width)
        + block_scratch(sizes, extras, specs),
        compiler_params=pltpu.CompilerParams(
            collective_id=collective_id, has_side_effects=True, vmem_limit_bytes=58 << 20
        ),
        name="attend",
    )(
        length, tokens, gain, w_proj, cosine, sine, gains, w_out, select, cot,
        *([select, cot] if early else []), *extras,
    )


def attend_back_kernel(sizes, heads, blocks, early, specs, *refs):
    count = len(specs)
    length_ref, proj_ref, low_ref, kv_ref, grad_ref, wo_ref, wq_ref, cos_ref, sin_ref, gains_ref = refs[:10]
    select_ref, back_ref, attn_any, o_any, ga_any, moe_any = refs[10:16]
    refs = list(refs[16:])

    def take(number):
        taken, refs[:number] = refs[:number], []
        return taken

    sources = take(count)
    part_ref, gains_out, gqkv_out, gout_out = take(4)
    results = take(count)
    gk_all, gv_all, go_ref, out_all, attn_all, o_all, ga_all, gqkv_stage, gout_stage, all_sem, out_sem = take(11)
    row_refs = take(4 if early else 0)
    sems = refs
    slots = moe_any.shape[2]

    def early_rows():
        return Rows(
            sizes, early, lambda b, i: moe_any.at[i, b], rows_at(row_refs[0], slots), row_refs[1:]
        )

    inward = [
        pltpu.make_async_copy(source, target, all_sem.at[i])
        for i, (source, target) in enumerate(((attn_any, attn_all), (o_any, o_all), (ga_any, ga_all)))
    ]
    step = pl.program_id(0)
    rows = proj_ref.shape[0]
    length = length_ref[0]
    cosine = cos_ref[...]
    sine = sin_ref[...]
    q_gain = gains_ref[0:1, :]
    k_gain = gains_ref[1:2, :]
    scale = HD ** (-0.5)
    block_at = blocks - 1 - step
    here = pl.ds(pl.multiple_of(block_at * rows, rows), rows)

    def back(raw, gain, grad):
        grad = turn(grad, cosine, -sine)
        factor = lax.rsqrt(jnp.mean(raw * raw, axis=-1, keepdims=True) + EPSILON)
        unit = raw * factor
        scaled = grad * gain
        inner = jnp.mean(scaled * unit, axis=-1, keepdims=True)
        return factor * (scaled - unit * inner), jnp.sum(grad * unit, axis=0, keepdims=True)

    @pl.when(step == 0)
    def _():
        greet(sizes)()
        Blocks(sizes, specs, sources, results, sems).start()
        for copy in inward:
            copy.start()
        if early:
            rows_away = early_rows()
            for b in range(early - 1, -1, -1):
                rows_away.start(b)
        gk_all[...] = jnp.zeros_like(gk_all)
        gv_all[...] = jnp.zeros_like(gv_all)
        gains_out[...] = jnp.zeros_like(gains_out)

    def arrive(at):
        go_ref[:, at] = lax.dot_general(
            grad_ref[...], wo_ref[at, :], (((1,), (1,)), ((), ())), preferred_element_type=F32
        ).astype(BF)

    tiles(heads * HD, 256, arrive)
    for block in range(blocks):
        @pl.when(block_at == block)
        def _():
            reach = (block + 1) * rows
            keys = kv_ref[:reach, :HD]
            values = kv_ref[:reach, HD:]

            def one(column):
                query = low_ref[:, column]
                grad_o = go_ref[:, column]
                probs = softmax_block(query, keys, block * rows, length, scale)
                grad_p = lax.dot_general(
                    grad_o, values, (((1,), (1,)), ((), ())), preferred_element_type=F32
                )
                inner = jnp.sum(probs * grad_p, axis=-1, keepdims=True)
                grad_s = (probs * (grad_p - inner)).astype(BF)
                grad_q = jnp.dot(grad_s, keys, preferred_element_type=F32) * scale
                gk_all[:reach, :] += lax.dot_general(
                    grad_s, query, (((0,), (0,)), ((), ())), preferred_element_type=F32
                )
                gv_all[:reach, :] += lax.dot_general(
                    probs.astype(BF), grad_o, (((0,), (0,)), ((), ())), preferred_element_type=F32
                )
                grad_raw, gained = back(proj_ref[:, column], q_gain, grad_q.astype(BF).astype(F32))
                out_all[here, column] = grad_raw.astype(BF)
                gains_out[0:1, :] += gained

            tiles(heads * HD, HD, one)

    grad_k = (gk_all[here, :] * scale).astype(BF).astype(F32)
    grad_raw, gained = back(proj_ref[:, heads * HD : (heads + 1) * HD], k_gain, grad_k)
    out_all[here, heads * HD : (heads + 1) * HD] = grad_raw.astype(BF)
    out_all[here, (heads + 1) * HD :] = gv_all[here, :].astype(BF)
    gains_out[1:2, :] += gained

    def leave(at):
        part_ref[0, :, at] = lax.dot_general(
            out_all[here, :], wq_ref[at, :], (((1,), (1,)), ((), ())), preferred_element_type=F32
        ).astype(BF)

    tiles(part_ref.shape[2], 256, leave)
    over_rows = (((0,), (0,)), ((), ()))

    def combine(rows_of):
        def one_part(at):
            part_ref[1, :, at] = lax.dot_general(
                select_ref[0], rows_of(at), over_rows, preferred_element_type=F32
            ).astype(BF)

        tiles(part_ref.shape[2], 512, one_part)

    @pl.when(block_at >= early)
    def _():
        combine(lambda at: back_ref[0, :, at])

    for b in range(early):
        @pl.when(block_at == b)
        def _():
            early_rows().wait(b)
            combine(lambda at: row_refs[0][b, :, at])


    @pl.when(step == blocks - 1)
    def _():
        for copy in inward:
            copy.wait()
        for i, (left, right, stage, result) in enumerate(
            ((attn_all, out_all, gqkv_stage, gqkv_out), (o_all, ga_all, gout_stage, gout_out))
        ):
            span = stage.shape[1]
            sent = []
            for n in range(left.shape[1] // span):
                if n >= 2:
                    sent[n - 2].wait()
                stage[n % 2] = lax.dot_general(
                    left[:, n * span : (n + 1) * span], right[...], over_rows,
                    preferred_element_type=F32,
                ).astype(BF)
                sent.append(
                    pltpu.make_async_copy(
                        stage.at[n % 2], result.at[pl.ds(n * span, span)], out_sem.at[i, n % 2]
                    )
                )
                sent[-1].start()
            for copy in sent[-2:]:
                copy.wait()
        Blocks(sizes, specs, sources, results, sems).wait()


def attend_back(
    length, projected, low, grad, w_out, w_proj, cosine, sine, gains, select, back, attn_low, o_low,
    moe_rows, heads, early, extras, specs, sizes, collective_id,
):
    total, own_width = projected.shape
    width = w_out.shape[1]
    blocks = select.shape[0]
    span = 256
    rows = total // blocks
    q_width = heads * HD

    def by_rows(columns):
        return pl.BlockSpec((rows, columns), lambda i: (blocks - 1 - i, 0))

    def by_block(array):
        return pl.BlockSpec((1,) + array.shape[1:], lambda i: (blocks - 1 - i, 0, 0))

    def whole(array):
        return pl.BlockSpec(array.shape, lambda i: (0, 0), pipeline_mode=pl.Buffered(1))

    return pl.pallas_call(
        functools.partial(attend_back_kernel, sizes, heads, blocks, early, specs),
        grid=(blocks,),
        out_shape=[
            jax.ShapeDtypeStruct((2, total, width), BF),
            jax.ShapeDtypeStruct((2, HD), F32),
            jax.ShapeDtypeStruct((width, own_width), BF),
            jax.ShapeDtypeStruct((q_width, width), BF),
        ] + block_outs(sizes, extras, specs),
        in_specs=[
            pl.BlockSpec(memory_space=pltpu.SMEM),
            by_rows(own_width),
            by_rows(q_width),
            pl.BlockSpec((total, 2 * HD), lambda i: (0, heads // 2)),
            by_rows(width),
            whole(w_out),
            whole(w_proj),
            by_rows(HD),
            by_rows(HD),
            whole(gains),
            by_block(select),
            pl.BlockSpec(
                (1,) + back.shape[1:], lambda i: (jnp.maximum(blocks - 1 - i - early, 0), 0, 0)
            ),
        ] + [ANY] * (4 + len(extras)),
        out_specs=[
            pl.BlockSpec((2, rows, width), lambda i: (0, blocks - 1 - i, 0)),
            pl.BlockSpec((2, HD), lambda i: (0, 0)),
        ] + [ANY] * (2 + len(extras)),
        scratch_shapes=[
            pltpu.VMEM((total, HD), F32),
            pltpu.VMEM((total, HD), F32),
            pltpu.VMEM((rows, q_width), BF),
            pltpu.VMEM((total, own_width), BF),
            pltpu.VMEM((total, width), BF),
            pltpu.VMEM((total, q_width), BF),
            pltpu.VMEM((total, width), BF),
            pltpu.VMEM((2, span, own_width), BF),
            pltpu.VMEM((2, span, width), BF),
            DMA((3,)),
            DMA((2, 2)),
        ]
        + row_scratch(sizes, early, moe_rows.shape[2], width)
        + block_scratch(sizes, extras, specs),
        compiler_params=pltpu.CompilerParams(
            collective_id=collective_id, has_side_effects=True, vmem_limit_bytes=58 << 20
        ),
        name="attend_back",
    )(
        length, projected, low, low, grad, w_out, w_proj, cosine, sine, gains, select, back,
        attn_low, o_low, grad, moe_rows, *extras,
    )


def rms_factor(values):
    return lax.rsqrt(jnp.mean(values * values, axis=-1, keepdims=True) + EPSILON)


def dot(left, right):
    return jnp.dot(left, right, preferred_element_type=F32)


def mm(form, left, right):
    return jnp.einsum(form, left, right, preferred_element_type=F32)


def whole_columns(blocks):
    parts, rows, _ = blocks.shape
    q_width = QH * HD // parts
    kv_width = KH * HD // parts
    moved = blocks.transpose(1, 0, 2)
    return jnp.concatenate(
        [
            moved[..., :q_width].reshape(rows, -1),
            moved[..., q_width : q_width + kv_width].reshape(rows, -1),
            moved[..., q_width + kv_width :].reshape(rows, -1),
        ],
        axis=-1,
    )


def lanes(flat, lead):
    width = flat.shape[-1]
    rows = -(-width // 2048) * 16
    return jnp.pad(flat, ((0, 0), (0, rows * 128 - width))).reshape(lead, rows, 128)


def per_device(
    tokens, cotangent, lengths, routes, slots, w_qkv, w_out, w_router, norm_gains, w_gate_up, w_down
):
    tok_count = tokens.shape[1]
    width = tokens.shape[2]
    S = lax.axis_size("seq")
    F = lax.axis_size("fsdp")
    N = S * F
    sizes = {"seq": S, "fsdp": F}
    local_experts = w_gate_up.shape[0]
    own_experts = local_experts // S
    expert_count = w_router.shape[1]
    capacity = tok_count * TOPK * 5 // (4 * expert_count)
    heads = QH // S
    seq_total = tok_count * S
    q_width = heads * HD
    own_width = q_width + 2 * HD
    seq_at = lax.axis_index("seq")
    w_rows = w_qkv.shape[0]
    small = norm_gains.shape[0]
    router_size = w_router.size
    part_width = w_gate_up.shape[1]
    down_width = w_down.shape[2]
    assert KH == S and own_experts == 1

    small_send = lanes(jnp.concatenate([w_router.reshape(-1), norm_gains])[None], 1)[0]
    table = jnp.concatenate([routes[0].T, slots[0].T])
    tok_all, cot_all, table_all, w_proj, out_own, small_all = entry(
        tokens[0], cotangent[0], table, w_qkv, w_out, small_send, sizes, 1
    )
    w_proj = w_proj.reshape(width, own_width)
    out_own = out_own.reshape(q_width, width)
    small_flat = small_all.reshape(N, -1)
    full_router = small_flat[:, :router_size].reshape(width, expert_count)
    gain_values = small_flat[:, router_size : router_size + small].reshape(-1).astype(F32)
    gain_attn = gain_values[:width]
    gain_ffn = gain_values[width : 2 * width][None]
    gain_heads = gain_values[2 * width :].reshape(2, HD)

    positions = jnp.arange(seq_total, dtype=jnp.int32)
    frequency = THETA ** (-jnp.arange(HD // 2, dtype=F32) / (HD // 2))
    angles = positions.astype(F32)[:, None] * frequency[None, :]
    cosine = jnp.concatenate([jnp.cos(angles)] * 2, axis=-1)
    sine = jnp.concatenate([-jnp.sin(angles), jnp.sin(angles)], axis=-1)
    expert_ids = jnp.arange(expert_count, dtype=jnp.int32)
    slot_ids = jnp.arange(capacity, dtype=jnp.int32)
    plane = (
        jnp.arange(F, dtype=jnp.int32)[:, None] * local_experts
        + seq_at * own_experts
        + jnp.arange(own_experts, dtype=jnp.int32)[None, :]
    ).reshape(-1)
    hit = table_all[:, None, :TOPK] == plane[None, :, None, None]
    plane_slots = jnp.max(jnp.where(hit, table_all[:, None, TOPK:], -1), axis=2)
    one_hot = plane_slots[:, :, None, :] == slot_ids[None, None, :, None]
    select = one_hot.astype(BF).reshape(S, F * own_experts * capacity, tok_count)
    grouped = (S, F, own_experts * capacity, width)

    fused = capacity % 16 == 0
    early = S // 2 if fused else 0
    attn_low, projected, qkv_low, o_low, o_part, cot_rows, *g_first, down_w = attend(
        lengths, tok_all.reshape(seq_total, width), gain_attn[None], w_proj, cosine, sine,
        gain_heads, out_own, select, cot_all, heads, early, [w_down.reshape((S, own_experts) + w_down.shape[1:])],
        ((("seq",), 0, "columns"),), sizes, 3,
    )
    o_part = o_part.reshape(1, S, tok_count, width)
    cot_rows = cot_rows.reshape((S - early,) + grouped[1:])

    residual, ffn_all, g_rows = line(
        "ffn", sizes, o_part, [tokens[0], gain_ffn], [cot_rows], ((("fsdp",), 1, 0),), 2
    )
    ffn_low = lax.dynamic_index_in_dim(ffn_all, seq_at, 0, keepdims=False)

    route_rows = routes[0]
    slot_rows = slots[0]
    router_scores = dot(ffn_low, full_router)
    picked = route_rows[:, :, None] == expert_ids[None, None, :]
    selected = jnp.sum(jnp.where(picked, router_scores[:, None, :], 0.0), axis=-1)
    gate_prob = jax.nn.softmax(selected, axis=-1)
    gate_table = jnp.sum(jnp.where(picked, gate_prob[:, :, None], 0.0), axis=1).T
    hit = table[None, :TOPK] == expert_ids[:, None, None]
    own_slots = jnp.max(jnp.where(hit, table[None, TOPK:], -1), axis=1)
    gate_slots = jnp.sum(
        jnp.where(
            own_slots[:, None, :] == slot_ids[None, :, None], gate_table[:, None, :], 0.0
        ),
        axis=-1,
    )
    by_device = (F, S, own_experts, capacity)

    def to_devices(values):
        return lanes(values.reshape(by_device).transpose(1, 0, 2, 3).reshape(N, -1), N)

    gate_send = to_devices(gate_slots)

    up_blocks = w_gate_up.reshape((S, own_experts) + w_gate_up.shape[1:])
    side_specs = ((("seq",), 0, 0), (EVERY, 0, 0))
    if fused:
        gate_up_w, gate_got, x_rows, through, g_flat = dispatch(
            [up_blocks, gate_send], side_specs, ffn_all, [*g_first, g_rows], down_w[0], select,
            sizes, 4,
        )
    else:
        ffn_rows = mm("brt,btd->brd", select, ffn_all).astype(BF).reshape(grouped)
        gate_up_w, gate_got, x_rows = exchange(
            [up_blocks, gate_send, ffn_rows], side_specs + ((("fsdp",), 1, 0),), sizes, 4
        )
        g_flat = g_rows.reshape(-1, width)
        through = mm("rd,hd->rh", g_flat, down_w[0])
    row_gate = gate_got.reshape(S, F, -1)[:, :, :capacity].transpose(1, 0, 2).reshape(-1, 1)
    x_flat = x_rows.reshape(-1, width)
    moe_rows, grad_rows, grad_gu_low, gated_hidden, prob_rows = expert(
        x_flat, row_gate, through, g_flat, gate_up_w.reshape(width, 2 * FF), down_w[0], 5
    )
    prob_send = prob_rows.reshape(F, S, -1).transpose(1, 0, 2).reshape(N, -1)
    back_blocks = [grad_rows.reshape(F, S, capacity, width), lanes(prob_send, N)]
    grad_back, prob_got, up_got, down_term, *grad_part = grads(
        back_blocks, ((("fsdp",), 0, 1), (EVERY, 0, 0)), x_flat, grad_gu_low, gated_hidden, g_flat,
        select if fused else None, sizes, 6,
    )
    if fused:
        (grad_part,) = grad_part
    else:
        grad_part = mm("brt,brd->btd", select, grad_back.reshape(S, -1, width)).astype(BF)
    moe_rows = moe_rows.reshape(F, S, capacity, width)
    prob_slots = prob_got.reshape(S, F, -1)[:, :, :capacity].transpose(1, 0, 2)
    prob_slots = prob_slots.reshape(expert_count, capacity)


    prob_of_route = jnp.einsum(
        "tke,ec->tkc", picked.astype(F32), prob_slots, precision=lax.Precision.HIGHEST
    )
    at_slot = slot_rows[:, :, None] == slot_ids[None, None, :]
    grad_prob = jnp.sum(jnp.where(at_slot, prob_of_route, 0.0), axis=-1)
    grad_selected = gate_prob * (grad_prob - jnp.sum(gate_prob * grad_prob, axis=-1, keepdims=True))
    grad_logits = jnp.sum(jnp.where(picked, grad_selected[:, :, None], 0.0), axis=1).astype(BF)
    grad_ffn_add = mm("te,de->td", grad_logits, full_router)
    grad_router_part = mm("td,te->de", ffn_low, grad_logits)
    valid = (seq_at * tok_count + jnp.arange(tok_count, dtype=jnp.int32)) < lengths[0]
    grad_final = jnp.where(valid[:, None], cotangent[0].astype(F32), 0.0)
    grad_residual, grad_gain_ffn, grad_attn_low, moe_back = line(
        "grad", sizes, grad_part[None], [grad_final, gain_ffn, residual, grad_ffn_add],
        [moe_rows], ((("fsdp",), (early, S - early), 1),), 7,
    )
    grad_attn_low = grad_attn_low.reshape(seq_total, width)

    early_gains = jnp.concatenate(
        [jnp.zeros((width,), F32), grad_gain_ffn[0], jnp.zeros((2 * HD,), F32)]
    )
    small_blocks = jnp.concatenate(
        [grad_router_part.reshape(N, -1), early_gains.reshape(N, -1)], axis=1
    )
    small_rows = -(-small_blocks.shape[1] // 1024) * 8
    small_blocks = jnp.pad(small_blocks, ((0, 0), (0, small_rows * 128 - small_blocks.shape[1])))
    small_blocks = small_blocks.reshape(N, small_rows, 128)
    last_parts, grad_gain_heads, grad_qkv_part, grad_out_part, down_got, small_got = attend_back(
        lengths, projected, qkv_low, grad_attn_low, out_own, w_proj, cosine, sine, gain_heads,
        select, moe_back.reshape(S - early, -1, width), attn_low, o_low, moe_rows, heads, early,
        [down_term[None], small_blocks], ((("seq",), "columns", 0), (EVERY, 0, 0)), sizes, 9,
    )
    grad_qkv_part = grad_qkv_part.reshape(S, F, w_rows, own_width)
    (
        grad_inputs, final, late_gains, grad_out, grad_qkv
    ) = line(
        "last", sizes, last_parts.reshape(2, S, tok_count, width),
        [
            grad_residual, gain_attn[None], residual, tokens[0], grad_gain_heads, lengths,
            grad_out_part.reshape(F, -1, width), grad_qkv_part,
        ],
        [], (), 8,
    )
    grad_gate_up, grad_down = widen(
        [up_got.reshape(w_gate_up.shape), down_got.reshape(w_down.shape)]
    )
    small_sum = jnp.sum(small_got, axis=0).reshape(-1)
    grad_router = small_sum[:router_size].reshape(w_router.shape)
    late_flat = jnp.sum(late_gains, axis=0).reshape(-1)
    late_sum = jnp.concatenate([late_flat[:width], jnp.zeros((width,), F32), late_flat[width:]])
    device_at = seq_at * F + lax.axis_index("fsdp")
    grad_gains = small_sum[router_size : router_size + small] + lax.dynamic_slice_in_dim(
        late_sum, device_at * small, small, 0
    )
    return (
        final[None],
        grad_inputs[None],
        grad_qkv,
        grad_out,
        grad_router,
        grad_gains,
        grad_gate_up,
        grad_down,
    )


def solution(mesh):
    in_specs = (
        P("fsdp", "seq", None),
        P("fsdp", "seq", None),
        P("fsdp"),
        P("fsdp", "seq", None),
        P("fsdp", "seq", None),
        P(("seq", "fsdp"), None),
        P(("seq", "fsdp"), None),
        P(("seq", "fsdp"), None),
        P(("seq", "fsdp")),
        P("fsdp", "seq", None),
        P("fsdp", None, "seq"),
    )
    out_specs = (
        P("fsdp", "seq", None),
        P("fsdp", "seq", None),
        P(("seq", "fsdp"), None),
        P(("seq", "fsdp"), None),
        P(("seq", "fsdp"), None),
        P(("seq", "fsdp")),
        P("fsdp", "seq", None),
        P("fsdp", None, "seq"),
    )
    return jax.shard_map(
        per_device, mesh=mesh, in_specs=in_specs, out_specs=out_specs, check_vma=False
    )
```

```python
import functools

import jax
import jax.numpy as jnp
from jax import lax
from jax.experimental import pallas as pl
from jax.experimental.pallas import tpu as pltpu
from jax.sharding import PartitionSpec as P

QH = 32
KH = 4
HD = 128
FF = 768
TOPK = 8
EPSILON = 1e-06
THETA = 1000000.0
MASKED = -1e30
AHEAD = 1
CHUNKS = 16
BF = jnp.bfloat16
F32 = jnp.float32
MESH = pl.DeviceIdType.MESH
ANY = pl.BlockSpec(memory_space=pl.ANY)
VM = pl.BlockSpec(memory_space=pltpu.VMEM)
DMA = pltpu.SemaphoreType.DMA
EVERY = ("seq", "fsdp")

def index_of(sizes, axes):
    at = 0
    for axis in axes:
        at = at * sizes[axis] + lax.axis_index(axis)
    return at


def count_of(sizes, axes):
    number = 1
    for axis in axes:
        number *= sizes[axis]
    return number


def place_of(sizes, axes, at):
    if len(axes) == 1:
        return {axes[0]: at}
    return {axes[0]: at // sizes[axes[1]], axes[1]: at % sizes[axes[1]]}


def each(total, body):
    @pl.loop(1, total)
    def _(step):
        body(step)


def greet(sizes):
    total = count_of(sizes, EVERY)
    me = index_of(sizes, EVERY)
    barrier = pltpu.get_barrier_semaphore()

    def signal(step):
        pl.semaphore_signal(
            barrier, inc=1, device_id=place_of(sizes, EVERY, lax.rem(me + step, total)),
            device_id_type=MESH,
        )

    each(total, signal)
    return lambda: pl.semaphore_wait(barrier, total - 1)


def block_of(ref, dim, at, total):
    if isinstance(dim, tuple):
        return ref.at[at, pl.ds(*dim)]
    if dim == "columns":
        width = ref.shape[-1] // total
        return ref.at[:, :, pl.ds(pl.multiple_of(at * width, 128), width)]
    return ref.at[at] if dim == 0 else ref.at[:, at]


class Blocks:
    def __init__(self, sizes, specs, sources, results, sems):
        self.own, self.parted = [], []
        if not specs:
            return
        send_sem, recv_sem, own_sem, *stages = sems
        for i, (axes, before, after) in enumerate(specs):
            me = index_of(sizes, axes)
            total = count_of(sizes, axes)
            source = block_of(sources[i], before, me, total)
            result = block_of(results[i], after, me, total)
            self.own.append(
                (
                    pltpu.make_async_copy(source, stages[i], own_sem.at[i, 0]),
                    pltpu.make_async_copy(stages[i], result, own_sem.at[i, 1]),
                )
            )

            def away(step, i=i, axes=axes, before=before, after=after, me=me, total=total):
                target = lax.rem(me + step, total)
                return pltpu.make_async_remote_copy(
                    src_ref=block_of(sources[i], before, target, total),
                    dst_ref=block_of(results[i], after, me, total),
                    send_sem=send_sem.at[i, step],
                    recv_sem=recv_sem.at[i, step],
                    device_id=place_of(sizes, axes, target),
                    device_id_type=MESH,
                )

            self.parted.append((total, away))

    def start(self):
        for total, away in self.parted:
            each(total, lambda step: away(step).start())
        for inward, _ in self.own:
            inward.start()

    def wait(self):
        for i in range(len(self.own)):
            self.wait_one(i)

    def wait_one(self, i):
        inward, outward = self.own[i]
        inward.wait()
        outward.start()
        outward.wait()
        total, away = self.parted[i]
        each(total, lambda step: away(step).wait())


def block_scratch(sizes, arrays, specs):
    if not specs:
        return []
    total = max(count_of(sizes, axes) for axes, _, _ in specs)
    stages = []
    for array, (axes, before, after) in zip(arrays, specs):
        shape = list(array.shape)
        if before == "columns":
            shape[-1] //= count_of(sizes, axes)
        elif isinstance(before, tuple):
            shape = [before[1]] + shape[2:]
        else:
            del shape[before]
        stages.append(pltpu.VMEM(tuple(shape), array.dtype))
    count = len(specs)
    return [DMA((count, total)), DMA((count, total)), DMA((count, 2))] + stages


def block_outs(sizes, arrays, specs):
    outs = []
    for array, (axes, before, after) in zip(arrays, specs):
        shape = list(array.shape)
        total = count_of(sizes, axes)
        if isinstance(before, tuple):
            shape = [before[1], shape[0]] + shape[2:]
        elif before == "columns":
            shape = [total, shape[0], shape[1], shape[2] // total]
        elif after == "columns":
            shape = [shape[1], shape[2], shape[3] * total]
        elif before != after:
            shape[0], shape[1] = shape[1], shape[0]
        outs.append(jax.ShapeDtypeStruct(tuple(shape), array.dtype))
    return outs


def exchange_kernel(sizes, specs, *refs):
    count = len(specs)
    met = greet(sizes)
    blocks = Blocks(sizes, specs, refs[:count], refs[count : 2 * count], refs[2 * count :])
    met()
    blocks.start()
    blocks.wait()


def exchange(arrays, specs, sizes, collective_id):
    count = len(arrays)
    return pl.pallas_call(
        functools.partial(exchange_kernel, sizes, specs),
        out_shape=block_outs(sizes, arrays, specs),
        in_specs=[ANY] * count,
        out_specs=[ANY] * count,
        scratch_shapes=block_scratch(sizes, arrays, specs),
        compiler_params=pltpu.CompilerParams(collective_id=collective_id, has_side_effects=True),
        name=f"exchange_{collective_id}",
    )(*arrays)


def entry_kernel(
    sizes, tok_ref, cot_ref, table_ref, wqkv_ref, wout_ref, small_ref,
    tok_out, cot_out, table_out, wq_out, wo_out, small_out,
    tok_send, tok_recv, tab_send, tab_recv, wq_zsend, wq_zrecv,
    pl_send, pl_recv, sib_send, sib_recv, sm_send, sm_recv, own_sem, *stages,
):
    S, F = sizes["seq"], sizes["fsdp"]
    s = lax.axis_index("seq")
    f = lax.axis_index("fsdp")
    N = S * F
    chips = F // 2
    me = s * F + f
    other = f + 1 - 2 * lax.rem(f, 2)
    rows = tok_ref.shape[0]
    chunks = tok_recv.shape[2]
    span = rows // chunks
    met = greet(sizes)
    kv = KH * HD // S
    q_width = QH * HD // S
    starts = (0, q_width * S, (q_width + kv) * S)
    widths = (q_width, kv, kv)
    offsets = (0, q_width, q_width + kv)

    def columns(z, p):
        return pl.ds(pl.multiple_of(starts[p] + z * widths[p], 128), widths[p])

    pairs = [
        (wqkv_ref.at[:, columns(s, p)], wq_out.at[s, f, :, pl.ds(offsets[p], widths[p])])
        for p in range(3)
    ] + [
        (wout_ref, wo_out.at[f]),
        (tok_ref, tok_out.at[s]),
        (cot_ref, cot_out.at[s]),
        (table_ref, table_out.at[s]),
        (small_ref, small_out.at[me]),
    ]
    inward = [
        pltpu.make_async_copy(source, stages[i], own_sem.at[i, 0])
        for i, (source, _) in enumerate(pairs)
    ]
    outward = [
        pltpu.make_async_copy(stages[i], result, own_sem.at[i, 1])
        for i, (_, result) in enumerate(pairs)
    ]
    for copy in inward:
        copy.start()
    met()

    def remote(src, dst, send_sem, recv_sem, where):
        return pltpu.make_async_remote_copy(
            src_ref=src, dst_ref=dst, send_sem=send_sem, recv_sem=recv_sem,
            device_id=where, device_id_type=MESH,
        )

    wq_line = []
    tables = []
    for step in range(1, S):
        target = lax.rem(s + step, S)
        for p in range(3):
            copy = remote(
                wqkv_ref.at[:, columns(target, p)],
                wq_out.at[s, f, :, pl.ds(offsets[p], widths[p])],
                wq_zsend.at[step, p], wq_zrecv.at[step, p], {"seq": target},
            )
            copy.start()
            wq_line.append(copy)
        copy = remote(
            table_ref, table_out.at[s], tab_send.at[step], tab_recv.at[step], {"seq": target}
        )
        copy.start()
        tables.append(copy)

    def along(a, block, c, way, hop):
        source, result = ((tok_ref, tok_out), (cot_ref, cot_out))[a]
        here = result.at[block, pl.ds(c * span, span)]
        src = source.at[pl.ds(c * span, span)] if hop == 1 else here
        return remote(
            src, here, tok_send.at[a, way, c, hop], tok_recv.at[a, way, c, hop],
            {"seq": s + 1 if way == 0 else s - 1},
        )

    def depart(a):
        for c in range(chunks):
            @pl.when(s < S - 1)
            def _():
                along(a, s, c, 0, 1).start()

            @pl.when(s > 0)
            def _():
                along(a, s, c, 1, 1).start()

    def relay(a, hop):
        for c in range(chunks):
            @pl.when(s >= hop)
            def _():
                along(a, s - hop, c, 0, hop).wait_recv()
                if hop < S - 1:
                    @pl.when(s < S - 1)
                    def _():
                        along(a, s - hop, c, 0, hop + 1).start()

            @pl.when(s < S - hop)
            def _():
                along(a, s + hop, c, 1, hop).wait_recv()
                if hop < S - 1:
                    @pl.when(s > 0)
                    def _():
                        along(a, s + hop, c, 1, hop + 1).start()

    depart(0)

    def plane_block(slot, owner):
        if slot == S:
            return wo_out.at[owner]
        return wq_out.at[lax.rem(s - slot + S, S), owner]

    def to_chip(slot, step):
        block = plane_block(slot, f)
        return remote(block, block, pl_send.at[slot, step], pl_recv.at[slot, step],
                      {"fsdp": lax.rem(f + 2 * step, F)})

    def to_other(slot, step):
        block = plane_block(slot, lax.rem(f - 2 * step + F, F))
        return remote(block, block, sib_send.at[slot, step], sib_recv.at[slot, step],
                      {"fsdp": other})

    def spread(slot):
        for step in range(1, chips):
            to_chip(slot, step).start()
        to_other(slot, 0).start()

    def forward(slot):
        for step in range(1, chips):
            to_chip(slot, step).wait_recv()
            to_other(slot, step).start()

    def small_copy(step):
        target = lax.rem(me + step, N)
        return remote(small_ref, small_out.at[me], sm_send.at[step], sm_recv.at[step],
                      place_of(sizes, EVERY, target))

    each(N, lambda step: small_copy(step).start())
    for i, copy in enumerate(inward):
        copy.wait()
        outward[i].start()
    for copy in outward[:3]:
        copy.wait()
    spread(0)
    outward[3].wait()
    spread(S)
    relay(0, 1)
    depart(1)
    for step in range(1, S):
        for p in range(3):
            wq_line[(step - 1) * 3 + p].wait()
        spread(step)
    for hop in range(2, S):
        relay(0, hop)
        relay(1, hop - 1)
    for slot in range(S + 1):
        forward(slot)
    relay(1, S - 1)
    for a in range(2):
        for hop in range(1, S):
            for c in range(chunks):
                @pl.when((s < S - 1) & (s >= hop - 1))
                def _():
                    along(a, s, c, 0, hop).wait_send()

                @pl.when((s > 0) & (s <= S - hop))
                def _():
                    along(a, s, c, 1, hop).wait_send()
    for copy in outward[4:]:
        copy.wait()
    for slot in range(S + 1):
        for step in range(1, chips):
            to_chip(slot, step).wait_send()
        for step in range(chips):
            to_other(slot, step).wait_send()
            block = plane_block(slot, lax.rem(other - 2 * step + F, F))
            remote(block, block, sib_send.at[slot, step], sib_recv.at[slot, step],
                   {"fsdp": other}).wait_recv()
    for copy in tables:
        copy.wait()
    each(N, lambda step: small_copy(step).wait())


def entry(tokens, cotangent, table, w_qkv, w_out, small, sizes, collective_id, chunks=4):
    S, F = sizes["seq"], sizes["fsdp"]
    own_width = w_qkv.shape[1] // S
    N = S * F
    line_out = jax.ShapeDtypeStruct((S,) + tokens.shape, tokens.dtype)
    q_width, kv = QH * HD // S, KH * HD // S
    stages = [
        pltpu.VMEM(shape, dtype)
        for shape, dtype in [
            ((w_qkv.shape[0], q_width), BF),
            ((w_qkv.shape[0], kv), BF),
            ((w_qkv.shape[0], kv), BF),
            (w_out.shape, BF),
            (tokens.shape, BF),
            (cotangent.shape, BF),
            (table.shape, table.dtype),
            (small.shape, BF),
        ]
    ]
    return pl.pallas_call(
        functools.partial(entry_kernel, sizes),
        out_shape=[
            line_out,
            line_out,
            jax.ShapeDtypeStruct((S,) + table.shape, table.dtype),
            jax.ShapeDtypeStruct((S, F, w_qkv.shape[0], own_width), w_qkv.dtype),
            jax.ShapeDtypeStruct((F,) + w_out.shape, w_out.dtype),
            jax.ShapeDtypeStruct((N,) + small.shape, small.dtype),
        ],
        in_specs=[ANY] * 6,
        out_specs=[ANY] * 6,
        scratch_shapes=[
            DMA((2, 2, chunks, S)), DMA((2, 2, chunks, S)), DMA((S,)), DMA((S,)),
            DMA((S, 3)), DMA((S, 3)), DMA((S + 1, F // 2)), DMA((S + 1, F // 2)),
            DMA((S + 1, F // 2)), DMA((S + 1, F // 2)), DMA((N,)), DMA((N,)), DMA((8, 2)),
        ] + stages,
        compiler_params=pltpu.CompilerParams(collective_id=collective_id, has_side_effects=True),
        name="entry",
    )(tokens, cotangent, table, w_qkv, w_out, small)


def grads_kernel(sizes, specs, combined, *refs):
    S = sizes["seq"]
    count = len(specs)
    refs = list(refs)

    def take(number):
        taken, refs[:number] = refs[:number], []
        return taken

    sources, (x_any, gu_any, ph_any, g_any) = take(count), take(4)
    combine = take(1) if combined else None
    results, (up_out, down_out) = take(count), take(2)
    part_out = take(1) if combined else None
    x_ref, gu_ref, ph_ref, g_ref, up_stage, down_stage = take(6)
    in_sem, up_send, up_recv, out_sem, back_sem, *sems = refs
    s = lax.axis_index("seq")
    inward = [
        pltpu.make_async_copy(source, target, in_sem.at[i])
        for i, (source, target) in enumerate(
            ((x_any, x_ref), (gu_any, gu_ref), (ph_any, ph_ref), (g_any, g_ref))
        )
    ]
    met = greet(sizes)
    for copy in inward:
        copy.start()
    blocks = Blocks(sizes, specs, sources, results, sems)
    met()
    blocks.start()
    inward[0].wait()
    inward[1].wait()
    part = up_stage.shape[1]
    over_rows = (((0,), (0,)), ((), ()))
    sent = []
    for turn_at in range(1, S + 1):
        target = lax.rem(s + turn_at, S)
        mine = pl.ds(pl.multiple_of(target * part, 128), part)
        block = up_stage.at[turn_at - 1]

        def one(at):
            block[:, at] = lax.dot_general(
                x_ref[:, mine], gu_ref[:, at], over_rows, preferred_element_type=F32
            ).astype(BF)

        tiles(gu_ref.shape[1], 256, one)
        if turn_at < S:
            copy = pltpu.make_async_remote_copy(
                src_ref=block, dst_ref=up_out.at[s],
                send_sem=up_send.at[turn_at], recv_sem=up_recv.at[turn_at],
                device_id={"seq": target}, device_id_type=MESH,
            )
        else:
            copy = pltpu.make_async_copy(block, up_out.at[s], out_sem.at[0])
        copy.start()
        sent.append(copy)
    inward[2].wait()
    inward[3].wait()

    def one_down(at):
        down_stage[:, at] = lax.dot_general(
            ph_ref[...], g_ref[:, at], over_rows, preferred_element_type=F32
        ).astype(BF)

    tiles(g_ref.shape[1], 256, one_down)
    copy = pltpu.make_async_copy(down_stage, down_out, out_sem.at[1])
    copy.start()
    sent.append(copy)
    blocks.wait_one(0)
    if combined:
        back = results[0]
        groups, slots = back.shape[1], back.shape[2]
        pieces = []
        for block_at in range(S):
            for group in range(groups):
                row = pl.ds((block_at * groups + group) * slots, slots)
                pieces.append(
                    pltpu.make_async_copy(
                        back.at[block_at, group], x_ref.at[row], back_sem.at[block_at, group]
                    )
                )
                pieces[-1].start()
        for copy in pieces:
            copy.wait()
        reach = groups * slots
        for block_at in range(S):

            def one_part(at):
                part_out[0][block_at, :, at] = lax.dot_general(
                    combine[0][block_at], x_ref[block_at * reach : (block_at + 1) * reach, at],
                    over_rows, preferred_element_type=F32,
                ).astype(BF)

            tiles(part_out[0].shape[2], 512, one_part)
    for i in range(1, count):
        blocks.wait_one(i)
    for copy in sent:
        copy.wait()


def grads(arrays, specs, rows, grad_gu, hidden, grad_out, select, sizes, collective_id):
    S = sizes["seq"]
    combined = select is not None
    groups = arrays[0].shape[0]
    part = rows.shape[1] // S
    up_block = (part, grad_gu.shape[1])
    down = (hidden.shape[1], grad_out.shape[1])
    inner = [rows, grad_gu, hidden, grad_out]
    return pl.pallas_call(
        functools.partial(grads_kernel, sizes, specs, combined),
        out_shape=block_outs(sizes, arrays, specs)
        + [jax.ShapeDtypeStruct((S,) + up_block, BF), jax.ShapeDtypeStruct(down, BF)]
        + ([jax.ShapeDtypeStruct((S, select.shape[2], rows.shape[1]), BF)] if combined else []),
        in_specs=[ANY] * (len(arrays) + 4) + [VM] * combined,
        out_specs=[ANY] * (len(arrays) + 2) + [VM] * combined,
        scratch_shapes=[pltpu.VMEM(array.shape, BF) for array in inner]
        + [pltpu.VMEM((S,) + up_block, BF), pltpu.VMEM(down, BF)]
        + [DMA((4,)), DMA((S,)), DMA((S,)), DMA((2,)), DMA((S, groups))]
        + block_scratch(sizes, arrays, specs),
        compiler_params=pltpu.CompilerParams(
            collective_id=collective_id, has_side_effects=True, vmem_limit_bytes=60 << 20
        ),
        name="grads",
    )(*arrays, *inner, *([select] if combined else []))


def dispatch_kernel(sizes, specs, parts, *refs):
    S, F = sizes["seq"], sizes["fsdp"]
    count = len(specs)
    refs = list(refs)

    def take(number):
        taken, refs[:number] = refs[:number], []
        return taken

    sources = take(count)
    tok_any, down_any, select_ref = take(3)
    g_parts = take(parts)
    results = take(count)
    rows_out, through_out, g_out = take(3)
    tok_ref, rows_ref, g_ref, down_ref, through_ref, row_send, row_recv, own_sem, in_sem, out_sem, g_sem, *sems = refs
    f = lax.axis_index("fsdp")
    slots = rows_out.shape[2]
    met = greet(sizes)
    inward = [pltpu.make_async_copy(tok_any.at[b], tok_ref.at[b], in_sem.at[b]) for b in range(S)]
    inward.append(pltpu.make_async_copy(down_any, down_ref, in_sem.at[S]))
    b = 0
    for g_any in g_parts:
        for j in range(g_any.shape[1]):
            for group in range(F):
                row = pl.ds((group * S + b) * slots, slots)
                inward.append(
                    pltpu.make_async_copy(g_any.at[group, j], g_ref.at[row], g_sem.at[b, group])
                )
            b += 1
    whole_g = pltpu.make_async_copy(g_ref, g_out, in_sem.at[S + 1])
    for copy in inward:
        copy.start()
    blocks = Blocks(sizes, specs, sources, results, sems)
    met()
    blocks.start()
    sent = []
    for b in range(S):
        inward[b].wait()

        def one(at):
            rows_ref[b, :, at] = jnp.dot(
                select_ref[b], tok_ref[b, :, at], preferred_element_type=F32
            ).astype(BF)

        tiles(rows_ref.shape[2], 512, one)
        for step in range(1, F):
            target = lax.rem(f + step, F)
            copy = pltpu.make_async_remote_copy(
                src_ref=rows_ref.at[b, pl.ds(pl.multiple_of(target * slots, 16), slots)],
                dst_ref=rows_out.at[f, b],
                send_sem=row_send.at[b, step], recv_sem=row_recv.at[b, step],
                device_id={"fsdp": target}, device_id_type=MESH,
            )
            copy.start()
            sent.append(copy)
        copy = pltpu.make_async_copy(
            rows_ref.at[b, pl.ds(pl.multiple_of(f * slots, 16), slots)], rows_out.at[f, b], own_sem.at[b]
        )
        copy.start()
        sent.append(copy)
    for copy in inward[S:]:
        copy.wait()
    whole_g.start()
    span = through_ref.shape[1]
    outward = []
    for n in range(g_ref.shape[0] // span):
        if n >= 2:
            outward[n - 2].wait()
        own = pl.ds(n * span, span)

        def one_through(at):
            through_ref[n % 2, :, at] = lax.dot_general(
                g_ref[own, :], down_ref[at, :], (((1,), (1,)), ((), ())), preferred_element_type=F32
            )

        tiles(through_ref.shape[2], 256, one_through)
        outward.append(pltpu.make_async_copy(through_ref.at[n % 2], through_out.at[own], out_sem.at[n % 2]))
        outward[-1].start()
    for copy in outward[-2:]:
        copy.wait()
    whole_g.wait()
    blocks.wait()
    for copy in sent:
        copy.wait()


def dispatch(arrays, specs, tokens, g_parts, w_down, select, sizes, collective_id):
    S, F = sizes["seq"], sizes["fsdp"]
    slots = select.shape[1] // F
    width = tokens.shape[2]
    count = F * S * slots
    hidden = w_down.shape[0]
    span = 512
    return pl.pallas_call(
        functools.partial(dispatch_kernel, sizes, specs, len(g_parts)),
        out_shape=block_outs(sizes, arrays, specs)
        + [
            jax.ShapeDtypeStruct((F, S, slots, width), BF),
            jax.ShapeDtypeStruct((count, hidden), F32),
            jax.ShapeDtypeStruct((count, width), BF),
        ],
        in_specs=[ANY] * (len(arrays) + 2) + [VM] + [ANY] * len(g_parts),
        out_specs=[ANY] * (len(arrays) + 3),
        scratch_shapes=[
            pltpu.VMEM(tokens.shape, BF),
            pltpu.VMEM((S, select.shape[1], width), BF),
            pltpu.VMEM((count, width), BF),
            pltpu.VMEM(w_down.shape, BF),
            pltpu.VMEM((2, span, hidden), F32),
            DMA((S, F)), DMA((S, F)), DMA((S,)), DMA((S + 2,)), DMA((2,)), DMA((S, F)),
        ] + block_scratch(sizes, arrays, specs),
        compiler_params=pltpu.CompilerParams(
            collective_id=collective_id, has_side_effects=True, vmem_limit_bytes=58 << 20
        ),
        name="dispatch",
    )(*arrays, tokens, w_down, select, *g_parts)


def expert_kernel(
    x_ref, gate_ref, through_ref, g_ref, up_w, down_w,
    moe_ref, back_ref, gu_ref, gated_ref, prob_ref, hidden_ref,
):
    hidden = hidden_ref.shape[1]
    width = x_ref.shape[1]
    row_gate = gate_ref[...]
    for at in range(0, hidden, 256):
        low = slice(at, at + 256)
        high = slice(hidden + at, hidden + at + 256)
        gate = jnp.dot(x_ref[...], up_w[:, low], preferred_element_type=F32)
        up = jnp.dot(x_ref[...], up_w[:, high], preferred_element_type=F32)
        sigmoid = jax.nn.sigmoid(gate)
        silu = gate * sigmoid
        value = (silu * up).astype(BF)
        hidden_ref[:, low] = value
        gated_ref[:, low] = (row_gate * value.astype(F32)).astype(BF)
        grad = (row_gate * through_ref[:, low]).astype(BF).astype(F32)
        gu_ref[:, low] = (grad * up * sigmoid * (1.0 + gate * (1.0 - sigmoid))).astype(BF)
        gu_ref[:, high] = (grad * silu).astype(BF)
    prob = jnp.zeros_like(row_gate)
    for at in range(0, width, 256):
        here = slice(at, at + 256)
        out = jnp.dot(hidden_ref[...], down_w[:, here], preferred_element_type=F32)
        out = out.astype(BF).astype(F32)
        moe_ref[:, here] = (row_gate * out).astype(BF)
        prob = prob + jnp.sum(out * g_ref[:, here].astype(F32), axis=-1, keepdims=True)
        back_ref[:, here] = lax.dot_general(
            gu_ref[...], up_w[here, :], (((1,), (1,)), ((), ())), preferred_element_type=F32
        ).astype(BF)
    prob_ref[...] = prob


def expert(x, row_gate, through, g, up_w, down_w, steps):
    count, width = x.shape
    hidden = down_w.shape[0]
    rows = count // steps

    def by_rows(columns):
        return pl.BlockSpec((rows, columns), lambda i: (i, 0))

    def whole(array):
        return pl.BlockSpec(array.shape, lambda i: (0, 0), pipeline_mode=pl.Buffered(1))

    return pl.pallas_call(
        expert_kernel,
        grid=(steps,),
        out_shape=[
            jax.ShapeDtypeStruct((count, width), BF),
            jax.ShapeDtypeStruct((count, width), BF),
            jax.ShapeDtypeStruct((count, 2 * hidden), BF),
            jax.ShapeDtypeStruct((count, hidden), BF),
            jax.ShapeDtypeStruct((count, 1), F32),
        ],
        in_specs=[by_rows(width), by_rows(1), by_rows(hidden), by_rows(width), whole(up_w), whole(down_w)],
        out_specs=[by_rows(width), by_rows(width), by_rows(2 * hidden), by_rows(hidden), by_rows(1)],
        scratch_shapes=[pltpu.VMEM((rows, hidden), BF)],
        compiler_params=pltpu.CompilerParams(vmem_limit_bytes=60 << 20),
        name="expert",
    )(x, row_gate, through, g, up_w, down_w)


def line_kernel(sizes, chunks, mode, extra, *refs):
    S, F = sizes["seq"], sizes["fsdp"]
    count = len(extra)
    names = {
        "ffn": (["base", "gain"], ["resid_out", "all_out"]),
        "grad": (["base", "gain", "resid", "add"], ["grad_out", "gain_out", "all_out"]),
        "last": (
            ["base", "gain", "resid", "inputs", "heads", "length", "gout", "gqkv"],
            ["grad_out", "low_out", "gains_all", "gout_out", "gqkv_out"],
        ),
    }[mode]
    refs = list(refs)

    def take(number):
        taken, refs[:number] = refs[:number], []
        return taken

    loaded = len(names[0]) + 1 - (3 if mode == "last" else 0)
    outside = take(loaded)
    kept = names[0][loaded - 1 :]
    given = dict(zip(kept, take(len(kept))))
    sources = take(count)
    given.update(zip(names[1], take(len(names[1]))))
    results = take(count)
    part, *inner = take(loaded)
    given.update(zip(names[0], inner))
    (load_sem,) = take(1)
    loads = [
        pltpu.make_async_copy(source, target, load_sem.at[i])
        for i, (source, target) in enumerate(zip(outside, [part] + inner))
    ]
    for copy in loads:
        copy.start()
    landings = take(2)
    gather = mode != "last"
    if gather:
        stage, rs_send, rs_recv, ag_send, ag_recv, own_sem = take(6)
        all_out = given["all_out"]
    else:
        gain_sum, gain_stage, gain_send, gain_recv, gain_own = take(5)
        plane_gout, plane_gqkv, gqkv_stage, gqkv_line, line_send, line_recv = take(6)
        plane_sems = take(5)
        rs_send, rs_recv = take(2)
    s = lax.axis_index("seq")
    f = lax.axis_index("fsdp")
    me = s * F + f
    N = S * F
    steps = chunks * part.shape[0]
    rows = part.shape[2]
    span = rows // chunks
    met = greet(sizes)
    blocks = Blocks(sizes, extra, sources, results, refs)
    met()
    for copy in loads:
        copy.wait()
    if mode == "grad":
        given["gain_out"][...] = jnp.zeros_like(given["gain_out"])
    if mode == "last":
        gain_sum[...] = jnp.zeros_like(gain_sum)

    def at(c):
        return pl.ds(pl.multiple_of((c % chunks) * span, span), span)

    def mine(d, c):
        return part.at[c // chunks, d, at(c)]

    def landed(way, d, c):
        return landings[way].at[c // chunks, d, at(c)]

    def rs_copy(d, c, way, src):
        return pltpu.make_async_remote_copy(
            src_ref=src, dst_ref=landed(way, d, c),
            send_sem=rs_send.at[way, d, c], recv_sem=rs_recv.at[way, d, c],
            device_id={"seq": s + 1 if way == 0 else s - 1}, device_id_type=MESH,
        )

    def ag_copy(block, c, way, hop):
        src = stage.at[at(c)] if hop == 1 else all_out.at[block, at(c)]
        return pltpu.make_async_remote_copy(
            src_ref=src, dst_ref=all_out.at[block, at(c)],
            send_sem=ag_send.at[way, c, hop], recv_sem=ag_recv.at[way, c, hop],
            device_id={"seq": s + 1 if way == 0 else s - 1}, device_id_type=MESH,
        )

    def end_step(c):
        @pl.when(s == 0)
        def _():
            for d in range(S - 1, 0, -1):
                rs_copy(d, c, 0, mine(d, c)).start()

        @pl.when(s == S - 1)
        def _():
            for d in range(S - 1):
                rs_copy(d, c, 1, mine(d, c)).start()

    def middle_step(way, c):
        for d in range(S - 1, 0, -1) if way == 0 else range(S - 1):
            @pl.when(d > s if way == 0 else d < s)
            def _():
                buffer = landed(way, d, c)
                rs_copy(d, c, way, buffer).wait_recv()
                total = buffer[...].astype(F32) + mine(d, c)[...].astype(F32)
                buffer[...] = total.astype(BF)
                rs_copy(d, c, way, buffer).start()

    def final_step(c):
        @pl.when(s > 0)
        def _():
            rs_copy(s, c, 0, mine(s, c)).wait_recv()

        @pl.when(s < S - 1)
        def _():
            rs_copy(s, c, 1, mine(s, c)).wait_recv()

        total = mine(s, c)[...].astype(F32)
        total = total + jnp.where(s > 0, landed(0, s, c)[...].astype(F32), 0.0)
        total = total + jnp.where(s < S - 1, landed(1, s, c)[...].astype(F32), 0.0)
        if mode == "last":
            @pl.when(c >= chunks)
            def _():
                row = s * rows + (c % chunks) * span
                row = row + lax.broadcasted_iota(jnp.int32, total.shape, 0)
                value = given["resid"][at(c), :] + total
                given["low_out"][at(c), :] = jnp.where(row < given["length"][0], value, 0.0).astype(BF)

            @pl.when(c < chunks)
            def _():
                value = given["inputs"][at(c), :].astype(F32)
                factor = lax.rsqrt(jnp.mean(value * value, axis=-1, keepdims=True) + EPSILON)
                normed = value * factor
                scaled = total * given["gain"][...]
                inner = jnp.mean(scaled * normed, axis=-1, keepdims=True)
                given["grad_out"][at(c), :] = given["base"][at(c), :] + factor * (scaled - normed * inner)
                gain_sum[...] += jnp.sum(total * normed, axis=0, keepdims=True)

            @pl.when(c == chunks - 1)
            def _():
                send_gains()

            return
        if mode == "ffn":
            value = given["base"][at(c), :].astype(F32) + total
            given["resid_out"][at(c), :] = value
            factor = lax.rsqrt(jnp.mean(value * value, axis=-1, keepdims=True) + EPSILON)
            low = (value * factor * given["gain"][...]).astype(BF)
        else:
            upstream = total + given["add"][at(c), :]
            value = given["resid"][at(c), :]
            factor = lax.rsqrt(jnp.mean(value * value, axis=-1, keepdims=True) + EPSILON)
            normed = value * factor
            scaled = upstream * given["gain"][...]
            inner = jnp.mean(scaled * normed, axis=-1, keepdims=True)
            result = given["base"][at(c), :] + factor * (scaled - normed * inner)
            given["grad_out"][at(c), :] = result
            given["gain_out"][...] += jnp.sum(upstream * normed, axis=0, keepdims=True)
            low = result.astype(BF)
        stage[at(c), :] = low
        pltpu.make_async_copy(stage.at[at(c)], all_out.at[s, at(c)], own_sem.at[c]).start()

        @pl.when(s < S - 1)
        def _():
            ag_copy(s, c, 0, 1).start()

        @pl.when(s > 0)
        def _():
            ag_copy(s, c, 1, 1).start()

    def gain_copy(step):
        return pltpu.make_async_remote_copy(
            src_ref=gain_stage, dst_ref=given["gains_all"].at[me],
            send_sem=gain_send.at[step], recv_sem=gain_recv.at[step],
            device_id=place_of(sizes, EVERY, lax.rem(me + step, N)), device_id_type=MESH,
        )

    def own_gains():
        return pltpu.make_async_copy(gain_stage, given["gains_all"].at[me], gain_own.at[0])

    def send_gains():
        number = gain_sum.shape[1] // 128
        for j in range(number):
            gain_stage[j : j + 1, :] = gain_sum[:, j * 128 : (j + 1) * 128]
        gain_stage[number:, :] = given["heads"][...]
        own_gains().start()
        each(N, lambda step: gain_copy(step).start())

    plane = None
    if mode == "last":
        plane = Blocks(
            sizes, ((("fsdp",), 0, 0), (("fsdp",), 1, 0)), [given["gout"], given["gqkv"]],
            [plane_gout, plane_gqkv], plane_sems,
        )

    def line_copy(step):
        return pltpu.make_async_remote_copy(
            src_ref=gqkv_stage.at[lax.rem(s + step, S)], dst_ref=gqkv_line.at[s],
            send_sem=line_send.at[step], recv_sem=line_recv.at[step],
            device_id={"seq": lax.rem(s + step, S)}, device_id_type=MESH,
        )

    def plane_step():
        plane.wait_one(1)
        for z in range(S):
            total = plane_gqkv[0, z].astype(F32)
            for owner in range(1, F):
                total = total + plane_gqkv[owner, z].astype(F32)
            gqkv_stage[z] = total.astype(BF)
        for step in range(1, S):
            line_copy(step).start()
        gqkv_line[s] = gqkv_stage[s]

    def rows_step():
        plane.wait_one(0)
        half = plane_gout.shape[1] // 2
        for part_at in range(2):
            own = pl.ds(part_at * half, half)
            total = plane_gout[0, own].astype(F32)
            for owner in range(1, F):
                total = total + plane_gout[owner, own].astype(F32)
            given["gout_out"][own, :] = total

    def columns_step():
        for step in range(1, S):
            line_copy(step).wait()
        result = given["gqkv_out"]
        q_width, kv = QH * HD // S, KH * HD // S
        for z in range(S):
            block = gqkv_line[z].astype(F32)
            result[:, z * q_width : (z + 1) * q_width] = block[:, :q_width]
            key_at = S * q_width + z * kv
            result[:, key_at : key_at + kv] = block[:, q_width : q_width + kv]
            value_at = S * (q_width + kv) + z * kv
            result[:, value_at : value_at + kv] = block[:, q_width + kv :]

    def relay_step(way, hop, c):
        block = s - hop if way == 0 else s + hop
        ag_copy(block, c, way, hop).wait_recv()
        if hop < S - 1:
            @pl.when(s < S - 1 if way == 0 else s > 0)
            def _():
                ag_copy(block, c, way, hop + 1).start()

    def final_lag(z):
        return 1 + jnp.maximum(jnp.maximum(z - 2, S - 3 - z), 0)

    ahead = min(steps, AHEAD if gather else steps)
    for c in range(ahead):
        end_step(c)
    if plane:
        plane.start()
    blocks.start()
    turns = steps + (2 * S - 2 if gather else S)

    def inside(c):
        return (c >= 0) & (c < steps)

    @pl.loop(0, turns)
    def _(t):
        for way in range(2):
            come = t - (s - 1 if way == 0 else S - 2 - s)

            @pl.when(inside(come) & ((s > 0) & (s < S - 1)))
            def _():
                middle_step(way, come)

        @pl.when(inside(t + ahead) & ((s == 0) | (s == S - 1)))
        def _():
            end_step(t + ahead)

        done = t - final_lag(s)

        @pl.when(inside(done))
        def _():
            final_step(done)

        if gather:
            for hop in range(1, S):
                for way in range(2):
                    block = s - hop if way == 0 else s + hop
                    passed = t - final_lag(block) - hop

                    @pl.when(inside(passed) & ((block >= 0) & (block < S)))
                    def _():
                        relay_step(way, hop, passed)
        else:
            @pl.when(t == steps * 13 // 16)
            def _():
                plane_step()

    if plane:
        rows_step()

    @pl.loop(0, steps)
    def _(c):
        for d in range(S - 1, 0, -1):
            @pl.when(d > s)
            def _():
                rs_copy(d, c, 0, mine(d, c)).wait_send()
        for d in range(S - 1):
            @pl.when(d < s)
            def _():
                rs_copy(d, c, 1, mine(d, c)).wait_send()
        if gather:
            pltpu.make_async_copy(stage.at[at(c)], all_out.at[s, at(c)], own_sem.at[c]).wait()
            for hop in range(1, S):
                @pl.when((s < S - 1) & (s >= hop - 1))
                def _():
                    ag_copy(s, c, 0, hop).wait_send()

                @pl.when((s > 0) & (s <= S - hop))
                def _():
                    ag_copy(s, c, 1, hop).wait_send()

    if mode == "last":
        columns_step()
        own_gains().wait()
        each(N, lambda step: gain_copy(step).wait())
    blocks.wait()


def line(mode, sizes, part, others, extras, specs, collective_id):
    chunks = CHUNKS if mode != "last" else CHUNKS // 2
    S, F = sizes["seq"], sizes["fsdp"]
    parts, _, rows, width = part.shape
    full = jax.ShapeDtypeStruct((rows, width), F32)
    everyone = jax.ShapeDtypeStruct((S, rows, width), BF)
    steps = chunks * parts
    loaded = [part] + list(others[:-3] if mode == "last" else others)
    scratch = [pltpu.VMEM(array.shape, array.dtype) for array in loaded] + [DMA((len(loaded),))]
    scratch += [pltpu.VMEM((parts, S, rows, width), BF)] * 2
    in_specs = [ANY] * (1 + len(others))
    sems = [DMA((2, S, steps)), DMA((2, S, steps))]
    if mode == "ffn":
        outs, out_specs = [full, everyone], [VM, ANY]
    elif mode == "grad":
        outs, out_specs = [full, jax.ShapeDtypeStruct((1, width), F32), everyone], [VM, VM, ANY]
    else:
        gout, gqkv = others[-2:]
        owned = gqkv.shape[2:]
        outs = [
            full,
            jax.ShapeDtypeStruct((rows, width), BF),
            jax.ShapeDtypeStruct((S * F, width // 128 + 2, 128), F32),
            jax.ShapeDtypeStruct(gout.shape[1:], F32),
            jax.ShapeDtypeStruct((owned[0], owned[1] * S), F32),
        ]
        out_specs = [VM, VM, ANY, VM, VM]
        N = S * F
        scratch += [pltpu.VMEM((1, width), F32), pltpu.VMEM((width // 128 + 2, 128), F32)]
        scratch += [DMA((N,)), DMA((N,)), DMA((1,))]
        scratch += [
            pltpu.VMEM(gout.shape, BF),
            pltpu.VMEM((F, S) + owned, BF),
            pltpu.VMEM((S,) + owned, BF),
            pltpu.VMEM((S,) + owned, BF),
            DMA((S,)),
            DMA((S,)),
        ]
        scratch += block_scratch(sizes, [gout, gqkv], ((("fsdp",), 0, 0), (("fsdp",), 1, 0)))
        in_specs[-3] = pl.BlockSpec(memory_space=pltpu.SMEM)
    if mode != "last":
        scratch.append(pltpu.VMEM((rows, width), BF))
        sems += [DMA((2, chunks, S)), DMA((2, chunks, S)), DMA((chunks,))]
    return pl.pallas_call(
        functools.partial(line_kernel, sizes, chunks, mode, specs),
        out_shape=outs + block_outs(sizes, extras, specs),
        in_specs=in_specs + [ANY] * len(extras),
        out_specs=out_specs + [ANY] * len(extras),
        scratch_shapes=scratch + sems + block_scratch(sizes, extras, specs),
        compiler_params=pltpu.CompilerParams(
            collective_id=collective_id, has_side_effects=True, vmem_limit_bytes=58 << 20
        ),
        name=f"line_{mode}",
    )(part, *others, *extras)


def widen_kernel(*refs):
    half = len(refs) // 2
    for narrow, wide in zip(refs[:half], refs[half:]):
        wide[...] = narrow[...].astype(F32)


def widen(arrays):
    specs = [pl.BlockSpec((1,) + array.shape[1:], lambda i: (i, 0, 0)) for array in arrays]
    return pl.pallas_call(
        widen_kernel,
        grid=(arrays[0].shape[0],),
        out_shape=[jax.ShapeDtypeStruct(array.shape, F32) for array in arrays],
        in_specs=specs,
        out_specs=specs,
        compiler_params=pltpu.CompilerParams(vmem_limit_bytes=40 << 20),
        name="widen",
    )(*arrays)


def turn(values, cosine, sine):
    return values * cosine + pltpu.roll(values, HD // 2, 1) * sine


def softmax_block(query, keys, first_row, length, scale):
    scores = lax.dot_general(
        query, keys, (((1,), (1,)), ((), ())), preferred_element_type=F32
    ) * scale
    row = first_row + lax.broadcasted_iota(jnp.int32, (scores.shape[0], 1), 0)
    column = lax.broadcasted_iota(jnp.int32, scores.shape, 1)
    scores = jnp.where(column <= jnp.minimum(row, length - 1), scores, MASKED)
    peak = jnp.max(scores, axis=-1, keepdims=True)
    weights = jnp.exp(scores - peak)
    return weights * (1.0 / jnp.sum(weights, axis=-1, keepdims=True))


def tiles(width, step, body):
    @pl.loop(0, width // step)
    def _(n):
        body(pl.ds(pl.multiple_of(n * step, step), step))


def each_head(heads, body):
    @pl.loop(0, heads)
    def _(n):
        body(pl.ds(pl.multiple_of(n * HD, HD), HD))


class Rows:
    def __init__(self, sizes, early, source, target, sems):
        F = sizes["fsdp"]
        f = lax.axis_index("fsdp")
        send_sem, recv_sem, own_sem = sems
        self.copies = []
        for b in range(early):
            own = pltpu.make_async_copy(source(b, f), target(b, f), own_sem.at[b])
            self.copies.append([own])
            for step in range(1, F):
                away = lax.rem(f + step, F)
                self.copies[b].append(
                    pltpu.make_async_remote_copy(
                        src_ref=source(b, away), dst_ref=target(b, f),
                        send_sem=send_sem.at[b, step], recv_sem=recv_sem.at[b, step],
                        device_id={"fsdp": away}, device_id_type=MESH,
                    )
                )

    def start(self, b):
        for copy in self.copies[b]:
            copy.start()

    def wait(self, b):
        for copy in self.copies[b]:
            copy.wait()


def row_scratch(sizes, early, slots, width):
    if not early:
        return []
    F = sizes["fsdp"]
    return [pltpu.VMEM((early, F * slots, width), BF), DMA((early, F)), DMA((early, F)), DMA((early,))]


def rows_at(ref, slots):
    return lambda b, i: ref.at[b, pl.ds(pl.multiple_of(i * slots, 16), slots)]


def attend_kernel(sizes, heads, blocks, early, specs, *refs):
    count = len(specs)
    length_ref, tok_ref, gain_ref, wq_ref, cos_ref, sin_ref, gains_ref, wo_ref = refs[:8]
    select_ref, cot_ref = refs[8:10]
    refs = list(refs[10:])

    def take(number):
        taken, refs[:number] = refs[:number], []
        return taken

    first = take(2 if early else 0)
    sources = take(count)
    attn_ref, proj_ref, low_ref, out_ref, part_ref, rows_ref = take(6)
    early_out = take(1 if early else 0)
    results = take(count)
    k_all, v_all = take(2)
    row_refs = take(4 if early else 0)
    sems = refs
    step = pl.program_id(0)

    def early_rows():
        slots = early_out[0].shape[2]
        return Rows(
            sizes, early, rows_at(row_refs[0], slots), lambda b, i: early_out[0].at[i, b], row_refs[1:]
        )

    @pl.when(step == 0)
    def _():
        greet(sizes)()
        Blocks(sizes, specs, sources, results, sems).start()
        if early:
            rows_away = early_rows()
            for b in range(early):

                def pick_first(at):
                    row_refs[0][b, :, at] = jnp.dot(
                        first[0][b], first[1][b, :, at], preferred_element_type=F32
                    ).astype(BF)

                tiles(row_refs[0].shape[2], 512, pick_first)
                rows_away.start(b)

    rows, width = proj_ref.shape
    length = length_ref[0]
    cosine = cos_ref[...]
    sine = sin_ref[...]
    q_gain = gains_ref[0:1, :]
    k_gain = gains_ref[1:2, :]
    scale = HD ** (-0.5)
    value = tok_ref[...].astype(F32)
    factor = lax.rsqrt(jnp.mean(value * value, axis=-1, keepdims=True) + EPSILON)
    attn_ref[...] = (value * factor * gain_ref[...]).astype(BF)

    def project(at):
        proj_ref[:, at] = jnp.dot(attn_ref[...], wq_ref[:, at], preferred_element_type=F32)

    tiles(width, 256, project)

    def normed(raw, gain):
        factor = lax.rsqrt(jnp.mean(raw * raw, axis=-1, keepdims=True) + EPSILON)
        return turn(raw * factor * gain, cosine, sine).astype(BF)

    key = normed(proj_ref[:, heads * HD : (heads + 1) * HD], k_gain)
    value_low = proj_ref[:, (heads + 1) * HD :].astype(BF)
    low_ref[:, heads * HD : (heads + 1) * HD] = key
    low_ref[:, (heads + 1) * HD :] = value_low
    here = pl.ds(pl.multiple_of(step * rows, rows), rows)
    k_all[here, :] = key
    v_all[here, :] = value_low
    for block in range(blocks):
        @pl.when(step == block)
        def _():
            reach = (block + 1) * rows

            def one(column):
                query = normed(proj_ref[:, column], q_gain)
                low_ref[:, column] = query
                probs = softmax_block(query, k_all[:reach, :], block * rows, length, scale)
                mixed = jnp.dot(probs.astype(BF), v_all[:reach, :], preferred_element_type=F32)
                out_ref[:, column] = mixed.astype(BF)

            each_head(heads, one)

    def leave(at):
        part_ref[:, at] = jnp.dot(
            out_ref[...], wo_ref[:, at], preferred_element_type=F32
        ).astype(BF)

    tiles(part_ref.shape[1], 256, leave)

    def pick(at):
        rows_ref[0, :, at] = jnp.dot(
            select_ref[0], cot_ref[0, :, at], preferred_element_type=F32
        ).astype(BF)

    @pl.when(step >= early)
    def _():
        tiles(rows_ref.shape[2], 512, pick)

    @pl.when(step == blocks - 1)
    def _():
        if early:
            rows_away = early_rows()
            for b in range(early):
                rows_away.wait(b)
        Blocks(sizes, specs, sources, results, sems).wait()


def attend(
    length, tokens, gain, w_proj, cosine, sine, gains, w_out, select, cot, heads, early, extras,
    specs, sizes, collective_id,
):
    total, width = tokens.shape
    blocks = select.shape[0]
    F = sizes["fsdp"]
    slots = select.shape[1] // F
    own_width = w_proj.shape[1]
    rows = total // blocks
    q_width = heads * HD

    def by_rows(columns):
        return pl.BlockSpec((rows, columns), lambda i: (i, 0))

    def leading(array):
        return pl.BlockSpec(
            (early,) + array.shape[1:], lambda i: (0, 0, 0), pipeline_mode=pl.Buffered(1)
        )

    def by_block(array):
        return pl.BlockSpec((1,) + array.shape[1:], lambda i: (i, 0, 0))

    def whole(array):
        return pl.BlockSpec(array.shape, lambda i: (0, 0), pipeline_mode=pl.Buffered(1))

    return pl.pallas_call(
        functools.partial(attend_kernel, sizes, heads, blocks, early, specs),
        grid=(blocks,),
        out_shape=[
            jax.ShapeDtypeStruct((total, width), BF),
            jax.ShapeDtypeStruct((total, own_width), F32),
            jax.ShapeDtypeStruct((total, own_width), BF),
            jax.ShapeDtypeStruct((total, q_width), BF),
            jax.ShapeDtypeStruct((total, width), BF),
            jax.ShapeDtypeStruct((blocks - early, select.shape[1], width), BF),
        ]
        + ([jax.ShapeDtypeStruct((F, early, slots, width), BF)] if early else [])
        + block_outs(sizes, extras, specs),
        in_specs=[
            pl.BlockSpec(memory_space=pltpu.SMEM),
            by_rows(width),
            whole(gain),
            whole(w_proj),
            by_rows(HD),
            by_rows(HD),
            whole(gains),
            whole(w_out),
            by_block(select),
            by_block(cot),
        ]
        + ([leading(select), leading(cot)] if early else [])
        + [ANY] * len(extras),
        out_specs=[
            by_rows(width), by_rows(own_width), by_rows(own_width), by_rows(q_width), by_rows(width),
            pl.BlockSpec((1, select.shape[1], width), lambda i: (jnp.maximum(i - early, 0), 0, 0)),
        ] + [ANY] * (len(extras) + (1 if early else 0)),
        scratch_shapes=[pltpu.VMEM((total, HD), BF), pltpu.VMEM((total, HD), BF)]
        + row_scratch(sizes, early, slots, width)
        + block_scratch(sizes, extras, specs),
        compiler_params=pltpu.CompilerParams(
            collective_id=collective_id, has_side_effects=True, vmem_limit_bytes=58 << 20
        ),
        name="attend",
    )(
        length, tokens, gain, w_proj, cosine, sine, gains, w_out, select, cot,
        *([select, cot] if early else []), *extras,
    )


def attend_back_kernel(sizes, heads, blocks, early, specs, *refs):
    count = len(specs)
    length_ref, proj_ref, low_ref, kv_ref, grad_ref, wo_ref, wq_ref, cos_ref, sin_ref, gains_ref = refs[:10]
    select_ref, back_ref, attn_any, o_any, ga_any, moe_any = refs[10:16]
    refs = list(refs[16:])

    def take(number):
        taken, refs[:number] = refs[:number], []
        return taken

    sources = take(count)
    part_ref, gains_out, gqkv_out, gout_out = take(4)
    results = take(count)
    gk_all, gv_all, go_ref, out_all, attn_all, o_all, ga_all, gqkv_stage, gout_stage, all_sem, out_sem = take(11)
    row_refs = take(4 if early else 0)
    sems = refs
    slots = moe_any.shape[2]

    def early_rows():
        return Rows(
            sizes, early, lambda b, i: moe_any.at[i, b], rows_at(row_refs[0], slots), row_refs[1:]
        )

    inward = [
        pltpu.make_async_copy(source, target, all_sem.at[i])
        for i, (source, target) in enumerate(((attn_any, attn_all), (o_any, o_all), (ga_any, ga_all)))
    ]
    step = pl.program_id(0)
    rows = proj_ref.shape[0]
    length = length_ref[0]
    cosine = cos_ref[...]
    sine = sin_ref[...]
    q_gain = gains_ref[0:1, :]
    k_gain = gains_ref[1:2, :]
    scale = HD ** (-0.5)
    block_at = blocks - 1 - step
    here = pl.ds(pl.multiple_of(block_at * rows, rows), rows)

    def back(raw, gain, grad):
        grad = turn(grad, cosine, -sine)
        factor = lax.rsqrt(jnp.mean(raw * raw, axis=-1, keepdims=True) + EPSILON)
        unit = raw * factor
        scaled = grad * gain
        inner = jnp.mean(scaled * unit, axis=-1, keepdims=True)
        return factor * (scaled - unit * inner), jnp.sum(grad * unit, axis=0, keepdims=True)

    @pl.when(step == 0)
    def _():
        greet(sizes)()
        Blocks(sizes, specs, sources, results, sems).start()
        for copy in inward:
            copy.start()
        if early:
            rows_away = early_rows()
            for b in range(early - 1, -1, -1):
                rows_away.start(b)
        gk_all[...] = jnp.zeros_like(gk_all)
        gv_all[...] = jnp.zeros_like(gv_all)
        gains_out[...] = jnp.zeros_like(gains_out)

    def arrive(at):
        go_ref[:, at] = lax.dot_general(
            grad_ref[...], wo_ref[at, :], (((1,), (1,)), ((), ())), preferred_element_type=F32
        ).astype(BF)

    tiles(heads * HD, 256, arrive)
    for block in range(blocks):
        @pl.when(block_at == block)
        def _():
            reach = (block + 1) * rows
            keys = kv_ref[:reach, :HD]
            values = kv_ref[:reach, HD:]

            def one(column):
                query = low_ref[:, column]
                grad_o = go_ref[:, column]
                probs = softmax_block(query, keys, block * rows, length, scale)
                grad_p = lax.dot_general(
                    grad_o, values, (((1,), (1,)), ((), ())), preferred_element_type=F32
                )
                inner = jnp.sum(probs * grad_p, axis=-1, keepdims=True)
                grad_s = (probs * (grad_p - inner)).astype(BF)
                grad_q = jnp.dot(grad_s, keys, preferred_element_type=F32) * scale
                gk_all[:reach, :] += lax.dot_general(
                    grad_s, query, (((0,), (0,)), ((), ())), preferred_element_type=F32
                )
                gv_all[:reach, :] += lax.dot_general(
                    probs.astype(BF), grad_o, (((0,), (0,)), ((), ())), preferred_element_type=F32
                )
                grad_raw, gained = back(proj_ref[:, column], q_gain, grad_q.astype(BF).astype(F32))
                out_all[here, column] = grad_raw.astype(BF)
                gains_out[0:1, :] += gained

            each_head(heads, one)

    grad_k = (gk_all[here, :] * scale).astype(BF).astype(F32)
    grad_raw, gained = back(proj_ref[:, heads * HD : (heads + 1) * HD], k_gain, grad_k)
    out_all[here, heads * HD : (heads + 1) * HD] = grad_raw.astype(BF)
    out_all[here, (heads + 1) * HD :] = gv_all[here, :].astype(BF)
    gains_out[1:2, :] += gained

    def leave(at):
        part_ref[0, :, at] = lax.dot_general(
            out_all[here, :], wq_ref[at, :], (((1,), (1,)), ((), ())), preferred_element_type=F32
        ).astype(BF)

    tiles(part_ref.shape[2], 256, leave)
    over_rows = (((0,), (0,)), ((), ()))

    def combine(rows_of):
        def one_part(at):
            part_ref[1, :, at] = lax.dot_general(
                select_ref[0], rows_of(at), over_rows, preferred_element_type=F32
            ).astype(BF)

        tiles(part_ref.shape[2], 512, one_part)

    @pl.when(block_at >= early)
    def _():
        combine(lambda at: back_ref[0, :, at])

    for b in range(early):
        @pl.when(block_at == b)
        def _():
            early_rows().wait(b)
            combine(lambda at: row_refs[0][b, :, at])


    @pl.when(step == blocks - 1)
    def _():
        for copy in inward:
            copy.wait()
        for i, (left, right, stage, result) in enumerate(
            ((attn_all, out_all, gqkv_stage, gqkv_out), (o_all, ga_all, gout_stage, gout_out))
        ):
            span = stage.shape[1]
            sent = []
            for n in range(left.shape[1] // span):
                if n >= 2:
                    sent[n - 2].wait()
                stage[n % 2] = lax.dot_general(
                    left[:, n * span : (n + 1) * span], right[...], over_rows,
                    preferred_element_type=F32,
                ).astype(BF)
                sent.append(
                    pltpu.make_async_copy(
                        stage.at[n % 2], result.at[pl.ds(n * span, span)], out_sem.at[i, n % 2]
                    )
                )
                sent[-1].start()
            for copy in sent[-2:]:
                copy.wait()
        Blocks(sizes, specs, sources, results, sems).wait()


def attend_back(
    length, projected, low, grad, w_out, w_proj, cosine, sine, gains, select, back, attn_low, o_low,
    moe_rows, heads, early, extras, specs, sizes, collective_id,
):
    total, own_width = projected.shape
    width = w_out.shape[1]
    blocks = select.shape[0]
    span = 256
    rows = total // blocks
    q_width = heads * HD

    def by_rows(columns):
        return pl.BlockSpec((rows, columns), lambda i: (blocks - 1 - i, 0))

    def by_block(array):
        return pl.BlockSpec((1,) + array.shape[1:], lambda i: (blocks - 1 - i, 0, 0))

    def whole(array):
        return pl.BlockSpec(array.shape, lambda i: (0, 0), pipeline_mode=pl.Buffered(1))

    return pl.pallas_call(
        functools.partial(attend_back_kernel, sizes, heads, blocks, early, specs),
        grid=(blocks,),
        out_shape=[
            jax.ShapeDtypeStruct((2, total, width), BF),
            jax.ShapeDtypeStruct((2, HD), F32),
            jax.ShapeDtypeStruct((width, own_width), BF),
            jax.ShapeDtypeStruct((q_width, width), BF),
        ] + block_outs(sizes, extras, specs),
        in_specs=[
            pl.BlockSpec(memory_space=pltpu.SMEM),
            by_rows(own_width),
            by_rows(q_width),
            pl.BlockSpec((total, 2 * HD), lambda i: (0, heads // 2)),
            by_rows(width),
            whole(w_out),
            whole(w_proj),
            by_rows(HD),
            by_rows(HD),
            whole(gains),
            by_block(select),
            pl.BlockSpec(
                (1,) + back.shape[1:], lambda i: (jnp.maximum(blocks - 1 - i - early, 0), 0, 0)
            ),
        ] + [ANY] * (4 + len(extras)),
        out_specs=[
            pl.BlockSpec((2, rows, width), lambda i: (0, blocks - 1 - i, 0)),
            pl.BlockSpec((2, HD), lambda i: (0, 0)),
        ] + [ANY] * (2 + len(extras)),
        scratch_shapes=[
            pltpu.VMEM((total, HD), F32),
            pltpu.VMEM((total, HD), F32),
            pltpu.VMEM((rows, q_width), BF),
            pltpu.VMEM((total, own_width), BF),
            pltpu.VMEM((total, width), BF),
            pltpu.VMEM((total, q_width), BF),
            pltpu.VMEM((total, width), BF),
            pltpu.VMEM((2, span, own_width), BF),
            pltpu.VMEM((2, span, width), BF),
            DMA((3,)),
            DMA((2, 2)),
        ]
        + row_scratch(sizes, early, moe_rows.shape[2], width)
        + block_scratch(sizes, extras, specs),
        compiler_params=pltpu.CompilerParams(
            collective_id=collective_id, has_side_effects=True, vmem_limit_bytes=58 << 20
        ),
        name="attend_back",
    )(
        length, projected, low, low, grad, w_out, w_proj, cosine, sine, gains, select, back,
        attn_low, o_low, grad, moe_rows, *extras,
    )


def rms_factor(values):
    return lax.rsqrt(jnp.mean(values * values, axis=-1, keepdims=True) + EPSILON)


def dot(left, right):
    return jnp.dot(left, right, preferred_element_type=F32)


def mm(form, left, right):
    return jnp.einsum(form, left, right, preferred_element_type=F32)


def whole_columns(blocks):
    parts, rows, _ = blocks.shape
    q_width = QH * HD // parts
    kv_width = KH * HD // parts
    moved = blocks.transpose(1, 0, 2)
    return jnp.concatenate(
        [
            moved[..., :q_width].reshape(rows, -1),
            moved[..., q_width : q_width + kv_width].reshape(rows, -1),
            moved[..., q_width + kv_width :].reshape(rows, -1),
        ],
        axis=-1,
    )


def lanes(flat, lead):
    width = flat.shape[-1]
    rows = -(-width // 2048) * 16
    return jnp.pad(flat, ((0, 0), (0, rows * 128 - width))).reshape(lead, rows, 128)


def per_device(
    tokens, cotangent, lengths, routes, slots, w_qkv, w_out, w_router, norm_gains, w_gate_up, w_down
):
    tok_count = tokens.shape[1]
    width = tokens.shape[2]
    S = lax.axis_size("seq")
    F = lax.axis_size("fsdp")
    N = S * F
    sizes = {"seq": S, "fsdp": F}
    local_experts = w_gate_up.shape[0]
    own_experts = local_experts // S
    expert_count = w_router.shape[1]
    capacity = tok_count * TOPK * 5 // (4 * expert_count)
    heads = QH // S
    seq_total = tok_count * S
    q_width = heads * HD
    own_width = q_width + 2 * HD
    seq_at = lax.axis_index("seq")
    w_rows = w_qkv.shape[0]
    small = norm_gains.shape[0]
    router_size = w_router.size
    part_width = w_gate_up.shape[1]
    down_width = w_down.shape[2]
    assert KH == S and own_experts == 1

    small_send = lanes(jnp.concatenate([w_router.reshape(-1), norm_gains])[None], 1)[0]
    table = jnp.concatenate([routes[0].T, slots[0].T])
    tok_all, cot_all, table_all, w_proj, out_own, small_all = entry(
        tokens[0], cotangent[0], table, w_qkv, w_out, small_send, sizes, 1
    )
    w_proj = w_proj.reshape(width, own_width)
    out_own = out_own.reshape(q_width, width)
    small_flat = small_all.reshape(N, -1)
    full_router = small_flat[:, :router_size].reshape(width, expert_count)
    gain_values = small_flat[:, router_size : router_size + small].reshape(-1).astype(F32)
    gain_attn = gain_values[:width]
    gain_ffn = gain_values[width : 2 * width][None]
    gain_heads = gain_values[2 * width :].reshape(2, HD)

    positions = jnp.arange(seq_total, dtype=jnp.int32)
    frequency = THETA ** (-jnp.arange(HD // 2, dtype=F32) / (HD // 2))
    angles = positions.astype(F32)[:, None] * frequency[None, :]
    cosine = jnp.concatenate([jnp.cos(angles)] * 2, axis=-1)
    sine = jnp.concatenate([-jnp.sin(angles), jnp.sin(angles)], axis=-1)
    expert_ids = jnp.arange(expert_count, dtype=jnp.int32)
    slot_ids = jnp.arange(capacity, dtype=jnp.int32)
    plane = (
        jnp.arange(F, dtype=jnp.int32)[:, None] * local_experts
        + seq_at * own_experts
        + jnp.arange(own_experts, dtype=jnp.int32)[None, :]
    ).reshape(-1)
    hit = table_all[:, None, :TOPK] == plane[None, :, None, None]
    plane_slots = jnp.max(jnp.where(hit, table_all[:, None, TOPK:], -1), axis=2)
    one_hot = plane_slots[:, :, None, :] == slot_ids[None, None, :, None]
    select = one_hot.astype(BF).reshape(S, F * own_experts * capacity, tok_count)
    grouped = (S, F, own_experts * capacity, width)

    fused = capacity % 16 == 0
    early = S // 2 if fused else 0
    attn_low, projected, qkv_low, o_low, o_part, cot_rows, *g_first, down_w = attend(
        lengths, tok_all.reshape(seq_total, width), gain_attn[None], w_proj, cosine, sine,
        gain_heads, out_own, select, cot_all, heads, early, [w_down.reshape((S, own_experts) + w_down.shape[1:])],
        ((("seq",), 0, "columns"),), sizes, 3,
    )
    o_part = o_part.reshape(1, S, tok_count, width)
    cot_rows = cot_rows.reshape((S - early,) + grouped[1:])

    residual, ffn_all, g_rows = line(
        "ffn", sizes, o_part, [tokens[0], gain_ffn], [cot_rows], ((("fsdp",), 1, 0),), 2
    )
    ffn_low = lax.dynamic_index_in_dim(ffn_all, seq_at, 0, keepdims=False)

    route_rows = routes[0]
    slot_rows = slots[0]
    router_scores = dot(ffn_low, full_router)
    picked = route_rows[:, :, None] == expert_ids[None, None, :]
    selected = jnp.sum(jnp.where(picked, router_scores[:, None, :], 0.0), axis=-1)
    gate_prob = jax.nn.softmax(selected, axis=-1)
    gate_table = jnp.sum(jnp.where(picked, gate_prob[:, :, None], 0.0), axis=1).T
    hit = table[None, :TOPK] == expert_ids[:, None, None]
    own_slots = jnp.max(jnp.where(hit, table[None, TOPK:], -1), axis=1)
    gate_slots = jnp.sum(
        jnp.where(
            own_slots[:, None, :] == slot_ids[None, :, None], gate_table[:, None, :], 0.0
        ),
        axis=-1,
    )
    by_device = (F, S, own_experts, capacity)

    def to_devices(values):
        return lanes(values.reshape(by_device).transpose(1, 0, 2, 3).reshape(N, -1), N)

    gate_send = to_devices(gate_slots)

    up_blocks = w_gate_up.reshape((S, own_experts) + w_gate_up.shape[1:])
    side_specs = ((("seq",), 0, 0), (EVERY, 0, 0))
    if fused:
        gate_up_w, gate_got, x_rows, through, g_flat = dispatch(
            [up_blocks, gate_send], side_specs, ffn_all, [*g_first, g_rows], down_w[0], select,
            sizes, 4,
        )
    else:
        ffn_rows = mm("brt,btd->brd", select, ffn_all).astype(BF).reshape(grouped)
        gate_up_w, gate_got, x_rows = exchange(
            [up_blocks, gate_send, ffn_rows], side_specs + ((("fsdp",), 1, 0),), sizes, 4
        )
        g_flat = g_rows.reshape(-1, width)
        through = mm("rd,hd->rh", g_flat, down_w[0])
    row_gate = gate_got.reshape(S, F, -1)[:, :, :capacity].transpose(1, 0, 2).reshape(-1, 1)
    x_flat = x_rows.reshape(-1, width)
    moe_rows, grad_rows, grad_gu_low, gated_hidden, prob_rows = expert(
        x_flat, row_gate, through, g_flat, gate_up_w.reshape(width, 2 * FF), down_w[0], 5
    )
    prob_send = prob_rows.reshape(F, S, -1).transpose(1, 0, 2).reshape(N, -1)
    back_blocks = [grad_rows.reshape(F, S, capacity, width), lanes(prob_send, N)]
    grad_back, prob_got, up_got, down_term, *grad_part = grads(
        back_blocks, ((("fsdp",), 0, 1), (EVERY, 0, 0)), x_flat, grad_gu_low, gated_hidden, g_flat,
        select if fused else None, sizes, 6,
    )
    if fused:
        (grad_part,) = grad_part
    else:
        grad_part = mm("brt,brd->btd", select, grad_back.reshape(S, -1, width)).astype(BF)
    moe_rows = moe_rows.reshape(F, S, capacity, width)
    prob_slots = prob_got.reshape(S, F, -1)[:, :, :capacity].transpose(1, 0, 2)
    prob_slots = prob_slots.reshape(expert_count, capacity)


    prob_of_route = jnp.einsum(
        "tke,ec->tkc", picked.astype(F32), prob_slots, precision=lax.Precision.HIGHEST
    )
    at_slot = slot_rows[:, :, None] == slot_ids[None, None, :]
    grad_prob = jnp.sum(jnp.where(at_slot, prob_of_route, 0.0), axis=-1)
    grad_selected = gate_prob * (grad_prob - jnp.sum(gate_prob * grad_prob, axis=-1, keepdims=True))
    grad_logits = jnp.sum(jnp.where(picked, grad_selected[:, :, None], 0.0), axis=1).astype(BF)
    grad_ffn_add = mm("te,de->td", grad_logits, full_router)
    grad_router_part = mm("td,te->de", ffn_low, grad_logits)
    valid = (seq_at * tok_count + jnp.arange(tok_count, dtype=jnp.int32)) < lengths[0]
    grad_final = jnp.where(valid[:, None], cotangent[0].astype(F32), 0.0)
    grad_residual, grad_gain_ffn, grad_attn_low, moe_back = line(
        "grad", sizes, grad_part[None], [grad_final, gain_ffn, residual, grad_ffn_add],
        [moe_rows], ((("fsdp",), (early, S - early), 1),), 7,
    )
    grad_attn_low = grad_attn_low.reshape(seq_total, width)

    early_gains = jnp.concatenate(
        [jnp.zeros((width,), F32), grad_gain_ffn[0], jnp.zeros((2 * HD,), F32)]
    )
    small_blocks = jnp.concatenate(
        [grad_router_part.reshape(N, -1), early_gains.reshape(N, -1)], axis=1
    )
    small_rows = -(-small_blocks.shape[1] // 1024) * 8
    small_blocks = jnp.pad(small_blocks, ((0, 0), (0, small_rows * 128 - small_blocks.shape[1])))
    small_blocks = small_blocks.reshape(N, small_rows, 128)
    last_parts, grad_gain_heads, grad_qkv_part, grad_out_part, down_got, small_got = attend_back(
        lengths, projected, qkv_low, grad_attn_low, out_own, w_proj, cosine, sine, gain_heads,
        select, moe_back.reshape(S - early, -1, width), attn_low, o_low, moe_rows, heads, early,
        [down_term[None], small_blocks], ((("seq",), "columns", 0), (EVERY, 0, 0)), sizes, 9,
    )
    grad_qkv_part = grad_qkv_part.reshape(S, F, w_rows, own_width)
    (
        grad_inputs, final, late_gains, grad_out, grad_qkv
    ) = line(
        "last", sizes, last_parts.reshape(2, S, tok_count, width),
        [
            grad_residual, gain_attn[None], residual, tokens[0], grad_gain_heads, lengths,
            grad_out_part.reshape(F, -1, width), grad_qkv_part,
        ],
        [], (), 8,
    )
    grad_gate_up, grad_down = widen(
        [up_got.reshape(w_gate_up.shape), down_got.reshape(w_down.shape)]
    )
    small_sum = jnp.sum(small_got, axis=0).reshape(-1)
    grad_router = small_sum[:router_size].reshape(w_router.shape)
    late_flat = jnp.sum(late_gains, axis=0).reshape(-1)
    late_sum = jnp.concatenate([late_flat[:width], jnp.zeros((width,), F32), late_flat[width:]])
    device_at = seq_at * F + lax.axis_index("fsdp")
    grad_gains = small_sum[router_size : router_size + small] + lax.dynamic_slice_in_dim(
        late_sum, device_at * small, small, 0
    )
    return (
        final[None],
        grad_inputs[None],
        grad_qkv,
        grad_out,
        grad_router,
        grad_gains,
        grad_gate_up,
        grad_down,
    )


def solution(mesh):
    in_specs = (
        P("fsdp", "seq", None),
        P("fsdp", "seq", None),
        P("fsdp"),
        P("fsdp", "seq", None),
        P("fsdp", "seq", None),
        P(("seq", "fsdp"), None),
        P(("seq", "fsdp"), None),
        P(("seq", "fsdp"), None),
        P(("seq", "fsdp")),
        P("fsdp", "seq", None),
        P("fsdp", None, "seq"),
    )
    out_specs = (
        P("fsdp", "seq", None),
        P("fsdp", "seq", None),
        P(("seq", "fsdp"), None),
        P(("seq", "fsdp"), None),
        P(("seq", "fsdp"), None),
        P(("seq", "fsdp")),
        P("fsdp", "seq", None),
        P("fsdp", None, "seq"),
    )
    return jax.shard_map(
        per_device, mesh=mesh, in_specs=in_specs, out_specs=out_specs, check_vma=False
    )
```
